32 devices in a mesh: data: 2 (over x), hid: 4 (over z), vocab: 4 (over y, core).
Axes of the slice: x: 2, y: 2, z: 4, core: 2. Of those that a mesh axis runs over, the one named last changes fastest.
Arguments:
- h_states: bfloat16 [2048, 2048], P('data', 'hid'), parts along dimension 0
- w_head: bfloat16 [2048, 100352], P('hid', 'vocab')
- inv_temp: float32 [2048], P('data'), parts along dimension 0
- tgt_ids: int32 [2048], P('data'), parts along dimension 0
Outputs:
- output 1: float32 [2048, 100352], P('data', ('vocab', 'hid')), parts along dimension 0
- output 2: float32 [2048], P('data'), parts along dimension 0
There are 2 independent parts. The reference program is written for one: setup_inputs(seed, part) draws one part's arguments, and reference() takes and returns one part's arrays. A program takes and returns all parts, laid end to end along the dimension named above; an argument that names none is the same for every part.
All inputs are finite; a program needn't handle non-finite values.
Results may differ from the reference program's by a relative error of at most 0.001.
Values are sent between devices in bfloat16 or wider.
A program may use at most 1 GiB of HBM per device.

```python
import jax
import jax.numpy as jnp
from jax import lax
import math

B = 1024
D = 2048
V = 100352


def setup_inputs(seed: int = 0, part: int = 0) -> dict:
    part_keys = jax.random.split(jax.random.fold_in(jax.random.key(seed), part), 5)
    shared_keys = jax.random.split(jax.random.key(seed + 1), 2)
    common_dir = jax.random.normal(shared_keys[0], (D,), jnp.float32)
    col_level = 140.0 - 2.5 * jnp.arange(V, dtype=jnp.float32) / V
    row_keys = jax.random.split(shared_keys[1], D // 128)
    dir_blocks = common_dir.reshape(D // 128, 128)

    def weight_block(block_args):
        blk_key, dir_part = block_args
        noise_blk = jax.random.normal(blk_key, (128, V), jnp.float32)
        w_part = noise_blk * (0.6 / math.sqrt(D)) + dir_part[:, None] * (col_level[None, :] / D)
        return w_part.astype(jnp.bfloat16)

    w_head = lax.map(weight_block, (row_keys, dir_blocks)).reshape(D, V)
    row_noise = jax.random.normal(part_keys[0], (B, D), jnp.float32)
    row_shift = jax.random.uniform(part_keys[1], (B,), jnp.float32, 1.0, 2.0)
    h_states = (row_noise + row_shift[:, None] * common_dir[None, :]).astype(jnp.bfloat16)
    inv_temp = jax.random.uniform(part_keys[2], (B,), jnp.float32, 0.7, 1.3)
    first_pick = jax.random.randint(part_keys[3], (B,), 0, V)
    second_pick = jax.random.randint(part_keys[4], (B,), 0, V)
    tgt_ids = jnp.maximum(first_pick, second_pick).at[0].set(0).at[1].set(V - 1)
    return {"h_states": h_states, "w_head": w_head, "inv_temp": inv_temp, "tgt_ids": tgt_ids}


def reference(h_states, w_head, inv_temp, tgt_ids):
    logits = jnp.dot(h_states, w_head, preferred_element_type=jnp.float32) * inv_temp[:, None]
    row_max = jnp.max(logits, axis=1, keepdims=True)
    exp_vals = jnp.exp(logits - row_max)
    row_sum = jnp.sum(exp_vals, axis=1, keepdims=True)
    prob_rows = exp_vals / row_sum
    cdf_table = jnp.cumsum(prob_rows, axis=1)
    cdf_at_tgt = jnp.take_along_axis(cdf_table, tgt_ids[:, None], axis=1)[:, 0]
    return (cdf_table, cdf_at_tgt)
```

```python
import functools

import jax
import jax.numpy as jnp
from jax import lax
from jax.experimental import pallas as pl
from jax.experimental.pallas import tpu as pltpu
from jax.sharding import PartitionSpec as P

MESH = pl.DeviceIdType.MESH
F32 = jnp.float32
BF16 = jnp.bfloat16
TILE = 256
LANES = 128
LOWEST = float(jnp.finfo(jnp.float32).min)


def chunks_of(tiles):
    sizes, left = [], tiles
    for size in (1, 1, 2, 2, 3):
        if left > size:
            sizes.append(size)
            left -= size
    while left > 0:
        sizes.append(min(4, left))
        left -= sizes[-1]
    starts, at = [], 0
    for size in reversed(sizes):
        starts.append((at, size))
        at += size
    return starts


def split3(e):
    hi = e.astype(BF16)
    rest = e - hi.astype(F32)
    mid = rest.astype(BF16)
    low = (rest - mid.astype(F32)).astype(BF16)
    return hi, mid, low


def prefix_kernel(
    n_cols, h_ref, w_ref, temp_ref, tgt_ref,
    c_ref, scale_ref, off_ref, tgt_out_ref,
    wbuf, hbuf, tri, tri_last, m_all, s_all, t_all, temp_col, rel_col, zmsg, vmsg, back,
    ws, wr, xs, xr, wl, hl, hs, hr, zs, zr, vs, vr,
):
    x, z, v = lax.axis_index("data"), lax.axis_index("hid"), lax.axis_index("vocab")
    rows, depth = h_ref.shape
    half, quarter = depth // 2, rows // 4
    n_tiles = pl.cdiv(n_cols, TILE)
    last_width = n_cols - (n_tiles - 1) * TILE
    plan = chunks_of(n_tiles)
    n_chunks = len(plan)

    side = z // 2
    outer_far, inner_far, near = 3 - 3 * side, 2 - side, 1 - z + 4 * side
    is_outer = jnp.where(z == side * 3, 1, 0)
    z_two, z_one = lax.rem(z + 2, 4), near
    v_two, v_one = lax.rem(v + 2, 4), v + 1 - 2 * lax.rem(v, 2)
    sources = (near, inner_far, outer_far)

    def cols_of(j):
        first, size = plan[j]
        start = first * TILE
        return start, min(n_cols, (first + size) * TILE) - start

    def w_rows(source, part):
        return pl.ds(pl.multiple_of(source * depth + part * half, half), half)

    def w_place(j, source, part):
        start, n = cols_of(j)
        return wbuf.at[w_rows(source, part), pl.ds(start, n)]

    def h_place(q, block=None):
        at = pl.ds(pl.multiple_of(q * quarter, quarter), quarter)
        if block is None:
            return hbuf.at[at]
        return hbuf.at[at, pl.ds(pl.multiple_of(block * depth, depth), depth)]

    def remote(src, dst, send, recv, **to):
        return pltpu.make_async_remote_copy(
            src_ref=src, dst_ref=dst, send_sem=send, recv_sem=recv, device_id=to, device_id_type=MESH
        )

    def direct(j, k, dest, slot):
        start, n = cols_of(j)
        src = w_ref.at[
            pl.ds(pl.multiple_of(x * half, half), half),
            pl.ds(pl.multiple_of(dest * n_cols + start, LANES), n),
        ]
        return remote(src, w_place(j, z, x), ws.at[j, k], wr.at[j, slot], hid=dest)

    def send_near(j):
        return direct(j, 0, near, 0)

    def send_inner(j):
        return direct(j, 1, inner_far, 1 + is_outer)

    def send_outer(j):
        return direct(j, 2, outer_far, 1 + is_outer)

    def landed(j, k):
        place = w_place(j, sources[k], x)
        remote(place, place, ws.at[j, k], wr.at[j, k], hid=sources[k]).wait_recv()

    def forward(j, k):
        place = w_place(j, sources[k], x)
        return remote(place, place, xs.at[j, k], xr.at[j, k], data=1 - x)

    def forwarded(j, k):
        place = w_place(j, sources[k], 1 - x)
        remote(place, place, xs.at[j, k], xr.at[j, k], data=1 - x).wait_recv()

    def own(j):
        start, n = cols_of(j)
        return pltpu.make_async_copy(
            w_ref.at[:, pl.ds(pl.multiple_of(z * n_cols + start, LANES), n)],
            wbuf.at[pl.ds(pl.multiple_of(z * depth, depth), depth), pl.ds(start, n)],
            wl.at[j],
        )

    h_mine = h_ref.at[pl.ds(pl.multiple_of(v * quarter, quarter), quarter)]
    h_own = pltpu.make_async_copy(h_mine, h_place(v, z), hl)
    h_two = remote(h_mine, h_place(v, z), hs.at[0], hr.at[0], hid=z_two)
    h_one = remote(h_mine, h_place(v, z), hs.at[1], hr.at[1], hid=z_one)
    h_relay = remote(h_place(v, z_two), h_place(v, z_two), hs.at[2], hr.at[2], hid=z_one)
    h_chip = remote(h_place(v), h_place(v), hs.at[3], hr.at[3], vocab=v_two)
    h_core = remote(h_place(v), h_place(v), hs.at[4], hr.at[4], vocab=v_one)
    h_both = remote(h_place(v_two), h_place(v_two), hs.at[5], hr.at[5], vocab=v_one)

    def arrived(place, i, **frm):
        remote(place, place, hs.at[i], hr.at[i], **frm).wait_recv()

    barrier = pltpu.get_barrier_semaphore()
    peers = [{"hid": lax.rem(z + d, 4)} for d in (1, 2, 3)]
    peers += [{"data": 1 - x}] + [{"vocab": lax.rem(v + d, 4)} for d in (1, 2, 3)]
    for peer in peers:
        pl.semaphore_signal(barrier, inc=1, device_id=peer, device_id_type=MESH)
    h_own.start()
    own(0).start()
    pl.semaphore_wait(barrier, len(peers))

    h_two.start()
    h_one.start()
    send_near(0).start()
    send_outer(0).start()

    def ones_below(ref, width):
        k = lax.broadcasted_iota(jnp.int32, (width, width), 0)
        c = lax.broadcasted_iota(jnp.int32, (width, width), 1)
        block = jnp.where(k <= c, 1.0, 0.0).astype(BF16)
        for i in range(3):
            ref[pl.ds(i * width, width), :] = block

    ones_below(tri, TILE)
    if last_width != TILE:
        ones_below(tri_last, last_width)
    base = (v * 4 + z) * n_cols
    back[0:1, :] = temp_ref[...]
    back[1:2, :] = (tgt_ref[...] - base).astype(F32)
    cols8 = back[...].T
    temp_col[...] = cols8[:, 0:1]
    rel_col[...] = cols8[:, 1:2].astype(jnp.int32)
    m_all[...] = jnp.full(m_all.shape, LOWEST, F32)
    s_all[...] = jnp.zeros(s_all.shape, F32)
    t_all[...] = jnp.zeros(t_all.shape, F32)

    arrived(h_place(v, z_two), 0, hid=z_two)
    h_relay.start()
    near_at = 1
    for j in range(n_chunks):
        while near_at < min(n_chunks, 3 + 2 * j):
            send_near(near_at).start()
            near_at += 1
        if j > 0:
            send_outer(j).start()
        send_inner(j).start()
    if n_chunks > 1:
        own(1).start()
    arrived(h_place(v, z_one), 1, hid=z_one)
    far = lax.rem(z_one + 2, 4)
    arrived(h_place(v, far), 2, hid=z_one)
    h_own.wait()
    h_chip.start()
    h_core.start()
    landed(0, 0)
    forward(0, 0).start()
    arrived(h_place(v_two), 3, vocab=v_two)
    h_both.start()

    def tile(t, start, width, table):
        span = pl.ds(start, width)
        part = min(rows, 512)

        @pl.loop(0, rows // part)
        def _(i):
            at = pl.ds(pl.multiple_of(i * part, part), part)
            c_ref[at, span] = jnp.dot(hbuf[at, :], wbuf[:, span], preferred_element_type=F32)

        few = min(rows, 256)

        @pl.loop(0, rows // few)
        def _(i):
            at = pl.ds(pl.multiple_of(i * few, few), few)
            logits = c_ref[at, span] * temp_col[at, :]
            top = jnp.max(logits, axis=1, keepdims=True)
            e = jnp.exp(logits - top)
            sums = jnp.dot(jnp.concatenate(split3(e), axis=1), table[...], preferred_element_type=F32)
            c_ref[at, span] = sums
            lane = lax.broadcasted_iota(jnp.int32, (few, width), 1)
            hit = jnp.where(lane == rel_col[at, :] - start, sums, 0.0)
            here = lax.broadcasted_iota(jnp.int32, (few, LANES), 1) == t
            m_all[at, :] = jnp.where(here, top, m_all[at, :])
            s_all[at, :] = jnp.where(here, sums[:, width - 1 : width], s_all[at, :])
            t_all[at, :] = jnp.where(here, jnp.sum(hit, axis=1, keepdims=True), t_all[at, :])

    def compute(j):
        first, size = plan[j]
        whole = size if first + size < n_tiles or last_width == TILE else size - 1
        if whole:

            @pl.loop(first, first + whole)
            def _(t):
                tile(t, pl.multiple_of(t * TILE, TILE), TILE, tri)

        if whole < size:
            tile(n_tiles - 1, (n_tiles - 1) * TILE, last_width, tri_last)

    def complete(j):
        for k in range(3):
            forwarded(j, k)
        own(j).wait()

    near_at = 1
    for j in range(n_chunks):
        while near_at < min(n_chunks, 2 + 2 * j):
            landed(near_at, 0)
            forward(near_at, 0).start()
            near_at += 1
        for k in (1, 2):
            landed(j, k)
            forward(j, k).start()
        if j == 0:
            arrived(h_place(v_one), 4, vocab=v_one)
            arrived(h_place(lax.rem(v_one + 2, 4)), 5, vocab=v_one)
        else:
            complete(j - 1)
            compute(j - 1)
        if j + 2 < n_chunks:
            own(j + 2).start()
    complete(n_chunks - 1)
    compute(n_chunks - 1)

    lane = lax.broadcasted_iota(jnp.int32, (rows, LANES), 1)
    top = jnp.max(m_all[...], axis=1, keepdims=True)
    shrink = jnp.exp(m_all[...] - top)
    parts = s_all[...] * shrink
    k = lax.broadcasted_iota(jnp.int32, (LANES, LANES), 0)
    c = lax.broadcasted_iota(jnp.int32, (LANES, LANES), 1)
    strict = jnp.where(k < c, 1.0, 0.0).astype(BF16)
    before = sum(jnp.dot(p, strict, preferred_element_type=F32) for p in split3(parts))
    s_all[...] = before
    rel = rel_col[...]
    holds = (rel >= lane * TILE) & (rel < (lane + 1) * TILE) & (rel < n_cols)
    found = t_all[...] * shrink + jnp.where(holds, before, 0.0)
    total = jnp.sum(parts, axis=1, keepdims=True)
    at_tgt = jnp.sum(found, axis=1, keepdims=True)
    packed = jnp.where(lane == 0, top, jnp.where(lane == 1, total, at_tgt))
    zmsg[z] = packed.T[0:4, :]

    for j in range(n_chunks):
        send_near(j).wait_send()
        send_inner(j).wait_send()
        send_outer(j).wait_send()
        for k in range(3):
            forward(j, k).wait_send()
    for copy in (h_two, h_one, h_relay, h_chip, h_core, h_both):
        copy.wait_send()

    def z_send(d):
        to = lax.rem(z + d, 4)
        return remote(zmsg.at[z], zmsg.at[z], zs.at[d - 1], zr.at[d - 1], hid=to)

    def v_send(d):
        to = lax.rem(v + d, 4)
        return remote(vmsg.at[v], vmsg.at[v], vs.at[d - 1], vr.at[d - 1], vocab=to)

    for d in (1, 2, 3):
        z_send(d).start()
    for d in (1, 2, 3):
        frm = lax.rem(z + 4 - d, 4)
        remote(zmsg.at[frm], zmsg.at[frm], zs.at[d - 1], zr.at[d - 1], hid=frm).wait_recv()

    ids = tgt_ref[...]
    maxes = [zmsg[h, 0:1, :] for h in range(4)]
    v_max = functools.reduce(jnp.maximum, maxes)
    v_sum = jnp.zeros((1, rows), F32)
    v_tgt = jnp.zeros((1, rows), F32)
    mine_before = jnp.zeros((1, rows), F32)
    for h in range(4):
        mine_before = jnp.where(h == z, v_sum, mine_before)
        f = jnp.exp(maxes[h] - v_max)
        low = (v * 4 + h) * n_cols
        inside = (ids >= low) & (ids < low + n_cols)
        v_tgt += jnp.where(inside, zmsg[h, 2:3, :] * f + v_sum, 0.0)
        v_sum += zmsg[h, 1:2, :] * f
    vmsg[v, 0:1, :] = v_max
    vmsg[v, 1:2, :] = v_sum
    vmsg[v, 2:3, :] = v_tgt
    vmsg[v, 3:4, :] = v_tgt

    for d in (1, 2, 3):
        z_send(d).wait_send()
    for d in (1, 2, 3):
        v_send(d).start()
    for d in (1, 2, 3):
        frm = lax.rem(v + 4 - d, 4)
        remote(vmsg.at[frm], vmsg.at[frm], vs.at[d - 1], vr.at[d - 1], vocab=frm).wait_recv()

    maxes = [vmsg[u, 0:1, :] for u in range(4)]
    g_max = functools.reduce(jnp.maximum, maxes)
    g_sum = jnp.zeros((1, rows), F32)
    g_tgt = jnp.zeros((1, rows), F32)
    g_before = jnp.zeros((1, rows), F32)
    for u in range(4):
        f = jnp.exp(maxes[u] - g_max)
        g_before = jnp.where(u == v, g_sum + mine_before * f, g_before)
        low = u * 4 * n_cols
        inside = (ids >= low) & (ids < low + 4 * n_cols)
        g_tgt += jnp.where(inside, vmsg[u, 2:3, :] * f + g_sum, 0.0)
        g_sum += vmsg[u, 1:2, :] * f
    tgt_out_ref[...] = g_tgt / g_sum
    back[0:1, :] = g_max
    back[1:2, :] = g_sum
    back[2:3, :] = g_before
    cols8 = back[...].T
    g_max, g_sum, g_before = cols8[:, 0:1], cols8[:, 1:2], cols8[:, 2:3]
    mine = jnp.max(m_all[...], axis=1, keepdims=True)
    scale_ref[...] = jnp.exp(m_all[...] - g_max) / g_sum
    off_ref[...] = (s_all[...] * jnp.exp(mine - g_max) + g_before) / g_sum
    for d in (1, 2, 3):
        v_send(d).wait_send()


def finish_kernel(c_ref, scale_ref, off_ref, tgt_ref, out_ref, tgt_out_ref):
    n, n_cols = out_ref.shape
    at = pl.ds(pl.multiple_of(pl.program_id(0) * n, n), n)
    for start in range(0, n_cols, TILE):
        t, stop = start // TILE, min(n_cols, start + TILE)
        out_ref[:, start:stop] = (
            c_ref[at, start:stop] * scale_ref[at, t : t + 1] + off_ref[at, t : t + 1]
        )
    tgt_out_ref[...] = tgt_ref[...]


def solution(mesh):
    n_hid, n_voc = mesh.shape["hid"], mesh.shape["vocab"]
    assert n_hid == 4 and n_voc == 4 and mesh.shape["data"] == 2

    def local_step(h_blk, w_blk, temp_blk, tgt_blk):
        rows, depth = h_blk.shape
        n_cols = w_blk.shape[1] // n_hid
        n_tiles = pl.cdiv(n_cols, TILE)
        last_width = n_cols - (n_tiles - 1) * TILE
        assert n_tiles <= LANES and n_cols % LANES == 0
        n_chunks = len(chunks_of(n_tiles))
        vmem = pl.BlockSpec(memory_space=pltpu.VMEM)
        hbm = pl.BlockSpec(memory_space=pltpu.HBM)
        dma = pltpu.SemaphoreType.DMA
        table = pltpu.VMEM((rows, LANES), F32)
        c, scale, off, tgt = pl.pallas_call(
            functools.partial(prefix_kernel, n_cols),
            out_shape=(
                pltpu.VMEM((rows, n_cols), F32),
                pltpu.VMEM((rows, LANES), F32),
                pltpu.VMEM((rows, LANES), F32),
                pltpu.VMEM((1, rows), F32),
            ),
            in_specs=[hbm, hbm, vmem, vmem],
            out_specs=[vmem] * 4,
            scratch_shapes=[
                pltpu.VMEM((4 * depth, n_cols), BF16),
                pltpu.VMEM((rows, 4 * depth), BF16),
                pltpu.VMEM((3 * TILE, TILE), BF16),
                pltpu.VMEM((3 * last_width, last_width), BF16),
                table,
                table,
                table,
                pltpu.VMEM((rows, 1), F32),
                pltpu.VMEM((rows, 1), jnp.int32),
                pltpu.VMEM((4, 4, rows), F32),
                pltpu.VMEM((4, 4, rows), F32),
                pltpu.VMEM((8, rows), F32),
                dma((n_chunks, 3)),
                dma((n_chunks, 3)),
                dma((n_chunks, 3)),
                dma((n_chunks, 3)),
                dma((n_chunks,)),
                dma,
                dma((6,)),
                dma((6,)),
                dma((3,)),
                dma((3,)),
                dma((3,)),
                dma((3,)),
            ],
            compiler_params=pltpu.CompilerParams(
                collective_id=0, has_side_effects=True, vmem_limit_bytes=37 << 20
            ),
            name="prefix",
        )(h_blk, w_blk, temp_blk.reshape(1, rows), tgt_blk.reshape(1, rows))
        n = min(rows, 128)
        cdf, cdf_tgt = pl.pallas_call(
            finish_kernel,
            grid=(rows // n,),
            out_shape=(
                jax.ShapeDtypeStruct((rows, n_cols), F32),
                jax.ShapeDtypeStruct((1, rows), F32),
            ),
            in_specs=[vmem] * 4,
            out_specs=[
                pl.BlockSpec((n, n_cols), lambda i: (i, 0)),
                pl.BlockSpec((1, rows), lambda i: (0, 0)),
            ],
            compiler_params=pltpu.CompilerParams(vmem_limit_bytes=9 << 20),
            name="finish",
        )(c, scale, off, tgt)
        return cdf, cdf_tgt.reshape(rows)

    return jax.shard_map(
        local_step,
        mesh=mesh,
        in_specs=(P("data", "hid"), P("hid", "vocab"), P("data"), P("data")),
        out_specs=(P("data", ("vocab", "hid")), P("data")),
        check_vma=False,
    )
```

```python
import functools

import jax
import jax.numpy as jnp
from jax import lax
from jax.experimental import pallas as pl
from jax.experimental.pallas import tpu as pltpu
from jax.sharding import PartitionSpec as P

MESH = pl.DeviceIdType.MESH
F32 = jnp.float32
BF16 = jnp.bfloat16
TILE = 256
LANES = 128
LOWEST = float(jnp.finfo(jnp.float32).min)


def chunks_of(tiles):
    sizes, left = [], tiles
    for size in (1, 1, 2, 2, 3):
        if left > size:
            sizes.append(size)
            left -= size
    while left > 0:
        sizes.append(min(4, left))
        left -= sizes[-1]
    starts, at = [], 0
    for size in reversed(sizes):
        starts.append((at, size))
        at += size
    return starts


def split3(e):
    hi = e.astype(BF16)
    rest = e - hi.astype(F32)
    mid = rest.astype(BF16)
    low = (rest - mid.astype(F32)).astype(BF16)
    return hi, mid, low


def prefix_kernel(
    n_cols, h_ref, w_ref, temp_ref, tgt_ref,
    c_ref, scale_ref, off_ref, tgt_out_ref,
    wbuf, hbuf, tri, tri_last, m_all, s_all, t_all, temp_col, rel_col, zmsg, vmsg, back,
    ws, wr, xs, xr, wl, hl, hs, hr, zs, zr, vs, vr,
):
    x, z, v = lax.axis_index("data"), lax.axis_index("hid"), lax.axis_index("vocab")
    rows, depth = h_ref.shape
    half, quarter = depth // 2, rows // 4
    n_tiles = pl.cdiv(n_cols, TILE)
    last_width = n_cols - (n_tiles - 1) * TILE
    plan = chunks_of(n_tiles)
    n_chunks = len(plan)

    side = z // 2
    outer_far, inner_far, near = 3 - 3 * side, 2 - side, 1 - z + 4 * side
    is_outer = jnp.where(z == side * 3, 1, 0)
    z_two, z_one = lax.rem(z + 2, 4), near
    v_two, v_one = lax.rem(v + 2, 4), v + 1 - 2 * lax.rem(v, 2)
    sources = (near, inner_far, outer_far)

    def cols_of(j):
        first, size = plan[j]
        start = first * TILE
        return start, min(n_cols, (first + size) * TILE) - start

    def w_rows(source, part):
        return pl.ds(pl.multiple_of(source * depth + part * half, half), half)

    def w_place(j, source, part):
        start, n = cols_of(j)
        return wbuf.at[w_rows(source, part), pl.ds(start, n)]

    def h_place(q, block=None):
        at = pl.ds(pl.multiple_of(q * quarter, quarter), quarter)
        if block is None:
            return hbuf.at[at]
        return hbuf.at[at, pl.ds(pl.multiple_of(block * depth, depth), depth)]

    def remote(src, dst, send, recv, **to):
        return pltpu.make_async_remote_copy(
            src_ref=src, dst_ref=dst, send_sem=send, recv_sem=recv, device_id=to, device_id_type=MESH
        )

    def direct(j, k, dest, slot):
        start, n = cols_of(j)
        src = w_ref.at[
            pl.ds(pl.multiple_of(x * half, half), half),
            pl.ds(pl.multiple_of(dest * n_cols + start, LANES), n),
        ]
        return remote(src, w_place(j, z, x), ws.at[j, k], wr.at[j, slot], hid=dest)

    def send_near(j):
        return direct(j, 0, near, 0)

    odd = lax.rem(v, 2)
    far_first = outer_far + odd * (inner_far - outer_far)
    far_second = inner_far + odd * (outer_far - inner_far)

    def send_inner(j):
        return direct(j, 1, far_second, 1 + is_outer)

    def send_outer(j):
        return direct(j, 2, far_first, 1 + is_outer)

    def landed(j, k):
        place = w_place(j, sources[k], x)
        remote(place, place, ws.at[j, k], wr.at[j, k], hid=sources[k]).wait_recv()

    def forward(j, k):
        place = w_place(j, sources[k], x)
        return remote(place, place, xs.at[j, k], xr.at[j, k], data=1 - x)

    def forwarded(j, k):
        place = w_place(j, sources[k], 1 - x)
        remote(place, place, xs.at[j, k], xr.at[j, k], data=1 - x).wait_recv()

    def own(j):
        start, n = cols_of(j)
        return pltpu.make_async_copy(
            w_ref.at[:, pl.ds(pl.multiple_of(z * n_cols + start, LANES), n)],
            wbuf.at[pl.ds(pl.multiple_of(z * depth, depth), depth), pl.ds(start, n)],
            wl.at[j],
        )

    h_mine = h_ref.at[pl.ds(pl.multiple_of(v * quarter, quarter), quarter)]
    h_own = pltpu.make_async_copy(h_mine, h_place(v, z), hl)
    h_two = remote(h_mine, h_place(v, z), hs.at[0], hr.at[0], hid=z_two)
    h_one = remote(h_mine, h_place(v, z), hs.at[1], hr.at[1], hid=z_one)
    h_relay = remote(h_place(v, z_two), h_place(v, z_two), hs.at[2], hr.at[2], hid=z_one)
    h_chip = remote(h_place(v), h_place(v), hs.at[3], hr.at[3], vocab=v_two)
    h_core = remote(h_place(v), h_place(v), hs.at[4], hr.at[4], vocab=v_one)
    h_both = remote(h_place(v_two), h_place(v_two), hs.at[5], hr.at[5], vocab=v_one)

    def arrived(place, i, **frm):
        remote(place, place, hs.at[i], hr.at[i], **frm).wait_recv()

    barrier = pltpu.get_barrier_semaphore()
    peers = [{"hid": lax.rem(z + d, 4)} for d in (1, 2, 3)]
    peers += [{"data": 1 - x}] + [{"vocab": lax.rem(v + d, 4)} for d in (1, 2, 3)]
    for peer in peers:
        pl.semaphore_signal(barrier, inc=1, device_id=peer, device_id_type=MESH)
    h_own.start()
    own(0).start()
    pl.semaphore_wait(barrier, len(peers))

    h_two.start()
    h_one.start()
    send_near(0).start()
    send_outer(0).start()

    def ones_below(ref, width):
        k = lax.broadcasted_iota(jnp.int32, (width, width), 0)
        c = lax.broadcasted_iota(jnp.int32, (width, width), 1)
        block = jnp.where(k <= c, 1.0, 0.0).astype(BF16)
        for i in range(3):
            ref[pl.ds(i * width, width), :] = block

    ones_below(tri, TILE)
    if last_width != TILE:
        ones_below(tri_last, last_width)
    base = (v * 4 + z) * n_cols
    back[0:1, :] = temp_ref[...]
    back[1:2, :] = (tgt_ref[...] - base).astype(F32)
    cols8 = back[...].T
    temp_col[...] = cols8[:, 0:1]
    rel_col[...] = cols8[:, 1:2].astype(jnp.int32)
    m_all[...] = jnp.full(m_all.shape, LOWEST, F32)
    s_all[...] = jnp.zeros(s_all.shape, F32)
    t_all[...] = jnp.zeros(t_all.shape, F32)

    arrived(h_place(v, z_two), 0, hid=z_two)
    h_relay.start()
    near_at = 1
    for j in range(n_chunks):
        while near_at < min(n_chunks, 3 + 2 * j):
            send_near(near_at).start()
            near_at += 1
        if j > 0:
            send_outer(j).start()
        send_inner(j).start()
    if n_chunks > 1:
        own(1).start()
    arrived(h_place(v, z_one), 1, hid=z_one)
    far = lax.rem(z_one + 2, 4)
    arrived(h_place(v, far), 2, hid=z_one)
    h_own.wait()
    h_chip.start()
    h_core.start()
    landed(0, 0)
    forward(0, 0).start()
    arrived(h_place(v_two), 3, vocab=v_two)
    h_both.start()

    def tile(t, start, width, table):
        span = pl.ds(start, width)
        part = min(rows, 512)

        @pl.loop(0, rows // part)
        def _(i):
            at = pl.ds(pl.multiple_of(i * part, part), part)
            c_ref[at, span] = jnp.dot(hbuf[at, :], wbuf[:, span], preferred_element_type=F32)

        few = min(rows, 256)

        @pl.loop(0, rows // few)
        def _(i):
            at = pl.ds(pl.multiple_of(i * few, few), few)
            logits = c_ref[at, span] * temp_col[at, :]
            top = jnp.max(logits, axis=1, keepdims=True)
            e = jnp.exp(logits - top)
            sums = jnp.dot(jnp.concatenate(split3(e), axis=1), table[...], preferred_element_type=F32)
            c_ref[at, span] = sums
            lane = lax.broadcasted_iota(jnp.int32, (few, width), 1)
            hit = jnp.where(lane == rel_col[at, :] - start, sums, 0.0)
            here = lax.broadcasted_iota(jnp.int32, (few, LANES), 1) == t
            m_all[at, :] = jnp.where(here, top, m_all[at, :])
            s_all[at, :] = jnp.where(here, sums[:, width - 1 : width], s_all[at, :])
            t_all[at, :] = jnp.where(here, jnp.sum(hit, axis=1, keepdims=True), t_all[at, :])

    def compute(j):
        first, size = plan[j]
        whole = size if first + size < n_tiles or last_width == TILE else size - 1
        if whole:

            @pl.loop(first, first + whole)
            def _(t):
                tile(t, pl.multiple_of(t * TILE, TILE), TILE, tri)

        if whole < size:
            tile(n_tiles - 1, (n_tiles - 1) * TILE, last_width, tri_last)

    def complete(j):
        for k in range(3):
            forwarded(j, k)
        own(j).wait()

    near_at = 1
    for j in range(n_chunks):
        while near_at < min(n_chunks, 2 + 2 * j):
            landed(near_at, 0)
            forward(near_at, 0).start()
            near_at += 1
        for k in (1, 2):
            landed(j, k)
            forward(j, k).start()
        if j == 0:
            arrived(h_place(v_one), 4, vocab=v_one)
            arrived(h_place(lax.rem(v_one + 2, 4)), 5, vocab=v_one)
        else:
            complete(j - 1)
            compute(j - 1)
        if j + 2 < n_chunks:
            own(j + 2).start()
    complete(n_chunks - 1)
    compute(n_chunks - 1)

    lane = lax.broadcasted_iota(jnp.int32, (rows, LANES), 1)
    top = jnp.max(m_all[...], axis=1, keepdims=True)
    shrink = jnp.exp(m_all[...] - top)
    parts = s_all[...] * shrink
    k = lax.broadcasted_iota(jnp.int32, (LANES, LANES), 0)
    c = lax.broadcasted_iota(jnp.int32, (LANES, LANES), 1)
    strict = jnp.where(k < c, 1.0, 0.0).astype(BF16)
    before = sum(jnp.dot(p, strict, preferred_element_type=F32) for p in split3(parts))
    s_all[...] = before
    rel = rel_col[...]
    holds = (rel >= lane * TILE) & (rel < (lane + 1) * TILE) & (rel < n_cols)
    found = t_all[...] * shrink + jnp.where(holds, before, 0.0)
    total = jnp.sum(parts, axis=1, keepdims=True)
    at_tgt = jnp.sum(found, axis=1, keepdims=True)
    packed = jnp.where(lane == 0, top, jnp.where(lane == 1, total, at_tgt))
    zmsg[z] = packed.T[0:4, :]

    for j in range(n_chunks):
        send_near(j).wait_send()
        send_inner(j).wait_send()
        send_outer(j).wait_send()
        for k in range(3):
            forward(j, k).wait_send()
    for copy in (h_two, h_one, h_relay, h_chip, h_core, h_both):
        copy.wait_send()

    def z_send(d):
        to = lax.rem(z + d, 4)
        return remote(zmsg.at[z], zmsg.at[z], zs.at[d - 1], zr.at[d - 1], hid=to)

    def v_send(d):
        to = lax.rem(v + d, 4)
        return remote(vmsg.at[v], vmsg.at[v], vs.at[d - 1], vr.at[d - 1], vocab=to)

    for d in (1, 2, 3):
        z_send(d).start()
    for d in (1, 2, 3):
        frm = lax.rem(z + 4 - d, 4)
        remote(zmsg.at[frm], zmsg.at[frm], zs.at[d - 1], zr.at[d - 1], hid=frm).wait_recv()

    ids = tgt_ref[...]
    maxes = [zmsg[h, 0:1, :] for h in range(4)]
    v_max = functools.reduce(jnp.maximum, maxes)
    v_sum = jnp.zeros((1, rows), F32)
    v_tgt = jnp.zeros((1, rows), F32)
    mine_before = jnp.zeros((1, rows), F32)
    for h in range(4):
        mine_before = jnp.where(h == z, v_sum, mine_before)
        f = jnp.exp(maxes[h] - v_max)
        low = (v * 4 + h) * n_cols
        inside = (ids >= low) & (ids < low + n_cols)
        v_tgt += jnp.where(inside, zmsg[h, 2:3, :] * f + v_sum, 0.0)
        v_sum += zmsg[h, 1:2, :] * f
    vmsg[v, 0:1, :] = v_max
    vmsg[v, 1:2, :] = v_sum
    vmsg[v, 2:3, :] = v_tgt
    vmsg[v, 3:4, :] = v_tgt

    for d in (1, 2, 3):
        z_send(d).wait_send()
    for d in (1, 2, 3):
        v_send(d).start()
    for d in (1, 2, 3):
        frm = lax.rem(v + 4 - d, 4)
        remote(vmsg.at[frm], vmsg.at[frm], vs.at[d - 1], vr.at[d - 1], vocab=frm).wait_recv()

    maxes = [vmsg[u, 0:1, :] for u in range(4)]
    g_max = functools.reduce(jnp.maximum, maxes)
    g_sum = jnp.zeros((1, rows), F32)
    g_tgt = jnp.zeros((1, rows), F32)
    g_before = jnp.zeros((1, rows), F32)
    for u in range(4):
        f = jnp.exp(maxes[u] - g_max)
        g_before = jnp.where(u == v, g_sum + mine_before * f, g_before)
        low = u * 4 * n_cols
        inside = (ids >= low) & (ids < low + 4 * n_cols)
        g_tgt += jnp.where(inside, vmsg[u, 2:3, :] * f + g_sum, 0.0)
        g_sum += vmsg[u, 1:2, :] * f
    tgt_out_ref[...] = g_tgt / g_sum
    back[0:1, :] = g_max
    back[1:2, :] = g_sum
    back[2:3, :] = g_before
    cols8 = back[...].T
    g_max, g_sum, g_before = cols8[:, 0:1], cols8[:, 1:2], cols8[:, 2:3]
    mine = jnp.max(m_all[...], axis=1, keepdims=True)
    scale_ref[...] = jnp.exp(m_all[...] - g_max) / g_sum
    off_ref[...] = (s_all[...] * jnp.exp(mine - g_max) + g_before) / g_sum
    for d in (1, 2, 3):
        v_send(d).wait_send()


def finish_kernel(c_ref, scale_ref, off_ref, tgt_ref, out_ref, tgt_out_ref):
    n, n_cols = out_ref.shape
    at = pl.ds(pl.multiple_of(pl.program_id(0) * n, n), n)
    for start in range(0, n_cols, TILE):
        t, stop = start // TILE, min(n_cols, start + TILE)
        out_ref[:, start:stop] = (
            c_ref[at, start:stop] * scale_ref[at, t : t + 1] + off_ref[at, t : t + 1]
        )
    tgt_out_ref[...] = tgt_ref[...]


def solution(mesh):
    n_hid, n_voc = mesh.shape["hid"], mesh.shape["vocab"]
    assert n_hid == 4 and n_voc == 4 and mesh.shape["data"] == 2

    def local_step(h_blk, w_blk, temp_blk, tgt_blk):
        rows, depth = h_blk.shape
        n_cols = w_blk.shape[1] // n_hid
        n_tiles = pl.cdiv(n_cols, TILE)
        last_width = n_cols - (n_tiles - 1) * TILE
        assert n_tiles <= LANES and n_cols % LANES == 0
        n_chunks = len(chunks_of(n_tiles))
        vmem = pl.BlockSpec(memory_space=pltpu.VMEM)
        hbm = pl.BlockSpec(memory_space=pltpu.HBM)
        dma = pltpu.SemaphoreType.DMA
        table = pltpu.VMEM((rows, LANES), F32)
        c, scale, off, tgt = pl.pallas_call(
            functools.partial(prefix_kernel, n_cols),
            out_shape=(
                pltpu.VMEM((rows, n_cols), F32),
                pltpu.VMEM((rows, LANES), F32),
                pltpu.VMEM((rows, LANES), F32),
                pltpu.VMEM((1, rows), F32),
            ),
            in_specs=[hbm, hbm, vmem, vmem],
            out_specs=[vmem] * 4,
            scratch_shapes=[
                pltpu.VMEM((4 * depth, n_cols), BF16),
                pltpu.VMEM((rows, 4 * depth), BF16),
                pltpu.VMEM((3 * TILE, TILE), BF16),
                pltpu.VMEM((3 * last_width, last_width), BF16),
                table,
                table,
                table,
                pltpu.VMEM((rows, 1), F32),
                pltpu.VMEM((rows, 1), jnp.int32),
                pltpu.VMEM((4, 4, rows), F32),
                pltpu.VMEM((4, 4, rows), F32),
                pltpu.VMEM((8, rows), F32),
                dma((n_chunks, 3)),
                dma((n_chunks, 3)),
                dma((n_chunks, 3)),
                dma((n_chunks, 3)),
                dma((n_chunks,)),
                dma,
                dma((6,)),
                dma((6,)),
                dma((3,)),
                dma((3,)),
                dma((3,)),
                dma((3,)),
            ],
            compiler_params=pltpu.CompilerParams(
                collective_id=0, has_side_effects=True, vmem_limit_bytes=37 << 20
            ),
            name="prefix",
        )(h_blk, w_blk, temp_blk.reshape(1, rows), tgt_blk.reshape(1, rows))
        n = min(rows, 128)
        cdf, cdf_tgt = pl.pallas_call(
            finish_kernel,
            grid=(rows // n,),
            out_shape=(
                jax.ShapeDtypeStruct((rows, n_cols), F32),
                jax.ShapeDtypeStruct((1, rows), F32),
            ),
            in_specs=[vmem] * 4,
            out_specs=[
                pl.BlockSpec((n, n_cols), lambda i: (i, 0)),
                pl.BlockSpec((1, rows), lambda i: (0, 0)),
            ],
            compiler_params=pltpu.CompilerParams(vmem_limit_bytes=9 << 20),
            name="finish",
        )(c, scale, off, tgt)
        return cdf, cdf_tgt.reshape(rows)

    return jax.shard_map(
        local_step,
        mesh=mesh,
        in_specs=(P("data", "hid"), P("hid", "vocab"), P("data"), P("data")),
        out_specs=(P("data", ("vocab", "hid")), P("data")),
        check_vma=False,
    )
```

```python
import functools

import jax
import jax.numpy as jnp
from jax import lax
from jax.experimental import pallas as pl
from jax.experimental.pallas import tpu as pltpu
from jax.sharding import PartitionSpec as P

MESH = pl.DeviceIdType.MESH
F32 = jnp.float32
BF16 = jnp.bfloat16
TILE = 256
LANES = 128
LOWEST = float(jnp.finfo(jnp.float32).min)


def chunks_of(tiles):
    sizes, left = [], tiles
    for size in (1, 1, 1, 2, 2):
        if left > size:
            sizes.append(size)
            left -= size
    while left > 0:
        sizes.append(min(3, left))
        left -= sizes[-1]
    starts, at = [], 0
    for size in reversed(sizes):
        starts.append((at, size))
        at += size
    return starts


def service_order(plan, tiles):
    half = tiles / 2
    events = [(0.5 * tiles, "h line", 0), (0.9 * tiles, "h chip", 0)]
    for j, (first, size) in enumerate(plan):
        end = first + size
        events.append((end, 0, j))
        events.append((2 * end if end < half else tiles + 4 * (end - half), 1, j))
        events.append((tiles + 4 * end if end < half else 3 * tiles + 2 * (end - half), 2, j))
    events.sort(key=lambda e: e[0])
    return [e[1:] for e in events]


def split3(e):
    hi = e.astype(BF16)
    rest = e - hi.astype(F32)
    mid = rest.astype(BF16)
    low = (rest - mid.astype(F32)).astype(BF16)
    return hi, mid, low


def prefix_kernel(
    n_cols, h_ref, w_ref, temp_ref, tgt_ref,
    c_ref, scale_ref, off_ref, tgt_out_ref, relay_ref,
    wbuf, hbuf, tri, tri_last, m_all, s_all, t_all, temp_col, rel_col, zmsg, vmsg, back,
    ws, wr, xs, xr, rs, rr, wl, hl, hs, hr, zs, zr, vs, vr,
):
    x, z, v = lax.axis_index("data"), lax.axis_index("hid"), lax.axis_index("vocab")
    rows, depth = h_ref.shape
    half, quarter = depth // 2, rows // 4
    n_tiles = pl.cdiv(n_cols, TILE)
    last_width = n_cols - (n_tiles - 1) * TILE
    plan = chunks_of(n_tiles)
    n_chunks = len(plan)

    side = z // 2
    outer_far, inner_far, near = 3 - 3 * side, 2 - side, 1 - z + 4 * side
    is_outer = jnp.where(z == side * 3, 1, 0)
    z_two, z_one = lax.rem(z + 2, 4), near
    v_two, v_one = lax.rem(v + 2, 4), v + 1 - 2 * lax.rem(v, 2)
    sources = (near, inner_far, outer_far)

    def cols_of(j):
        first, size = plan[j]
        start = first * TILE
        return start, min(n_cols, (first + size) * TILE) - start

    def w_rows(source, part):
        return pl.ds(pl.multiple_of(source * depth + part * half, half), half)

    def w_place(j, source, part):
        start, n = cols_of(j)
        return wbuf.at[w_rows(source, part), pl.ds(start, n)]

    def h_place(q, block=None):
        at = pl.ds(pl.multiple_of(q * quarter, quarter), quarter)
        if block is None:
            return hbuf.at[at]
        return hbuf.at[at, pl.ds(pl.multiple_of(block * depth, depth), depth)]

    def remote(src, dst, send, recv, **to):
        return pltpu.make_async_remote_copy(
            src_ref=src, dst_ref=dst, send_sem=send, recv_sem=recv, device_id=to, device_id_type=MESH
        )

    def direct(j, k, dest, slot):
        start, n = cols_of(j)
        src = w_ref.at[
            pl.ds(pl.multiple_of(x * half, half), half),
            pl.ds(pl.multiple_of(dest * n_cols + start, LANES), n),
        ]
        return remote(src, w_place(j, z, x), ws.at[j, k], wr.at[j, slot], hid=dest)

    def send_near(j):
        return direct(j, 0, near, 0)

    def send_inner(j):
        return direct(j, 1, inner_far, 1 + is_outer)

    def relay_place(j, s):
        start, n = cols_of(j)
        return relay_ref.at[s, :, pl.ds(start, n)]

    def send_outer(j):
        start, n = cols_of(j)
        src = w_ref.at[
            pl.ds(pl.multiple_of(x * half, half), half),
            pl.ds(pl.multiple_of(outer_far * n_cols + start, LANES), n),
        ]
        return remote(src, relay_place(j, is_outer), ws.at[j, 2], rr.at[j, is_outer], hid=inner_far)

    def relay_landed(j, s):
        place = relay_place(j, s)
        remote(place, place, ws.at[j, 2], rr.at[j, s], hid=inner_far).wait_recv()

    def relay(j, s):
        return remote(relay_place(j, s), w_place(j, sources[1 + s], x), rs.at[j, s], wr.at[j, 1 + s], hid=near)

    def landed(j, k):
        place = w_place(j, sources[k], x)
        remote(place, place, ws.at[j, k], wr.at[j, k], hid=sources[k]).wait_recv()

    def forward(j, k):
        place = w_place(j, sources[k], x)
        return remote(place, place, xs.at[j, k], xr.at[j, k], data=1 - x)

    def forwarded(j, k):
        place = w_place(j, sources[k], 1 - x)
        remote(place, place, xs.at[j, k], xr.at[j, k], data=1 - x).wait_recv()

    def own(j):
        start, n = cols_of(j)
        return pltpu.make_async_copy(
            w_ref.at[:, pl.ds(pl.multiple_of(z * n_cols + start, LANES), n)],
            wbuf.at[pl.ds(pl.multiple_of(z * depth, depth), depth), pl.ds(start, n)],
            wl.at[j],
        )

    h_mine = h_ref.at[pl.ds(pl.multiple_of(v * quarter, quarter), quarter)]
    h_own = pltpu.make_async_copy(h_mine, h_place(v, z), hl)
    h_two = remote(h_mine, h_place(v, z), hs.at[0], hr.at[0], hid=z_two)
    h_one = remote(h_mine, h_place(v, z), hs.at[1], hr.at[1], hid=z_one)
    h_relay = remote(h_place(v, z_two), h_place(v, z_two), hs.at[2], hr.at[2], hid=z_one)
    h_chip = remote(h_place(v), h_place(v), hs.at[3], hr.at[3], vocab=v_two)
    h_core = remote(h_place(v), h_place(v), hs.at[4], hr.at[4], vocab=v_one)
    h_both = remote(h_place(v_two), h_place(v_two), hs.at[5], hr.at[5], vocab=v_one)

    def arrived(place, i, **frm):
        remote(place, place, hs.at[i], hr.at[i], **frm).wait_recv()

    barrier = pltpu.get_barrier_semaphore()
    peers = [{"hid": lax.rem(z + d, 4)} for d in (1, 2, 3)]
    peers += [{"data": 1 - x}] + [{"vocab": lax.rem(v + d, 4)} for d in (1, 2, 3)]
    for peer in peers:
        pl.semaphore_signal(barrier, inc=1, device_id=peer, device_id_type=MESH)
    h_own.start()
    own(0).start()
    pl.semaphore_wait(barrier, len(peers))

    h_two.start()
    h_one.start()
    send_near(0).start()
    send_outer(0).start()

    def ones_below(ref, width):
        k = lax.broadcasted_iota(jnp.int32, (width, width), 0)
        c = lax.broadcasted_iota(jnp.int32, (width, width), 1)
        block = jnp.where(k <= c, 1.0, 0.0).astype(BF16)
        for i in range(3):
            ref[pl.ds(i * width, width), :] = block

    ones_below(tri, TILE)
    if last_width != TILE:
        ones_below(tri_last, last_width)
    base = (v * 4 + z) * n_cols
    back[0:1, :] = temp_ref[...]
    back[1:2, :] = (tgt_ref[...] - base).astype(F32)
    cols8 = back[...].T
    temp_col[...] = cols8[:, 0:1]
    rel_col[...] = cols8[:, 1:2].astype(jnp.int32)
    m_all[...] = jnp.full(m_all.shape, LOWEST, F32)
    s_all[...] = jnp.zeros(s_all.shape, F32)
    t_all[...] = jnp.zeros(t_all.shape, F32)

    arrived(h_place(v, z_two), 0, hid=z_two)
    h_relay.start()
    for j in range(1, n_chunks):
        send_near(j).start()
    send_inner(0).start()
    for j in range(1, n_chunks):
        send_outer(j).start()
        send_inner(j).start()
    if n_chunks > 1:
        own(1).start()

    def tile(t, start, width, table):
        span = pl.ds(start, width)
        part = min(rows, 512)

        @pl.loop(0, rows // part)
        def _(i):
            at = pl.ds(pl.multiple_of(i * part, part), part)
            c_ref[at, span] = jnp.dot(hbuf[at, :], wbuf[:, span], preferred_element_type=F32)

        few = min(rows, 256)

        @pl.loop(0, rows // few)
        def _(i):
            at = pl.ds(pl.multiple_of(i * few, few), few)
            logits = c_ref[at, span] * temp_col[at, :]
            top = jnp.max(logits, axis=1, keepdims=True)
            e = jnp.exp(logits - top)
            sums = jnp.dot(jnp.concatenate(split3(e), axis=1), table[...], preferred_element_type=F32)
            c_ref[at, span] = sums
            lane = lax.broadcasted_iota(jnp.int32, (few, width), 1)
            hit = jnp.where(lane == rel_col[at, :] - start, sums, 0.0)
            here = lax.broadcasted_iota(jnp.int32, (few, LANES), 1) == t
            m_all[at, :] = jnp.where(here, top, m_all[at, :])
            s_all[at, :] = jnp.where(here, sums[:, width - 1 : width], s_all[at, :])
            t_all[at, :] = jnp.where(here, jnp.sum(hit, axis=1, keepdims=True), t_all[at, :])

    def compute(j):
        first, size = plan[j]
        whole = size if first + size < n_tiles or last_width == TILE else size - 1
        if whole:

            @pl.loop(first, first + whole)
            def _(t):
                tile(t, pl.multiple_of(t * TILE, TILE), TILE, tri)

        if whole < size:
            tile(n_tiles - 1, (n_tiles - 1) * TILE, last_width, tri_last)

    def complete(j):
        for k in range(3):
            forwarded(j, k)
        own(j).wait()

    def pass_on(j, k):
        if k > 0:

            @pl.when(is_outer == 0)
            def _():
                relay_landed(j, k - 1)
                relay(j, k - 1).start()

        landed(j, k)
        forward(j, k).start()

    for what, j in service_order(plan, n_tiles):
        if what == "h line":
            arrived(h_place(v, z_one), 1, hid=z_one)
            arrived(h_place(v, lax.rem(z_one + 2, 4)), 2, hid=z_one)
            h_own.wait()
            h_chip.start()
            h_core.start()
        elif what == "h chip":
            arrived(h_place(v_two), 3, vocab=v_two)
            h_both.start()
        else:
            pass_on(j, what)
            if what == 2 and j == 0:
                arrived(h_place(v_one), 4, vocab=v_one)
                arrived(h_place(lax.rem(v_one + 2, 4)), 5, vocab=v_one)
            elif what == 2:
                complete(j - 1)
                compute(j - 1)
            if what == 2 and j + 2 < n_chunks:
                own(j + 2).start()
    complete(n_chunks - 1)
    compute(n_chunks - 1)

    lane = lax.broadcasted_iota(jnp.int32, (rows, LANES), 1)
    top = jnp.max(m_all[...], axis=1, keepdims=True)
    shrink = jnp.exp(m_all[...] - top)
    parts = s_all[...] * shrink
    k = lax.broadcasted_iota(jnp.int32, (LANES, LANES), 0)
    c = lax.broadcasted_iota(jnp.int32, (LANES, LANES), 1)
    strict = jnp.where(k < c, 1.0, 0.0).astype(BF16)
    before = sum(jnp.dot(p, strict, preferred_element_type=F32) for p in split3(parts))
    s_all[...] = before
    rel = rel_col[...]
    holds = (rel >= lane * TILE) & (rel < (lane + 1) * TILE) & (rel < n_cols)
    found = t_all[...] * shrink + jnp.where(holds, before, 0.0)
    total = jnp.sum(parts, axis=1, keepdims=True)
    at_tgt = jnp.sum(found, axis=1, keepdims=True)
    packed = jnp.where(lane == 0, top, jnp.where(lane == 1, total, at_tgt))
    zmsg[z] = packed.T[0:4, :]

    for j in range(n_chunks):
        send_near(j).wait_send()
        send_inner(j).wait_send()
        send_outer(j).wait_send()
        for k in range(3):
            forward(j, k).wait_send()

    @pl.when(is_outer == 0)
    def _():
        for j in range(n_chunks):
            for s in range(2):
                relay(j, s).wait_send()

    for copy in (h_two, h_one, h_relay, h_chip, h_core, h_both):
        copy.wait_send()

    def z_send(d):
        to = lax.rem(z + d, 4)
        return remote(zmsg.at[z], zmsg.at[z], zs.at[d - 1], zr.at[d - 1], hid=to)

    def v_send(d):
        to = lax.rem(v + d, 4)
        return remote(vmsg.at[v], vmsg.at[v], vs.at[d - 1], vr.at[d - 1], vocab=to)

    for d in (1, 2, 3):
        z_send(d).start()
    for d in (1, 2, 3):
        frm = lax.rem(z + 4 - d, 4)
        remote(zmsg.at[frm], zmsg.at[frm], zs.at[d - 1], zr.at[d - 1], hid=frm).wait_recv()

    ids = tgt_ref[...]
    maxes = [zmsg[h, 0:1, :] for h in range(4)]
    v_max = functools.reduce(jnp.maximum, maxes)
    v_sum = jnp.zeros((1, rows), F32)
    v_tgt = jnp.zeros((1, rows), F32)
    mine_before = jnp.zeros((1, rows), F32)
    for h in range(4):
        mine_before = jnp.where(h == z, v_sum, mine_before)
        f = jnp.exp(maxes[h] - v_max)
        low = (v * 4 + h) * n_cols
        inside = (ids >= low) & (ids < low + n_cols)
        v_tgt += jnp.where(inside, zmsg[h, 2:3, :] * f + v_sum, 0.0)
        v_sum += zmsg[h, 1:2, :] * f
    vmsg[v, 0:1, :] = v_max
    vmsg[v, 1:2, :] = v_sum
    vmsg[v, 2:3, :] = v_tgt
    vmsg[v, 3:4, :] = v_tgt

    for d in (1, 2, 3):
        z_send(d).wait_send()
    for d in (1, 2, 3):
        v_send(d).start()
    for d in (1, 2, 3):
        frm = lax.rem(v + 4 - d, 4)
        remote(vmsg.at[frm], vmsg.at[frm], vs.at[d - 1], vr.at[d - 1], vocab=frm).wait_recv()

    maxes = [vmsg[u, 0:1, :] for u in range(4)]
    g_max = functools.reduce(jnp.maximum, maxes)
    g_sum = jnp.zeros((1, rows), F32)
    g_tgt = jnp.zeros((1, rows), F32)
    g_before = jnp.zeros((1, rows), F32)
    for u in range(4):
        f = jnp.exp(maxes[u] - g_max)
        g_before = jnp.where(u == v, g_sum + mine_before * f, g_before)
        low = u * 4 * n_cols
        inside = (ids >= low) & (ids < low + 4 * n_cols)
        g_tgt += jnp.where(inside, vmsg[u, 2:3, :] * f + g_sum, 0.0)
        g_sum += vmsg[u, 1:2, :] * f
    tgt_out_ref[...] = g_tgt / g_sum
    back[0:1, :] = g_max
    back[1:2, :] = g_sum
    back[2:3, :] = g_before
    cols8 = back[...].T
    g_max, g_sum, g_before = cols8[:, 0:1], cols8[:, 1:2], cols8[:, 2:3]
    mine = jnp.max(m_all[...], axis=1, keepdims=True)
    scale_ref[...] = jnp.exp(m_all[...] - g_max) / g_sum
    off_ref[...] = (s_all[...] * jnp.exp(mine - g_max) + g_before) / g_sum
    for d in (1, 2, 3):
        v_send(d).wait_send()


def finish_kernel(c_ref, scale_ref, off_ref, tgt_ref, out_ref, tgt_out_ref, buf, sems):
    slots, n, n_cols = buf.shape
    steps = c_ref.shape[0] // n

    def put(i):
        slot = lax.rem(i, slots)
        at = pl.ds(pl.multiple_of(i * n, n), n)
        return pltpu.make_async_copy(buf.at[slot], out_ref.at[at], sems.at[slot])

    @pl.loop(0, steps)
    def _(i):
        slot = lax.rem(i, slots)
        at = pl.ds(pl.multiple_of(i * n, n), n)

        @pl.when(i >= slots)
        def _():
            put(i - slots).wait()

        for start in range(0, n_cols, TILE):
            t, stop = start // TILE, min(n_cols, start + TILE)
            buf[slot, :, start:stop] = (
                c_ref[at, start:stop] * scale_ref[at, t : t + 1] + off_ref[at, t : t + 1]
            )
        put(i).start()

    tgt_out_ref[...] = tgt_ref[...]
    for i in range(max(0, steps - slots), steps):
        put(i).wait()


def solution(mesh):
    n_hid, n_voc = mesh.shape["hid"], mesh.shape["vocab"]
    assert n_hid == 4 and n_voc == 4 and mesh.shape["data"] == 2

    def local_step(h_blk, w_blk, temp_blk, tgt_blk):
        rows, depth = h_blk.shape
        n_cols = w_blk.shape[1] // n_hid
        n_tiles = pl.cdiv(n_cols, TILE)
        last_width = n_cols - (n_tiles - 1) * TILE
        assert n_tiles <= LANES and n_cols % LANES == 0
        n_chunks = len(chunks_of(n_tiles))
        vmem = pl.BlockSpec(memory_space=pltpu.VMEM)
        hbm = pl.BlockSpec(memory_space=pltpu.HBM)
        dma = pltpu.SemaphoreType.DMA
        table = pltpu.VMEM((rows, LANES), F32)
        c, scale, off, tgt, _ = pl.pallas_call(
            functools.partial(prefix_kernel, n_cols),
            out_shape=(
                pltpu.VMEM((rows, n_cols), F32),
                pltpu.VMEM((rows, LANES), F32),
                pltpu.VMEM((rows, LANES), F32),
                pltpu.VMEM((1, rows), F32),
                jax.ShapeDtypeStruct((2, depth // 2, n_cols), BF16),
            ),
            in_specs=[hbm, hbm, vmem, vmem],
            out_specs=[vmem] * 4 + [hbm],
            scratch_shapes=[
                pltpu.VMEM((4 * depth, n_cols), BF16),
                pltpu.VMEM((rows, 4 * depth), BF16),
                pltpu.VMEM((3 * TILE, TILE), BF16),
                pltpu.VMEM((3 * last_width, last_width), BF16),
                table,
                table,
                table,
                pltpu.VMEM((rows, 1), F32),
                pltpu.VMEM((rows, 1), jnp.int32),
                pltpu.VMEM((4, 4, rows), F32),
                pltpu.VMEM((4, 4, rows), F32),
                pltpu.VMEM((8, rows), F32),
                dma((n_chunks, 3)),
                dma((n_chunks, 3)),
                dma((n_chunks, 3)),
                dma((n_chunks, 3)),
                dma((n_chunks, 2)),
                dma((n_chunks, 2)),
                dma((n_chunks,)),
                dma,
                dma((6,)),
                dma((6,)),
                dma((3,)),
                dma((3,)),
                dma((3,)),
                dma((3,)),
            ],
            compiler_params=pltpu.CompilerParams(
                collective_id=0, has_side_effects=True, vmem_limit_bytes=37 << 20
            ),
            name="prefix",
        )(h_blk, w_blk, temp_blk.reshape(1, rows), tgt_blk.reshape(1, rows))
        n = min(rows, 64)
        cdf, cdf_tgt = pl.pallas_call(
            finish_kernel,
            out_shape=(
                jax.ShapeDtypeStruct((rows, n_cols), F32),
                jax.ShapeDtypeStruct((1, rows), F32),
            ),
            in_specs=[vmem] * 4,
            out_specs=[hbm, vmem],
            scratch_shapes=[pltpu.VMEM((4, n, n_cols), F32), dma((4,))],
            compiler_params=pltpu.CompilerParams(vmem_limit_bytes=9 << 20),
            name="finish",
        )(c, scale, off, tgt)
        return cdf, cdf_tgt.reshape(rows)

    return jax.shard_map(
        local_step,
        mesh=mesh,
        in_specs=(P("data", "hid"), P("hid", "vocab"), P("data"), P("data")),
        out_specs=(P("data", ("vocab", "hid")), P("data")),
        check_vma=False,
    )
```

```python
import functools

import jax
import jax.numpy as jnp
from jax import lax
from jax.experimental import pallas as pl
from jax.experimental.pallas import tpu as pltpu
from jax.sharding import PartitionSpec as P

MESH = pl.DeviceIdType.MESH
F32 = jnp.float32
BF16 = jnp.bfloat16
TILE = 256
LANES = 128
LOWEST = float(jnp.finfo(jnp.float32).min)


def chunks_of(tiles):
    sizes, left = [], tiles
    for size in (1, 1, 1, 2, 2):
        if left > size:
            sizes.append(size)
            left -= size
    while left > 0:
        sizes.append(min(3, left))
        left -= sizes[-1]
    starts, at = [], 0
    for size in reversed(sizes):
        starts.append((at, size))
        at += size
    return starts


def service_order(plan, tiles):
    events = [(0.15 * tiles, "h line", 0), (0.28 * tiles, "h chip", 0)]
    for j, (first, size) in enumerate(plan):
        end = first + size
        events.append((first + size / 3 + 1, 0, j))
        events.append((end + 1, 2, j))
        events.append((min(1.86 * end, 0.68 * tiles + 0.6 * end) + 1, 1, j))
    events.sort(key=lambda e: e[0])
    order = [e[1:] for e in events]
    for j in range(len(plan)):
        at = max(order.index((k, j)) for k in (0, 1, 2))
        order.remove((1, j))
        order.insert(at, (1, j))
    return order


def split3(e):
    hi = e.astype(BF16)
    rest = e - hi.astype(F32)
    mid = rest.astype(BF16)
    low = (rest - mid.astype(F32)).astype(BF16)
    return hi, mid, low


def prefix_kernel(
    n_cols, h_ref, w_ref, temp_ref, tgt_ref,
    c_ref, scale_ref, off_ref, tgt_out_ref,
    wbuf, hbuf, zbuf, tri, tri_last, m_all, s_all, t_all, temp_col, rel_col, zmsg, vmsg, back,
    ws, wr, xs, xr, wl, hl, hs, hr, zs, zr, vs, vr,
):
    x, z, v = lax.axis_index("data"), lax.axis_index("hid"), lax.axis_index("vocab")
    rows, depth = h_ref.shape
    half, quarter = depth // 2, rows // 4
    n_tiles = pl.cdiv(n_cols, TILE)
    last_width = n_cols - (n_tiles - 1) * TILE
    plan = chunks_of(n_tiles)
    n_chunks = len(plan)

    side = z // 2
    outer_far, inner_far, near = 3 - 3 * side, 2 - side, 1 - z + 4 * side
    is_outer = jnp.where(z == side * 3, 1, 0)
    z_two, z_one = lax.rem(z + 2, 4), near
    v_two, v_one = lax.rem(v + 2, 4), v + 1 - 2 * lax.rem(v, 2)
    sources = (near, inner_far, outer_far)

    def cols_of(j):
        first, size = plan[j]
        start = first * TILE
        return start, min(n_cols, (first + size) * TILE) - start

    def w_rows(source, part):
        return pl.ds(pl.multiple_of(source * depth + part * half, half), half)

    def w_place(j, source, part):
        start, n = cols_of(j)
        return wbuf.at[w_rows(source, part), pl.ds(start, n)]

    def h_place(q, block=None):
        at = pl.ds(pl.multiple_of(q * quarter, quarter), quarter)
        if block is None:
            return hbuf.at[at]
        return hbuf.at[at, pl.ds(pl.multiple_of(block * depth, depth), depth)]

    def remote(src, dst, send, recv, **to):
        return pltpu.make_async_remote_copy(
            src_ref=src, dst_ref=dst, send_sem=send, recv_sem=recv, device_id=to, device_id_type=MESH
        )

    def direct(j, k, dest, slot):
        start, n = cols_of(j)
        src = w_ref.at[
            pl.ds(pl.multiple_of(x * half, half), half),
            pl.ds(pl.multiple_of(dest * n_cols + start, LANES), n),
        ]
        return remote(src, w_place(j, z, x), ws.at[j, k], wr.at[j, slot], hid=dest)

    def send_near(j):
        return direct(j, 0, near, 0)

    odd = lax.rem(v, 2)
    far_first = outer_far + odd * (inner_far - outer_far)
    far_second = inner_far + odd * (outer_far - inner_far)

    def send_far(j, i):
        return direct(j, 1 + i, (far_first, far_second)[i], 1 + is_outer)

    def landed(j, k):
        place = w_place(j, sources[k], x)
        remote(place, place, ws.at[j, k], wr.at[j, k], hid=sources[k]).wait_recv()

    def forward(j, k):
        place = w_place(j, sources[k], x)
        return remote(place, place, xs.at[j, k], xr.at[j, k], data=1 - x)

    def forwarded(j, k):
        place = w_place(j, sources[k], 1 - x)
        remote(place, place, xs.at[j, k], xr.at[j, k], data=1 - x).wait_recv()

    def own(j):
        start, n = cols_of(j)
        return pltpu.make_async_copy(
            w_ref.at[:, pl.ds(pl.multiple_of(z * n_cols + start, LANES), n)],
            wbuf.at[pl.ds(pl.multiple_of(z * depth, depth), depth), pl.ds(start, n)],
            wl.at[j],
        )

    h_mine = h_ref.at[pl.ds(pl.multiple_of(v * quarter, quarter), quarter)]
    h_own = pltpu.make_async_copy(h_mine, h_place(v, z), hl)
    h_two = remote(h_mine, h_place(v, z), hs.at[0], hr.at[0], hid=z_two)
    h_one = remote(h_mine, h_place(v, z), hs.at[1], hr.at[1], hid=z_one)
    h_relay = remote(h_place(v, z_two), h_place(v, z_two), hs.at[2], hr.at[2], hid=z_one)
    h_chip = remote(h_place(v), h_place(v), hs.at[3], hr.at[3], vocab=v_two)
    h_core = remote(h_place(v), h_place(v), hs.at[4], hr.at[4], vocab=v_one)
    h_both = remote(h_place(v_two), h_place(v_two), hs.at[5], hr.at[5], vocab=v_one)

    def arrived(place, i, **frm):
        remote(place, place, hs.at[i], hr.at[i], **frm).wait_recv()

    barrier = pltpu.get_barrier_semaphore()
    peers = [{"hid": lax.rem(z + d, 4)} for d in (1, 2, 3)]
    peers += [{"data": 1 - x}] + [{"vocab": lax.rem(v + d, 4)} for d in (1, 2, 3)]
    for peer in peers:
        pl.semaphore_signal(barrier, inc=1, device_id=peer, device_id_type=MESH)
    h_own.start()
    own(0).start()
    with jax.named_scope("bar"):
        pl.semaphore_wait(barrier, len(peers))

    h_two.start()
    h_one.start()
    send_near(0).start()
    send_far(0, 0).start()

    def ones_below(ref, width):
        k = lax.broadcasted_iota(jnp.int32, (width, width), 0)
        c = lax.broadcasted_iota(jnp.int32, (width, width), 1)
        block = jnp.where(k <= c, 1.0, 0.0).astype(BF16)
        for i in range(3):
            ref[pl.ds(i * width, width), :] = block

    ones_below(tri, TILE)
    if last_width != TILE:
        ones_below(tri_last, last_width)
    base = (v * 4 + z) * n_cols
    back[0:1, :] = temp_ref[...]
    back[1:2, :] = (tgt_ref[...] - base).astype(F32)
    cols8 = back[...].T
    temp_col[...] = jnp.broadcast_to(cols8[:, 0:1], temp_col.shape)
    rel_col[...] = jnp.broadcast_to(cols8[:, 1:2], rel_col.shape).astype(jnp.int32)
    m_all[...] = jnp.full(m_all.shape, LOWEST, F32)
    s_all[...] = jnp.zeros(s_all.shape, F32)
    t_all[...] = jnp.zeros(t_all.shape, F32)

    with jax.named_scope("h0"):
        arrived(h_place(v, z_two), 0, hid=z_two)
    h_relay.start()
    send_far(0, 1).start()
    for j in range(1, n_chunks):
        send_near(j).start()
        send_far(j, 0).start()
        send_far(j, 1).start()
    if n_chunks > 1:
        own(1).start()

    part, few = min(rows, 512), min(rows, 128)

    def logits_and_sums(product, sums):
        @pl.loop(0, rows // part)
        def _(i):
            if product is not None:
                _, new_start, new_width = product
                at = pl.ds(pl.multiple_of(i * part, part), part)
                new = jnp.dot(
                    hbuf[at, :], wbuf[:, pl.ds(new_start, new_width)], preferred_element_type=F32
                )
            for k in range(0, part, few) if sums is not None else ():
                prefix(pl.ds(pl.multiple_of(i * part + k, few), few), *sums)
            if product is not None:
                zbuf[at, 0:new_width] = new

    def prefix(at, t, start, width):
        pieces = width // LANES
        logits = zbuf[at, 0:width] * jnp.concatenate([temp_col[at, :]] * pieces, axis=1)
        lane = lax.broadcasted_iota(jnp.int32, (few, LANES), 1)
        here = lane == t
        top = jnp.max(logits, axis=1, keepdims=True)
        m_all[at, :] = jnp.where(here, top, m_all[at, :])
        e = jnp.exp(logits - top)
        total = jnp.sum(e, axis=1, keepdims=True)
        s_all[at, :] = jnp.where(here, total, s_all[at, :])
        table = tri if width == TILE else tri_last
        run = jnp.dot(jnp.concatenate(split3(e), axis=1), table[...], preferred_element_type=F32)
        c_ref[at, pl.ds(start, width)] = run
        rel = rel_col[at, :] - start
        hit = t_all[at, :]
        for p in range(pieces):
            hit += jnp.where(lane == rel - p * LANES, run[:, p * LANES : (p + 1) * LANES], 0.0)
        t_all[at, :] = hit

    def whole(t):
        return t, pl.multiple_of(t * TILE, TILE), TILE

    last = (n_tiles - 1, (n_tiles - 1) * TILE, last_width)

    def compute(j):
        first, size = plan[j]
        stop = first + size
        if first == 0:
            logits_and_sums(whole(0) if n_tiles > 1 else last, None)
            first = 1
        if first < min(stop, n_tiles - 1):

            @pl.loop(first, min(stop, n_tiles - 1))
            def _(t):
                logits_and_sums(whole(t), whole(t - 1))

        if stop == n_tiles:
            if n_tiles > 1:
                logits_and_sums(last, whole(n_tiles - 2))
            logits_and_sums(None, last)

    def complete(j):
        for k in range(3):
            forwarded(j, k)
        own(j).wait()

    for what, j in service_order(plan, n_tiles):
        if what == "h line":
            with jax.named_scope("hline"):
                arrived(h_place(v, z_one), 1, hid=z_one)
                arrived(h_place(v, lax.rem(z_one + 2, 4)), 2, hid=z_one)
                h_own.wait()
            h_chip.start()
            h_core.start()
        elif what == "h chip":
            with jax.named_scope("hchip"):
                arrived(h_place(v_two), 3, vocab=v_two)
            h_both.start()
        else:
            with jax.named_scope(f"w{what}_{j}"):
                landed(j, what)
            forward(j, what).start()
            if what != 1:
                continue
            if j == 1:
                with jax.named_scope("hcore"):
                    arrived(h_place(v_one), 4, vocab=v_one)
                    arrived(h_place(lax.rem(v_one + 2, 4)), 5, vocab=v_one)
            if j > 0:
                with jax.named_scope(f"x{j - 1}"):
                    complete(j - 1)
                with jax.named_scope(f"c{j - 1}"):
                    compute(j - 1)
            if j + 2 < n_chunks:
                own(j + 2).start()
    with jax.named_scope("xlast"):
        complete(n_chunks - 1)
    with jax.named_scope("clast"):
        compute(n_chunks - 1)

    lane = lax.broadcasted_iota(jnp.int32, (rows, LANES), 1)
    top = jnp.max(m_all[...], axis=1, keepdims=True)
    shrink = jnp.exp(m_all[...] - top)
    parts = s_all[...] * shrink
    k = lax.broadcasted_iota(jnp.int32, (LANES, LANES), 0)
    c = lax.broadcasted_iota(jnp.int32, (LANES, LANES), 1)
    strict = jnp.where(k < c, 1.0, 0.0).astype(BF16)
    before = sum(jnp.dot(p, strict, preferred_element_type=F32) for p in split3(parts))
    s_all[...] = before
    rel = rel_col[...]
    holds = (rel >= lane * TILE) & (rel < (lane + 1) * TILE) & (rel < n_cols)
    at_tgt = jnp.sum(t_all[...], axis=1, keepdims=True)
    found = jnp.where(holds, at_tgt * shrink + before, 0.0)
    total = jnp.sum(parts, axis=1, keepdims=True)
    at_tgt = jnp.sum(found, axis=1, keepdims=True)
    packed = jnp.where(lane == 0, top, jnp.where(lane == 1, total, at_tgt))
    zmsg[z] = packed.T[0:4, :]

    for j in range(n_chunks):
        send_near(j).wait_send()
        send_far(j, 0).wait_send()
        send_far(j, 1).wait_send()
        for k in range(3):
            forward(j, k).wait_send()

    for copy in (h_two, h_one, h_relay, h_chip, h_core, h_both):
        copy.wait_send()

    def z_send(d):
        to = lax.rem(z + d, 4)
        return remote(zmsg.at[z], zmsg.at[z], zs.at[d - 1], zr.at[d - 1], hid=to)

    def v_send(d):
        to = lax.rem(v + d, 4)
        return remote(vmsg.at[v], vmsg.at[v], vs.at[d - 1], vr.at[d - 1], vocab=to)

    for d in (1, 2, 3):
        z_send(d).start()
    for d in (1, 2, 3):
        frm = lax.rem(z + 4 - d, 4)
        with jax.named_scope(f"z{d}"):
            remote(zmsg.at[frm], zmsg.at[frm], zs.at[d - 1], zr.at[d - 1], hid=frm).wait_recv()

    ids = tgt_ref[...]
    maxes = [zmsg[h, 0:1, :] for h in range(4)]
    v_max = functools.reduce(jnp.maximum, maxes)
    v_sum = jnp.zeros((1, rows), F32)
    v_tgt = jnp.zeros((1, rows), F32)
    mine_before = jnp.zeros((1, rows), F32)
    for h in range(4):
        mine_before = jnp.where(h == z, v_sum, mine_before)
        f = jnp.exp(maxes[h] - v_max)
        low = (v * 4 + h) * n_cols
        inside = (ids >= low) & (ids < low + n_cols)
        v_tgt += jnp.where(inside, zmsg[h, 2:3, :] * f + v_sum, 0.0)
        v_sum += zmsg[h, 1:2, :] * f
    vmsg[v, 0:1, :] = v_max
    vmsg[v, 1:2, :] = v_sum
    vmsg[v, 2:3, :] = v_tgt
    vmsg[v, 3:4, :] = v_tgt

    for d in (1, 2, 3):
        z_send(d).wait_send()
    for d in (1, 2, 3):
        v_send(d).start()
    for d in (1, 2, 3):
        frm = lax.rem(v + 4 - d, 4)
        with jax.named_scope(f"v{d}"):
            remote(vmsg.at[frm], vmsg.at[frm], vs.at[d - 1], vr.at[d - 1], vocab=frm).wait_recv()

    maxes = [vmsg[u, 0:1, :] for u in range(4)]
    g_max = functools.reduce(jnp.maximum, maxes)
    g_sum = jnp.zeros((1, rows), F32)
    g_tgt = jnp.zeros((1, rows), F32)
    g_before = jnp.zeros((1, rows), F32)
    for u in range(4):
        f = jnp.exp(maxes[u] - g_max)
        g_before = jnp.where(u == v, g_sum + mine_before * f, g_before)
        low = u * 4 * n_cols
        inside = (ids >= low) & (ids < low + 4 * n_cols)
        g_tgt += jnp.where(inside, vmsg[u, 2:3, :] * f + g_sum, 0.0)
        g_sum += vmsg[u, 1:2, :] * f
    tgt_out_ref[...] = g_tgt / g_sum
    back[0:1, :] = g_max
    back[1:2, :] = g_sum
    back[2:3, :] = g_before
    cols8 = back[...].T
    g_max, g_sum, g_before = cols8[:, 0:1], cols8[:, 1:2], cols8[:, 2:3]
    mine = jnp.max(m_all[...], axis=1, keepdims=True)
    scale_ref[...] = jnp.exp(m_all[...] - g_max) / g_sum
    off_ref[...] = (s_all[...] * jnp.exp(mine - g_max) + g_before) / g_sum
    for d in (1, 2, 3):
        v_send(d).wait_send()


def finish_kernel(c_ref, scale_ref, off_ref, tgt_ref, out_ref, tgt_out_ref, buf, sems):
    slots, n, n_cols = buf.shape
    steps = c_ref.shape[0] // n

    def put(i):
        slot = lax.rem(i, slots)
        at = pl.ds(pl.multiple_of(i * n, n), n)
        return pltpu.make_async_copy(buf.at[slot], out_ref.at[at], sems.at[slot])

    @pl.loop(0, steps)
    def _(i):
        slot = lax.rem(i, slots)
        at = pl.ds(pl.multiple_of(i * n, n), n)

        @pl.when(i >= slots)
        def _():
            put(i - slots).wait()

        for start in range(0, n_cols, TILE):
            t, stop = start // TILE, min(n_cols, start + TILE)
            buf[slot, :, start:stop] = (
                c_ref[at, start:stop] * scale_ref[at, t : t + 1] + off_ref[at, t : t + 1]
            )
        put(i).start()

    tgt_out_ref[...] = tgt_ref[...]
    for i in range(max(0, steps - slots), steps):
        put(i).wait()


def solution(mesh):
    n_hid, n_voc = mesh.shape["hid"], mesh.shape["vocab"]
    assert n_hid == 4 and n_voc == 4 and mesh.shape["data"] == 2

    def local_step(h_blk, w_blk, temp_blk, tgt_blk):
        rows, depth = h_blk.shape
        n_cols = w_blk.shape[1] // n_hid
        n_tiles = pl.cdiv(n_cols, TILE)
        last_width = n_cols - (n_tiles - 1) * TILE
        assert n_tiles <= LANES and n_cols % LANES == 0
        n_chunks = len(chunks_of(n_tiles))
        vmem = pl.BlockSpec(memory_space=pltpu.VMEM)
        hbm = pl.BlockSpec(memory_space=pltpu.HBM)
        dma = pltpu.SemaphoreType.DMA
        table = pltpu.VMEM((rows, LANES), F32)
        c, scale, off, tgt = pl.pallas_call(
            functools.partial(prefix_kernel, n_cols),
            out_shape=(
                pltpu.VMEM((rows, n_cols), F32),
                pltpu.VMEM((rows, LANES), F32),
                pltpu.VMEM((rows, LANES), F32),
                pltpu.VMEM((1, rows), F32),
            ),
            in_specs=[hbm, hbm, vmem, vmem],
            out_specs=[vmem] * 4,
            scratch_shapes=[
                pltpu.VMEM((4 * depth, n_cols), BF16),
                pltpu.VMEM((rows, 4 * depth), BF16),
                pltpu.VMEM((rows, TILE), F32),
                pltpu.VMEM((3 * TILE, TILE), BF16),
                pltpu.VMEM((3 * last_width, last_width), BF16),
                table,
                table,
                table,
                table,
                pltpu.VMEM((rows, LANES), jnp.int32),
                pltpu.VMEM((4, 4, rows), F32),
                pltpu.VMEM((4, 4, rows), F32),
                pltpu.VMEM((8, rows), F32),
                dma((n_chunks, 3)),
                dma((n_chunks, 3)),
                dma((n_chunks, 3)),
                dma((n_chunks, 3)),
                dma((n_chunks,)),
                dma,
                dma((6,)),
                dma((6,)),
                dma((3,)),
                dma((3,)),
                dma((3,)),
                dma((3,)),
            ],
            compiler_params=pltpu.CompilerParams(
                collective_id=0, has_side_effects=True, vmem_limit_bytes=37 << 20
            ),
            name="prefix",
        )(h_blk, w_blk, temp_blk.reshape(1, rows), tgt_blk.reshape(1, rows))
        n = min(rows, 64)
        cdf, cdf_tgt = pl.pallas_call(
            finish_kernel,
            out_shape=(
                jax.ShapeDtypeStruct((rows, n_cols), F32),
                jax.ShapeDtypeStruct((1, rows), F32),
            ),
            in_specs=[vmem] * 4,
            out_specs=[hbm, vmem],
            scratch_shapes=[pltpu.VMEM((4, n, n_cols), F32), dma((4,))],
            compiler_params=pltpu.CompilerParams(vmem_limit_bytes=9 << 20),
            name="finish",
        )(c, scale, off, tgt)
        return cdf, cdf_tgt.reshape(rows)

    return jax.shard_map(
        local_step,
        mesh=mesh,
        in_specs=(P("data", "hid"), P("hid", "vocab"), P("data"), P("data")),
        out_specs=(P("data", ("vocab", "hid")), P("data")),
        check_vma=False,
    )
```

```python
import functools

import jax
import jax.numpy as jnp
from jax import lax
from jax.experimental import pallas as pl
from jax.experimental.pallas import tpu as pltpu
from jax.sharding import PartitionSpec as P

MESH = pl.DeviceIdType.MESH
F32 = jnp.float32
BF16 = jnp.bfloat16
TILE = 256
LANES = 128
LOWEST = float(jnp.finfo(jnp.float32).min)


def chunks_of(tiles):
    sizes, left = [], tiles
    for size in (1, 1, 1, 2, 2):
        if left > size:
            sizes.append(size)
            left -= size
    while left > 0:
        sizes.append(min(3, left))
        left -= sizes[-1]
    starts, at = [], 0
    for size in reversed(sizes):
        starts.append((at, size))
        at += size
    return starts


def service_order(plan, tiles):
    events = [(0.15 * tiles, "h line", 0), (0.28 * tiles, "h chip", 0)]
    for j, (first, size) in enumerate(plan):
        end = first + size
        events.append((first + size / 3 + 1, 0, j))
        events.append((end + 1, 2, j))
        events.append((min(1.86 * end, 0.68 * tiles + 0.6 * end) + 1, 1, j))
    events.sort(key=lambda e: e[0])
    order = [e[1:] for e in events]
    for j in range(len(plan)):
        at = max(order.index((k, j)) for k in (0, 1, 2))
        order.remove((1, j))
        order.insert(at, (1, j))
    return order


def folds_of(plan):
    n, folds, at = len(plan), [], 0
    for j in (3 * n // 11, 5 * n // 11):
        stop = sum(plan[j]) - 1
        if j < n - 2 and stop > at:
            folds.append((j, at, stop))
            at = stop
    return folds


def split3(e):
    hi = e.astype(BF16)
    rest = e - hi.astype(F32)
    mid = rest.astype(BF16)
    low = (rest - mid.astype(F32)).astype(BF16)
    return hi, mid, low


def prefix_kernel(
    n_cols, h_ref, w_ref, temp_ref, tgt_ref,
    c_ref, scale_ref, off_ref, factor_ref, tgt_out_ref,
    wbuf, hbuf, zbuf, zpre, tri, tri_last, m_all, s_all, t_all, temp_col, rel_col, zmsg, vmsg, back,
    ws, wr, xs, xr, wl, hl, hs, hr, zs, zr, vs, vr,
):
    x, z, v = lax.axis_index("data"), lax.axis_index("hid"), lax.axis_index("vocab")
    rows, depth = h_ref.shape
    half, quarter = depth // 2, rows // 4
    n_tiles = pl.cdiv(n_cols, TILE)
    last_width = n_cols - (n_tiles - 1) * TILE
    plan = chunks_of(n_tiles)
    n_chunks = len(plan)

    side = z // 2
    outer_far, inner_far, near = 3 - 3 * side, 2 - side, 1 - z + 4 * side
    is_outer = jnp.where(z == side * 3, 1, 0)
    z_two, z_one = lax.rem(z + 2, 4), near
    v_two, v_one = lax.rem(v + 2, 4), v + 1 - 2 * lax.rem(v, 2)
    sources = (near, inner_far, outer_far)

    def cols_of(j):
        first, size = plan[j]
        start = first * TILE
        return start, min(n_cols, (first + size) * TILE) - start

    def w_rows(source, part):
        return pl.ds(pl.multiple_of(source * depth + part * half, half), half)

    def w_place(j, source, part):
        start, n = cols_of(j)
        return wbuf.at[w_rows(source, part), pl.ds(start, n)]

    def h_place(q, block=None):
        at = pl.ds(pl.multiple_of(q * quarter, quarter), quarter)
        if block is None:
            return hbuf.at[at]
        return hbuf.at[at, pl.ds(pl.multiple_of(block * depth, depth), depth)]

    def remote(src, dst, send, recv, **to):
        return pltpu.make_async_remote_copy(
            src_ref=src, dst_ref=dst, send_sem=send, recv_sem=recv, device_id=to, device_id_type=MESH
        )

    def direct(j, k, dest, slot):
        start, n = cols_of(j)
        src = w_ref.at[
            pl.ds(pl.multiple_of(x * half, half), half),
            pl.ds(pl.multiple_of(dest * n_cols + start, LANES), n),
        ]
        return remote(src, w_place(j, z, x), ws.at[j, k], wr.at[j, slot], hid=dest)

    def send_near(j):
        return direct(j, 0, near, 0)

    odd = lax.rem(v, 2)
    far_first = outer_far + odd * (inner_far - outer_far)
    far_second = inner_far + odd * (outer_far - inner_far)

    def send_far(j, i):
        return direct(j, 1 + i, (far_first, far_second)[i], 1 + is_outer)

    def landed(j, k):
        place = w_place(j, sources[k], x)
        remote(place, place, ws.at[j, k], wr.at[j, k], hid=sources[k]).wait_recv()

    def forward(j, k):
        place = w_place(j, sources[k], x)
        return remote(place, place, xs.at[j, k], xr.at[j, k], data=1 - x)

    def forwarded(j, k):
        place = w_place(j, sources[k], 1 - x)
        remote(place, place, xs.at[j, k], xr.at[j, k], data=1 - x).wait_recv()

    def own(j):
        start, n = cols_of(j)
        return pltpu.make_async_copy(
            w_ref.at[:, pl.ds(pl.multiple_of(z * n_cols + start, LANES), n)],
            wbuf.at[pl.ds(pl.multiple_of(z * depth, depth), depth), pl.ds(start, n)],
            wl.at[j],
        )

    h_mine = h_ref.at[pl.ds(pl.multiple_of(v * quarter, quarter), quarter)]
    h_own = pltpu.make_async_copy(h_mine, h_place(v, z), hl)
    h_two = remote(h_mine, h_place(v, z), hs.at[0], hr.at[0], hid=z_two)
    h_one = remote(h_mine, h_place(v, z), hs.at[1], hr.at[1], hid=z_one)
    h_relay = remote(h_place(v, z_two), h_place(v, z_two), hs.at[2], hr.at[2], hid=z_one)
    h_chip = remote(h_place(v), h_place(v), hs.at[3], hr.at[3], vocab=v_two)
    h_core = remote(h_place(v), h_place(v), hs.at[4], hr.at[4], vocab=v_one)
    h_both = remote(h_place(v_two), h_place(v_two), hs.at[5], hr.at[5], vocab=v_one)

    def arrived(place, i, **frm):
        remote(place, place, hs.at[i], hr.at[i], **frm).wait_recv()

    barrier = pltpu.get_barrier_semaphore()
    peers = [{"hid": lax.rem(z + d, 4)} for d in (1, 2, 3)]
    peers += [{"data": 1 - x}] + [{"vocab": lax.rem(v + d, 4)} for d in (1, 2, 3)]
    for peer in peers:
        pl.semaphore_signal(barrier, inc=1, device_id=peer, device_id_type=MESH)
    h_own.start()
    own(0).start()
    with jax.named_scope("bar"):
        pl.semaphore_wait(barrier, len(peers))

    h_two.start()
    h_one.start()
    send_near(0).start()
    send_far(0, 0).start()

    def ones_below(ref, width):
        k = lax.broadcasted_iota(jnp.int32, (width, width), 0)
        c = lax.broadcasted_iota(jnp.int32, (width, width), 1)
        block = jnp.where(k <= c, 1.0, 0.0).astype(BF16)
        for i in range(3):
            ref[pl.ds(i * width, width), :] = block

    ones_below(tri, TILE)
    if last_width != TILE:
        ones_below(tri_last, last_width)
    base = (v * 4 + z) * n_cols
    back[0:1, :] = temp_ref[...]
    back[1:2, :] = (tgt_ref[...] - base).astype(F32)
    cols8 = back[...].T
    temp_col[...] = jnp.broadcast_to(cols8[:, 0:1], temp_col.shape)
    rel_col[...] = jnp.broadcast_to(cols8[:, 1:2], rel_col.shape).astype(jnp.int32)
    m_all[...] = jnp.full(m_all.shape, LOWEST, F32)
    s_all[...] = jnp.zeros(s_all.shape, F32)
    t_all[...] = jnp.zeros(t_all.shape, F32)

    with jax.named_scope("h0"):
        arrived(h_place(v, z_two), 0, hid=z_two)
    h_relay.start()
    send_far(0, 1).start()
    for j in range(1, n_chunks):
        send_near(j).start()
        send_far(j, 0).start()
        send_far(j, 1).start()
    if n_chunks > 1:
        own(1).start()

    part, few = min(rows, 512), min(rows, 128)

    def logits_and_sums(product, sums):
        @pl.loop(0, rows // part)
        def _(i):
            if product is not None:
                _, new_start, new_width = product
                at = pl.ds(pl.multiple_of(i * part, part), part)
                new = jnp.dot(
                    hbuf[at, :], wbuf[:, pl.ds(new_start, new_width)], preferred_element_type=F32
                )
            for k in range(0, part, few) if sums is not None else ():
                prefix(pl.ds(pl.multiple_of(i * part + k, few), few), *sums)
            if product is not None:
                zbuf[at, 0:new_width] = new

    def prefix(at, t, start, width):
        pieces = width // LANES
        logits = zbuf[at, 0:width] * jnp.concatenate([temp_col[at, :]] * pieces, axis=1)
        lane = lax.broadcasted_iota(jnp.int32, (few, LANES), 1)
        here = lane == t
        top = jnp.max(logits, axis=1, keepdims=True)
        m_all[at, :] = jnp.where(here, top, m_all[at, :])
        e = jnp.exp(logits - top)
        total = jnp.sum(e, axis=1, keepdims=True)
        s_all[at, :] = jnp.where(here, total, s_all[at, :])
        table = tri if width == TILE else tri_last
        run = jnp.dot(jnp.concatenate(split3(e), axis=1), table[...], preferred_element_type=F32)
        c_ref[at, pl.ds(start, width)] = run
        rel = rel_col[at, :] - start
        hit = t_all[at, :]
        for p in range(pieces):
            hit += jnp.where(lane == rel - p * LANES, run[:, p * LANES : (p + 1) * LANES], 0.0)
        t_all[at, :] = hit

    def whole(t):
        return t, pl.multiple_of(t * TILE, TILE), TILE

    ends = [(n_tiles - 2, (n_tiles - 2) * TILE, TILE), (n_tiles - 1, (n_tiles - 1) * TILE, last_width)]

    def compute(j):
        first, size = plan[j]
        stop = first + size
        if first == 0:
            logits_and_sums(whole(0), None)
            first = 1
        if first < stop:

            @pl.loop(first, stop)
            def _(t):
                logits_and_sums(whole(t), whole(t - 1))

        if stop == n_tiles - 2:
            logits_and_sums(None, whole(stop - 1))

    def block_dot(at, block, start, width):
        lanes = pl.ds(pl.multiple_of(block * depth, depth), depth)
        return jnp.dot(hbuf[at, lanes], wbuf[lanes, start : start + width], preferred_element_type=F32)

    def begin_end(i):
        _, start, width = ends[i]

        @pl.loop(0, rows // part)
        def _(k):
            at = pl.ds(pl.multiple_of(k * part, part), part)
            zpre[at, i * TILE : i * TILE + width] = (
                block_dot(at, z, start, width)
                + block_dot(at, near, start, width)
                + block_dot(at, outer_far, start, width)
            )

    def finish_end(i):
        _, start, width = ends[i]

        @pl.loop(0, rows // part)
        def _(k):
            at = pl.ds(pl.multiple_of(k * part, part), part)
            zbuf[at, 0:width] = zpre[at, i * TILE : i * TILE + width] + block_dot(at, inner_far, start, width)
            for q in range(0, part, few):
                prefix(pl.ds(pl.multiple_of(k * part + q, few), few), *ends[i])

    def fold(g0, g1):
        @pl.loop(0, rows // few)
        def _(i):
            at = pl.ds(pl.multiple_of(i * few, few), few)
            lane = lax.broadcasted_iota(jnp.int32, (few, LANES), 1)
            group = (lane >= g0) & (lane < g1)
            m, s = m_all[at, :], s_all[at, :]
            top = jnp.max(jnp.where(group, m, LOWEST), axis=1, keepdims=True)
            shrink = jnp.where(group, jnp.exp(m - top), 0.0)
            parts = s * shrink
            before = prefix_before(parts)
            for t in range(g0, g1):
                span = slice(t * TILE, (t + 1) * TILE)
                c_ref[at, span] = c_ref[at, span] * shrink[:, t : t + 1] + before[:, t : t + 1]
            rel = rel_col[at, :]
            holds = (rel >= lane * TILE) & (rel < (lane + 1) * TILE)
            old = t_all[at, :]
            moved = jnp.sum(old, axis=1, keepdims=True) * shrink + before
            inside = (rel >= g0 * TILE) & (rel < g1 * TILE)
            t_all[at, :] = jnp.where(inside, jnp.where(holds, moved, 0.0), old)
            m_all[at, :] = jnp.where(group, top, m)
            total = jnp.sum(parts, axis=1, keepdims=True)
            s_all[at, :] = jnp.where(group, jnp.where(lane == g1 - 1, total, 0.0), s)

    def prefix_before(parts):
        k = lax.broadcasted_iota(jnp.int32, (LANES, LANES), 0)
        c = lax.broadcasted_iota(jnp.int32, (LANES, LANES), 1)
        strict = jnp.where(k < c, 1.0, 0.0).astype(BF16)
        return sum(jnp.dot(p, strict, preferred_element_type=F32) for p in split3(parts))

    def complete(j):
        for k in range(3):
            forwarded(j, k)
        own(j).wait()

    order = service_order(plan, n_tiles)
    folds = {j: (g0, g1) for j, g0, g1 in folds_of(plan)}
    known = max(order.index((k, j)) for k in (0, 2) for j in (n_chunks - 2, n_chunks - 1))
    early = min(j for j in range(max(0, n_chunks - 5), n_chunks - 1) if order.index((1, j + 1)) > known)
    assert n_chunks > 2 and early < n_chunks - 2

    for what, j in order:
        if what == "h line":
            with jax.named_scope("hline"):
                arrived(h_place(v, z_one), 1, hid=z_one)
                arrived(h_place(v, lax.rem(z_one + 2, 4)), 2, hid=z_one)
                h_own.wait()
            h_chip.start()
            h_core.start()
        elif what == "h chip":
            with jax.named_scope("hchip"):
                arrived(h_place(v_two), 3, vocab=v_two)
            h_both.start()
        else:
            with jax.named_scope(f"w{what}_{j}"):
                landed(j, what)
            forward(j, what).start()
            if what != 1:
                continue
            if j == 1:
                with jax.named_scope("hcore"):
                    arrived(h_place(v_one), 4, vocab=v_one)
                    arrived(h_place(lax.rem(v_one + 2, 4)), 5, vocab=v_one)
            if 0 < j < n_chunks - 1:
                with jax.named_scope(f"x{j - 1}"):
                    complete(j - 1)
                with jax.named_scope(f"c{j - 1}"):
                    compute(j - 1)
                if j - 1 in folds:
                    with jax.named_scope(f"f{j - 1}"):
                        fold(*folds[j - 1])
            if j == 0:
                for i in range(2, n_chunks):
                    own(i).start()
            if j - 1 == early:
                for i in (0, 1):
                    with jax.named_scope(f"b{i}"):
                        own(n_chunks - 2 + i).wait()
                        forwarded(n_chunks - 2 + i, 0)
                        forwarded(n_chunks - 2 + i, 2)
                    with jax.named_scope(f"p{i}"):
                        begin_end(i)
    for i in (0, 1):
        with jax.named_scope(f"xe{i}"):
            forwarded(n_chunks - 2 + i, 1)
        with jax.named_scope(f"ce{i}"):
            finish_end(i)

    lane = lax.broadcasted_iota(jnp.int32, (rows, LANES), 1)
    top = jnp.max(m_all[...], axis=1, keepdims=True)
    shrink = jnp.exp(m_all[...] - top)
    scale_ref[...] = shrink
    parts = s_all[...] * shrink
    before = prefix_before(parts)
    off_ref[...] = before
    rel = rel_col[...]
    holds = (rel >= lane * TILE) & (rel < (lane + 1) * TILE) & (rel < n_cols)
    at_tgt = jnp.sum(t_all[...], axis=1, keepdims=True)
    found = jnp.where(holds, at_tgt * shrink + before, 0.0)
    total = jnp.sum(parts, axis=1, keepdims=True)
    at_tgt = jnp.sum(found, axis=1, keepdims=True)
    packed = jnp.where(lane == 0, top, jnp.where(lane == 1, total, at_tgt))
    zmsg[z] = packed.T[0:4, :]

    for j in range(n_chunks):
        send_near(j).wait_send()
        send_far(j, 0).wait_send()
        send_far(j, 1).wait_send()
        for k in range(3):
            forward(j, k).wait_send()

    for copy in (h_two, h_one, h_relay, h_chip, h_core, h_both):
        copy.wait_send()

    def z_send(i):
        slot = (0, 1 + is_outer, 1 + is_outer)[i]
        return remote(zmsg.at[z], zmsg.at[z], zs.at[i], zr.at[slot], hid=(near, inner_far, outer_far)[i])

    def v_send(d):
        to = lax.rem(v + d, 4)
        return remote(vmsg.at[v], vmsg.at[v], vs.at[d - 1], vr.at[d - 1], vocab=to)

    for i in (2, 1, 0):
        z_send(i).start()
    for i, frm in enumerate(sources):
        with jax.named_scope(f"z{i}"):
            remote(zmsg.at[frm], zmsg.at[frm], zs.at[i], zr.at[i], hid=frm).wait_recv()

    ids = tgt_ref[...]
    maxes = [zmsg[h, 0:1, :] for h in range(4)]
    v_max = functools.reduce(jnp.maximum, maxes)
    v_sum = jnp.zeros((1, rows), F32)
    v_tgt = jnp.zeros((1, rows), F32)
    mine_before = jnp.zeros((1, rows), F32)
    for h in range(4):
        mine_before = jnp.where(h == z, v_sum, mine_before)
        f = jnp.exp(maxes[h] - v_max)
        low = (v * 4 + h) * n_cols
        inside = (ids >= low) & (ids < low + n_cols)
        v_tgt += jnp.where(inside, zmsg[h, 2:3, :] * f + v_sum, 0.0)
        v_sum += zmsg[h, 1:2, :] * f
    vmsg[v, 0:1, :] = v_max
    vmsg[v, 1:2, :] = v_sum
    vmsg[v, 2:3, :] = v_tgt
    vmsg[v, 3:4, :] = v_tgt

    for i in range(3):
        z_send(i).wait_send()
    for d in (1, 2, 3):
        v_send(d).start()
    for d in (1, 2, 3):
        frm = lax.rem(v + 4 - d, 4)
        with jax.named_scope(f"v{d}"):
            remote(vmsg.at[frm], vmsg.at[frm], vs.at[d - 1], vr.at[d - 1], vocab=frm).wait_recv()

    maxes = [vmsg[u, 0:1, :] for u in range(4)]
    g_max = functools.reduce(jnp.maximum, maxes)
    g_sum = jnp.zeros((1, rows), F32)
    g_tgt = jnp.zeros((1, rows), F32)
    g_before = jnp.zeros((1, rows), F32)
    for u in range(4):
        f = jnp.exp(maxes[u] - g_max)
        g_before = jnp.where(u == v, g_sum + mine_before * f, g_before)
        low = u * 4 * n_cols
        inside = (ids >= low) & (ids < low + 4 * n_cols)
        g_tgt += jnp.where(inside, vmsg[u, 2:3, :] * f + g_sum, 0.0)
        g_sum += vmsg[u, 1:2, :] * f
    tgt_out_ref[...] = g_tgt / g_sum
    factor_ref[0:1, :] = jnp.exp(zmsg[z, 0:1, :] - g_max) / g_sum
    factor_ref[1:2, :] = g_before / g_sum
    for d in (1, 2, 3):
        v_send(d).wait_send()


def finish_kernel(lanes, c_ref, scale_ref, off_ref, factor_ref, tgt_ref, out_ref, tgt_out_ref, buf, factor_col, sems):
    slots, n, n_cols = buf.shape
    steps = c_ref.shape[0] // n
    factor_col[...] = factor_ref[...].T

    def put(i):
        slot = lax.rem(i, slots)
        at = pl.ds(pl.multiple_of(i * n, n), n)
        return pltpu.make_async_copy(buf.at[slot], out_ref.at[at], sems.at[slot])

    @pl.loop(0, steps)
    def _(i):
        slot = lax.rem(i, slots)

        @pl.when(i >= slots)
        def _():
            put(i - slots).wait()

        at = pl.ds(pl.multiple_of(i * n, n), n)
        factor = factor_col[at, 0:1]
        scale = scale_ref[at, :] * factor
        off = off_ref[at, :] * factor + factor_col[at, 1:2]
        for t, lane in enumerate(lanes):
            span = slice(t * TILE, min(n_cols, (t + 1) * TILE))
            buf[slot, :, span] = c_ref[at, span] * scale[:, lane : lane + 1] + off[:, lane : lane + 1]
        put(i).start()

    tgt_out_ref[...] = tgt_ref[...]
    for i in range(max(0, steps - slots), steps):
        put(i).wait()


def solution(mesh):
    n_hid, n_voc = mesh.shape["hid"], mesh.shape["vocab"]
    assert n_hid == 4 and n_voc == 4 and mesh.shape["data"] == 2

    def local_step(h_blk, w_blk, temp_blk, tgt_blk):
        rows, depth = h_blk.shape
        n_cols = w_blk.shape[1] // n_hid
        n_tiles = pl.cdiv(n_cols, TILE)
        last_width = n_cols - (n_tiles - 1) * TILE
        assert n_tiles <= LANES and n_cols % LANES == 0
        plan = chunks_of(n_tiles)
        n_chunks = len(plan)
        vmem = pl.BlockSpec(memory_space=pltpu.VMEM)
        hbm = pl.BlockSpec(memory_space=pltpu.HBM)
        dma = pltpu.SemaphoreType.DMA
        table = pltpu.VMEM((rows, LANES), F32)
        c, scale, off, factor, tgt = pl.pallas_call(
            functools.partial(prefix_kernel, n_cols),
            out_shape=(
                pltpu.VMEM((rows, n_cols), F32),
                pltpu.VMEM((rows, LANES), F32),
                pltpu.VMEM((rows, LANES), F32),
                pltpu.VMEM((8, rows), F32),
                pltpu.VMEM((1, rows), F32),
            ),
            in_specs=[hbm, hbm, vmem, vmem],
            out_specs=[vmem] * 5,
            scratch_shapes=[
                pltpu.VMEM((4 * depth, n_cols), BF16),
                pltpu.VMEM((rows, 4 * depth), BF16),
                pltpu.VMEM((rows, TILE), F32),
                pltpu.VMEM((rows, TILE + last_width), F32),
                pltpu.VMEM((3 * TILE, TILE), BF16),
                pltpu.VMEM((3 * last_width, last_width), BF16),
                table,
                table,
                table,
                table,
                pltpu.VMEM((rows, LANES), jnp.int32),
                pltpu.VMEM((4, 4, rows), F32),
                pltpu.VMEM((4, 4, rows), F32),
                pltpu.VMEM((8, rows), F32),
                dma((n_chunks, 3)),
                dma((n_chunks, 3)),
                dma((n_chunks, 3)),
                dma((n_chunks, 3)),
                dma((n_chunks,)),
                dma,
                dma((6,)),
                dma((6,)),
                dma((3,)),
                dma((3,)),
                dma((3,)),
                dma((3,)),
            ],
            compiler_params=pltpu.CompilerParams(
                collective_id=0, has_side_effects=True, vmem_limit_bytes=37 << 20
            ),
            name="prefix",
        )(h_blk, w_blk, temp_blk.reshape(1, rows), tgt_blk.reshape(1, rows))
        n = min(rows, 64)
        lanes = list(range(n_tiles))
        for _, g0, g1 in folds_of(plan):
            lanes[g0:g1] = [g0] * (g1 - g0)
        cdf, cdf_tgt = pl.pallas_call(
            functools.partial(finish_kernel, lanes),
            out_shape=(
                jax.ShapeDtypeStruct((rows, n_cols), F32),
                jax.ShapeDtypeStruct((1, rows), F32),
            ),
            in_specs=[vmem] * 5,
            out_specs=[hbm, vmem],
            scratch_shapes=[pltpu.VMEM((4, n, n_cols), F32), pltpu.VMEM((rows, 8), F32), dma((4,))],
            compiler_params=pltpu.CompilerParams(vmem_limit_bytes=9 << 20),
            name="finish",
        )(c, scale, off, factor, tgt)
        return cdf, cdf_tgt.reshape(rows)

    return jax.shard_map(
        local_step,
        mesh=mesh,
        in_specs=(P("data", "hid"), P("hid", "vocab"), P("data"), P("data")),
        out_specs=(P("data", ("vocab", "hid")), P("data")),
        check_vma=False,
    )
```

```python
import functools

import jax
import jax.numpy as jnp
from jax import lax
from jax.experimental import pallas as pl
from jax.experimental.pallas import tpu as pltpu
from jax.sharding import PartitionSpec as P

MESH = pl.DeviceIdType.MESH
F32 = jnp.float32
BF16 = jnp.bfloat16
TILE = 256
LANES = 128
LOWEST = float(jnp.finfo(jnp.float32).min)


def chunks_of(blocks):
    sizes, left = [], blocks
    for size in (blocks % 2 or 2, 1, 1, 1, 1, 2, 4, 4):
        if left > size:
            sizes.append(size)
            left -= size
    while left > 0:
        sizes.append(min(6, left))
        left -= sizes[-1]
    starts, at = [], 0
    for size in reversed(sizes):
        starts.append((at, size))
        at += size
    return starts


def service_order(plan, blocks):
    events = [(0.15 * blocks, "h line", 0), (0.28 * blocks, "h chip", 0)]
    for j, (first, size) in enumerate(plan):
        end = first + size
        events.append((first + size / 3 + 2, 0, j))
        events.append((end + 2, 2, j))
        events.append((min(1.86 * end, 0.68 * blocks + 0.6 * end) + 2, 1, j))
    events.sort(key=lambda e: e[0])
    order = [e[1:] for e in events]
    for j in range(len(plan)):
        at = max(order.index((k, j)) for k in (0, 1, 2))
        order.remove((1, j))
        order.insert(at, (1, j))
    return order


def folds_of(plan):
    n, folds, at = len(plan), [], 0
    for j in (3 * n // 13, 5 * n // 13):
        stop = sum(plan[j]) // 2 - 1
        if j < n - 5 and stop > at:
            folds.append((j, at, stop))
            at = stop
    return folds


def split3(e):
    hi = e.astype(BF16)
    rest = e - hi.astype(F32)
    mid = rest.astype(BF16)
    low = (rest - mid.astype(F32)).astype(BF16)
    return hi, mid, low


def prefix_kernel(
    n_cols, h_ref, w_ref, temp_hbm, tgt_hbm,
    c_ref, scale_ref, off_ref, factor_ref, tgt_out_ref,
    wbuf, hbuf, zbuf, tri, tri_last, m_all, s_all, t_all, temp_col, rel_col, temp_ref, tgt_ref, zmsg, vmsg, back,
    ws, wr, xs, xr, wl, hl, hs, hr, zs, zr, vs, vr, rl,
):
    x, z, v = lax.axis_index("data"), lax.axis_index("hid"), lax.axis_index("vocab")
    rows, depth = h_ref.shape
    half, quarter = depth // 2, rows // 4
    n_tiles = pl.cdiv(n_cols, TILE)
    last_width = n_cols - (n_tiles - 1) * TILE
    plan = chunks_of(n_cols // LANES)
    n_chunks = len(plan)

    side = z // 2
    outer_far, inner_far, near = 3 - 3 * side, 2 - side, 1 - z + 4 * side
    is_outer = jnp.where(z == side * 3, 1, 0)
    z_two, z_one = lax.rem(z + 2, 4), near
    v_two, v_one = lax.rem(v + 2, 4), v + 1 - 2 * lax.rem(v, 2)
    sources = (near, inner_far, outer_far)

    def cols_of(j):
        first, size = plan[j]
        return first * LANES, size * LANES

    def w_rows(source, part):
        return pl.ds(pl.multiple_of(source * depth + part * half, half), half)

    def w_place(j, source, part):
        start, n = cols_of(j)
        return wbuf.at[w_rows(source, part), pl.ds(start, n)]

    def h_place(q, block=None):
        at = pl.ds(pl.multiple_of(q * quarter, quarter), quarter)
        if block is None:
            return hbuf.at[at]
        return hbuf.at[at, pl.ds(pl.multiple_of(block * depth, depth), depth)]

    def remote(src, dst, send, recv, **to):
        return pltpu.make_async_remote_copy(
            src_ref=src, dst_ref=dst, send_sem=send, recv_sem=recv, device_id=to, device_id_type=MESH
        )

    def direct(j, k, dest, slot):
        start, n = cols_of(j)
        src = w_ref.at[
            pl.ds(pl.multiple_of(x * half, half), half),
            pl.ds(pl.multiple_of(dest * n_cols + start, LANES), n),
        ]
        return remote(src, w_place(j, z, x), ws.at[k], wr.at[j, slot], hid=dest)

    def send_near(j):
        return direct(j, 0, near, 0)

    odd = lax.rem(v, 2)
    far_first = outer_far + odd * (inner_far - outer_far)
    far_second = inner_far + odd * (outer_far - inner_far)

    def send_far(j, i):
        return direct(j, 1 + i, (far_first, far_second)[i], 1 + is_outer)

    def landed(j, k):
        place = w_place(j, sources[k], x)
        remote(place, place, ws.at[k], wr.at[j, k], hid=sources[k]).wait_recv()

    def forward(j, k):
        place = w_place(j, sources[k], x)
        return remote(place, place, xs.at[k], xr.at[j, k], data=1 - x)

    def forwarded(j, k):
        place = w_place(j, sources[k], 1 - x)
        remote(place, place, xs.at[k], xr.at[j, k], data=1 - x).wait_recv()

    def own(j):
        start, n = cols_of(j)
        return pltpu.make_async_copy(
            w_ref.at[:, pl.ds(pl.multiple_of(z * n_cols + start, LANES), n)],
            wbuf.at[pl.ds(pl.multiple_of(z * depth, depth), depth), pl.ds(start, n)],
            wl,
        )

    h_mine = h_ref.at[pl.ds(pl.multiple_of(v * quarter, quarter), quarter)]
    h_own = pltpu.make_async_copy(h_mine, h_place(v, z), hl)
    h_two = remote(h_mine, h_place(v, z), hs.at[0], hr.at[0], hid=z_two)
    h_one = remote(h_mine, h_place(v, z), hs.at[1], hr.at[1], hid=z_one)
    h_relay = remote(h_place(v, z_two), h_place(v, z_two), hs.at[2], hr.at[2], hid=z_one)
    h_chip = remote(h_place(v), h_place(v), hs.at[3], hr.at[3], vocab=v_two)
    h_core = remote(h_place(v), h_place(v), hs.at[4], hr.at[4], vocab=v_one)
    h_both = remote(h_place(v_two), h_place(v_two), hs.at[5], hr.at[5], vocab=v_one)

    def arrived(place, i, **frm):
        remote(place, place, hs.at[i], hr.at[i], **frm).wait_recv()

    barrier = pltpu.get_barrier_semaphore()
    peers = [{"hid": lax.rem(z + d, 4)} for d in (1, 2, 3)]
    peers += [{"data": 1 - x}] + [{"vocab": lax.rem(v + d, 4)} for d in (1, 2, 3)]
    for peer in peers:
        pl.semaphore_signal(barrier, inc=1, device_id=peer, device_id_type=MESH)
    row_copies = [
        pltpu.make_async_copy(temp_hbm, temp_ref, rl.at[0]),
        pltpu.make_async_copy(tgt_hbm, tgt_ref, rl.at[1]),
    ]
    for copy in (h_own, *row_copies):
        copy.start()
    for j in range(n_chunks):
        own(j).start()
    with jax.named_scope("bar"):
        pl.semaphore_wait(barrier, len(peers))

    h_two.start()
    h_one.start()
    send_near(0).start()
    send_far(0, 0).start()

    def ones_below(ref, width):
        k = lax.broadcasted_iota(jnp.int32, (width, width), 0)
        c = lax.broadcasted_iota(jnp.int32, (width, width), 1)
        block = jnp.where(k <= c, 1.0, 0.0).astype(BF16)
        for i in range(3):
            ref[pl.ds(i * width, width), :] = block

    ones_below(tri, TILE)
    if last_width != TILE:
        ones_below(tri_last, last_width)
    base = (v * 4 + z) * n_cols
    for copy in row_copies:
        copy.wait()
    back[0:1, :] = temp_ref[...]
    back[1:2, :] = (tgt_ref[...] - base).astype(F32)
    cols8 = back[...].T
    temp_col[...] = jnp.broadcast_to(cols8[:, 0:1], temp_col.shape)
    rel_col[...] = jnp.broadcast_to(cols8[:, 1:2], rel_col.shape).astype(jnp.int32)
    m_all[...] = jnp.full(m_all.shape, LOWEST, F32)
    s_all[...] = jnp.zeros(s_all.shape, F32)
    t_all[...] = jnp.zeros(t_all.shape, F32)

    with jax.named_scope("h0"):
        arrived(h_place(v, z_two), 0, hid=z_two)
    h_relay.start()
    send_far(0, 1).start()
    for j in range(1, n_chunks):
        send_near(j).start()
        send_far(j, 0).start()
        send_far(j, 1).start()

    part, few = min(rows, 512), min(rows, 128)

    def logits_and_sums(product, sums):
        @pl.loop(0, rows // part)
        def _(i):
            if product is not None:
                _, new_start, new_width = product
                at = pl.ds(pl.multiple_of(i * part, part), part)
                new = jnp.dot(
                    hbuf[at, :], wbuf[:, pl.ds(new_start, new_width)], preferred_element_type=F32
                )
            for k in range(0, part, few) if sums is not None else ():
                prefix(pl.ds(pl.multiple_of(i * part + k, few), few), *sums)
            if product is not None:
                zbuf[at, 0:new_width] = new

    def prefix(at, t, start, width):
        pieces = width // LANES
        logits = zbuf[at, 0:width] * jnp.concatenate([temp_col[at, :]] * pieces, axis=1)
        lane = lax.broadcasted_iota(jnp.int32, (few, LANES), 1)
        here = lane == t
        top = jnp.max(logits, axis=1, keepdims=True)
        m_all[at, :] = jnp.where(here, top, m_all[at, :])
        e = jnp.exp(logits - top)
        total = jnp.sum(e, axis=1, keepdims=True)
        s_all[at, :] = jnp.where(here, total, s_all[at, :])
        table = tri if width == TILE else tri_last
        run = jnp.dot(jnp.concatenate(split3(e), axis=1), table[...], preferred_element_type=F32)
        c_ref[at, pl.ds(start, width)] = run
        rel = rel_col[at, :] - start
        hit = t_all[at, :]
        for p in range(pieces):
            hit += jnp.where(lane == rel - p * LANES, run[:, p * LANES : (p + 1) * LANES], 0.0)
        t_all[at, :] = hit

    def whole(t):
        return t, pl.multiple_of(t * TILE, TILE), TILE

    ends = [
        (n_chunks - 4, n_tiles - 3, (n_tiles - 3) * TILE, TILE),
        (n_chunks - 2, n_tiles - 2, (n_tiles - 2) * TILE, TILE),
        (n_chunks - 1, n_tiles - 1, (n_tiles - 1) * TILE, last_width),
    ]

    def compute(j):
        first, size = (n // 2 for n in plan[j])
        stop = first + size
        if first == 0:
            logits_and_sums(whole(0), None)
            first = 1
        if first < stop:

            @pl.loop(first, stop)
            def _(t):
                logits_and_sums(whole(t), whole(t - 1))

        if stop == n_tiles - 3:
            logits_and_sums(None, whole(stop - 1))

    def block_dot(at, block, start, width):
        lanes = pl.ds(pl.multiple_of(block * depth, depth), depth)
        return jnp.dot(hbuf[at, lanes], wbuf[lanes, start : start + width], preferred_element_type=F32)

    def begin_end(i):
        _, _, start, width = ends[i]

        @pl.loop(0, rows // part)
        def _(k):
            at = pl.ds(pl.multiple_of(k * part, part), part)
            c_ref[at, start : start + width] = (
                block_dot(at, z, start, width)
                + block_dot(at, near, start, width)
                + block_dot(at, outer_far, start, width)
            )

    def finish_end(i):
        _, _, start, width = ends[i]

        @pl.loop(0, rows // part)
        def _(k):
            at = pl.ds(pl.multiple_of(k * part, part), part)
            zbuf[at, 0:width] = c_ref[at, start : start + width] + block_dot(at, inner_far, start, width)
            for q in range(0, part, few):
                prefix(pl.ds(pl.multiple_of(k * part + q, few), few), *ends[i][1:])

    def fold(g0, g1):
        @pl.loop(0, rows // few)
        def _(i):
            at = pl.ds(pl.multiple_of(i * few, few), few)
            lane = lax.broadcasted_iota(jnp.int32, (few, LANES), 1)
            group = (lane >= g0) & (lane < g1)
            m, s = m_all[at, :], s_all[at, :]
            top = jnp.max(jnp.where(group, m, LOWEST), axis=1, keepdims=True)
            shrink = jnp.where(group, jnp.exp(m - top), 0.0)
            parts = s * shrink
            before = prefix_before(parts)
            for t in range(g0, g1):
                span = slice(t * TILE, (t + 1) * TILE)
                c_ref[at, span] = c_ref[at, span] * shrink[:, t : t + 1] + before[:, t : t + 1]
            rel = rel_col[at, :]
            holds = (rel >= lane * TILE) & (rel < (lane + 1) * TILE)
            old = t_all[at, :]
            moved = jnp.sum(old, axis=1, keepdims=True) * shrink + before
            inside = (rel >= g0 * TILE) & (rel < g1 * TILE)
            t_all[at, :] = jnp.where(inside, jnp.where(holds, moved, 0.0), old)
            m_all[at, :] = jnp.where(group, top, m)
            total = jnp.sum(parts, axis=1, keepdims=True)
            s_all[at, :] = jnp.where(group, jnp.where(lane == g1 - 1, total, 0.0), s)

    def close(i):
        first = ends[i - 1][0] + 1 if i else n_chunks - 5
        with jax.named_scope(f"xe{i}"):
            for j in range(first, ends[i][0] + 1):
                forwarded(j, 1)
        with jax.named_scope(f"ce{i}"):
            finish_end(i)

    def prefix_before(parts):
        k = lax.broadcasted_iota(jnp.int32, (LANES, LANES), 0)
        c = lax.broadcasted_iota(jnp.int32, (LANES, LANES), 1)
        strict = jnp.where(k < c, 1.0, 0.0).astype(BF16)
        return sum(jnp.dot(p, strict, preferred_element_type=F32) for p in split3(parts))

    def complete(j):
        for k in range(3):
            forwarded(j, k)

    def own_complete():
        place = wbuf.at[pl.ds(pl.multiple_of(z * depth, depth), depth)]
        pltpu.make_async_copy(place, place, wl).wait()

    order = service_order(plan, n_cols // LANES)
    folds = {j: (g0, g1) for j, g0, g1 in folds_of(plan)}
    tail = range(n_chunks - 5, n_chunks)
    known = max(order.index((k, j)) for k in (0, 2) for j in tail)
    early = min(j for j in range(max(0, n_chunks - 7), n_chunks - 1) if order.index((1, j + 1)) > known)
    assert n_chunks > 5 and early < n_chunks - 5

    for what, j in order:
        if what == "h line":
            with jax.named_scope("hline"):
                arrived(h_place(v, z_one), 1, hid=z_one)
                arrived(h_place(v, lax.rem(z_one + 2, 4)), 2, hid=z_one)
                h_own.wait()
            h_chip.start()
            h_core.start()
        elif what == "h chip":
            with jax.named_scope("hchip"):
                arrived(h_place(v_two), 3, vocab=v_two)
            h_both.start()
        else:
            with jax.named_scope(f"w{what}_{j}"):
                landed(j, what)
            forward(j, what).start()
            if what != 1:
                continue
            if j == 1:
                with jax.named_scope("hcore"):
                    arrived(h_place(v_one), 4, vocab=v_one)
                    arrived(h_place(lax.rem(v_one + 2, 4)), 5, vocab=v_one)
                    own_complete()
            if 0 < j <= n_chunks - 5:
                with jax.named_scope(f"x{j - 1}"):
                    complete(j - 1)
                with jax.named_scope(f"c{j - 1}"):
                    compute(j - 1)
                if j - 1 in folds:
                    with jax.named_scope(f"f{j - 1}"):
                        fold(*folds[j - 1])
            if j - 1 == early:
                with jax.named_scope("begin"):
                    for i in tail:
                        forwarded(i, 0)
                        forwarded(i, 2)
                    for i in range(len(ends)):
                        begin_end(i)
    for i in range(len(ends)):
        close(i)

    lane = lax.broadcasted_iota(jnp.int32, (rows, LANES), 1)
    top = jnp.max(m_all[...], axis=1, keepdims=True)
    shrink = jnp.exp(m_all[...] - top)
    scale_ref[...] = shrink
    parts = s_all[...] * shrink
    before = prefix_before(parts)
    off_ref[...] = before
    rel = rel_col[...]
    holds = (rel >= lane * TILE) & (rel < (lane + 1) * TILE) & (rel < n_cols)
    at_tgt = jnp.sum(t_all[...], axis=1, keepdims=True)
    found = jnp.where(holds, at_tgt * shrink + before, 0.0)
    total = jnp.sum(parts, axis=1, keepdims=True)
    at_tgt = jnp.sum(found, axis=1, keepdims=True)
    packed = jnp.where(lane == 0, top, jnp.where(lane == 1, total, at_tgt))
    zmsg[z] = packed.T[0:3, :]

    for k in range(3):
        mine = wbuf.at[w_rows(sources[k], x)]
        remote(mine, mine, ws.at[k], wr.at[0, k], hid=near).wait_send()
        remote(mine, mine, xs.at[k], xr.at[0, k], data=1 - x).wait_send()
    for copy in (h_two, h_one, h_relay, h_chip, h_core, h_both):
        copy.wait_send()

    def z_send(i):
        slot = (0, 1 + is_outer, 1 + is_outer)[i]
        return remote(zmsg.at[z], zmsg.at[z], zs.at[i], zr.at[slot], hid=(near, inner_far, outer_far)[i])

    def v_send(d):
        to = lax.rem(v + d, 4)
        return remote(vmsg.at[v], vmsg.at[v], vs.at[d - 1], vr.at[d - 1], vocab=to)

    for i in (2, 1, 0):
        z_send(i).start()
    for i, frm in enumerate(sources):
        with jax.named_scope(f"z{i}"):
            remote(zmsg.at[frm], zmsg.at[frm], zs.at[i], zr.at[i], hid=frm).wait_recv()

    ids = tgt_ref[...]
    maxes = [zmsg[h, 0:1, :] for h in range(4)]
    v_max = functools.reduce(jnp.maximum, maxes)
    v_sum = jnp.zeros((1, rows), F32)
    v_tgt = jnp.zeros((1, rows), F32)
    mine_before = jnp.zeros((1, rows), F32)
    for h in range(4):
        mine_before = jnp.where(h == z, v_sum, mine_before)
        f = jnp.exp(maxes[h] - v_max)
        low = (v * 4 + h) * n_cols
        inside = (ids >= low) & (ids < low + n_cols)
        v_tgt += jnp.where(inside, zmsg[h, 2:3, :] * f + v_sum, 0.0)
        v_sum += zmsg[h, 1:2, :] * f
    vmsg[v, 0:1, :] = v_max
    vmsg[v, 1:2, :] = v_sum
    vmsg[v, 2:3, :] = v_tgt

    for i in range(3):
        z_send(i).wait_send()
    for d in (2, 1, 3):
        v_send(d).start()
    for d in (1, 2, 3):
        frm = lax.rem(v + 4 - d, 4)
        with jax.named_scope(f"v{d}"):
            remote(vmsg.at[frm], vmsg.at[frm], vs.at[d - 1], vr.at[d - 1], vocab=frm).wait_recv()

    maxes = [vmsg[u, 0:1, :] for u in range(4)]
    g_max = functools.reduce(jnp.maximum, maxes)
    g_sum = jnp.zeros((1, rows), F32)
    g_tgt = jnp.zeros((1, rows), F32)
    g_before = jnp.zeros((1, rows), F32)
    for u in range(4):
        f = jnp.exp(maxes[u] - g_max)
        g_before = jnp.where(u == v, g_sum + mine_before * f, g_before)
        low = u * 4 * n_cols
        inside = (ids >= low) & (ids < low + 4 * n_cols)
        g_tgt += jnp.where(inside, vmsg[u, 2:3, :] * f + g_sum, 0.0)
        g_sum += vmsg[u, 1:2, :] * f
    tgt_out_ref[...] = g_tgt / g_sum
    factor_ref[0:1, :] = jnp.exp(zmsg[z, 0:1, :] - g_max) / g_sum
    factor_ref[1:2, :] = g_before / g_sum
    for d in (1, 2, 3):
        v_send(d).wait_send()


def finish_kernel(lanes, c_ref, scale_ref, off_ref, factor_ref, tgt_ref, out_ref, tgt_out_ref, buf, factor_col, sems):
    slots, n, n_cols = buf.shape
    steps = c_ref.shape[0] // n
    factor_col[...] = factor_ref[...].T

    def put(i):
        slot = lax.rem(i, slots)
        at = pl.ds(pl.multiple_of(i * n, n), n)
        return pltpu.make_async_copy(buf.at[slot], out_ref.at[at], sems.at[slot])

    @pl.loop(0, steps)
    def _(i):
        slot = lax.rem(i, slots)

        @pl.when(i >= slots)
        def _():
            put(i - slots).wait()

        at = pl.ds(pl.multiple_of(i * n, n), n)
        factor = factor_col[at, 0:1]
        scale = scale_ref[at, :] * factor
        off = off_ref[at, :] * factor + factor_col[at, 1:2]
        for t, lane in enumerate(lanes):
            span = slice(t * TILE, min(n_cols, (t + 1) * TILE))
            buf[slot, :, span] = c_ref[at, span] * scale[:, lane : lane + 1] + off[:, lane : lane + 1]
        put(i).start()

    tgt_out_ref[...] = tgt_ref[...]
    for i in range(max(0, steps - slots), steps):
        put(i).wait()


def solution(mesh):
    n_hid, n_voc = mesh.shape["hid"], mesh.shape["vocab"]
    assert n_hid == 4 and n_voc == 4 and mesh.shape["data"] == 2

    def local_step(h_blk, w_blk, temp_blk, tgt_blk):
        rows, depth = h_blk.shape
        n_cols = w_blk.shape[1] // n_hid
        n_tiles = pl.cdiv(n_cols, TILE)
        last_width = n_cols - (n_tiles - 1) * TILE
        assert n_tiles <= LANES and n_cols % LANES == 0
        plan = chunks_of(n_cols // LANES)
        n_chunks = len(plan)
        vmem = pl.BlockSpec(memory_space=pltpu.VMEM)
        hbm = pl.BlockSpec(memory_space=pltpu.HBM)
        dma = pltpu.SemaphoreType.DMA
        table = pltpu.VMEM((rows, LANES), F32)
        c, scale, off, factor, tgt = pl.pallas_call(
            functools.partial(prefix_kernel, n_cols),
            out_shape=(
                pltpu.VMEM((rows, n_cols), F32),
                pltpu.VMEM((rows, LANES), F32),
                pltpu.VMEM((rows, LANES), F32),
                pltpu.VMEM((8, rows), F32),
                pltpu.VMEM((1, rows), F32),
            ),
            in_specs=[hbm] * 4,
            out_specs=[vmem] * 5,
            scratch_shapes=[
                pltpu.VMEM((4 * depth, n_cols), BF16),
                pltpu.VMEM((rows, 4 * depth), BF16),
                pltpu.VMEM((rows, TILE), F32),
                pltpu.VMEM((3 * TILE, TILE), BF16),
                pltpu.VMEM((3 * last_width, last_width), BF16),
                table,
                table,
                table,
                table,
                pltpu.VMEM((rows, LANES), jnp.int32),
                pltpu.VMEM((1, rows), F32),
                pltpu.VMEM((1, rows), jnp.int32),
                pltpu.VMEM((4, 3, rows), F32),
                pltpu.VMEM((4, 3, rows), F32),
                pltpu.VMEM((8, rows), F32),
                dma((3,)),
                dma((n_chunks, 3)),
                dma((3,)),
                dma((n_chunks, 3)),
                dma,
                dma,
                dma((6,)),
                dma((6,)),
                dma((3,)),
                dma((3,)),
                dma((3,)),
                dma((3,)),
                dma((2,)),
            ],
            compiler_params=pltpu.CompilerParams(
                collective_id=0, has_side_effects=True, vmem_limit_bytes=37 << 20
            ),
            name="prefix",
        )(h_blk, w_blk, temp_blk.reshape(1, rows), tgt_blk.reshape(1, rows))
        n = min(rows, 64)
        lanes = list(range(n_tiles))
        for _, g0, g1 in folds_of(plan):
            lanes[g0:g1] = [g0] * (g1 - g0)
        cdf, cdf_tgt = pl.pallas_call(
            functools.partial(finish_kernel, lanes),
            out_shape=(
                jax.ShapeDtypeStruct((rows, n_cols), F32),
                jax.ShapeDtypeStruct((1, rows), F32),
            ),
            in_specs=[vmem] * 5,
            out_specs=[hbm, vmem],
            scratch_shapes=[pltpu.VMEM((4, n, n_cols), F32), pltpu.VMEM((rows, 8), F32), dma((4,))],
            compiler_params=pltpu.CompilerParams(vmem_limit_bytes=9 << 20),
            name="finish",
        )(c, scale, off, factor, tgt)
        return cdf, cdf_tgt.reshape(rows)

    return jax.shard_map(
        local_step,
        mesh=mesh,
        in_specs=(P("data", "hid"), P("hid", "vocab"), P("data"), P("data")),
        out_specs=(P("data", ("vocab", "hid")), P("data")),
        check_vma=False,
    )
```

```python
import functools

import jax
import jax.numpy as jnp
from jax import lax
from jax.experimental import pallas as pl
from jax.experimental.pallas import tpu as pltpu
from jax.sharding import PartitionSpec as P

MESH = pl.DeviceIdType.MESH
F32 = jnp.float32
BF16 = jnp.bfloat16
TILE = 256
LANES = 128
LOWEST = float(jnp.finfo(jnp.float32).min)


def chunks_of(blocks):
    sizes, left = [], blocks
    for size in (blocks % 2 or 2, 1, 1, 1, 1, 2, 4, 4):
        if left > size:
            sizes.append(size)
            left -= size
    while left > 0:
        sizes.append(min(6, left))
        left -= sizes[-1]
    starts, at = [], 0
    for size in reversed(sizes):
        starts.append((at, size))
        at += size
    return starts


def service_order(plan, blocks):
    events = [(0.15 * blocks, "h line", 0), (0.28 * blocks, "h chip", 0)]
    for j, (first, size) in enumerate(plan):
        end = first + size
        events.append((first + size / 3 + 2, 0, j))
        events.append((end + 2, 2, j))
        events.append((min(1.86 * end, 0.68 * blocks + 0.6 * end) + 2, 1, j))
    events.sort(key=lambda e: e[0])
    order = [e[1:] for e in events]
    for j in range(len(plan)):
        at = max(order.index((k, j)) for k in (0, 1, 2))
        order.remove((1, j))
        order.insert(at, (1, j))
    return order


def folds_of(plan):
    n, folds, at = len(plan), [], 0
    for j in (3 * n // 13, 5 * n // 13):
        stop = sum(plan[j]) // 2 - 1
        if j < n - 5 and stop > at:
            folds.append((j, at, stop))
            at = stop
    return folds


def split3(e):
    hi = e.astype(BF16)
    rest = e - hi.astype(F32)
    mid = rest.astype(BF16)
    low = (rest - mid.astype(F32)).astype(BF16)
    return hi, mid, low


def prefix_kernel(
    n_cols, h_ref, w_ref, temp_hbm, tgt_hbm,
    c_ref, scale_ref, off_ref, factor_ref, tgt_out_ref,
    wbuf, hbuf, zbuf, tri, tri_last, m_all, s_all, t_all, temp_col, rel_col, temp_ref, tgt_ref, zmsg, vmsg, back,
    ws, wr, xs, xr, wl, hl, hs, hr, zs, zr, vs, vr, rl,
):
    x, z, v = lax.axis_index("data"), lax.axis_index("hid"), lax.axis_index("vocab")
    rows, depth = h_ref.shape
    half, quarter = depth // 2, rows // 4
    n_tiles = pl.cdiv(n_cols, TILE)
    last_width = n_cols - (n_tiles - 1) * TILE
    plan = chunks_of(n_cols // LANES)
    n_chunks = len(plan)

    side = z // 2
    outer_far, inner_far, near = 3 - 3 * side, 2 - side, 1 - z + 4 * side
    is_outer = jnp.where(z == side * 3, 1, 0)
    z_two, z_one = lax.rem(z + 2, 4), near
    v_two, v_one = lax.rem(v + 2, 4), v + 1 - 2 * lax.rem(v, 2)
    sources = (near, inner_far, outer_far)

    def cols_of(j):
        first, size = plan[j]
        return first * LANES, size * LANES

    def w_rows(source, part):
        return pl.ds(pl.multiple_of(source * depth + part * half, half), half)

    def w_place(j, source, part):
        start, n = cols_of(j)
        return wbuf.at[w_rows(source, part), pl.ds(start, n)]

    def h_place(q, block=None):
        at = pl.ds(pl.multiple_of(q * quarter, quarter), quarter)
        if block is None:
            return hbuf.at[at]
        return hbuf.at[at, pl.ds(pl.multiple_of(block * depth, depth), depth)]

    def remote(src, dst, send, recv, **to):
        return pltpu.make_async_remote_copy(
            src_ref=src, dst_ref=dst, send_sem=send, recv_sem=recv, device_id=to, device_id_type=MESH
        )

    def direct(j, k, dest, slot):
        start, n = cols_of(j)
        src = w_ref.at[
            pl.ds(pl.multiple_of(x * half, half), half),
            pl.ds(pl.multiple_of(dest * n_cols + start, LANES), n),
        ]
        return remote(src, w_place(j, z, x), ws.at[k], wr.at[j, slot], hid=dest)

    def send_near(j):
        return direct(j, 0, near, 0)

    odd = lax.rem(v, 2)
    far_first = outer_far + odd * (inner_far - outer_far)
    far_second = inner_far + odd * (outer_far - inner_far)

    def send_far(j, i):
        return direct(j, 1 + i, (far_first, far_second)[i], 1 + is_outer)

    def landed(j, k):
        place = w_place(j, sources[k], x)
        remote(place, place, ws.at[k], wr.at[j, k], hid=sources[k]).wait_recv()

    def forward(j, k):
        place = w_place(j, sources[k], x)
        return remote(place, place, xs.at[k], xr.at[j, k], data=1 - x)

    def forwarded(j, k):
        place = w_place(j, sources[k], 1 - x)
        remote(place, place, xs.at[k], xr.at[j, k], data=1 - x).wait_recv()

    def own(j):
        start, n = cols_of(j)
        return pltpu.make_async_copy(
            w_ref.at[:, pl.ds(pl.multiple_of(z * n_cols + start, LANES), n)],
            wbuf.at[pl.ds(pl.multiple_of(z * depth, depth), depth), pl.ds(start, n)],
            wl,
        )

    h_mine = h_ref.at[pl.ds(pl.multiple_of(v * quarter, quarter), quarter)]
    h_own = pltpu.make_async_copy(h_mine, h_place(v, z), hl)
    h_two = remote(h_mine, h_place(v, z), hs.at[0], hr.at[0], hid=z_two)
    h_one = remote(h_mine, h_place(v, z), hs.at[1], hr.at[1], hid=z_one)
    h_relay = remote(h_place(v, z_two), h_place(v, z_two), hs.at[2], hr.at[2], hid=z_one)
    h_chip = remote(h_place(v), h_place(v), hs.at[3], hr.at[3], vocab=v_two)
    h_core = remote(h_place(v), h_place(v), hs.at[4], hr.at[4], vocab=v_one)
    h_both = remote(h_place(v_two), h_place(v_two), hs.at[5], hr.at[5], vocab=v_one)

    def arrived(place, i, **frm):
        remote(place, place, hs.at[i], hr.at[i], **frm).wait_recv()

    barrier = pltpu.get_barrier_semaphore()
    peers = [{"hid": lax.rem(z + d, 4)} for d in (1, 2, 3)]
    peers += [{"data": 1 - x}] + [{"vocab": lax.rem(v + d, 4)} for d in (1, 2, 3)]
    for peer in peers:
        pl.semaphore_signal(barrier, inc=1, device_id=peer, device_id_type=MESH)
    row_copies = [
        pltpu.make_async_copy(temp_hbm, temp_ref, rl.at[0]),
        pltpu.make_async_copy(tgt_hbm, tgt_ref, rl.at[1]),
    ]
    for copy in (h_own, *row_copies):
        copy.start()
    for j in range(n_chunks):
        own(j).start()
    with jax.named_scope("bar"):
        pl.semaphore_wait(barrier, len(peers))

    h_two.start()
    h_one.start()
    send_near(0).start()
    send_far(0, 0).start()

    def ones_below(ref, width):
        k = lax.broadcasted_iota(jnp.int32, (width, width), 0)
        c = lax.broadcasted_iota(jnp.int32, (width, width), 1)
        block = jnp.where(k <= c, 1.0, 0.0).astype(BF16)
        for i in range(3):
            ref[pl.ds(i * width, width), :] = block

    ones_below(tri, TILE)
    if last_width != TILE:
        ones_below(tri_last, last_width)
    base = (v * 4 + z) * n_cols
    for copy in row_copies:
        copy.wait()
    back[0:1, :] = temp_ref[...]
    back[1:2, :] = (tgt_ref[...] - base).astype(F32)
    cols8 = back[...].T
    temp_col[...] = jnp.broadcast_to(cols8[:, 0:1], temp_col.shape)
    rel_col[...] = jnp.broadcast_to(cols8[:, 1:2], rel_col.shape).astype(jnp.int32)
    m_all[...] = jnp.full(m_all.shape, LOWEST, F32)
    s_all[...] = jnp.zeros(s_all.shape, F32)
    t_all[...] = jnp.zeros(t_all.shape, F32)

    with jax.named_scope("h0"):
        arrived(h_place(v, z_two), 0, hid=z_two)
    h_relay.start()
    send_far(0, 1).start()
    for j in range(1, n_chunks):
        send_near(j).start()
        send_far(j, 0).start()
        send_far(j, 1).start()

    part, few = min(rows, 512), min(rows, 128)

    def logits_and_sums(product, sums):
        @pl.loop(0, rows // part)
        def _(i):
            if product is not None:
                _, new_start, new_width = product
                at = pl.ds(pl.multiple_of(i * part, part), part)
                new = jnp.dot(
                    hbuf[at, :], wbuf[:, pl.ds(new_start, new_width)], preferred_element_type=F32
                )
            for k in range(0, part, few) if sums is not None else ():
                prefix(pl.ds(pl.multiple_of(i * part + k, few), few), *sums)
            if product is not None:
                zbuf[at, 0:new_width] = new

    def prefix(at, t, start, width):
        pieces = width // LANES
        logits = zbuf[at, 0:width] * jnp.concatenate([temp_col[at, :]] * pieces, axis=1)
        lane = lax.broadcasted_iota(jnp.int32, (few, LANES), 1)
        here = lane == t
        top = jnp.max(logits, axis=1, keepdims=True)
        m_all[at, :] = jnp.where(here, top, m_all[at, :])
        e = jnp.exp(logits - top)
        total = jnp.sum(e, axis=1, keepdims=True)
        s_all[at, :] = jnp.where(here, total, s_all[at, :])
        table = tri if width == TILE else tri_last
        run = jnp.dot(jnp.concatenate(split3(e), axis=1), table[...], preferred_element_type=F32)
        c_ref[at, pl.ds(start, width)] = run
        rel = rel_col[at, :] - start
        hit = t_all[at, :]
        for p in range(pieces):
            hit += jnp.where(lane == rel - p * LANES, run[:, p * LANES : (p + 1) * LANES], 0.0)
        t_all[at, :] = hit

    def whole(t):
        return t, pl.multiple_of(t * TILE, TILE), TILE

    ends = [
        (n_chunks - 4, n_tiles - 3, (n_tiles - 3) * TILE, TILE),
        (n_chunks - 2, n_tiles - 2, (n_tiles - 2) * TILE, TILE),
        (n_chunks - 1, n_tiles - 1, (n_tiles - 1) * TILE, last_width),
    ]

    def compute(j):
        first, size = (n // 2 for n in plan[j])
        stop = first + size
        if first == 0:
            logits_and_sums(whole(0), None)
            first = 1
        if first < stop:

            @pl.loop(first, stop)
            def _(t):
                logits_and_sums(whole(t), whole(t - 1))

        if stop == n_tiles - 3:
            logits_and_sums(None, whole(stop - 1))

    def block_dot(at, block, start, width):
        lanes = pl.ds(pl.multiple_of(block * depth, depth), depth)
        return jnp.dot(hbuf[at, lanes], wbuf[lanes, start : start + width], preferred_element_type=F32)

    def begin_end(i):
        _, _, start, width = ends[i]

        @pl.loop(0, rows // part)
        def _(k):
            at = pl.ds(pl.multiple_of(k * part, part), part)
            c_ref[at, start : start + width] = (
                block_dot(at, z, start, width)
                + block_dot(at, near, start, width)
                + block_dot(at, outer_far, start, width)
            )

    def finish_end(i):
        _, _, start, width = ends[i]

        every = slice(0, rows)
        zbuf[:, 0:width] = c_ref[:, start : start + width] + block_dot(every, inner_far, start, width)
        logits_and_sums(None, ends[i][1:])

    def fold(g0, g1):
        @pl.loop(0, rows // few)
        def _(i):
            at = pl.ds(pl.multiple_of(i * few, few), few)
            lane = lax.broadcasted_iota(jnp.int32, (few, LANES), 1)
            group = (lane >= g0) & (lane < g1)
            m, s = m_all[at, :], s_all[at, :]
            top = jnp.max(jnp.where(group, m, LOWEST), axis=1, keepdims=True)
            shrink = jnp.where(group, jnp.exp(m - top), 0.0)
            parts = s * shrink
            before = prefix_before(parts)
            for t in range(g0, g1):
                span = slice(t * TILE, (t + 1) * TILE)
                c_ref[at, span] = c_ref[at, span] * shrink[:, t : t + 1] + before[:, t : t + 1]
            rel = rel_col[at, :]
            holds = (rel >= lane * TILE) & (rel < (lane + 1) * TILE)
            old = t_all[at, :]
            moved = jnp.sum(old, axis=1, keepdims=True) * shrink + before
            inside = (rel >= g0 * TILE) & (rel < g1 * TILE)
            t_all[at, :] = jnp.where(inside, jnp.where(holds, moved, 0.0), old)
            m_all[at, :] = jnp.where(group, top, m)
            total = jnp.sum(parts, axis=1, keepdims=True)
            s_all[at, :] = jnp.where(group, jnp.where(lane == g1 - 1, total, 0.0), s)

    def close(i):
        first = ends[i - 1][0] + 1 if i else n_chunks - 5
        with jax.named_scope(f"xe{i}"):
            for j in range(first, ends[i][0] + 1):
                forwarded(j, 1)
        with jax.named_scope(f"ce{i}"):
            finish_end(i)

    def prefix_before(parts):
        k = lax.broadcasted_iota(jnp.int32, (LANES, LANES), 0)
        c = lax.broadcasted_iota(jnp.int32, (LANES, LANES), 1)
        strict = jnp.where(k < c, 1.0, 0.0).astype(BF16)
        return sum(jnp.dot(p, strict, preferred_element_type=F32) for p in split3(parts))

    def complete(j):
        for k in range(3):
            forwarded(j, k)

    def own_complete():
        place = wbuf.at[pl.ds(pl.multiple_of(z * depth, depth), depth)]
        pltpu.make_async_copy(place, place, wl).wait()

    order = service_order(plan, n_cols // LANES)
    folds = {j: (g0, g1) for j, g0, g1 in folds_of(plan)}
    tail = range(n_chunks - 5, n_chunks)
    known = max(order.index((k, j)) for k in (0, 2) for j in tail)
    early = min(j for j in range(max(0, n_chunks - 10), n_chunks - 1) if order.index((1, j + 1)) > known)
    assert n_chunks > 5 and early < n_chunks - 5

    for what, j in order:
        if what == "h line":
            with jax.named_scope("hline"):
                arrived(h_place(v, z_one), 1, hid=z_one)
                arrived(h_place(v, lax.rem(z_one + 2, 4)), 2, hid=z_one)
                h_own.wait()
            h_chip.start()
            h_core.start()
        elif what == "h chip":
            with jax.named_scope("hchip"):
                arrived(h_place(v_two), 3, vocab=v_two)
            h_both.start()
        else:
            with jax.named_scope(f"w{what}_{j}"):
                landed(j, what)
            forward(j, what).start()
            if what != 1:
                continue
            if j == 1:
                with jax.named_scope("hcore"):
                    arrived(h_place(v_one), 4, vocab=v_one)
                    arrived(h_place(lax.rem(v_one + 2, 4)), 5, vocab=v_one)
                    own_complete()
            if 0 < j <= n_chunks - 5:
                with jax.named_scope(f"x{j - 1}"):
                    complete(j - 1)
                with jax.named_scope(f"c{j - 1}"):
                    compute(j - 1)
                if j - 1 in folds:
                    with jax.named_scope(f"f{j - 1}"):
                        fold(*folds[j - 1])
            if j - 1 == early:
                with jax.named_scope("begin"):
                    for i in tail:
                        forwarded(i, 0)
                        forwarded(i, 2)
                    for i in range(len(ends)):
                        begin_end(i)
            if j == n_chunks - 2:
                close(0)
    close(1)
    close(2)

    lane = lax.broadcasted_iota(jnp.int32, (rows, LANES), 1)
    top = jnp.max(m_all[...], axis=1, keepdims=True)
    shrink = jnp.exp(m_all[...] - top)
    scale_ref[...] = shrink
    parts = s_all[...] * shrink
    before = prefix_before(parts)
    off_ref[...] = before
    rel = rel_col[...]
    holds = (rel >= lane * TILE) & (rel < (lane + 1) * TILE) & (rel < n_cols)
    at_tgt = jnp.sum(t_all[...], axis=1, keepdims=True)
    found = jnp.where(holds, at_tgt * shrink + before, 0.0)
    total = jnp.sum(parts, axis=1, keepdims=True)
    at_tgt = jnp.sum(found, axis=1, keepdims=True)
    packed = jnp.where(lane == 0, top, jnp.where(lane == 1, total, at_tgt))
    zmsg[z] = packed.T[0:3, :]

    for k in range(3):
        mine = wbuf.at[w_rows(sources[k], x)]
        remote(mine, mine, ws.at[k], wr.at[0, k], hid=near).wait_send()
        remote(mine, mine, xs.at[k], xr.at[0, k], data=1 - x).wait_send()
    for copy in (h_two, h_one, h_relay, h_chip, h_core, h_both):
        copy.wait_send()

    def z_send(i):
        slot = (0, 1 + is_outer, 1 + is_outer)[i]
        return remote(zmsg.at[z], zmsg.at[z], zs.at[i], zr.at[slot], hid=(near, inner_far, outer_far)[i])

    def v_send(d):
        to = lax.rem(v + d, 4)
        return remote(vmsg.at[v], vmsg.at[v], vs.at[d - 1], vr.at[d - 1], vocab=to)

    for i in (2, 1, 0):
        z_send(i).start()
    for i, frm in enumerate(sources):
        with jax.named_scope(f"z{i}"):
            remote(zmsg.at[frm], zmsg.at[frm], zs.at[i], zr.at[i], hid=frm).wait_recv()

    ids = tgt_ref[...]
    maxes = [zmsg[h, 0:1, :] for h in range(4)]
    v_max = functools.reduce(jnp.maximum, maxes)
    v_sum = jnp.zeros((1, rows), F32)
    v_tgt = jnp.zeros((1, rows), F32)
    mine_before = jnp.zeros((1, rows), F32)
    for h in range(4):
        mine_before = jnp.where(h == z, v_sum, mine_before)
        f = jnp.exp(maxes[h] - v_max)
        low = (v * 4 + h) * n_cols
        inside = (ids >= low) & (ids < low + n_cols)
        v_tgt += jnp.where(inside, zmsg[h, 2:3, :] * f + v_sum, 0.0)
        v_sum += zmsg[h, 1:2, :] * f
    vmsg[v, 0:1, :] = v_max
    vmsg[v, 1:2, :] = v_sum
    vmsg[v, 2:3, :] = v_tgt

    for i in range(3):
        z_send(i).wait_send()
    for d in (2, 1, 3):
        v_send(d).start()
    for d in (1, 2, 3):
        frm = lax.rem(v + 4 - d, 4)
        with jax.named_scope(f"v{d}"):
            remote(vmsg.at[frm], vmsg.at[frm], vs.at[d - 1], vr.at[d - 1], vocab=frm).wait_recv()

    maxes = [vmsg[u, 0:1, :] for u in range(4)]
    g_max = functools.reduce(jnp.maximum, maxes)
    g_sum = jnp.zeros((1, rows), F32)
    g_tgt = jnp.zeros((1, rows), F32)
    g_before = jnp.zeros((1, rows), F32)
    for u in range(4):
        f = jnp.exp(maxes[u] - g_max)
        g_before = jnp.where(u == v, g_sum + mine_before * f, g_before)
        low = u * 4 * n_cols
        inside = (ids >= low) & (ids < low + 4 * n_cols)
        g_tgt += jnp.where(inside, vmsg[u, 2:3, :] * f + g_sum, 0.0)
        g_sum += vmsg[u, 1:2, :] * f
    tgt_out_ref[...] = g_tgt / g_sum
    factor_ref[0:1, :] = jnp.exp(zmsg[z, 0:1, :] - g_max) / g_sum
    factor_ref[1:2, :] = g_before / g_sum
    for d in (1, 2, 3):
        v_send(d).wait_send()


def finish_kernel(lanes, c_ref, scale_ref, off_ref, factor_ref, tgt_ref, out_ref, tgt_out_ref, buf, factor_col, sems):
    slots, n, n_cols = buf.shape
    steps = c_ref.shape[0] // n
    factor_col[...] = factor_ref[...].T

    def put(i):
        slot = lax.rem(i, slots)
        at = pl.ds(pl.multiple_of(i * n, n), n)
        return pltpu.make_async_copy(buf.at[slot], out_ref.at[at], sems.at[slot])

    @pl.loop(0, steps)
    def _(i):
        slot = lax.rem(i, slots)

        @pl.when(i >= slots)
        def _():
            put(i - slots).wait()

        at = pl.ds(pl.multiple_of(i * n, n), n)
        factor = factor_col[at, 0:1]
        scale = scale_ref[at, :] * factor
        off = off_ref[at, :] * factor + factor_col[at, 1:2]
        for t, lane in enumerate(lanes):
            span = slice(t * TILE, min(n_cols, (t + 1) * TILE))
            buf[slot, :, span] = c_ref[at, span] * scale[:, lane : lane + 1] + off[:, lane : lane + 1]
        @pl.when(lax.rem(i, 2) == 0)
        def _():
            put(i).start()

        @pl.when(lax.rem(i, 2) == 1)
        def _():
            put(i).start(priority=1)

    tgt_out_ref[...] = tgt_ref[...]
    for i in range(max(0, steps - slots), steps):
        put(i).wait()


def solution(mesh):
    n_hid, n_voc = mesh.shape["hid"], mesh.shape["vocab"]
    assert n_hid == 4 and n_voc == 4 and mesh.shape["data"] == 2

    def local_step(h_blk, w_blk, temp_blk, tgt_blk):
        rows, depth = h_blk.shape
        n_cols = w_blk.shape[1] // n_hid
        n_tiles = pl.cdiv(n_cols, TILE)
        last_width = n_cols - (n_tiles - 1) * TILE
        assert n_tiles <= LANES and n_cols % LANES == 0
        plan = chunks_of(n_cols // LANES)
        n_chunks = len(plan)
        vmem = pl.BlockSpec(memory_space=pltpu.VMEM)
        hbm = pl.BlockSpec(memory_space=pltpu.HBM)
        dma = pltpu.SemaphoreType.DMA
        table = pltpu.VMEM((rows, LANES), F32)
        c, scale, off, factor, tgt = pl.pallas_call(
            functools.partial(prefix_kernel, n_cols),
            out_shape=(
                pltpu.VMEM((rows, n_cols), F32),
                pltpu.VMEM((rows, LANES), F32),
                pltpu.VMEM((rows, LANES), F32),
                pltpu.VMEM((8, rows), F32),
                pltpu.VMEM((1, rows), F32),
            ),
            in_specs=[hbm] * 4,
            out_specs=[vmem] * 5,
            scratch_shapes=[
                pltpu.VMEM((4 * depth, n_cols), BF16),
                pltpu.VMEM((rows, 4 * depth), BF16),
                pltpu.VMEM((rows, TILE), F32),
                pltpu.VMEM((3 * TILE, TILE), BF16),
                pltpu.VMEM((3 * last_width, last_width), BF16),
                table,
                table,
                table,
                table,
                pltpu.VMEM((rows, LANES), jnp.int32),
                pltpu.VMEM((1, rows), F32),
                pltpu.VMEM((1, rows), jnp.int32),
                pltpu.VMEM((4, 3, rows), F32),
                pltpu.VMEM((4, 3, rows), F32),
                pltpu.VMEM((8, rows), F32),
                dma((3,)),
                dma((n_chunks, 3)),
                dma((3,)),
                dma((n_chunks, 3)),
                dma,
                dma,
                dma((6,)),
                dma((6,)),
                dma((3,)),
                dma((3,)),
                dma((3,)),
                dma((3,)),
                dma((2,)),
            ],
            compiler_params=pltpu.CompilerParams(
                collective_id=0, has_side_effects=True, vmem_limit_bytes=37 << 20
            ),
            name="prefix",
        )(h_blk, w_blk, temp_blk.reshape(1, rows), tgt_blk.reshape(1, rows))
        n = min(rows, 64)
        lanes = list(range(n_tiles))
        for _, g0, g1 in folds_of(plan):
            lanes[g0:g1] = [g0] * (g1 - g0)
        cdf, cdf_tgt = pl.pallas_call(
            functools.partial(finish_kernel, lanes),
            out_shape=(
                jax.ShapeDtypeStruct((rows, n_cols), F32),
                jax.ShapeDtypeStruct((1, rows), F32),
            ),
            in_specs=[vmem] * 5,
            out_specs=[hbm, vmem],
            scratch_shapes=[pltpu.VMEM((4, n, n_cols), F32), pltpu.VMEM((rows, 8), F32), dma((4,))],
            compiler_params=pltpu.CompilerParams(vmem_limit_bytes=9 << 20),
            name="finish",
        )(c, scale, off, factor, tgt)
        return cdf, cdf_tgt.reshape(rows)

    return jax.shard_map(
        local_step,
        mesh=mesh,
        in_specs=(P("data", "hid"), P("hid", "vocab"), P("data"), P("data")),
        out_specs=(P("data", ("vocab", "hid")), P("data")),
        check_vma=False,
    )
```

```python
import functools

import jax
import jax.numpy as jnp
from jax import lax
from jax.experimental import pallas as pl
from jax.experimental.pallas import tpu as pltpu
from jax.sharding import PartitionSpec as P

MESH = pl.DeviceIdType.MESH
F32 = jnp.float32
BF16 = jnp.bfloat16
TILE = 256
LANES = 128
LOWEST = float(jnp.finfo(jnp.float32).min)


def chunks_of(blocks):
    sizes, left = [], blocks
    for size in (blocks % 2 or 2, 1, 1, 1, 1, 2, 4, 4):
        if left > size:
            sizes.append(size)
            left -= size
    while left > 0:
        sizes.append(min(6, left))
        left -= sizes[-1]
    starts, at = [], 0
    for size in reversed(sizes):
        starts.append((at, size, 0, 2))
        at += size
    first, size, _, _ = starts.pop()
    return starts + [(first, size, 0, 1), (first, size, 1, 1)]


def service_order(plan, blocks):
    events = [(0.15 * blocks, "h line", 0), (0.28 * blocks, "h chip", 0)]
    for j, (first, size, _, _) in enumerate(plan):
        end = first + size
        events.append((first + size / 3 + 2, 0, j))
        events.append((end + 2, 2, j))
        events.append((min(1.86 * end, 0.68 * blocks + 0.6 * end) + 2, 1, j))
    events.sort(key=lambda e: e[0])
    order = [e[1:] for e in events]
    for j in range(len(plan)):
        at = max(order.index((k, j)) for k in (0, 1, 2))
        order.remove((1, j))
        order.insert(at, (1, j))
    return order


def folds_of(plan):
    n, folds, at = len(plan), [], 0
    for j in (3 * n // 14, 5 * n // 14):
        stop = sum(plan[j][:2]) // 2 - 1
        if j < n - 6 and stop > at:
            folds.append((j, at, stop))
            at = stop
    return folds


def split3(e):
    hi = e.astype(BF16)
    rest = e - hi.astype(F32)
    mid = rest.astype(BF16)
    low = (rest - mid.astype(F32)).astype(BF16)
    return hi, mid, low


def prefix_kernel(
    n_cols, h_ref, w_ref, temp_hbm, tgt_hbm,
    c_ref, scale_ref, off_ref, factor_ref, tgt_out_ref,
    wbuf, hbuf, zbuf, tri, tri_last, m_all, s_all, t_all, temp_col, rel_col, temp_ref, tgt_ref, zmsg, vmsg, back,
    ws, wr, xs, xr, ts, tr, wl, hl, hs, hr, zs, zr, vs, vr, rl,
):
    x, z, v = lax.axis_index("data"), lax.axis_index("hid"), lax.axis_index("vocab")
    rows, depth = h_ref.shape
    half, quarter = depth // 2, rows // 4
    n_tiles = pl.cdiv(n_cols, TILE)
    last_width = n_cols - (n_tiles - 1) * TILE
    plan = chunks_of(n_cols // LANES)
    n_chunks = len(plan)

    side = z // 2
    outer_far, inner_far, near = 3 - 3 * side, 2 - side, 1 - z + 4 * side
    is_outer = jnp.where(z == side * 3, 1, 0)
    z_two, z_one = lax.rem(z + 2, 4), near
    v_two, v_one = lax.rem(v + 2, 4), v + 1 - 2 * lax.rem(v, 2)
    sources = (near, inner_far, outer_far)

    def cols_of(j):
        first, size, _, _ = plan[j]
        return first * LANES, size * LANES

    def w_rows(source, part, j=None):
        at, n = (0, half) if j is None else (plan[j][2] * (half // 2), plan[j][3] * (half // 2))
        return pl.ds(pl.multiple_of(source * depth + part * half + at, half // 2), n)

    def w_place(j, source, part):
        start, n = cols_of(j)
        return wbuf.at[w_rows(source, part, j), pl.ds(start, n)]

    def h_place(q, block=None):
        at = pl.ds(pl.multiple_of(q * quarter, quarter), quarter)
        if block is None:
            return hbuf.at[at]
        return hbuf.at[at, pl.ds(pl.multiple_of(block * depth, depth), depth)]

    def remote(src, dst, send, recv, **to):
        return pltpu.make_async_remote_copy(
            src_ref=src, dst_ref=dst, send_sem=send, recv_sem=recv, device_id=to, device_id_type=MESH
        )

    def w_source(j, part, dest):
        start, n = cols_of(j)
        return w_ref.at[w_rows(0, part, j), pl.ds(pl.multiple_of(dest * n_cols + start, LANES), n)]

    def direct(j, k, dest, slot):
        return remote(w_source(j, x, dest), w_place(j, z, x), ws.at[k], wr.at[j, slot], hid=dest)

    def send_near(j):
        return direct(j, 0, near, 0)

    odd = lax.rem(v, 2)
    far_first = outer_far + odd * (inner_far - outer_far)
    far_second = inner_far + odd * (outer_far - inner_far)

    def send_far(j, i):
        return direct(j, 1 + i, (far_first, far_second)[i], 1 + is_outer)

    def send_twin(i):
        dest = (far_first, far_second)[i]
        return remote(w_source(n_chunks - 1, 1 - x, dest), w_place(n_chunks - 1, z, 1 - x), ts.at[i], tr, hid=dest)

    def twin_landed():
        place = w_place(n_chunks - 1, inner_far, 1 - x)
        remote(place, place, ts.at[0], tr, hid=inner_far).wait_recv()

    def landed(j, k):
        place = w_place(j, sources[k], x)
        remote(place, place, ws.at[k], wr.at[j, k], hid=sources[k]).wait_recv()

    def forward(j, k):
        place = w_place(j, sources[k], x)
        send = 3 if k == 1 and j == n_chunks - 2 else k
        return remote(place, place, xs.at[send], xr.at[j, k], data=1 - x)

    def forwarded(j, k):
        place = w_place(j, sources[k], 1 - x)
        remote(place, place, xs.at[k], xr.at[j, k], data=1 - x).wait_recv()

    def own(j):
        start, n = cols_of(j)
        return pltpu.make_async_copy(
            w_ref.at[:, pl.ds(pl.multiple_of(z * n_cols + start, LANES), n)],
            wbuf.at[pl.ds(pl.multiple_of(z * depth, depth), depth), pl.ds(start, n)],
            wl,
        )

    h_mine = h_ref.at[pl.ds(pl.multiple_of(v * quarter, quarter), quarter)]
    h_own = pltpu.make_async_copy(h_mine, h_place(v, z), hl)
    h_two = remote(h_mine, h_place(v, z), hs.at[0], hr.at[0], hid=z_two)
    h_one = remote(h_mine, h_place(v, z), hs.at[1], hr.at[1], hid=z_one)
    h_relay = remote(h_place(v, z_two), h_place(v, z_two), hs.at[2], hr.at[2], hid=z_one)
    h_chip = remote(h_place(v), h_place(v), hs.at[3], hr.at[3], vocab=v_two)
    h_core = remote(h_place(v), h_place(v), hs.at[4], hr.at[4], vocab=v_one)
    h_both = remote(h_place(v_two), h_place(v_two), hs.at[5], hr.at[5], vocab=v_one)

    def arrived(place, i, **frm):
        remote(place, place, hs.at[i], hr.at[i], **frm).wait_recv()

    barrier = pltpu.get_barrier_semaphore()
    peers = [{"hid": lax.rem(z + d, 4)} for d in (1, 2, 3)]
    peers += [{"data": 1 - x}] + [{"vocab": lax.rem(v + d, 4)} for d in (1, 2, 3)]
    for peer in peers:
        pl.semaphore_signal(barrier, inc=1, device_id=peer, device_id_type=MESH)
    row_copies = [
        pltpu.make_async_copy(temp_hbm, temp_ref, rl.at[0]),
        pltpu.make_async_copy(tgt_hbm, tgt_ref, rl.at[1]),
    ]
    for copy in (h_own, *row_copies):
        copy.start()
    for j in range(n_chunks - 1):
        own(j).start()
    with jax.named_scope("bar"):
        pl.semaphore_wait(barrier, len(peers))

    h_two.start()
    h_one.start()
    send_near(0).start()
    send_far(0, 0).start()

    def ones_below(ref, width):
        k = lax.broadcasted_iota(jnp.int32, (width, width), 0)
        c = lax.broadcasted_iota(jnp.int32, (width, width), 1)
        block = jnp.where(k <= c, 1.0, 0.0).astype(BF16)
        for i in range(3):
            ref[pl.ds(i * width, width), :] = block

    ones_below(tri, TILE)
    if last_width != TILE:
        ones_below(tri_last, last_width)
    base = (v * 4 + z) * n_cols
    for copy in row_copies:
        copy.wait()
    back[0:1, :] = temp_ref[...]
    back[1:2, :] = (tgt_ref[...] - base).astype(F32)
    cols8 = back[...].T
    temp_col[...] = jnp.broadcast_to(cols8[:, 0:1], temp_col.shape)
    rel_col[...] = jnp.broadcast_to(cols8[:, 1:2], rel_col.shape).astype(jnp.int32)
    m_all[...] = jnp.full(m_all.shape, LOWEST, F32)
    s_all[...] = jnp.zeros(s_all.shape, F32)
    t_all[...] = jnp.zeros(t_all.shape, F32)

    with jax.named_scope("h0"):
        arrived(h_place(v, z_two), 0, hid=z_two)
    h_relay.start()
    send_far(0, 1).start()
    for j in range(1, n_chunks):
        send_near(j).start()
        send_far(j, 0).start()
        send_far(j, 1).start()

    @pl.when(is_outer == 0)
    def _():
        send_twin(0).start()
        send_twin(1).start()


    part, few = min(rows, 512), min(rows, 128)

    def logits_and_sums(product, sums):
        @pl.loop(0, rows // part)
        def _(i):
            if product is not None:
                _, new_start, new_width = product
                at = pl.ds(pl.multiple_of(i * part, part), part)
                new = jnp.dot(
                    hbuf[at, :], wbuf[:, pl.ds(new_start, new_width)], preferred_element_type=F32
                )
            for k in range(0, part, few) if sums is not None else ():
                prefix(pl.ds(pl.multiple_of(i * part + k, few), few), *sums)
            if product is not None:
                zbuf[at, 0:new_width] = new

    def prefix(at, t, start, width):
        pieces = width // LANES
        logits = zbuf[at, 0:width] * jnp.concatenate([temp_col[at, :]] * pieces, axis=1)
        lane = lax.broadcasted_iota(jnp.int32, (few, LANES), 1)
        here = lane == t
        top = jnp.max(logits, axis=1, keepdims=True)
        m_all[at, :] = jnp.where(here, top, m_all[at, :])
        e = jnp.exp(logits - top)
        total = jnp.sum(e, axis=1, keepdims=True)
        s_all[at, :] = jnp.where(here, total, s_all[at, :])
        table = tri if width == TILE else tri_last
        run = jnp.dot(jnp.concatenate(split3(e), axis=1), table[...], preferred_element_type=F32)
        c_ref[at, pl.ds(start, width)] = run
        rel = rel_col[at, :] - start
        hit = t_all[at, :]
        for p in range(pieces):
            hit += jnp.where(lane == rel - p * LANES, run[:, p * LANES : (p + 1) * LANES], 0.0)
        t_all[at, :] = hit

    def whole(t):
        return t, pl.multiple_of(t * TILE, TILE), TILE

    ends = [
        (n_chunks - 5, n_tiles - 3, (n_tiles - 3) * TILE, TILE),
        (n_chunks - 3, n_tiles - 2, (n_tiles - 2) * TILE, TILE),
        (n_chunks - 1, n_tiles - 1, (n_tiles - 1) * TILE, last_width),
    ]

    def compute(j):
        first, size = (n // 2 for n in plan[j][:2])
        stop = first + size
        if first == 0:
            logits_and_sums(whole(0), None)
            first = 1
        if first < stop:

            @pl.loop(first, stop)
            def _(t):
                logits_and_sums(whole(t), whole(t - 1))

        if stop == n_tiles - 3:
            logits_and_sums(None, whole(stop - 1))

    def block_dot(at, block, start, width):
        lanes = pl.ds(pl.multiple_of(block * depth, depth), depth)
        return jnp.dot(hbuf[at, lanes], wbuf[lanes, start : start + width], preferred_element_type=F32)

    def begin_end(i):
        _, _, start, width = ends[i]

        @pl.loop(0, rows // part)
        def _(k):
            at = pl.ds(pl.multiple_of(k * part, part), part)
            c_ref[at, start : start + width] = (
                block_dot(at, z, start, width)
                + block_dot(at, near, start, width)
                + block_dot(at, outer_far, start, width)
            )

    def finish_end(i):
        _, _, start, width = ends[i]

        every = slice(0, rows)
        zbuf[:, 0:width] = c_ref[:, start : start + width] + block_dot(every, inner_far, start, width)
        logits_and_sums(None, ends[i][1:])

    def fold(g0, g1):
        @pl.loop(0, rows // few)
        def _(i):
            at = pl.ds(pl.multiple_of(i * few, few), few)
            lane = lax.broadcasted_iota(jnp.int32, (few, LANES), 1)
            group = (lane >= g0) & (lane < g1)
            m, s = m_all[at, :], s_all[at, :]
            top = jnp.max(jnp.where(group, m, LOWEST), axis=1, keepdims=True)
            shrink = jnp.where(group, jnp.exp(m - top), 0.0)
            parts = s * shrink
            before = prefix_before(parts)
            for t in range(g0, g1):
                span = slice(t * TILE, (t + 1) * TILE)
                c_ref[at, span] = c_ref[at, span] * shrink[:, t : t + 1] + before[:, t : t + 1]
            rel = rel_col[at, :]
            holds = (rel >= lane * TILE) & (rel < (lane + 1) * TILE)
            old = t_all[at, :]
            moved = jnp.sum(old, axis=1, keepdims=True) * shrink + before
            inside = (rel >= g0 * TILE) & (rel < g1 * TILE)
            t_all[at, :] = jnp.where(inside, jnp.where(holds, moved, 0.0), old)
            m_all[at, :] = jnp.where(group, top, m)
            total = jnp.sum(parts, axis=1, keepdims=True)
            s_all[at, :] = jnp.where(group, jnp.where(lane == g1 - 1, total, 0.0), s)

    def close(i):
        first = ends[i - 1][0] + 1 if i else n_chunks - 6
        with jax.named_scope(f"xe{i}"):
            for j in range(first, ends[i][0] + 1):
                if j < n_chunks - 1:
                    forwarded(j, 1)
                else:
                    twin_landed()
        with jax.named_scope(f"ce{i}"):
            finish_end(i)

    def prefix_before(parts):
        k = lax.broadcasted_iota(jnp.int32, (LANES, LANES), 0)
        c = lax.broadcasted_iota(jnp.int32, (LANES, LANES), 1)
        strict = jnp.where(k < c, 1.0, 0.0).astype(BF16)
        return sum(jnp.dot(p, strict, preferred_element_type=F32) for p in split3(parts))

    def complete(j):
        for k in range(3):
            forwarded(j, k)

    def own_complete():
        place = wbuf.at[pl.ds(pl.multiple_of(z * depth, depth), depth)]
        pltpu.make_async_copy(place, place, wl).wait()

    order = service_order(plan, n_cols // LANES)
    folds = {j: (g0, g1) for j, g0, g1 in folds_of(plan)}
    tail = range(n_chunks - 6, n_chunks)
    known = max(order.index((k, j)) for k in (0, 2) for j in tail)
    early = min(j for j in range(max(0, n_chunks - 11), n_chunks - 1) if order.index((1, j + 1)) > known)
    assert n_chunks > 6 and early < n_chunks - 6

    for what, j in order:
        if what == "h line":
            with jax.named_scope("hline"):
                arrived(h_place(v, z_one), 1, hid=z_one)
                arrived(h_place(v, lax.rem(z_one + 2, 4)), 2, hid=z_one)
                h_own.wait()
            h_chip.start()
            h_core.start()
        elif what == "h chip":
            with jax.named_scope("hchip"):
                arrived(h_place(v_two), 3, vocab=v_two)
            h_both.start()
        else:
            with jax.named_scope(f"w{what}_{j}"):
                landed(j, what)
            if (what, j) != (1, n_chunks - 1):
                forward(j, what).start()
            if what != 1:
                continue
            if j == 1:
                with jax.named_scope("hcore"):
                    arrived(h_place(v_one), 4, vocab=v_one)
                    arrived(h_place(lax.rem(v_one + 2, 4)), 5, vocab=v_one)
                    own_complete()
            if 0 < j <= n_chunks - 6:
                with jax.named_scope(f"x{j - 1}"):
                    complete(j - 1)
                with jax.named_scope(f"c{j - 1}"):
                    compute(j - 1)
                if j - 1 in folds:
                    with jax.named_scope(f"f{j - 1}"):
                        fold(*folds[j - 1])
            if j - 1 == early:
                with jax.named_scope("begin"):
                    for i in tail:
                        forwarded(i, 0)
                        forwarded(i, 2)
                    for i in range(len(ends)):
                        begin_end(i)
            if j == n_chunks - 3:
                close(0)
    close(1)
    close(2)

    lane = lax.broadcasted_iota(jnp.int32, (rows, LANES), 1)
    top = jnp.max(m_all[...], axis=1, keepdims=True)
    shrink = jnp.exp(m_all[...] - top)
    scale_ref[...] = shrink
    parts = s_all[...] * shrink
    total = jnp.sum(parts, axis=1, keepdims=True)
    rel = rel_col[...]
    holds = (rel >= lane * TILE) & (rel < (lane + 1) * TILE) & (rel < n_cols)
    ahead = ((lane + 1) * TILE <= rel) & (rel < n_cols)
    at_tgt = jnp.sum(t_all[...], axis=1, keepdims=True)
    found = jnp.where(holds, at_tgt * shrink, jnp.where(ahead, parts, 0.0))
    at_tgt = jnp.sum(found, axis=1, keepdims=True)
    packed = jnp.where(lane == 0, top, jnp.where(lane == 1, total, at_tgt))
    zmsg[z] = packed.T[0:3, :]

    for k in range(3):
        mine = wbuf.at[w_rows(sources[k], x)]
        remote(mine, mine, ws.at[k], wr.at[0, k], hid=near).wait_send()
        if k == 1:
            mine = wbuf.at[w_rows(sources[k], x), pl.ds(0, n_cols - last_width)]
        remote(mine, mine, xs.at[k], xr.at[0, k], data=1 - x).wait_send()
    forward(n_chunks - 2, 1).wait_send()

    @pl.when(is_outer == 0)
    def _():
        send_twin(0).wait_send()
        send_twin(1).wait_send()

    for copy in (h_two, h_one, h_relay, h_chip, h_core, h_both):
        copy.wait_send()

    def z_send(i):
        slot = (0, 1 + is_outer, 1 + is_outer)[i]
        return remote(zmsg.at[z], zmsg.at[z], zs.at[i], zr.at[slot], hid=(near, inner_far, outer_far)[i])

    def v_send(d):
        to = lax.rem(v + d, 4)
        return remote(vmsg.at[v], vmsg.at[v], vs.at[d - 1], vr.at[d - 1], vocab=to)

    for i in (2, 1, 0):
        z_send(i).start()
    off_ref[...] = prefix_before(s_all[...] * scale_ref[...])
    for i, frm in enumerate(sources):
        with jax.named_scope(f"z{i}"):
            remote(zmsg.at[frm], zmsg.at[frm], zs.at[i], zr.at[i], hid=frm).wait_recv()

    ids = tgt_ref[...]
    maxes = [zmsg[h, 0:1, :] for h in range(4)]
    v_max = functools.reduce(jnp.maximum, maxes)
    v_sum = jnp.zeros((1, rows), F32)
    v_tgt = jnp.zeros((1, rows), F32)
    mine_before = jnp.zeros((1, rows), F32)
    for h in range(4):
        mine_before = jnp.where(h == z, v_sum, mine_before)
        f = jnp.exp(maxes[h] - v_max)
        low = (v * 4 + h) * n_cols
        inside = (ids >= low) & (ids < low + n_cols)
        v_tgt += jnp.where(inside, zmsg[h, 2:3, :] * f + v_sum, 0.0)
        v_sum += zmsg[h, 1:2, :] * f
    vmsg[v, 0:1, :] = v_max
    vmsg[v, 1:2, :] = v_sum
    vmsg[v, 2:3, :] = v_tgt

    for i in range(3):
        z_send(i).wait_send()
    for d in (2, 1, 3):
        v_send(d).start()
    for d in (1, 2, 3):
        frm = lax.rem(v + 4 - d, 4)
        with jax.named_scope(f"v{d}"):
            remote(vmsg.at[frm], vmsg.at[frm], vs.at[d - 1], vr.at[d - 1], vocab=frm).wait_recv()

    maxes = [vmsg[u, 0:1, :] for u in range(4)]
    g_max = functools.reduce(jnp.maximum, maxes)
    g_sum = jnp.zeros((1, rows), F32)
    g_tgt = jnp.zeros((1, rows), F32)
    g_before = jnp.zeros((1, rows), F32)
    for u in range(4):
        f = jnp.exp(maxes[u] - g_max)
        g_before = jnp.where(u == v, g_sum + mine_before * f, g_before)
        low = u * 4 * n_cols
        inside = (ids >= low) & (ids < low + 4 * n_cols)
        g_tgt += jnp.where(inside, vmsg[u, 2:3, :] * f + g_sum, 0.0)
        g_sum += vmsg[u, 1:2, :] * f
    tgt_out_ref[...] = g_tgt / g_sum
    factor_ref[0:1, :] = jnp.exp(zmsg[z, 0:1, :] - g_max) / g_sum
    factor_ref[1:2, :] = g_before / g_sum
    for d in (1, 2, 3):
        v_send(d).wait_send()


def finish_kernel(lanes, c_ref, scale_ref, off_ref, factor_ref, tgt_ref, out_ref, tgt_out_ref, buf, factor_col, sems):
    slots, n, n_cols = buf.shape
    steps = c_ref.shape[0] // n
    factor_col[...] = factor_ref[...].T

    def put(i):
        slot = lax.rem(i, slots)
        at = pl.ds(pl.multiple_of(i * n, n), n)
        return pltpu.make_async_copy(buf.at[slot], out_ref.at[at], sems.at[slot])

    @pl.loop(0, steps)
    def _(i):
        slot = lax.rem(i, slots)

        @pl.when(i >= slots)
        def _():
            put(i - slots).wait()

        at = pl.ds(pl.multiple_of(i * n, n), n)
        factor = factor_col[at, 0:1]
        scale = scale_ref[at, :] * factor
        off = off_ref[at, :] * factor + factor_col[at, 1:2]
        for t, lane in enumerate(lanes):
            span = slice(t * TILE, min(n_cols, (t + 1) * TILE))
            buf[slot, :, span] = c_ref[at, span] * scale[:, lane : lane + 1] + off[:, lane : lane + 1]
        put(i).start()

    tgt_out_ref[...] = tgt_ref[...]
    for i in range(max(0, steps - slots), steps):
        put(i).wait()


def solution(mesh):
    n_hid, n_voc = mesh.shape["hid"], mesh.shape["vocab"]
    assert n_hid == 4 and n_voc == 4 and mesh.shape["data"] == 2

    def local_step(h_blk, w_blk, temp_blk, tgt_blk):
        rows, depth = h_blk.shape
        n_cols = w_blk.shape[1] // n_hid
        n_tiles = pl.cdiv(n_cols, TILE)
        last_width = n_cols - (n_tiles - 1) * TILE
        assert n_tiles <= LANES and n_cols % LANES == 0
        plan = chunks_of(n_cols // LANES)
        n_chunks = len(plan)
        vmem = pl.BlockSpec(memory_space=pltpu.VMEM)
        hbm = pl.BlockSpec(memory_space=pltpu.HBM)
        dma = pltpu.SemaphoreType.DMA
        table = pltpu.VMEM((rows, LANES), F32)
        c, scale, off, factor, tgt = pl.pallas_call(
            functools.partial(prefix_kernel, n_cols),
            out_shape=(
                pltpu.VMEM((rows, n_cols), F32),
                pltpu.VMEM((rows, LANES), F32),
                pltpu.VMEM((rows, LANES), F32),
                pltpu.VMEM((8, rows), F32),
                pltpu.VMEM((1, rows), F32),
            ),
            in_specs=[hbm] * 4,
            out_specs=[vmem] * 5,
            scratch_shapes=[
                pltpu.VMEM((4 * depth, n_cols), BF16),
                pltpu.VMEM((rows, 4 * depth), BF16),
                pltpu.VMEM((rows, TILE), F32),
                pltpu.VMEM((3 * TILE, TILE), BF16),
                pltpu.VMEM((3 * last_width, last_width), BF16),
                table,
                table,
                table,
                table,
                pltpu.VMEM((rows, LANES), jnp.int32),
                pltpu.VMEM((1, rows), F32),
                pltpu.VMEM((1, rows), jnp.int32),
                pltpu.VMEM((4, 3, rows), F32),
                pltpu.VMEM((4, 3, rows), F32),
                pltpu.VMEM((8, rows), F32),
                dma((3,)),
                dma((n_chunks, 3)),
                dma((4,)),
                dma((n_chunks, 3)),
                dma((2,)),
                dma,
                dma,
                dma,
                dma((6,)),
                dma((6,)),
                dma((3,)),
                dma((3,)),
                dma((3,)),
                dma((3,)),
                dma((2,)),
            ],
            compiler_params=pltpu.CompilerParams(
                collective_id=0, has_side_effects=True, vmem_limit_bytes=37 << 20
            ),
            name="prefix",
        )(h_blk, w_blk, temp_blk.reshape(1, rows), tgt_blk.reshape(1, rows))
        n = min(rows, 64)
        lanes = list(range(n_tiles))
        for _, g0, g1 in folds_of(plan):
            lanes[g0:g1] = [g0] * (g1 - g0)
        cdf, cdf_tgt = pl.pallas_call(
            functools.partial(finish_kernel, lanes),
            out_shape=(
                jax.ShapeDtypeStruct((rows, n_cols), F32),
                jax.ShapeDtypeStruct((1, rows), F32),
            ),
            in_specs=[vmem] * 5,
            out_specs=[hbm, vmem],
            scratch_shapes=[pltpu.VMEM((4, n, n_cols), F32), pltpu.VMEM((rows, 8), F32), dma((4,))],
            compiler_params=pltpu.CompilerParams(vmem_limit_bytes=9 << 20),
            name="finish",
        )(c, scale, off, factor, tgt)
        return cdf, cdf_tgt.reshape(rows)

    return jax.shard_map(
        local_step,
        mesh=mesh,
        in_specs=(P("data", "hid"), P("hid", "vocab"), P("data"), P("data")),
        out_specs=(P("data", ("vocab", "hid")), P("data")),
        check_vma=False,
    )
```

```python
import functools

import jax
import jax.numpy as jnp
from jax import lax
from jax.experimental import pallas as pl
from jax.experimental.pallas import tpu as pltpu
from jax.sharding import PartitionSpec as P

MESH = pl.DeviceIdType.MESH
F32 = jnp.float32
BF16 = jnp.bfloat16
TILE = 256
LANES = 128
SLOTS = 32
LOWEST = float(jnp.finfo(jnp.float32).min)


def chunks_of(blocks):
    sizes, left = [], blocks
    for size in (blocks % 2 or 2, 1, 1, 1, 1, 2, 4, 4):
        if left > size:
            sizes.append(size)
            left -= size
    while left > 0:
        sizes.append(min(6, left))
        left -= sizes[-1]
    starts, at = [], 0
    for size in reversed(sizes):
        starts.append((at, size, 0, 2))
        at += size
    first, size, _, _ = starts.pop()
    return starts + [(first, size, 0, 1), (first, size, 1, 1)]


def service_order(plan, blocks):
    events = [(0.15 * blocks, "h line", 0), (0.28 * blocks, "h chip", 0)]
    for j, (first, size, _, _) in enumerate(plan):
        end = first + size
        events.append((first + size / 3 + 2, 0, j))
        events.append((end + 2, 2, j))
        events.append((min(1.86 * end, 0.68 * blocks + 0.6 * end) + 2, 1, j))
    events.sort(key=lambda e: e[0])
    order = [e[1:] for e in events]
    for j in range(len(plan)):
        at = max(order.index((k, j)) for k in (0, 1, 2))
        order.remove((1, j))
        order.insert(at, (1, j))
    return order


def folds_of(plan):
    n, folds, at = len(plan), [], 0
    for j in (3 * n // 14, 5 * n // 14):
        stop = sum(plan[j][:2]) // 2 - 1
        if j < n - 6 and stop > at:
            folds.append((j, at, stop))
            at = stop
    return folds


def split3(e):
    hi = e.astype(BF16)
    rest = e - hi.astype(F32)
    mid = rest.astype(BF16)
    low = (rest - mid.astype(F32)).astype(BF16)
    return hi, mid, low


def prefix_kernel(
    n_cols, h_ref, w_ref, temp_hbm, tgt_hbm,
    c_ref, coef_ref, factor_ref, tgt_out_ref,
    wbuf, hbuf, zbuf, tri, tri_last, stats, t_all, temp_col, rel_col, temp_ref, tgt_ref, zmsg, vmsg, back,
    ws, wr, xs, xr, ts, tr, wl, hl, hs, hr, zs, zr, vs, vr, rl,
):
    x, z, v = lax.axis_index("data"), lax.axis_index("hid"), lax.axis_index("vocab")
    rows, depth = h_ref.shape
    half, quarter = depth // 2, rows // 4
    n_tiles = pl.cdiv(n_cols, TILE)
    last_width = n_cols - (n_tiles - 1) * TILE
    plan = chunks_of(n_cols // LANES)
    n_chunks = len(plan)
    first_end = n_chunks - 6

    side = z // 2
    outer_far, inner_far, near = 3 - 3 * side, 2 - side, 1 - z + 4 * side
    is_outer = jnp.where(z == side * 3, 1, 0)
    z_two, z_one = lax.rem(z + 2, 4), near
    v_two, v_one = lax.rem(v + 2, 4), v + 1 - 2 * lax.rem(v, 2)
    sources = (near, inner_far, outer_far)

    def cols_of(j):
        first, size, _, _ = plan[j]
        return first * LANES, size * LANES

    def w_rows(source, part, j=None):
        at, n = (0, half) if j is None else (plan[j][2] * (half // 2), plan[j][3] * (half // 2))
        return pl.ds(pl.multiple_of(source * depth + part * half + at, half // 2), n)

    def w_place(j, source, part):
        start, n = cols_of(j)
        return wbuf.at[w_rows(source, part, j), pl.ds(start, n)]

    def h_place(q, block=None):
        at = pl.ds(pl.multiple_of(q * quarter, quarter), quarter)
        if block is None:
            return hbuf.at[at]
        return hbuf.at[at, pl.ds(pl.multiple_of(block * depth, depth), depth)]

    def remote(src, dst, send, recv, **to):
        return pltpu.make_async_remote_copy(
            src_ref=src, dst_ref=dst, send_sem=send, recv_sem=recv, device_id=to, device_id_type=MESH
        )

    def w_source(j, part, dest):
        start, n = cols_of(j)
        return w_ref.at[w_rows(0, part, j), pl.ds(pl.multiple_of(dest * n_cols + start, LANES), n)]

    def direct(j, k, dest, slot):
        return remote(w_source(j, x, dest), w_place(j, z, x), ws.at[k], wr.at[j, slot], hid=dest)

    def send_near(j):
        return direct(j, 0, near, 0)

    odd = lax.rem(v, 2)
    far_first = outer_far + odd * (inner_far - outer_far)
    far_second = inner_far + odd * (outer_far - inner_far)

    def send_far(j, i):
        return direct(j, 1 + i, (far_first, far_second)[i], 1 + is_outer)

    def send_twin(i):
        dest = (far_first, far_second)[i]
        return remote(w_source(n_chunks - 1, 1 - x, dest), w_place(n_chunks - 1, z, 1 - x), ts.at[i], tr, hid=dest)

    def twin_landed():
        place = w_place(n_chunks - 1, inner_far, 1 - x)
        remote(place, place, ts.at[0], tr, hid=inner_far).wait_recv()

    def landed(j, k):
        place = w_place(j, sources[k], x)
        remote(place, place, ws.at[k], wr.at[j, k], hid=sources[k]).wait_recv()

    def forward(j, k):
        place = w_place(j, sources[k], x)
        send = 3 if k == 1 and j == n_chunks - 2 else k
        return remote(place, place, xs.at[send], xr.at[cross(j, k)], data=1 - x)

    def cross(j, k):
        if j < first_end:
            return j
        return first_end if k != 1 else 1 + j

    def cross_wait(slot, count, start, stop):
        place = wbuf.at[pl.ds(0, count), pl.ds(start, stop - start)]
        remote(place, place, xs.at[0], xr.at[slot], data=1 - x).wait_recv()

    def forwarded(j):
        place = w_place(j, inner_far, 1 - x)
        remote(place, place, xs.at[1], xr.at[cross(j, 1)], data=1 - x).wait_recv()

    def own(j):
        start, n = cols_of(j)
        return pltpu.make_async_copy(
            w_ref.at[:, pl.ds(pl.multiple_of(z * n_cols + start, LANES), n)],
            wbuf.at[pl.ds(pl.multiple_of(z * depth, depth), depth), pl.ds(start, n)],
            wl,
        )

    h_mine = h_ref.at[pl.ds(pl.multiple_of(v * quarter, quarter), quarter)]
    h_own = pltpu.make_async_copy(h_mine, h_place(v, z), hl)
    h_two = remote(h_mine, h_place(v, z), hs.at[0], hr.at[0], hid=z_two)
    h_one = remote(h_mine, h_place(v, z), hs.at[1], hr.at[1], hid=z_one)
    h_relay = remote(h_place(v, z_two), h_place(v, z_two), hs.at[2], hr.at[2], hid=z_one)
    h_chip = remote(h_place(v), h_place(v), hs.at[3], hr.at[3], vocab=v_two)
    h_core = remote(h_place(v), h_place(v), hs.at[4], hr.at[4], vocab=v_one)
    h_both = remote(h_place(v_two), h_place(v_two), hs.at[5], hr.at[5], vocab=v_one)

    def arrived(place, i, **frm):
        remote(place, place, hs.at[i], hr.at[i], **frm).wait_recv()

    barrier = pltpu.get_barrier_semaphore()
    peers = [{"hid": lax.rem(z + d, 4)} for d in (1, 2, 3)]
    peers += [{"data": 1 - x}] + [{"vocab": lax.rem(v + d, 4)} for d in (1, 2, 3)]
    for peer in peers:
        pl.semaphore_signal(barrier, inc=1, device_id=peer, device_id_type=MESH)
    row_copies = [
        pltpu.make_async_copy(temp_hbm, temp_ref, rl.at[0]),
        pltpu.make_async_copy(tgt_hbm, tgt_ref, rl.at[1]),
    ]
    for copy in (h_own, *row_copies):
        copy.start()
    for j in range(n_chunks - 1):
        own(j).start()
    with jax.named_scope("bar"):
        pl.semaphore_wait(barrier, len(peers))

    h_two.start()
    h_one.start()
    send_near(0).start()
    send_far(0, 0).start()

    def ones_below(ref, width):
        k = lax.broadcasted_iota(jnp.int32, (width, width), 0)
        c = lax.broadcasted_iota(jnp.int32, (width, width), 1)
        block = jnp.where(k <= c, 1.0, 0.0).astype(BF16)
        for i in range(3):
            ref[pl.ds(i * width, width), :] = block

    ones_below(tri, TILE)
    if last_width != TILE:
        ones_below(tri_last, last_width)
    base = (v * 4 + z) * n_cols
    for copy in row_copies:
        copy.wait()
    back[0:1, :] = temp_ref[...]
    back[1:2, :] = (tgt_ref[...] - base).astype(F32)
    cols8 = back[...].T
    temp_col[...] = jnp.broadcast_to(cols8[:, 0:1], temp_col.shape)
    rel_col[...] = jnp.broadcast_to(cols8[:, 1:2], rel_col.shape).astype(jnp.int32)
    slot = lax.broadcasted_iota(jnp.int32, stats.shape, 1)
    stats[...] = jnp.where(slot < SLOTS, LOWEST, 0.0)
    t_all[...] = jnp.zeros(t_all.shape, F32)

    with jax.named_scope("h0"):
        arrived(h_place(v, z_two), 0, hid=z_two)
    h_relay.start()
    send_far(0, 1).start()
    for j in range(1, n_chunks):
        send_near(j).start()
        send_far(j, 0).start()
        send_far(j, 1).start()

    @pl.when(is_outer == 0)
    def _():
        send_twin(0).start()
        send_twin(1).start()


    part, few = min(rows, 512), min(rows, 128)

    def logits_and_sums(product, sums):
        @pl.loop(0, rows // part)
        def _(i):
            if product is not None:
                _, new_start, new_width = product
                at = pl.ds(pl.multiple_of(i * part, part), part)
                new = jnp.dot(
                    hbuf[at, :], wbuf[:, pl.ds(new_start, new_width)], preferred_element_type=F32
                )
            for k in range(0, part, few) if sums is not None else ():
                prefix(pl.ds(pl.multiple_of(i * part + k, few), few), *sums)
            if product is not None:
                zbuf[at, 0:new_width] = new

    def prefix(at, t, start, width):
        pieces = width // LANES
        logits = zbuf[at, 0:width] * jnp.concatenate([temp_col[at, :]] * pieces, axis=1)
        lane = lax.broadcasted_iota(jnp.int32, (few, LANES), 1)
        top = jnp.max(logits, axis=1, keepdims=True)
        e = jnp.exp(logits - top)
        total = jnp.sum(e, axis=1, keepdims=True)
        stats[at, :] = jnp.where(lane == t, top, jnp.where(lane == SLOTS + t, total, stats[at, :]))
        table = tri if width == TILE else tri_last
        run = jnp.dot(jnp.concatenate(split3(e), axis=1), table[...], preferred_element_type=F32)
        c_ref[at, pl.ds(start, width)] = run
        rel = rel_col[at, :] - start
        hit = t_all[at, :]
        for p in range(pieces):
            hit += jnp.where(lane == rel - p * LANES, run[:, p * LANES : (p + 1) * LANES], 0.0)
        t_all[at, :] = hit

    def whole(t):
        return t, pl.multiple_of(t * TILE, TILE), TILE

    ends = [
        (n_chunks - 5, n_tiles - 3, (n_tiles - 3) * TILE, TILE),
        (n_chunks - 3, n_tiles - 2, (n_tiles - 2) * TILE, TILE),
        (n_chunks - 1, n_tiles - 1, (n_tiles - 1) * TILE, last_width),
    ]

    def compute(j):
        first, size = (n // 2 for n in plan[j][:2])
        stop = first + size
        if first == 0:
            logits_and_sums(whole(0), None)
            first = 1
        if first < stop:

            @pl.loop(first, stop)
            def _(t):
                logits_and_sums(whole(t), whole(t - 1))

        if stop == n_tiles - 3:
            logits_and_sums(None, whole(stop - 1))

    def block_dot(at, block, start, width):
        lanes = pl.ds(pl.multiple_of(block * depth, depth), depth)
        return jnp.dot(hbuf[at, lanes], wbuf[lanes, start : start + width], preferred_element_type=F32)

    def begin_end(i):
        _, _, start, width = ends[i]

        @pl.loop(0, rows // part)
        def _(k):
            at = pl.ds(pl.multiple_of(k * part, part), part)
            c_ref[at, start : start + width] = (
                block_dot(at, z, start, width)
                + block_dot(at, near, start, width)
                + block_dot(at, outer_far, start, width)
            )

    def finish_end(i):
        _, _, start, width = ends[i]

        every = slice(0, rows)
        zbuf[:, 0:width] = c_ref[:, start : start + width] + block_dot(every, inner_far, start, width)
        logits_and_sums(None, ends[i][1:])

    def fold(g0, g1):
        @pl.loop(0, rows // few)
        def _(i):
            at = pl.ds(pl.multiple_of(i * few, few), few)
            lane = lax.broadcasted_iota(jnp.int32, (few, LANES), 1)
            group = (lane >= g0) & (lane < g1)
            m = stats[at, :]
            s = pltpu.roll(m, LANES - SLOTS, 1)
            top = jnp.max(jnp.where(group, m, LOWEST), axis=1, keepdims=True)
            shrink = jnp.where(group, jnp.exp(m - top), 0.0)
            parts = jnp.where(group, s, 0.0) * shrink
            before = prefix_before(parts)
            for t in range(g0, g1):
                span = slice(t * TILE, (t + 1) * TILE)
                c_ref[at, span] = c_ref[at, span] * shrink[:, t : t + 1] + before[:, t : t + 1]
            rel = rel_col[at, :]
            holds = (rel >= lane * TILE) & (rel < (lane + 1) * TILE)
            old = t_all[at, :]
            moved = jnp.sum(old, axis=1, keepdims=True) * shrink + before
            inside = (rel >= g0 * TILE) & (rel < g1 * TILE)
            t_all[at, :] = jnp.where(inside, jnp.where(holds, moved, 0.0), old)
            total = jnp.sum(parts, axis=1, keepdims=True)
            sums = jnp.where(lane == SLOTS + g1 - 1, total, 0.0)
            of_sums = (lane >= SLOTS + g0) & (lane < SLOTS + g1)
            stats[at, :] = jnp.where(group, top, jnp.where(of_sums, sums, m))

    def close(i):
        first = ends[i - 1][0] + 1 if i else n_chunks - 6
        with jax.named_scope(f"xe{i}"):
            for j in range(first, ends[i][0] + 1):
                if j < n_chunks - 1:
                    forwarded(j)
                else:
                    twin_landed()
        with jax.named_scope(f"ce{i}"):
            finish_end(i)

    def prefix_before(parts):
        k = lax.broadcasted_iota(jnp.int32, (LANES, LANES), 0)
        c = lax.broadcasted_iota(jnp.int32, (LANES, LANES), 1)
        strict = jnp.where(k < c, 1.0, 0.0).astype(BF16)
        return sum(jnp.dot(p, strict, preferred_element_type=F32) for p in split3(parts))

    def complete(j):
        start, n = cols_of(j)
        cross_wait(j, 3 * half, start, start + n)

    def own_complete():
        place = wbuf.at[pl.ds(pl.multiple_of(z * depth, depth), depth)]
        pltpu.make_async_copy(place, place, wl).wait()

    order = service_order(plan, n_cols // LANES)
    folds = {j: (g0, g1) for j, g0, g1 in folds_of(plan)}
    tail = range(n_chunks - 6, n_chunks)
    known = max(order.index((k, j)) for k in (0, 2) for j in tail)
    early = min(j for j in range(max(0, n_chunks - 11), n_chunks - 1) if order.index((1, j + 1)) > known)
    assert n_chunks > 6 and early < n_chunks - 6

    for what, j in order:
        if what == "h line":
            with jax.named_scope("hline"):
                arrived(h_place(v, z_one), 1, hid=z_one)
                arrived(h_place(v, lax.rem(z_one + 2, 4)), 2, hid=z_one)
                h_own.wait()
            h_chip.start()
            h_core.start()
        elif what == "h chip":
            with jax.named_scope("hchip"):
                arrived(h_place(v_two), 3, vocab=v_two)
            h_both.start()
        else:
            with jax.named_scope(f"w{what}_{j}"):
                landed(j, what)
            if (what, j) != (1, n_chunks - 1):
                forward(j, what).start()
            if what != 1:
                continue
            if j == 1:
                with jax.named_scope("hcore"):
                    arrived(h_place(v_one), 4, vocab=v_one)
                    arrived(h_place(lax.rem(v_one + 2, 4)), 5, vocab=v_one)
                    own_complete()
            if 0 < j <= n_chunks - 6:
                with jax.named_scope(f"x{j - 1}"):
                    complete(j - 1)
                with jax.named_scope(f"c{j - 1}"):
                    compute(j - 1)
                if j - 1 in folds:
                    with jax.named_scope(f"f{j - 1}"):
                        fold(*folds[j - 1])
            if j - 1 == early:
                with jax.named_scope("begin"):
                    cross_wait(first_end, 2 * half, cols_of(first_end)[0], n_cols)
                    for i in range(len(ends)):
                        begin_end(i)
            if j == n_chunks - 3:
                close(0)
    close(1)
    close(2)

    lane = lax.broadcasted_iota(jnp.int32, (rows, LANES), 1)
    at_tgt = jnp.sum(t_all[...], axis=1, keepdims=True)
    turned = jnp.where(lane == 2 * SLOTS, at_tgt, stats[...]).T
    m, at_tgt = turned[0:SLOTS, :], turned[2 * SLOTS : 2 * SLOTS + 1, :]
    top = jnp.max(m, axis=0, keepdims=True)
    shrink = jnp.exp(m - top)
    parts = turned[SLOTS : 2 * SLOTS, :] * shrink
    start = lax.broadcasted_iota(jnp.int32, (SLOTS, rows), 0) * TILE
    rel = tgt_ref[...] - base
    known = rel < n_cols
    holds = (rel >= start) & (rel < start + TILE) & known
    ahead = (start + TILE <= rel) & known
    found = jnp.where(holds, at_tgt * shrink, jnp.where(ahead, parts, 0.0))
    zmsg[z, 0:1, :] = top
    zmsg[z, 1:2, :] = jnp.sum(parts, axis=0, keepdims=True)
    zmsg[z, 2:3, :] = jnp.sum(found, axis=0, keepdims=True)

    for k in range(3):
        mine = wbuf.at[w_rows(sources[k], x)]
        remote(mine, mine, ws.at[k], wr.at[0, k], hid=near).wait_send()
        if k == 1:
            mine = wbuf.at[w_rows(sources[k], x), pl.ds(0, n_cols - last_width)]
        remote(mine, mine, xs.at[k], xr.at[0], data=1 - x).wait_send()
    forward(n_chunks - 2, 1).wait_send()

    @pl.when(is_outer == 0)
    def _():
        send_twin(0).wait_send()
        send_twin(1).wait_send()

    for copy in (h_two, h_one, h_relay, h_chip, h_core, h_both):
        copy.wait_send()

    def z_send(i):
        slot = (0, 1 + is_outer, 1 + is_outer)[i]
        return remote(zmsg.at[z], zmsg.at[z], zs.at[i], zr.at[slot], hid=(near, inner_far, outer_far)[i])

    def v_send(d):
        to = lax.rem(v + d, 4)
        return remote(vmsg.at[v], vmsg.at[v], vs.at[d - 1], vr.at[d - 1], vocab=to)

    for i in (2, 1, 0):
        z_send(i).start()
    k = lax.broadcasted_iota(jnp.int32, (SLOTS, SLOTS), 0)
    c = lax.broadcasted_iota(jnp.int32, (SLOTS, SLOTS), 1)
    strict = jnp.where(c < k, 1.0, 0.0).astype(BF16)
    before = sum(jnp.dot(strict, p, preferred_element_type=F32) for p in split3(parts))
    rest = jnp.zeros((LANES - 2 * SLOTS, rows), F32)
    coef_ref[...] = jnp.concatenate([shrink, before, rest], axis=0).T
    for i, frm in enumerate(sources):
        with jax.named_scope(f"z{i}"):
            remote(zmsg.at[frm], zmsg.at[frm], zs.at[i], zr.at[i], hid=frm).wait_recv()

    ids = tgt_ref[...]
    maxes = [zmsg[h, 0:1, :] for h in range(4)]
    v_max = functools.reduce(jnp.maximum, maxes)
    v_sum = jnp.zeros((1, rows), F32)
    v_tgt = jnp.zeros((1, rows), F32)
    mine_before = jnp.zeros((1, rows), F32)
    for h in range(4):
        mine_before = jnp.where(h == z, v_sum, mine_before)
        f = jnp.exp(maxes[h] - v_max)
        low = (v * 4 + h) * n_cols
        inside = (ids >= low) & (ids < low + n_cols)
        v_tgt += jnp.where(inside, zmsg[h, 2:3, :] * f + v_sum, 0.0)
        v_sum += zmsg[h, 1:2, :] * f
    vmsg[v, 0:1, :] = v_max
    vmsg[v, 1:2, :] = v_sum
    vmsg[v, 2:3, :] = v_tgt

    for i in range(3):
        z_send(i).wait_send()
    for d in (2, 1, 3):
        v_send(d).start()
    for d in (1, 2, 3):
        frm = lax.rem(v + 4 - d, 4)
        with jax.named_scope(f"v{d}"):
            remote(vmsg.at[frm], vmsg.at[frm], vs.at[d - 1], vr.at[d - 1], vocab=frm).wait_recv()

    maxes = [vmsg[u, 0:1, :] for u in range(4)]
    g_max = functools.reduce(jnp.maximum, maxes)
    g_sum = jnp.zeros((1, rows), F32)
    g_tgt = jnp.zeros((1, rows), F32)
    g_before = jnp.zeros((1, rows), F32)
    for u in range(4):
        f = jnp.exp(maxes[u] - g_max)
        g_before = jnp.where(u == v, g_sum + mine_before * f, g_before)
        low = u * 4 * n_cols
        inside = (ids >= low) & (ids < low + 4 * n_cols)
        g_tgt += jnp.where(inside, vmsg[u, 2:3, :] * f + g_sum, 0.0)
        g_sum += vmsg[u, 1:2, :] * f
    tgt_out_ref[...] = g_tgt / g_sum
    factor_ref[0:1, :] = jnp.exp(zmsg[z, 0:1, :] - g_max) / g_sum
    factor_ref[1:2, :] = g_before / g_sum
    for d in (1, 2, 3):
        v_send(d).wait_send()


def finish_kernel(lanes, c_ref, coef_ref, factor_ref, tgt_ref, out_ref, tgt_out_ref, buf, factor_col, sems):
    slots, n, n_cols = buf.shape
    steps = c_ref.shape[0] // n
    factor_col[...] = factor_ref[...].T

    def put(i):
        slot = lax.rem(i, slots)
        at = pl.ds(pl.multiple_of(i * n, n), n)
        return pltpu.make_async_copy(buf.at[slot], out_ref.at[at], sems.at[slot])

    @pl.loop(0, steps)
    def _(i):
        slot = lax.rem(i, slots)

        @pl.when(i >= slots)
        def _():
            put(i - slots).wait()

        at = pl.ds(pl.multiple_of(i * n, n), n)
        lane = lax.broadcasted_iota(jnp.int32, (n, LANES), 1)
        coef = coef_ref[at, :] * factor_col[at, 0:1] + jnp.where(lane < SLOTS, 0.0, factor_col[at, 1:2])
        for t, k in enumerate(lanes):
            span = slice(t * TILE, min(n_cols, (t + 1) * TILE))
            buf[slot, :, span] = c_ref[at, span] * coef[:, k : k + 1] + coef[:, SLOTS + k : SLOTS + k + 1]
        put(i).start()

    tgt_out_ref[...] = tgt_ref[...]
    for i in range(max(0, steps - slots), steps):
        put(i).wait()


def solution(mesh):
    n_hid, n_voc = mesh.shape["hid"], mesh.shape["vocab"]
    assert n_hid == 4 and n_voc == 4 and mesh.shape["data"] == 2

    def local_step(h_blk, w_blk, temp_blk, tgt_blk):
        rows, depth = h_blk.shape
        n_cols = w_blk.shape[1] // n_hid
        n_tiles = pl.cdiv(n_cols, TILE)
        last_width = n_cols - (n_tiles - 1) * TILE
        assert n_tiles <= SLOTS and n_cols % LANES == 0
        plan = chunks_of(n_cols // LANES)
        n_chunks = len(plan)
        vmem = pl.BlockSpec(memory_space=pltpu.VMEM)
        hbm = pl.BlockSpec(memory_space=pltpu.HBM)
        dma = pltpu.SemaphoreType.DMA
        table = pltpu.VMEM((rows, LANES), F32)
        c, coef, factor, tgt = pl.pallas_call(
            functools.partial(prefix_kernel, n_cols),
            out_shape=(
                pltpu.VMEM((rows, n_cols), F32),
                pltpu.VMEM((rows, LANES), F32),
                pltpu.VMEM((8, rows), F32),
                pltpu.VMEM((1, rows), F32),
            ),
            in_specs=[hbm] * 4,
            out_specs=[vmem] * 4,
            scratch_shapes=[
                pltpu.VMEM((4 * depth, n_cols), BF16),
                pltpu.VMEM((rows, 4 * depth), BF16),
                pltpu.VMEM((rows, TILE), F32),
                pltpu.VMEM((3 * TILE, TILE), BF16),
                pltpu.VMEM((3 * last_width, last_width), BF16),
                table,
                table,
                table,
                pltpu.VMEM((rows, LANES), jnp.int32),
                pltpu.VMEM((1, rows), F32),
                pltpu.VMEM((1, rows), jnp.int32),
                pltpu.VMEM((4, 3, rows), F32),
                pltpu.VMEM((4, 3, rows), F32),
                pltpu.VMEM((8, rows), F32),
                dma((3,)),
                dma((n_chunks, 3)),
                dma((4,)),
                dma((n_chunks,)),
                dma((2,)),
                dma,
                dma,
                dma,
                dma((6,)),
                dma((6,)),
                dma((3,)),
                dma((3,)),
                dma((3,)),
                dma((3,)),
                dma((2,)),
            ],
            compiler_params=pltpu.CompilerParams(
                collective_id=0, has_side_effects=True, vmem_limit_bytes=37 << 20
            ),
            name="prefix",
        )(h_blk, w_blk, temp_blk.reshape(1, rows), tgt_blk.reshape(1, rows))
        n = min(rows, 64)
        lanes = list(range(n_tiles))
        for _, g0, g1 in folds_of(plan):
            lanes[g0:g1] = [g0] * (g1 - g0)
        cdf, cdf_tgt = pl.pallas_call(
            functools.partial(finish_kernel, lanes),
            out_shape=(
                jax.ShapeDtypeStruct((rows, n_cols), F32),
                jax.ShapeDtypeStruct((1, rows), F32),
            ),
            in_specs=[vmem] * 4,
            out_specs=[hbm, vmem],
            scratch_shapes=[pltpu.VMEM((4, n, n_cols), F32), pltpu.VMEM((rows, 8), F32), dma((4,))],
            compiler_params=pltpu.CompilerParams(vmem_limit_bytes=9 << 20),
            name="finish",
        )(c, coef, factor, tgt)
        return cdf, cdf_tgt.reshape(rows)

    return jax.shard_map(
        local_step,
        mesh=mesh,
        in_specs=(P("data", "hid"), P("hid", "vocab"), P("data"), P("data")),
        out_specs=(P("data", ("vocab", "hid")), P("data")),
        check_vma=False,
    )
```

```python
import functools

import jax
import jax.numpy as jnp
from jax import lax
from jax.experimental import pallas as pl
from jax.experimental.pallas import tpu as pltpu
from jax.sharding import PartitionSpec as P

MESH = pl.DeviceIdType.MESH
F32 = jnp.float32
BF16 = jnp.bfloat16
TILE = 256
LANES = 128
SLOTS = 32
LOWEST = float(jnp.finfo(jnp.float32).min)


def tiles_of(blocks):
    whole = (blocks - 3) // 2
    tiles = [(t * TILE, TILE) for t in range(whole)]
    return tiles + [(b * LANES, LANES) for b in range(2 * whole, blocks)]


def chunks_of(blocks):
    whole = (blocks - 3) // 2
    sizes, left = [], 2 * whole - 2
    for size in (2, 4, 4):
        if left > size:
            sizes.append(size)
            left -= size
    while left > 0:
        sizes.append(min(6, left))
        left -= sizes[-1]
    plan, at = [], 0
    for size in reversed(sizes):
        plan.append((at, size, 0, 2))
        at += size
    plan += [(b, 1, 0, 2) for b in range(at, blocks - 2)]
    return plan + [(b, 1, r, 1) for b in (blocks - 2, blocks - 1) for r in (0, 1)]


def service_order(plan, blocks):
    events = [(0.15 * blocks, "h line", 0), (0.28 * blocks, "h chip", 0)]
    for j, (first, size, _, _) in enumerate(plan):
        end = first + size
        events.append((first + size / 3 + 2, 0, j))
        events.append((end + 2, 2, j))
        events.append((min(1.86 * end, 0.68 * blocks + 0.6 * end) + 2, 1, j))
    events.sort(key=lambda e: e[0])
    order = [e[1:] for e in events]
    for j in range(len(plan)):
        at = max(order.index((k, j)) for k in (0, 1, 2))
        order.remove((1, j))
        order.insert(at, (1, j))
    return order


def folds_of(plan, first_end):
    folds, at = [], 0
    for j in (first_end // 3, 5 * first_end // 9):
        stop = sum(plan[j][:2]) // 2 - 1
        if j < first_end and stop > at:
            folds.append((j, at, stop))
            at = stop
    return folds


def split3(e):
    hi = e.astype(BF16)
    rest = e - hi.astype(F32)
    mid = rest.astype(BF16)
    low = (rest - mid.astype(F32)).astype(BF16)
    return hi, mid, low


def prefix_kernel(
    n_cols, h_ref, w_ref, temp_hbm, tgt_hbm,
    c_ref, coef_ref, factor_ref, tgt_out_ref,
    wbuf, hbuf, zbuf, tri, tri_last, stats, t_all, temp_col, rel_col, temp_ref, tgt_ref, zmsg, vmsg, back,
    ws, wr, xs, xr, ts, tr, wl, hl, hs, hr, zs, zr, vs, vr, rl,
):
    x, z, v = lax.axis_index("data"), lax.axis_index("hid"), lax.axis_index("vocab")
    rows, depth = h_ref.shape
    half, quarter = depth // 2, rows // 4
    tiles = tiles_of(n_cols // LANES)
    n_tiles = len(tiles)
    n_whole = sum(width == TILE for _, width in tiles)
    plan = chunks_of(n_cols // LANES)
    n_chunks = len(plan)
    ends = [[j for j, (first, *_) in enumerate(plan) if first * LANES < sum(tiles[t])][-1] for t in range(n_whole - 1, n_tiles)]
    first_end = ends[0] - 1

    side = z // 2
    outer_far, inner_far, near = 3 - 3 * side, 2 - side, 1 - z + 4 * side
    is_outer = jnp.where(z == side * 3, 1, 0)
    z_two, z_one = lax.rem(z + 2, 4), near
    v_two, v_one = lax.rem(v + 2, 4), v + 1 - 2 * lax.rem(v, 2)
    sources = (near, inner_far, outer_far)

    def cols_of(j):
        first, size, _, _ = plan[j]
        return first * LANES, size * LANES

    def w_rows(source, part, j=None):
        at, n = (0, half) if j is None else (plan[j][2] * (half // 2), plan[j][3] * (half // 2))
        return pl.ds(pl.multiple_of(source * depth + part * half + at, half // 2), n)

    def w_place(j, source, part):
        start, n = cols_of(j)
        return wbuf.at[w_rows(source, part, j), pl.ds(start, n)]

    def h_place(q, block=None):
        at = pl.ds(pl.multiple_of(q * quarter, quarter), quarter)
        if block is None:
            return hbuf.at[at]
        return hbuf.at[at, pl.ds(pl.multiple_of(block * depth, depth), depth)]

    def remote(src, dst, send, recv, **to):
        return pltpu.make_async_remote_copy(
            src_ref=src, dst_ref=dst, send_sem=send, recv_sem=recv, device_id=to, device_id_type=MESH
        )

    def w_source(j, part, dest):
        start, n = cols_of(j)
        return w_ref.at[w_rows(0, part, j), pl.ds(pl.multiple_of(dest * n_cols + start, LANES), n)]

    def direct(j, k, dest, slot):
        return remote(w_source(j, x, dest), w_place(j, z, x), ws.at[k], wr.at[j, slot], hid=dest)

    def send_near(j):
        return direct(j, 0, near, 0)

    odd = lax.rem(v, 2)
    far_first = outer_far + odd * (inner_far - outer_far)
    far_second = inner_far + odd * (outer_far - inner_far)

    def send_far(j, i):
        return direct(j, 1 + i, (far_first, far_second)[i], 1 + is_outer)

    def send_twin(i):
        dest = (far_first, far_second)[i]
        return remote(w_source(n_chunks - 1, 1 - x, dest), w_place(n_chunks - 1, z, 1 - x), ts.at[i], tr, hid=dest)

    def twin_landed():
        place = w_place(n_chunks - 1, inner_far, 1 - x)
        remote(place, place, ts.at[0], tr, hid=inner_far).wait_recv()

    def landed(j, k):
        place = w_place(j, sources[k], x)
        remote(place, place, ws.at[k], wr.at[j, k], hid=sources[k]).wait_recv()

    def forward(j, k):
        place = w_place(j, sources[k], x)
        send = 3 if k == 1 and j == n_chunks - 2 else k
        return remote(place, place, xs.at[send], xr.at[cross(j, k)], data=1 - x)

    def cross(j, k):
        if j < first_end:
            return j
        return first_end if k != 1 else 1 + j

    def cross_wait(slot, count, start, stop):
        place = wbuf.at[pl.ds(0, count), pl.ds(start, stop - start)]
        remote(place, place, xs.at[0], xr.at[slot], data=1 - x).wait_recv()

    def forwarded(j):
        place = w_place(j, inner_far, 1 - x)
        remote(place, place, xs.at[1], xr.at[cross(j, 1)], data=1 - x).wait_recv()

    def own(j):
        start, n = cols_of(j)
        return pltpu.make_async_copy(
            w_ref.at[:, pl.ds(pl.multiple_of(z * n_cols + start, LANES), n)],
            wbuf.at[pl.ds(pl.multiple_of(z * depth, depth), depth), pl.ds(start, n)],
            wl,
        )

    h_mine = h_ref.at[pl.ds(pl.multiple_of(v * quarter, quarter), quarter)]
    h_own = pltpu.make_async_copy(h_mine, h_place(v, z), hl)
    h_two = remote(h_mine, h_place(v, z), hs.at[0], hr.at[0], hid=z_two)
    h_one = remote(h_mine, h_place(v, z), hs.at[1], hr.at[1], hid=z_one)
    h_relay = remote(h_place(v, z_two), h_place(v, z_two), hs.at[2], hr.at[2], hid=z_one)
    h_chip = remote(h_place(v), h_place(v), hs.at[3], hr.at[3], vocab=v_two)
    h_core = remote(h_place(v), h_place(v), hs.at[4], hr.at[4], vocab=v_one)
    h_both = remote(h_place(v_two), h_place(v_two), hs.at[5], hr.at[5], vocab=v_one)

    def arrived(place, i, **frm):
        remote(place, place, hs.at[i], hr.at[i], **frm).wait_recv()

    barrier = pltpu.get_barrier_semaphore()
    peers = [{"hid": lax.rem(z + d, 4)} for d in (1, 2, 3)]
    peers += [{"data": 1 - x}] + [{"vocab": lax.rem(v + d, 4)} for d in (1, 2, 3)]
    for peer in peers:
        pl.semaphore_signal(barrier, inc=1, device_id=peer, device_id_type=MESH)
    row_copies = [
        pltpu.make_async_copy(temp_hbm, temp_ref, rl.at[0]),
        pltpu.make_async_copy(tgt_hbm, tgt_ref, rl.at[1]),
    ]
    for copy in (h_own, *row_copies):
        copy.start()
    for j in range(n_chunks):
        if plan[j][2] == 0:
            own(j).start()
    with jax.named_scope("bar"):
        pl.semaphore_wait(barrier, len(peers))

    h_two.start()
    h_one.start()
    send_near(0).start()
    send_far(0, 0).start()

    def ones_below(ref, width):
        k = lax.broadcasted_iota(jnp.int32, (width, width), 0)
        c = lax.broadcasted_iota(jnp.int32, (width, width), 1)
        block = jnp.where(k <= c, 1.0, 0.0).astype(BF16)
        for i in range(3):
            ref[pl.ds(i * width, width), :] = block

    ones_below(tri, TILE)
    ones_below(tri_last, LANES)
    base = (v * 4 + z) * n_cols
    for copy in row_copies:
        copy.wait()
    back[0:1, :] = temp_ref[...]
    back[1:2, :] = (tgt_ref[...] - base).astype(F32)
    cols8 = back[...].T
    temp_col[...] = jnp.broadcast_to(cols8[:, 0:1], temp_col.shape)
    rel_col[...] = jnp.broadcast_to(cols8[:, 1:2], rel_col.shape).astype(jnp.int32)
    slot = lax.broadcasted_iota(jnp.int32, stats.shape, 1)
    stats[...] = jnp.where(slot < SLOTS, LOWEST, 0.0)
    t_all[...] = jnp.zeros(t_all.shape, F32)

    with jax.named_scope("h0"):
        arrived(h_place(v, z_two), 0, hid=z_two)
    h_relay.start()
    send_far(0, 1).start()
    for j in range(1, n_chunks):
        send_near(j).start()
        send_far(j, 0).start()
        send_far(j, 1).start()

    @pl.when(is_outer == 0)
    def _():
        send_twin(0).start()
        send_twin(1).start()


    part, few = min(rows, 512), min(rows, 128)

    def logits_and_sums(product, sums):
        @pl.loop(0, rows // part)
        def _(i):
            if product is not None:
                _, new_start, new_width = product
                at = pl.ds(pl.multiple_of(i * part, part), part)
                new = jnp.dot(
                    hbuf[at, :], wbuf[:, pl.ds(new_start, new_width)], preferred_element_type=F32
                )
            for k in range(0, part, few) if sums is not None else ():
                prefix(pl.ds(pl.multiple_of(i * part + k, few), few), *sums)
            if product is not None:
                zbuf[at, 0:new_width] = new

    def prefix(at, t, start, width):
        pieces = width // LANES
        logits = zbuf[at, 0:width] * jnp.concatenate([temp_col[at, :]] * pieces, axis=1)
        lane = lax.broadcasted_iota(jnp.int32, (few, LANES), 1)
        top = jnp.max(logits, axis=1, keepdims=True)
        e = jnp.exp(logits - top)
        total = jnp.sum(e, axis=1, keepdims=True)
        stats[at, :] = jnp.where(lane == t, top, jnp.where(lane == SLOTS + t, total, stats[at, :]))
        table = tri if width == TILE else tri_last
        run = jnp.dot(jnp.concatenate(split3(e), axis=1), table[...], preferred_element_type=F32)
        c_ref[at, pl.ds(start, width)] = run
        rel = rel_col[at, :] - start
        hit = t_all[at, :]
        for p in range(pieces):
            hit += jnp.where(lane == rel - p * LANES, run[:, p * LANES : (p + 1) * LANES], 0.0)
        t_all[at, :] = hit

    def whole(t):
        return t, pl.multiple_of(t * TILE, TILE), TILE

    def compute(j):
        first, size = (n // 2 for n in plan[j][:2])
        stop = first + size
        if first == 0:
            logits_and_sums(whole(0), None)
            first = 1
        if first < stop:

            @pl.loop(first, stop)
            def _(t):
                logits_and_sums(whole(t), whole(t - 1))

        if j == first_end - 1:
            logits_and_sums(None, whole(stop - 1))

    def block_dot(at, block, start, width):
        lanes = pl.ds(pl.multiple_of(block * depth, depth), depth)
        return jnp.dot(hbuf[at, lanes], wbuf[lanes, start : start + width], preferred_element_type=F32)

    def begin_end(i):
        start, width = tiles[n_whole - 1 + i]

        @pl.loop(0, rows // part)
        def _(k):
            at = pl.ds(pl.multiple_of(k * part, part), part)
            c_ref[at, start : start + width] = (
                block_dot(at, z, start, width)
                + block_dot(at, near, start, width)
                + block_dot(at, outer_far, start, width)
            )

    def finish_end(i):
        t = n_whole - 1 + i
        start, width = tiles[t]
        every = slice(0, rows)
        zbuf[:, 0:width] = c_ref[:, start : start + width] + block_dot(every, inner_far, start, width)
        logits_and_sums(None, (t, start, width))

    def fold(g0, g1):
        @pl.loop(0, rows // few)
        def _(i):
            at = pl.ds(pl.multiple_of(i * few, few), few)
            lane = lax.broadcasted_iota(jnp.int32, (few, LANES), 1)
            group = (lane >= g0) & (lane < g1)
            m = stats[at, :]
            s = pltpu.roll(m, LANES - SLOTS, 1)
            top = jnp.max(jnp.where(group, m, LOWEST), axis=1, keepdims=True)
            shrink = jnp.where(group, jnp.exp(m - top), 0.0)
            parts = jnp.where(group, s, 0.0) * shrink
            before = prefix_before(parts)
            for t in range(g0, g1):
                span = slice(t * TILE, (t + 1) * TILE)
                c_ref[at, span] = c_ref[at, span] * shrink[:, t : t + 1] + before[:, t : t + 1]
            rel = rel_col[at, :]
            holds = (rel >= lane * TILE) & (rel < (lane + 1) * TILE)
            old = t_all[at, :]
            moved = jnp.sum(old, axis=1, keepdims=True) * shrink + before
            inside = (rel >= g0 * TILE) & (rel < g1 * TILE)
            t_all[at, :] = jnp.where(inside, jnp.where(holds, moved, 0.0), old)
            total = jnp.sum(parts, axis=1, keepdims=True)
            sums = jnp.where(lane == SLOTS + g1 - 1, total, 0.0)
            of_sums = (lane >= SLOTS + g0) & (lane < SLOTS + g1)
            stats[at, :] = jnp.where(group, top, jnp.where(of_sums, sums, m))

    def close(i):
        first = ends[i - 1] + 1 if i else first_end
        with jax.named_scope(f"xe{i}"):
            for j in range(first, ends[i] + 1):
                if j < n_chunks - 1:
                    forwarded(j)
                else:
                    twin_landed()
        with jax.named_scope(f"ce{i}"):
            finish_end(i)

    def prefix_before(parts):
        k = lax.broadcasted_iota(jnp.int32, (LANES, LANES), 0)
        c = lax.broadcasted_iota(jnp.int32, (LANES, LANES), 1)
        strict = jnp.where(k < c, 1.0, 0.0).astype(BF16)
        return sum(jnp.dot(p, strict, preferred_element_type=F32) for p in split3(parts))

    def complete(j):
        start, n = cols_of(j)
        cross_wait(j, 3 * half, start, start + n)

    def own_complete():
        place = wbuf.at[pl.ds(pl.multiple_of(z * depth, depth), depth)]
        pltpu.make_async_copy(place, place, wl).wait()

    order = service_order(plan, n_cols // LANES)
    folds = {j: (g0, g1) for j, g0, g1 in folds_of(plan, first_end)}
    tail = range(first_end, n_chunks)
    known = max(order.index((k, j)) for k in (0, 2) for j in tail)
    early = min(j for j in range(max(0, first_end - 5), n_chunks - 1) if order.index((1, j + 1)) > known)
    assert early < first_end
    m = len(ends) - 1
    closes = {ends[i + 1]: i for i in range(m - 2)} | {n_chunks - 2: m - 2, n_chunks - 1: m - 1}

    for what, j in order:
        if what == "h line":
            with jax.named_scope("hline"):
                arrived(h_place(v, z_one), 1, hid=z_one)
                arrived(h_place(v, lax.rem(z_one + 2, 4)), 2, hid=z_one)
                h_own.wait()
            h_chip.start()
            h_core.start()
        elif what == "h chip":
            with jax.named_scope("hchip"):
                arrived(h_place(v_two), 3, vocab=v_two)
            h_both.start()
        else:
            with jax.named_scope(f"w{what}_{j}"):
                landed(j, what)
            if (what, j) != (1, n_chunks - 1):
                forward(j, what).start()
            if what != 1:
                continue
            if j == 1:
                with jax.named_scope("hcore"):
                    arrived(h_place(v_one), 4, vocab=v_one)
                    arrived(h_place(lax.rem(v_one + 2, 4)), 5, vocab=v_one)
                    own_complete()
            if 0 < j <= first_end:
                with jax.named_scope(f"x{j - 1}"):
                    complete(j - 1)
                with jax.named_scope(f"c{j - 1}"):
                    compute(j - 1)
                if j - 1 in folds:
                    with jax.named_scope(f"f{j - 1}"):
                        fold(*folds[j - 1])
            if j - 1 == early:
                with jax.named_scope("begin"):
                    cross_wait(first_end, 2 * half, cols_of(first_end)[0], n_cols)
                    for i in range(len(ends)):
                        begin_end(i)
            if j in closes:
                close(closes[j])
    close(m)

    lane = lax.broadcasted_iota(jnp.int32, (rows, LANES), 1)
    at_tgt = jnp.sum(t_all[...], axis=1, keepdims=True)
    turned = jnp.where(lane == 2 * SLOTS, at_tgt, stats[...]).T
    m, at_tgt = turned[0:SLOTS, :], turned[2 * SLOTS : 2 * SLOTS + 1, :]
    top = jnp.max(m, axis=0, keepdims=True)
    shrink = jnp.exp(m - top)
    parts = turned[SLOTS : 2 * SLOTS, :] * shrink
    t = lax.broadcasted_iota(jnp.int32, (SLOTS, rows), 0)
    start = jnp.where(t < n_whole, t * TILE, n_whole * (TILE - LANES) + t * LANES)
    stop = start + jnp.where(t < n_whole, TILE, LANES)
    rel = tgt_ref[...] - base
    known = rel < n_cols
    holds = (rel >= start) & (rel < stop) & known
    ahead = (stop <= rel) & known
    found = jnp.where(holds, at_tgt * shrink, jnp.where(ahead, parts, 0.0))
    zmsg[z, 0:1, :] = top
    zmsg[z, 1:2, :] = jnp.sum(parts, axis=0, keepdims=True)
    zmsg[z, 2:3, :] = jnp.sum(found, axis=0, keepdims=True)

    for k in range(3):
        mine = wbuf.at[w_rows(sources[k], x)]
        remote(mine, mine, ws.at[k], wr.at[0, k], hid=near).wait_send()
        if k == 1:
            mine = wbuf.at[w_rows(sources[k], x), pl.ds(0, n_cols - LANES)]
        remote(mine, mine, xs.at[k], xr.at[0], data=1 - x).wait_send()
    forward(n_chunks - 2, 1).wait_send()

    @pl.when(is_outer == 0)
    def _():
        send_twin(0).wait_send()
        send_twin(1).wait_send()

    for copy in (h_two, h_one, h_relay, h_chip, h_core, h_both):
        copy.wait_send()

    def z_send(i):
        slot = (0, 1 + is_outer, 1 + is_outer)[i]
        return remote(zmsg.at[z], zmsg.at[z], zs.at[i], zr.at[slot], hid=(near, inner_far, outer_far)[i])

    def v_send(d):
        to = lax.rem(v + d, 4)
        return remote(vmsg.at[v], vmsg.at[v], vs.at[d - 1], vr.at[d - 1], vocab=to)

    for i in (2, 1, 0):
        z_send(i).start()
    k = lax.broadcasted_iota(jnp.int32, (SLOTS, SLOTS), 0)
    c = lax.broadcasted_iota(jnp.int32, (SLOTS, SLOTS), 1)
    strict = jnp.where(c < k, 1.0, 0.0).astype(BF16)
    before = sum(jnp.dot(strict, p, preferred_element_type=F32) for p in split3(parts))
    rest = jnp.zeros((LANES - 2 * SLOTS, rows), F32)
    coef_ref[...] = jnp.concatenate([shrink, before, rest], axis=0).T
    for i, frm in enumerate(sources):
        with jax.named_scope(f"z{i}"):
            remote(zmsg.at[frm], zmsg.at[frm], zs.at[i], zr.at[i], hid=frm).wait_recv()

    ids = tgt_ref[...]
    maxes = [zmsg[h, 0:1, :] for h in range(4)]
    v_max = functools.reduce(jnp.maximum, maxes)
    v_sum = jnp.zeros((1, rows), F32)
    v_tgt = jnp.zeros((1, rows), F32)
    mine_before = jnp.zeros((1, rows), F32)
    for h in range(4):
        mine_before = jnp.where(h == z, v_sum, mine_before)
        f = jnp.exp(maxes[h] - v_max)
        low = (v * 4 + h) * n_cols
        inside = (ids >= low) & (ids < low + n_cols)
        v_tgt += jnp.where(inside, zmsg[h, 2:3, :] * f + v_sum, 0.0)
        v_sum += zmsg[h, 1:2, :] * f
    vmsg[v, 0:1, :] = v_max
    vmsg[v, 1:2, :] = v_sum
    vmsg[v, 2:3, :] = v_tgt

    for i in range(3):
        z_send(i).wait_send()
    for d in (2, 1, 3):
        v_send(d).start()
    for d in (1, 2, 3):
        frm = lax.rem(v + 4 - d, 4)
        with jax.named_scope(f"v{d}"):
            remote(vmsg.at[frm], vmsg.at[frm], vs.at[d - 1], vr.at[d - 1], vocab=frm).wait_recv()

    maxes = [vmsg[u, 0:1, :] for u in range(4)]
    g_max = functools.reduce(jnp.maximum, maxes)
    g_sum = jnp.zeros((1, rows), F32)
    g_tgt = jnp.zeros((1, rows), F32)
    g_before = jnp.zeros((1, rows), F32)
    for u in range(4):
        f = jnp.exp(maxes[u] - g_max)
        g_before = jnp.where(u == v, g_sum + mine_before * f, g_before)
        low = u * 4 * n_cols
        inside = (ids >= low) & (ids < low + 4 * n_cols)
        g_tgt += jnp.where(inside, vmsg[u, 2:3, :] * f + g_sum, 0.0)
        g_sum += vmsg[u, 1:2, :] * f
    tgt_out_ref[...] = g_tgt / g_sum
    factor_ref[0:1, :] = jnp.exp(zmsg[z, 0:1, :] - g_max) / g_sum
    factor_ref[1:2, :] = g_before / g_sum
    for d in (1, 2, 3):
        v_send(d).wait_send()


def finish_kernel(tiles, lanes, c_ref, coef_ref, factor_ref, tgt_ref, out_ref, tgt_out_ref, buf, factor_col, sems):
    slots, n, n_cols = buf.shape
    steps = c_ref.shape[0] // n

    def put(i):
        slot = lax.rem(i, slots)
        at = pl.ds(pl.multiple_of(i * n, n), n)
        return pltpu.make_async_copy(buf.at[slot], out_ref.at[at], sems.at[slot])

    @pl.loop(0, steps)
    def _(i):
        slot = lax.rem(i, slots)

        @pl.when(i >= slots)
        def _():
            put(i - slots).wait()

        at = pl.ds(pl.multiple_of(i * n, n), n)
        turn = max(n, LANES)

        @pl.when(lax.rem(i, turn // n) == 0)
        def _():
            some = pl.ds(pl.multiple_of(i // (turn // n) * turn, turn), turn)
            factor_col[some, :] = factor_ref[:, some].T

        lane = lax.broadcasted_iota(jnp.int32, (n, LANES), 1)
        coef = coef_ref[at, :] * factor_col[at, 0:1] + jnp.where(lane < SLOTS, 0.0, factor_col[at, 1:2])
        for (start, width), k in zip(tiles, lanes):
            span = slice(start, start + width)
            buf[slot, :, span] = c_ref[at, span] * coef[:, k : k + 1] + coef[:, SLOTS + k : SLOTS + k + 1]
        put(i).start()

    tgt_out_ref[...] = tgt_ref[...]
    for i in range(max(0, steps - slots), steps):
        put(i).wait()


def solution(mesh):
    n_hid, n_voc = mesh.shape["hid"], mesh.shape["vocab"]
    assert n_hid == 4 and n_voc == 4 and mesh.shape["data"] == 2

    def local_step(h_blk, w_blk, temp_blk, tgt_blk):
        rows, depth = h_blk.shape
        n_cols = w_blk.shape[1] // n_hid
        assert n_cols % LANES == 0
        tiles = tiles_of(n_cols // LANES)
        n_tiles = len(tiles)
        assert n_tiles <= SLOTS
        plan = chunks_of(n_cols // LANES)
        n_chunks = len(plan)
        vmem = pl.BlockSpec(memory_space=pltpu.VMEM)
        hbm = pl.BlockSpec(memory_space=pltpu.HBM)
        dma = pltpu.SemaphoreType.DMA
        table = pltpu.VMEM((rows, LANES), F32)
        c, coef, factor, tgt = pl.pallas_call(
            functools.partial(prefix_kernel, n_cols),
            out_shape=(
                pltpu.VMEM((rows, n_cols), F32),
                pltpu.VMEM((rows, LANES), F32),
                pltpu.VMEM((8, rows), F32),
                pltpu.VMEM((1, rows), F32),
            ),
            in_specs=[hbm] * 4,
            out_specs=[vmem] * 4,
            scratch_shapes=[
                pltpu.VMEM((4 * depth, n_cols), BF16),
                pltpu.VMEM((rows, 4 * depth), BF16),
                pltpu.VMEM((rows, TILE), F32),
                pltpu.VMEM((3 * TILE, TILE), BF16),
                pltpu.VMEM((3 * LANES, LANES), BF16),
                table,
                table,
                table,
                pltpu.VMEM((rows, LANES), jnp.int32),
                pltpu.VMEM((1, rows), F32),
                pltpu.VMEM((1, rows), jnp.int32),
                pltpu.VMEM((4, 3, rows), F32),
                pltpu.VMEM((4, 3, rows), F32),
                pltpu.VMEM((8, rows), F32),
                dma((3,)),
                dma((n_chunks, 3)),
                dma((4,)),
                dma((n_chunks,)),
                dma((2,)),
                dma,
                dma,
                dma,
                dma((6,)),
                dma((6,)),
                dma((3,)),
                dma((3,)),
                dma((3,)),
                dma((3,)),
                dma((2,)),
            ],
            compiler_params=pltpu.CompilerParams(
                collective_id=0, has_side_effects=True, vmem_limit_bytes=37 << 20
            ),
            name="prefix",
        )(h_blk, w_blk, temp_blk.reshape(1, rows), tgt_blk.reshape(1, rows))
        n = min(rows, 64)
        lanes = list(range(n_tiles))
        last_whole = sum(width == TILE for _, width in tiles) - 1
        first_end = [first for first, *_ in plan].index(2 * last_whole)
        for _, g0, g1 in folds_of(plan, first_end):
            lanes[g0:g1] = [g0] * (g1 - g0)
        cdf, cdf_tgt = pl.pallas_call(
            functools.partial(finish_kernel, tiles, lanes),
            out_shape=(
                jax.ShapeDtypeStruct((rows, n_cols), F32),
                jax.ShapeDtypeStruct((1, rows), F32),
            ),
            in_specs=[vmem] * 4,
            out_specs=[hbm, vmem],
            scratch_shapes=[pltpu.VMEM((4, n, n_cols), F32), pltpu.VMEM((rows, 8), F32), dma((4,))],
            compiler_params=pltpu.CompilerParams(vmem_limit_bytes=9 << 20),
            name="finish",
        )(c, coef, factor, tgt)
        return cdf, cdf_tgt.reshape(rows)

    return jax.shard_map(
        local_step,
        mesh=mesh,
        in_specs=(P("data", "hid"), P("hid", "vocab"), P("data"), P("data")),
        out_specs=(P("data", ("vocab", "hid")), P("data")),
        check_vma=False,
    )
```

```python
import functools

import jax
import jax.numpy as jnp
from jax import lax
from jax.experimental import pallas as pl
from jax.experimental.pallas import tpu as pltpu
from jax.sharding import PartitionSpec as P

MESH = pl.DeviceIdType.MESH
F32 = jnp.float32
BF16 = jnp.bfloat16
TILE = 256
LANES = 128
SLOTS = 32
LOWEST = float(jnp.finfo(jnp.float32).min)


def tiles_of(blocks):
    whole = (blocks - 3) // 2
    tiles = [(t * TILE, TILE) for t in range(whole)]
    return tiles + [(b * LANES, LANES) for b in range(2 * whole, blocks)]


def chunks_of(blocks):
    whole = (blocks - 3) // 2
    sizes, left = [], 2 * whole - 2
    for size in (2, 2, 2, 2, 4, 4):
        if left > size:
            sizes.append(size)
            left -= size
    while left > 0:
        sizes.append(min(6, left))
        left -= sizes[-1]
    plan, at = [], 0
    for size in reversed(sizes):
        plan.append((at, size, 0, 2))
        at += size
    plan += [(b, 1, 0, 2) for b in range(at, blocks - 2)]
    return plan + [(b, 1, r, 1) for b in (blocks - 2, blocks - 1) for r in (0, 1)]


def service_order(plan, blocks):
    events = [(0.15 * blocks, "h line", 0), (0.28 * blocks, "h chip", 0)]
    for j, (first, size, _, _) in enumerate(plan):
        end = first + size
        events.append((first + size / 3 + 2, 0, j))
        events.append((end + 2, 2, j))
        events.append((min(1.86 * end, 0.68 * blocks + 0.6 * end) + 2, 1, j))
    events.sort(key=lambda e: e[0])
    order = [e[1:] for e in events]
    for j in range(len(plan)):
        at = max(order.index((k, j)) for k in (0, 1, 2))
        order.remove((1, j))
        order.insert(at, (1, j))
    return order


def folds_of(plan, first_end):
    folds, at = [], 0
    for j in (first_end // 3, 3 * first_end // 5):
        stop = sum(plan[j][:2]) // 2 - 1
        if j < first_end and stop > at:
            folds.append((j, at, stop))
            at = stop
    return folds


def split3(e):
    hi = e.astype(BF16)
    rest = e - hi.astype(F32)
    mid = rest.astype(BF16)
    low = (rest - mid.astype(F32)).astype(BF16)
    return hi, mid, low


def prefix_kernel(
    n_cols, h_ref, w_ref, temp_hbm, tgt_hbm,
    c_ref, coef_ref, factor_ref, tgt_out_ref,
    wbuf, hbuf, zbuf, tri, tri_last, stats, t_all, temp_col, rel_col, temp_ref, tgt_ref, zmsg, vmsg, back,
    ws, wr, xs, xr, ts, tr, wl, hl, hs, hr, zs, zr, vs, vr, rl,
):
    x, z, v = lax.axis_index("data"), lax.axis_index("hid"), lax.axis_index("vocab")
    rows, depth = h_ref.shape
    half, quarter = depth // 2, rows // 4
    tiles = tiles_of(n_cols // LANES)
    n_tiles = len(tiles)
    n_whole = sum(width == TILE for _, width in tiles)
    plan = chunks_of(n_cols // LANES)
    n_chunks = len(plan)
    ends = [[j for j, (first, *_) in enumerate(plan) if first * LANES < sum(tiles[t])][-1] for t in range(n_whole - 1, n_tiles)]
    first_end = ends[0] - 1

    side = z // 2
    outer_far, inner_far, near = 3 - 3 * side, 2 - side, 1 - z + 4 * side
    is_outer = jnp.where(z == side * 3, 1, 0)
    z_two, z_one = lax.rem(z + 2, 4), near
    v_two, v_one = lax.rem(v + 2, 4), v + 1 - 2 * lax.rem(v, 2)
    sources = (near, inner_far, outer_far)

    def cols_of(j):
        first, size, _, _ = plan[j]
        return first * LANES, size * LANES

    def w_rows(source, part, j=None):
        at, n = (0, half) if j is None else (plan[j][2] * (half // 2), plan[j][3] * (half // 2))
        return pl.ds(pl.multiple_of(source * depth + part * half + at, half // 2), n)

    def w_place(j, source, part):
        start, n = cols_of(j)
        return wbuf.at[w_rows(source, part, j), pl.ds(start, n)]

    def h_place(q, block=None):
        at = pl.ds(pl.multiple_of(q * quarter, quarter), quarter)
        if block is None:
            return hbuf.at[at]
        return hbuf.at[at, pl.ds(pl.multiple_of(block * depth, depth), depth)]

    def remote(src, dst, send, recv, **to):
        return pltpu.make_async_remote_copy(
            src_ref=src, dst_ref=dst, send_sem=send, recv_sem=recv, device_id=to, device_id_type=MESH
        )

    def w_source(j, part, dest):
        start, n = cols_of(j)
        return w_ref.at[w_rows(0, part, j), pl.ds(pl.multiple_of(dest * n_cols + start, LANES), n)]

    def direct(j, k, dest, slot):
        return remote(w_source(j, x, dest), w_place(j, z, x), ws.at[k], wr.at[j, slot], hid=dest)

    def send_near(j):
        return direct(j, 0, near, 0)

    odd = lax.rem(v, 2)
    far_first = outer_far + odd * (inner_far - outer_far)
    far_second = inner_far + odd * (outer_far - inner_far)

    def send_far(j, i):
        return direct(j, 1 + i, (far_first, far_second)[i], 1 + is_outer)

    def send_twin(i):
        dest = (far_first, far_second)[i]
        return remote(w_source(n_chunks - 1, 1 - x, dest), w_place(n_chunks - 1, z, 1 - x), ts.at[i], tr, hid=dest)

    def twin_landed():
        place = w_place(n_chunks - 1, inner_far, 1 - x)
        remote(place, place, ts.at[0], tr, hid=inner_far).wait_recv()

    def landed(j, k):
        place = w_place(j, sources[k], x)
        remote(place, place, ws.at[k], wr.at[j, k], hid=sources[k]).wait_recv()

    def forward(j, k):
        place = w_place(j, sources[k], x)
        send = 3 if k == 1 and j == n_chunks - 2 else k
        return remote(place, place, xs.at[send], xr.at[cross(j, k)], data=1 - x)

    def cross(j, k):
        if j < first_end:
            return j
        return first_end if k != 1 else 1 + j

    def cross_wait(slot, count, start, stop):
        place = wbuf.at[pl.ds(0, count), pl.ds(start, stop - start)]
        remote(place, place, xs.at[0], xr.at[slot], data=1 - x).wait_recv()

    def forwarded(j):
        place = w_place(j, inner_far, 1 - x)
        remote(place, place, xs.at[1], xr.at[cross(j, 1)], data=1 - x).wait_recv()

    def own(j):
        start, n = cols_of(j)
        return pltpu.make_async_copy(
            w_ref.at[:, pl.ds(pl.multiple_of(z * n_cols + start, LANES), n)],
            wbuf.at[pl.ds(pl.multiple_of(z * depth, depth), depth), pl.ds(start, n)],
            wl,
        )

    h_mine = h_ref.at[pl.ds(pl.multiple_of(v * quarter, quarter), quarter)]
    h_own = pltpu.make_async_copy(h_mine, h_place(v, z), hl)
    h_two = remote(h_mine, h_place(v, z), hs.at[0], hr.at[0], hid=z_two)
    h_one = remote(h_mine, h_place(v, z), hs.at[1], hr.at[1], hid=z_one)
    h_relay = remote(h_place(v, z_two), h_place(v, z_two), hs.at[2], hr.at[2], hid=z_one)
    h_chip = remote(h_place(v), h_place(v), hs.at[3], hr.at[3], vocab=v_two)
    h_core = remote(h_place(v), h_place(v), hs.at[4], hr.at[4], vocab=v_one)
    h_both = remote(h_place(v_two), h_place(v_two), hs.at[5], hr.at[5], vocab=v_one)

    def arrived(place, i, **frm):
        remote(place, place, hs.at[i], hr.at[i], **frm).wait_recv()

    barrier = pltpu.get_barrier_semaphore()
    peers = [{"hid": lax.rem(z + d, 4)} for d in (1, 2, 3)]
    peers += [{"data": 1 - x}] + [{"vocab": lax.rem(v + d, 4)} for d in (1, 2, 3)]
    for peer in peers:
        pl.semaphore_signal(barrier, inc=1, device_id=peer, device_id_type=MESH)
    row_copies = [
        pltpu.make_async_copy(temp_hbm, temp_ref, rl.at[0]),
        pltpu.make_async_copy(tgt_hbm, tgt_ref, rl.at[1]),
    ]
    for copy in (h_own, *row_copies):
        copy.start()
    for j in range(n_chunks):
        if plan[j][2] == 0:
            own(j).start()
    with jax.named_scope("bar"):
        pl.semaphore_wait(barrier, len(peers))

    h_two.start()
    h_one.start()
    send_near(0).start()
    send_far(0, 0).start()

    def ones_below(ref, width):
        k = lax.broadcasted_iota(jnp.int32, (width, width), 0)
        c = lax.broadcasted_iota(jnp.int32, (width, width), 1)
        block = jnp.where(k <= c, 1.0, 0.0).astype(BF16)
        for i in range(3):
            ref[pl.ds(i * width, width), :] = block

    ones_below(tri, TILE)
    ones_below(tri_last, LANES)
    base = (v * 4 + z) * n_cols
    for copy in row_copies:
        copy.wait()
    back[0:1, :] = temp_ref[...]
    back[1:2, :] = (tgt_ref[...] - base).astype(F32)
    cols8 = back[...].T
    temp_col[...] = jnp.broadcast_to(cols8[:, 0:1], temp_col.shape)
    rel_col[...] = jnp.broadcast_to(cols8[:, 1:2], rel_col.shape).astype(jnp.int32)
    slot = lax.broadcasted_iota(jnp.int32, stats.shape, 1)
    stats[...] = jnp.where(slot < SLOTS, LOWEST, 0.0)
    t_all[...] = jnp.zeros(t_all.shape, F32)

    with jax.named_scope("h0"):
        arrived(h_place(v, z_two), 0, hid=z_two)
    h_relay.start()
    send_far(0, 1).start()
    for j in range(1, n_chunks):
        send_near(j).start()
        send_far(j, 0).start()
        send_far(j, 1).start()

    @pl.when(is_outer == 0)
    def _():
        send_twin(0).start()
        send_twin(1).start()


    part, few = min(rows, 512), min(rows, 128)

    def logits_and_sums(product, sums):
        @pl.loop(0, rows // part)
        def _(i):
            if product is not None:
                _, new_start, new_width = product
                at = pl.ds(pl.multiple_of(i * part, part), part)
                new = jnp.dot(
                    hbuf[at, :], wbuf[:, pl.ds(new_start, new_width)], preferred_element_type=F32
                )
            for k in range(0, part, few) if sums is not None else ():
                prefix(pl.ds(pl.multiple_of(i * part + k, few), few), *sums)
            if product is not None:
                zbuf[at, 0:new_width] = new

    def prefix(at, t, start, width):
        pieces = width // LANES
        logits = zbuf[at, 0:width] * jnp.concatenate([temp_col[at, :]] * pieces, axis=1)
        lane = lax.broadcasted_iota(jnp.int32, (few, LANES), 1)
        top = jnp.max(logits, axis=1, keepdims=True)
        e = jnp.exp(logits - top)
        total = jnp.sum(e, axis=1, keepdims=True)
        stats[at, :] = jnp.where(lane == t, top, jnp.where(lane == SLOTS + t, total, stats[at, :]))
        table = tri if width == TILE else tri_last
        run = jnp.dot(jnp.concatenate(split3(e), axis=1), table[...], preferred_element_type=F32)
        c_ref[at, pl.ds(start, width)] = run
        rel = rel_col[at, :] - start
        hit = t_all[at, :]
        for p in range(pieces):
            hit += jnp.where(lane == rel - p * LANES, run[:, p * LANES : (p + 1) * LANES], 0.0)
        t_all[at, :] = hit

    def whole(t):
        return t, pl.multiple_of(t * TILE, TILE), TILE

    def compute(j):
        first, size = (n // 2 for n in plan[j][:2])
        stop = first + size
        if first == 0:
            logits_and_sums(whole(0), None)
            first = 1
        if first < stop:

            @pl.loop(first, stop)
            def _(t):
                logits_and_sums(whole(t), whole(t - 1))

        if j == first_end - 1:
            logits_and_sums(None, whole(stop - 1))

    def block_dot(at, block, start, width):
        lanes = pl.ds(pl.multiple_of(block * depth, depth), depth)
        return jnp.dot(hbuf[at, lanes], wbuf[lanes, start : start + width], preferred_element_type=F32)

    def begin_end(i):
        start, width = tiles[n_whole - 1 + i]

        @pl.loop(0, rows // part)
        def _(k):
            at = pl.ds(pl.multiple_of(k * part, part), part)
            c_ref[at, start : start + width] = (
                block_dot(at, z, start, width)
                + block_dot(at, near, start, width)
                + block_dot(at, outer_far, start, width)
            )

    def finish_end(i):
        t = n_whole - 1 + i
        start, width = tiles[t]
        every = slice(0, rows)
        zbuf[:, 0:width] = c_ref[:, start : start + width] + block_dot(every, inner_far, start, width)
        logits_and_sums(None, (t, start, width))

    def fold(g0, g1):
        @pl.loop(0, rows // few)
        def _(i):
            at = pl.ds(pl.multiple_of(i * few, few), few)
            lane = lax.broadcasted_iota(jnp.int32, (few, LANES), 1)
            group = (lane >= g0) & (lane < g1)
            m = stats[at, :]
            s = pltpu.roll(m, LANES - SLOTS, 1)
            top = jnp.max(jnp.where(group, m, LOWEST), axis=1, keepdims=True)
            shrink = jnp.where(group, jnp.exp(m - top), 0.0)
            parts = jnp.where(group, s, 0.0) * shrink
            before = prefix_before(parts)
            for t in range(g0, g1):
                span = slice(t * TILE, (t + 1) * TILE)
                c_ref[at, span] = c_ref[at, span] * shrink[:, t : t + 1] + before[:, t : t + 1]
            rel = rel_col[at, :]
            holds = (rel >= lane * TILE) & (rel < (lane + 1) * TILE)
            old = t_all[at, :]
            moved = jnp.sum(old, axis=1, keepdims=True) * shrink + before
            inside = (rel >= g0 * TILE) & (rel < g1 * TILE)
            t_all[at, :] = jnp.where(inside, jnp.where(holds, moved, 0.0), old)
            total = jnp.sum(parts, axis=1, keepdims=True)
            sums = jnp.where(lane == SLOTS + g1 - 1, total, 0.0)
            of_sums = (lane >= SLOTS + g0) & (lane < SLOTS + g1)
            stats[at, :] = jnp.where(group, top, jnp.where(of_sums, sums, m))

    def close(i):
        first = ends[i - 1] + 1 if i else first_end
        with jax.named_scope(f"xe{i}"):
            for j in range(first, ends[i] + 1):
                if j < n_chunks - 1:
                    forwarded(j)
                else:
                    twin_landed()
        with jax.named_scope(f"ce{i}"):
            finish_end(i)

    def prefix_before(parts):
        k = lax.broadcasted_iota(jnp.int32, (LANES, LANES), 0)
        c = lax.broadcasted_iota(jnp.int32, (LANES, LANES), 1)
        strict = jnp.where(k < c, 1.0, 0.0).astype(BF16)
        return sum(jnp.dot(p, strict, preferred_element_type=F32) for p in split3(parts))

    def complete(j):
        start, n = cols_of(j)
        cross_wait(j, 3 * half, start, start + n)

    def own_complete():
        place = wbuf.at[pl.ds(pl.multiple_of(z * depth, depth), depth)]
        pltpu.make_async_copy(place, place, wl).wait()

    order = service_order(plan, n_cols // LANES)
    folds = {j: (g0, g1) for j, g0, g1 in folds_of(plan, first_end)}
    tail = range(first_end, n_chunks)
    known = max(order.index((k, j)) for k in (0, 2) for j in tail)
    early = min(j for j in range(max(0, first_end - 7), n_chunks - 1) if order.index((1, j + 1)) > known)
    assert early < first_end
    m = len(ends) - 1
    closes = {n_chunks - 3: range(m - 2), n_chunks - 2: [m - 2], n_chunks - 1: [m - 1]}

    for what, j in order:
        if what == "h line":
            with jax.named_scope("hline"):
                arrived(h_place(v, z_one), 1, hid=z_one)
                arrived(h_place(v, lax.rem(z_one + 2, 4)), 2, hid=z_one)
                h_own.wait()
            h_chip.start()
            h_core.start()
        elif what == "h chip":
            with jax.named_scope("hchip"):
                arrived(h_place(v_two), 3, vocab=v_two)
            h_both.start()
        else:
            with jax.named_scope(f"w{what}_{j}"):
                landed(j, what)
            if (what, j) != (1, n_chunks - 1):
                forward(j, what).start()
            if what != 1:
                continue
            if j == 1:
                with jax.named_scope("hcore"):
                    arrived(h_place(v_one), 4, vocab=v_one)
                    arrived(h_place(lax.rem(v_one + 2, 4)), 5, vocab=v_one)
                    own_complete()
            if 0 < j <= first_end:
                with jax.named_scope(f"x{j - 1}"):
                    complete(j - 1)
                with jax.named_scope(f"c{j - 1}"):
                    compute(j - 1)
                if j - 1 in folds:
                    with jax.named_scope(f"f{j - 1}"):
                        fold(*folds[j - 1])
            if j - 1 == early:
                with jax.named_scope("begin"):
                    cross_wait(first_end, 2 * half, cols_of(first_end)[0], n_cols)
                    for i in range(len(ends)):
                        begin_end(i)
            for i in closes.get(j, ()):
                close(i)
    close(m)

    lane = lax.broadcasted_iota(jnp.int32, (rows, LANES), 1)
    at_tgt = jnp.sum(t_all[...], axis=1, keepdims=True)
    turned = jnp.where(lane == 2 * SLOTS, at_tgt, stats[...]).T
    m, at_tgt = turned[0:SLOTS, :], turned[2 * SLOTS : 2 * SLOTS + 1, :]
    top = jnp.max(m, axis=0, keepdims=True)
    shrink = jnp.exp(m - top)
    parts = turned[SLOTS : 2 * SLOTS, :] * shrink
    t = lax.broadcasted_iota(jnp.int32, (SLOTS, rows), 0)
    start = jnp.where(t < n_whole, t * TILE, n_whole * (TILE - LANES) + t * LANES)
    stop = start + jnp.where(t < n_whole, TILE, LANES)
    rel = tgt_ref[...] - base
    known = rel < n_cols
    holds = (rel >= start) & (rel < stop) & known
    ahead = (stop <= rel) & known
    found = jnp.where(holds, at_tgt * shrink, jnp.where(ahead, parts, 0.0))
    zmsg[z, 0:1, :] = top
    zmsg[z, 1:2, :] = jnp.sum(parts, axis=0, keepdims=True)
    zmsg[z, 2:3, :] = jnp.sum(found, axis=0, keepdims=True)

    for k in range(3):
        mine = wbuf.at[w_rows(sources[k], x)]
        remote(mine, mine, ws.at[k], wr.at[0, k], hid=near).wait_send()
        if k == 1:
            mine = wbuf.at[w_rows(sources[k], x), pl.ds(0, n_cols - LANES)]
        remote(mine, mine, xs.at[k], xr.at[0], data=1 - x).wait_send()
    forward(n_chunks - 2, 1).wait_send()

    @pl.when(is_outer == 0)
    def _():
        send_twin(0).wait_send()
        send_twin(1).wait_send()

    for copy in (h_two, h_one, h_relay, h_chip, h_core, h_both):
        copy.wait_send()

    def z_send(i):
        slot = (0, 1 + is_outer, 1 + is_outer)[i]
        return remote(zmsg.at[z], zmsg.at[z], zs.at[i], zr.at[slot], hid=(near, inner_far, outer_far)[i])

    def v_send(d):
        to = lax.rem(v + d, 4)
        return remote(vmsg.at[v], vmsg.at[v], vs.at[d - 1], vr.at[d - 1], vocab=to)

    for i in (2, 1, 0):
        z_send(i).start()
    k = lax.broadcasted_iota(jnp.int32, (SLOTS, SLOTS), 0)
    c = lax.broadcasted_iota(jnp.int32, (SLOTS, SLOTS), 1)
    strict = jnp.where(c < k, 1.0, 0.0).astype(BF16)
    before = sum(jnp.dot(strict, p, preferred_element_type=F32) for p in split3(parts))
    rest = jnp.zeros((LANES - 2 * SLOTS, rows), F32)
    coef_ref[...] = jnp.concatenate([shrink, before, rest], axis=0).T
    for i, frm in enumerate(sources):
        with jax.named_scope(f"z{i}"):
            remote(zmsg.at[frm], zmsg.at[frm], zs.at[i], zr.at[i], hid=frm).wait_recv()

    ids = tgt_ref[...]
    maxes = [zmsg[h, 0:1, :] for h in range(4)]
    v_max = functools.reduce(jnp.maximum, maxes)
    v_sum = jnp.zeros((1, rows), F32)
    v_tgt = jnp.zeros((1, rows), F32)
    mine_before = jnp.zeros((1, rows), F32)
    for h in range(4):
        mine_before = jnp.where(h == z, v_sum, mine_before)
        f = jnp.exp(maxes[h] - v_max)
        low = (v * 4 + h) * n_cols
        inside = (ids >= low) & (ids < low + n_cols)
        v_tgt += jnp.where(inside, zmsg[h, 2:3, :] * f + v_sum, 0.0)
        v_sum += zmsg[h, 1:2, :] * f
    vmsg[v, 0:1, :] = v_max
    vmsg[v, 1:2, :] = v_sum
    vmsg[v, 2:3, :] = v_tgt

    for i in range(3):
        z_send(i).wait_send()
    for d in (2, 1, 3):
        v_send(d).start()
    for d in (1, 2, 3):
        frm = lax.rem(v + 4 - d, 4)
        with jax.named_scope(f"v{d}"):
            remote(vmsg.at[frm], vmsg.at[frm], vs.at[d - 1], vr.at[d - 1], vocab=frm).wait_recv()

    maxes = [vmsg[u, 0:1, :] for u in range(4)]
    g_max = functools.reduce(jnp.maximum, maxes)
    g_sum = jnp.zeros((1, rows), F32)
    g_tgt = jnp.zeros((1, rows), F32)
    g_before = jnp.zeros((1, rows), F32)
    for u in range(4):
        f = jnp.exp(maxes[u] - g_max)
        g_before = jnp.where(u == v, g_sum + mine_before * f, g_before)
        low = u * 4 * n_cols
        inside = (ids >= low) & (ids < low + 4 * n_cols)
        g_tgt += jnp.where(inside, vmsg[u, 2:3, :] * f + g_sum, 0.0)
        g_sum += vmsg[u, 1:2, :] * f
    tgt_out_ref[...] = g_tgt / g_sum
    factor_ref[0:1, :] = jnp.exp(zmsg[z, 0:1, :] - g_max) / g_sum
    factor_ref[1:2, :] = g_before / g_sum
    for d in (1, 2, 3):
        v_send(d).wait_send()


def finish_kernel(tiles, lanes, c_ref, coef_ref, factor_ref, tgt_ref, out_ref, tgt_out_ref, buf, factor_col, sems):
    slots, n, n_cols = buf.shape
    steps = c_ref.shape[0] // n

    def put(i):
        slot = lax.rem(i, slots)
        at = pl.ds(pl.multiple_of(i * n, n), n)
        return pltpu.make_async_copy(buf.at[slot], out_ref.at[at], sems.at[slot])

    @pl.loop(0, steps)
    def _(i):
        slot = lax.rem(i, slots)

        @pl.when(i >= slots)
        def _():
            put(i - slots).wait()

        at = pl.ds(pl.multiple_of(i * n, n), n)
        turn = max(n, LANES)

        @pl.when(lax.rem(i, turn // n) == 0)
        def _():
            some = pl.ds(pl.multiple_of(i // (turn // n) * turn, turn), turn)
            factor_col[some, :] = factor_ref[:, some].T

        lane = lax.broadcasted_iota(jnp.int32, (n, LANES), 1)
        coef = coef_ref[at, :] * factor_col[at, 0:1] + jnp.where(lane < SLOTS, 0.0, factor_col[at, 1:2])
        for (start, width), k in zip(tiles, lanes):
            span = slice(start, start + width)
            buf[slot, :, span] = c_ref[at, span] * coef[:, k : k + 1] + coef[:, SLOTS + k : SLOTS + k + 1]
        put(i).start()

    tgt_out_ref[...] = tgt_ref[...]
    for i in range(max(0, steps - slots), steps):
        put(i).wait()


def solution(mesh):
    n_hid, n_voc = mesh.shape["hid"], mesh.shape["vocab"]
    assert n_hid == 4 and n_voc == 4 and mesh.shape["data"] == 2

    def local_step(h_blk, w_blk, temp_blk, tgt_blk):
        rows, depth = h_blk.shape
        n_cols = w_blk.shape[1] // n_hid
        assert n_cols % LANES == 0
        tiles = tiles_of(n_cols // LANES)
        n_tiles = len(tiles)
        assert n_tiles <= SLOTS
        plan = chunks_of(n_cols // LANES)
        n_chunks = len(plan)
        vmem = pl.BlockSpec(memory_space=pltpu.VMEM)
        hbm = pl.BlockSpec(memory_space=pltpu.HBM)
        dma = pltpu.SemaphoreType.DMA
        table = pltpu.VMEM((rows, LANES), F32)
        c, coef, factor, tgt = pl.pallas_call(
            functools.partial(prefix_kernel, n_cols),
            out_shape=(
                pltpu.VMEM((rows, n_cols), F32),
                pltpu.VMEM((rows, LANES), F32),
                pltpu.VMEM((8, rows), F32),
                pltpu.VMEM((1, rows), F32),
            ),
            in_specs=[hbm] * 4,
            out_specs=[vmem] * 4,
            scratch_shapes=[
                pltpu.VMEM((4 * depth, n_cols), BF16),
                pltpu.VMEM((rows, 4 * depth), BF16),
                pltpu.VMEM((rows, TILE), F32),
                pltpu.VMEM((3 * TILE, TILE), BF16),
                pltpu.VMEM((3 * LANES, LANES), BF16),
                table,
                table,
                table,
                pltpu.VMEM((rows, LANES), jnp.int32),
                pltpu.VMEM((1, rows), F32),
                pltpu.VMEM((1, rows), jnp.int32),
                pltpu.VMEM((4, 3, rows), F32),
                pltpu.VMEM((4, 3, rows), F32),
                pltpu.VMEM((8, rows), F32),
                dma((3,)),
                dma((n_chunks, 3)),
                dma((4,)),
                dma((n_chunks,)),
                dma((2,)),
                dma,
                dma,
                dma,
                dma((6,)),
                dma((6,)),
                dma((3,)),
                dma((3,)),
                dma((3,)),
                dma((3,)),
                dma((2,)),
            ],
            compiler_params=pltpu.CompilerParams(
                collective_id=0, has_side_effects=True, vmem_limit_bytes=37 << 20
            ),
            name="prefix",
        )(h_blk, w_blk, temp_blk.reshape(1, rows), tgt_blk.reshape(1, rows))
        n = min(rows, 64)
        lanes = list(range(n_tiles))
        last_whole = sum(width == TILE for _, width in tiles) - 1
        first_end = [first for first, *_ in plan].index(2 * last_whole)
        for _, g0, g1 in folds_of(plan, first_end):
            lanes[g0:g1] = [g0] * (g1 - g0)
        cdf, cdf_tgt = pl.pallas_call(
            functools.partial(finish_kernel, tiles, lanes),
            out_shape=(
                jax.ShapeDtypeStruct((rows, n_cols), F32),
                jax.ShapeDtypeStruct((1, rows), F32),
            ),
            in_specs=[vmem] * 4,
            out_specs=[hbm, vmem],
            scratch_shapes=[pltpu.VMEM((4, n, n_cols), F32), pltpu.VMEM((rows, 8), F32), dma((4,))],
            compiler_params=pltpu.CompilerParams(vmem_limit_bytes=9 << 20),
            name="finish",
        )(c, coef, factor, tgt)
        return cdf, cdf_tgt.reshape(rows)

    return jax.shard_map(
        local_step,
        mesh=mesh,
        in_specs=(P("data", "hid"), P("hid", "vocab"), P("data"), P("data")),
        out_specs=(P("data", ("vocab", "hid")), P("data")),
        check_vma=False,
    )
```

```python
import functools

import jax
import jax.numpy as jnp
from jax import lax
from jax.experimental import pallas as pl
from jax.experimental.pallas import tpu as pltpu
from jax.sharding import PartitionSpec as P

MESH = pl.DeviceIdType.MESH
F32 = jnp.float32
BF16 = jnp.bfloat16
TILE = 256
LANES = 128
SLOTS = 32
LOWEST = float(jnp.finfo(jnp.float32).min)


def tiles_of(blocks):
    whole = (blocks - 3) // 2
    tiles = [(t * TILE, TILE) for t in range(whole)]
    return tiles + [(b * LANES, LANES) for b in range(2 * whole, blocks)]


def chunks_of(blocks):
    whole = (blocks - 3) // 2
    sizes, left = [], 2 * whole - 2
    for size in (2, 2, 2, 2, 4, 4):
        if left > size:
            sizes.append(size)
            left -= size
    while left > 0:
        sizes.append(min(6, left))
        left -= sizes[-1]
    plan, at = [], 0
    for size in reversed(sizes):
        plan.append((at, size, 0, 2))
        at += size
    plan += [(b, 1, 0, 2) for b in range(at, blocks - 2)]
    return plan + [(b, 1, r, 1) for b in (blocks - 2, blocks - 1) for r in (0, 1)]


def service_order(plan, blocks):
    events = [(0.15 * blocks, "h line", 0), (0.28 * blocks, "h chip", 0)]
    for j, (first, size, _, _) in enumerate(plan):
        end = first + size
        events.append((first + size / 3 + 2, 0, j))
        events.append((end + 2, 2, j))
        events.append((min(1.86 * end, 0.68 * blocks + 0.6 * end) + 2, 1, j))
    events.sort(key=lambda e: e[0])
    order = [e[1:] for e in events]
    for j in range(len(plan)):
        at = max(order.index((k, j)) for k in (0, 1, 2))
        order.remove((1, j))
        order.insert(at, (1, j))
    return order


def folds_of(plan, first_end):
    folds, at = [], 0
    for j in (first_end // 3, 3 * first_end // 5):
        stop = sum(plan[j][:2]) // 2 - 1
        if j < first_end and stop > at:
            folds.append((j, at, stop))
            at = stop
    return folds


def split3(e):
    hi = e.astype(BF16)
    rest = e - hi.astype(F32)
    mid = rest.astype(BF16)
    low = (rest - mid.astype(F32)).astype(BF16)
    return hi, mid, low


def prefix_kernel(
    n_cols, h_ref, w_ref, temp_hbm, tgt_hbm,
    c_ref, coef_ref, factor_ref, tgt_out_ref,
    wbuf, hbuf, zbuf, tri, tri_last, stats, t_all, temp_col, rel_col, temp_ref, tgt_ref, zmsg, vmsg, back,
    ws, wr, xs, xr, ts, tr, wl, hl, hs, hr, zs, zr, vs, vr, rl,
):
    x, z, v = lax.axis_index("data"), lax.axis_index("hid"), lax.axis_index("vocab")
    rows, depth = h_ref.shape
    half, quarter = depth // 2, rows // 4
    tiles = tiles_of(n_cols // LANES)
    n_tiles = len(tiles)
    n_whole = sum(width == TILE for _, width in tiles)
    plan = chunks_of(n_cols // LANES)
    n_chunks = len(plan)
    ends = [[j for j, (first, *_) in enumerate(plan) if first * LANES < sum(tiles[t])][-1] for t in range(n_whole - 1, n_tiles)]
    first_end = ends[0] - 1

    side = z // 2
    outer_far, inner_far, near = 3 - 3 * side, 2 - side, 1 - z + 4 * side
    is_outer = jnp.where(z == side * 3, 1, 0)
    z_two, z_one = lax.rem(z + 2, 4), near
    v_two, v_one = lax.rem(v + 2, 4), v + 1 - 2 * lax.rem(v, 2)
    sources = (near, inner_far, outer_far)

    def cols_of(j):
        first, size, _, _ = plan[j]
        return first * LANES, size * LANES

    def w_rows(source, part, j=None):
        at, n = (0, half) if j is None else (plan[j][2] * (half // 2), plan[j][3] * (half // 2))
        return pl.ds(pl.multiple_of(source * depth + part * half + at, half // 2), n)

    def w_place(j, source, part):
        start, n = cols_of(j)
        return wbuf.at[w_rows(source, part, j), pl.ds(start, n)]

    def h_place(q, block=None):
        at = pl.ds(pl.multiple_of(q * quarter, quarter), quarter)
        if block is None:
            return hbuf.at[at]
        return hbuf.at[at, pl.ds(pl.multiple_of(block * depth, depth), depth)]

    def remote(src, dst, send, recv, **to):
        return pltpu.make_async_remote_copy(
            src_ref=src, dst_ref=dst, send_sem=send, recv_sem=recv, device_id=to, device_id_type=MESH
        )

    def w_source(j, part, dest):
        start, n = cols_of(j)
        return w_ref.at[w_rows(0, part, j), pl.ds(pl.multiple_of(dest * n_cols + start, LANES), n)]

    def direct(j, k, dest, slot):
        return remote(w_source(j, x, dest), w_place(j, z, x), ws.at[k], wr.at[j, slot], hid=dest)

    def send_near(j):
        return direct(j, 0, near, 0)

    odd = lax.rem(v, 2)
    far_first = outer_far + odd * (inner_far - outer_far)
    far_second = inner_far + odd * (outer_far - inner_far)

    def send_far(j, i):
        return direct(j, 1 + i, (far_first, far_second)[i], 1 + is_outer)

    def send_twin(i):
        dest = (far_first, far_second)[i]
        return remote(w_source(n_chunks - 1, 1 - x, dest), w_place(n_chunks - 1, z, 1 - x), ts.at[i], tr, hid=dest)

    def twin_landed():
        place = w_place(n_chunks - 1, inner_far, 1 - x)
        remote(place, place, ts.at[0], tr, hid=inner_far).wait_recv()

    def landed(j, k):
        place = w_place(j, sources[k], x)
        remote(place, place, ws.at[k], wr.at[j, k], hid=sources[k]).wait_recv()

    def forward(j, k):
        place = w_place(j, sources[k], x)
        send = 3 if k == 1 and j == n_chunks - 2 else k
        return remote(place, place, xs.at[send], xr.at[cross(j, k)], data=1 - x)

    def cross(j, k):
        if j < first_end:
            return j
        return first_end if k != 1 else 1 + j

    def cross_wait(slot, count, start, stop):
        place = wbuf.at[pl.ds(0, count), pl.ds(start, stop - start)]
        remote(place, place, xs.at[0], xr.at[slot], data=1 - x).wait_recv()

    def forwarded(j):
        place = w_place(j, inner_far, 1 - x)
        remote(place, place, xs.at[1], xr.at[cross(j, 1)], data=1 - x).wait_recv()

    def own(j):
        start, n = cols_of(j)
        return pltpu.make_async_copy(
            w_ref.at[:, pl.ds(pl.multiple_of(z * n_cols + start, LANES), n)],
            wbuf.at[pl.ds(pl.multiple_of(z * depth, depth), depth), pl.ds(start, n)],
            wl,
        )

    h_mine = h_ref.at[pl.ds(pl.multiple_of(v * quarter, quarter), quarter)]
    h_own = pltpu.make_async_copy(h_mine, h_place(v, z), hl)
    h_two = remote(h_mine, h_place(v, z), hs.at[0], hr.at[0], hid=z_two)
    h_one = remote(h_mine, h_place(v, z), hs.at[1], hr.at[1], hid=z_one)
    h_relay = remote(h_place(v, z_two), h_place(v, z_two), hs.at[2], hr.at[2], hid=z_one)
    h_chip = remote(h_place(v), h_place(v), hs.at[3], hr.at[3], vocab=v_two)
    h_core = remote(h_place(v), h_place(v), hs.at[4], hr.at[4], vocab=v_one)
    h_both = remote(h_place(v_two), h_place(v_two), hs.at[5], hr.at[5], vocab=v_one)

    def arrived(place, i, **frm):
        remote(place, place, hs.at[i], hr.at[i], **frm).wait_recv()

    barrier = pltpu.get_barrier_semaphore()
    peers = [{"hid": lax.rem(z + d, 4)} for d in (1, 2, 3)]
    peers += [{"data": 1 - x}] + [{"vocab": lax.rem(v + d, 4)} for d in (1, 2, 3)]
    for peer in peers:
        pl.semaphore_signal(barrier, inc=1, device_id=peer, device_id_type=MESH)
    row_copies = [
        pltpu.make_async_copy(temp_hbm, temp_ref, rl.at[0]),
        pltpu.make_async_copy(tgt_hbm, tgt_ref, rl.at[1]),
    ]
    for copy in (h_own, *row_copies):
        copy.start()
    for j in range(n_chunks):
        if plan[j][2] == 0:
            own(j).start()
    with jax.named_scope("bar"):
        pl.semaphore_wait(barrier, len(peers))

    h_two.start()
    h_one.start()
    send_near(0).start()
    send_far(0, 0).start()

    def ones_below(ref, width):
        k = lax.broadcasted_iota(jnp.int32, (width, width), 0)
        c = lax.broadcasted_iota(jnp.int32, (width, width), 1)
        block = jnp.where(k <= c, 1.0, 0.0).astype(BF16)
        for i in range(3):
            ref[pl.ds(i * width, width), :] = block

    ones_below(tri, TILE)
    ones_below(tri_last, LANES)
    base = (v * 4 + z) * n_cols
    for copy in row_copies:
        copy.wait()
    back[0:1, :] = temp_ref[...]
    back[1:2, :] = (tgt_ref[...] - base).astype(F32)
    cols8 = back[...].T
    temp_col[...] = jnp.broadcast_to(cols8[:, 0:1], temp_col.shape)
    rel_col[...] = jnp.broadcast_to(cols8[:, 1:2], rel_col.shape).astype(jnp.int32)
    slot = lax.broadcasted_iota(jnp.int32, stats.shape, 1)
    stats[...] = jnp.where(slot < SLOTS, LOWEST, 0.0)
    t_all[...] = jnp.zeros(t_all.shape, F32)

    with jax.named_scope("h0"):
        arrived(h_place(v, z_two), 0, hid=z_two)
    h_relay.start()
    send_far(0, 1).start()
    for j in range(1, n_chunks):
        send_near(j).start()
        send_far(j, 0).start()
        send_far(j, 1).start()

    @pl.when(is_outer == 0)
    def _():
        send_twin(0).start()
        send_twin(1).start()


    part, few = min(rows, 512), min(rows, 128)

    def logits_and_sums(product, sums):
        some = part if product is not None or sums[2] == TILE else min(rows, 2 * part)

        @pl.loop(0, rows // some)
        def _(i):
            if product is not None:
                _, new_start, new_width = product
                at = pl.ds(pl.multiple_of(i * part, part), part)
                new = jnp.dot(
                    hbuf[at, :], wbuf[:, pl.ds(new_start, new_width)], preferred_element_type=F32
                )
            for k in range(0, some, few) if sums is not None else ():
                prefix(pl.ds(pl.multiple_of(i * some + k, few), few), *sums)
            if product is not None:
                zbuf[at, 0:new_width] = new

    def prefix(at, t, start, width):
        pieces = width // LANES
        logits = zbuf[at, 0:width] * jnp.concatenate([temp_col[at, :]] * pieces, axis=1)
        lane = lax.broadcasted_iota(jnp.int32, (few, LANES), 1)
        top = jnp.max(logits, axis=1, keepdims=True)
        e = jnp.exp(logits - top)
        total = jnp.sum(e, axis=1, keepdims=True)
        stats[at, :] = jnp.where(lane == t, top, jnp.where(lane == SLOTS + t, total, stats[at, :]))
        table = tri if width == TILE else tri_last
        run = jnp.dot(jnp.concatenate(split3(e), axis=1), table[...], preferred_element_type=F32)
        c_ref[at, pl.ds(start, width)] = run
        rel = rel_col[at, :] - start
        hit = t_all[at, :]
        for p in range(pieces):
            hit += jnp.where(lane == rel - p * LANES, run[:, p * LANES : (p + 1) * LANES], 0.0)
        t_all[at, :] = hit

    def whole(t):
        return t, pl.multiple_of(t * TILE, TILE), TILE

    def compute(j):
        first, size = (n // 2 for n in plan[j][:2])
        stop = first + size
        if first == 0:
            logits_and_sums(whole(0), None)
            first = 1
        if first < stop:

            @pl.loop(first, stop)
            def _(t):
                logits_and_sums(whole(t), whole(t - 1))

        if j == first_end - 1:
            logits_and_sums(None, whole(stop - 1))

    def block_dot(at, block, start, width):
        lanes = pl.ds(pl.multiple_of(block * depth, depth), depth)
        return jnp.dot(hbuf[at, lanes], wbuf[lanes, start : start + width], preferred_element_type=F32)

    def begin_end(i):
        start, width = tiles[n_whole - 1 + i]

        @pl.loop(0, rows // part)
        def _(k):
            at = pl.ds(pl.multiple_of(k * part, part), part)
            c_ref[at, start : start + width] = (
                block_dot(at, z, start, width)
                + block_dot(at, near, start, width)
                + block_dot(at, outer_far, start, width)
            )

    def finish_end(i):
        t = n_whole - 1 + i
        start, width = tiles[t]
        every = slice(0, rows)
        zbuf[:, 0:width] = c_ref[:, start : start + width] + block_dot(every, inner_far, start, width)
        logits_and_sums(None, (t, start, width))

    def fold(g0, g1):
        @pl.loop(0, rows // few)
        def _(i):
            at = pl.ds(pl.multiple_of(i * few, few), few)
            lane = lax.broadcasted_iota(jnp.int32, (few, LANES), 1)
            group = (lane >= g0) & (lane < g1)
            m = stats[at, :]
            s = pltpu.roll(m, LANES - SLOTS, 1)
            top = jnp.max(jnp.where(group, m, LOWEST), axis=1, keepdims=True)
            shrink = jnp.where(group, jnp.exp(m - top), 0.0)
            parts = jnp.where(group, s, 0.0) * shrink
            before = prefix_before(parts)
            for t in range(g0, g1):
                span = slice(t * TILE, (t + 1) * TILE)
                c_ref[at, span] = c_ref[at, span] * shrink[:, t : t + 1] + before[:, t : t + 1]
            rel = rel_col[at, :]
            holds = (rel >= lane * TILE) & (rel < (lane + 1) * TILE)
            old = t_all[at, :]
            moved = jnp.sum(old, axis=1, keepdims=True) * shrink + before
            inside = (rel >= g0 * TILE) & (rel < g1 * TILE)
            t_all[at, :] = jnp.where(inside, jnp.where(holds, moved, 0.0), old)
            total = jnp.sum(parts, axis=1, keepdims=True)
            sums = jnp.where(lane == SLOTS + g1 - 1, total, 0.0)
            of_sums = (lane >= SLOTS + g0) & (lane < SLOTS + g1)
            stats[at, :] = jnp.where(group, top, jnp.where(of_sums, sums, m))

    def close(i):
        first = ends[i - 1] + 1 if i else first_end
        with jax.named_scope(f"xe{i}"):
            for j in range(first, ends[i] + 1):
                if j < n_chunks - 1:
                    forwarded(j)
                else:
                    twin_landed()
        with jax.named_scope(f"ce{i}"):
            finish_end(i)

    def prefix_before(parts):
        k = lax.broadcasted_iota(jnp.int32, (LANES, LANES), 0)
        c = lax.broadcasted_iota(jnp.int32, (LANES, LANES), 1)
        strict = jnp.where(k < c, 1.0, 0.0).astype(BF16)
        return sum(jnp.dot(p, strict, preferred_element_type=F32) for p in split3(parts))

    def complete(j):
        start, n = cols_of(j)
        cross_wait(j, 3 * half, start, start + n)

    def own_complete():
        place = wbuf.at[pl.ds(pl.multiple_of(z * depth, depth), depth)]
        pltpu.make_async_copy(place, place, wl).wait()

    order = service_order(plan, n_cols // LANES)
    folds = {j: (g0, g1) for j, g0, g1 in folds_of(plan, first_end)}
    tail = range(first_end, n_chunks)
    known = max(order.index((k, j)) for k in (0, 2) for j in tail)
    early = min(j for j in range(max(0, first_end - 7), n_chunks - 1) if order.index((1, j + 1)) > known)
    assert early < first_end
    m = len(ends) - 1
    closes = {n_chunks - 3: range(m - 2), n_chunks - 2: [m - 2], n_chunks - 1: [m - 1]}

    for what, j in order:
        if what == "h line":
            with jax.named_scope("hline"):
                arrived(h_place(v, z_one), 1, hid=z_one)
                arrived(h_place(v, lax.rem(z_one + 2, 4)), 2, hid=z_one)
                h_own.wait()
            h_chip.start()
            h_core.start()
        elif what == "h chip":
            with jax.named_scope("hchip"):
                arrived(h_place(v_two), 3, vocab=v_two)
            h_both.start()
        else:
            with jax.named_scope(f"w{what}_{j}"):
                landed(j, what)
            if (what, j) != (1, n_chunks - 1):
                forward(j, what).start()
            if what != 1:
                continue
            if j == 1:
                with jax.named_scope("hcore"):
                    arrived(h_place(v_one), 4, vocab=v_one)
                    arrived(h_place(lax.rem(v_one + 2, 4)), 5, vocab=v_one)
                    own_complete()
            if 0 < j <= first_end:
                with jax.named_scope(f"x{j - 1}"):
                    complete(j - 1)
                with jax.named_scope(f"c{j - 1}"):
                    compute(j - 1)
                if j - 1 in folds:
                    with jax.named_scope(f"f{j - 1}"):
                        fold(*folds[j - 1])
            if j - 1 == early:
                with jax.named_scope("begin"):
                    cross_wait(first_end, 2 * half, cols_of(first_end)[0], n_cols)
                    for i in range(len(ends)):
                        begin_end(i)
            for i in closes.get(j, ()):
                close(i)
    close(m)

    lane = lax.broadcasted_iota(jnp.int32, (rows, LANES), 1)
    at_tgt = jnp.sum(t_all[...], axis=1, keepdims=True)
    turned = jnp.where(lane == 2 * SLOTS, at_tgt, stats[...]).T
    m, at_tgt = turned[0:SLOTS, :], turned[2 * SLOTS : 2 * SLOTS + 1, :]
    top = jnp.max(m, axis=0, keepdims=True)
    shrink = jnp.exp(m - top)
    parts = turned[SLOTS : 2 * SLOTS, :] * shrink
    t = lax.broadcasted_iota(jnp.int32, (SLOTS, rows), 0)
    start = jnp.where(t < n_whole, t * TILE, n_whole * (TILE - LANES) + t * LANES)
    stop = start + jnp.where(t < n_whole, TILE, LANES)
    rel = tgt_ref[...] - base
    known = rel < n_cols
    holds = (rel >= start) & (rel < stop) & known
    ahead = (stop <= rel) & known
    found = jnp.where(holds, at_tgt * shrink, jnp.where(ahead, parts, 0.0))
    zmsg[z, 0:1, :] = top
    zmsg[z, 1:2, :] = jnp.sum(parts, axis=0, keepdims=True)
    zmsg[z, 2:3, :] = jnp.sum(found, axis=0, keepdims=True)

    for k in range(3):
        mine = wbuf.at[w_rows(sources[k], x)]
        remote(mine, mine, ws.at[k], wr.at[0, k], hid=near).wait_send()
        if k == 1:
            mine = wbuf.at[w_rows(sources[k], x), pl.ds(0, n_cols - LANES)]
        remote(mine, mine, xs.at[k], xr.at[0], data=1 - x).wait_send()
    forward(n_chunks - 2, 1).wait_send()

    @pl.when(is_outer == 0)
    def _():
        send_twin(0).wait_send()
        send_twin(1).wait_send()

    for copy in (h_two, h_one, h_relay, h_chip, h_core, h_both):
        copy.wait_send()

    def z_send(i):
        slot = (0, 1 + is_outer, 1 + is_outer)[i]
        return remote(zmsg.at[z], zmsg.at[z], zs.at[i], zr.at[slot], hid=(near, inner_far, outer_far)[i])

    def v_send(d):
        to = lax.rem(v + d, 4)
        return remote(vmsg.at[v], vmsg.at[v], vs.at[d - 1], vr.at[d - 1], vocab=to)

    for i in (2, 1, 0):
        z_send(i).start()
    k = lax.broadcasted_iota(jnp.int32, (SLOTS, SLOTS), 0)
    c = lax.broadcasted_iota(jnp.int32, (SLOTS, SLOTS), 1)
    strict = jnp.where(c < k, 1.0, 0.0).astype(BF16)
    before = sum(jnp.dot(strict, p, preferred_element_type=F32) for p in split3(parts))
    rest = jnp.zeros((LANES - 2 * SLOTS, rows), F32)
    coef_ref[...] = jnp.concatenate([shrink, before, rest], axis=0).T
    for i, frm in enumerate(sources):
        with jax.named_scope(f"z{i}"):
            remote(zmsg.at[frm], zmsg.at[frm], zs.at[i], zr.at[i], hid=frm).wait_recv()

    ids = tgt_ref[...]
    maxes = [zmsg[h, 0:1, :] for h in range(4)]
    v_max = functools.reduce(jnp.maximum, maxes)
    v_sum = jnp.zeros((1, rows), F32)
    v_tgt = jnp.zeros((1, rows), F32)
    mine_before = jnp.zeros((1, rows), F32)
    for h in range(4):
        mine_before = jnp.where(h == z, v_sum, mine_before)
        f = jnp.exp(maxes[h] - v_max)
        low = (v * 4 + h) * n_cols
        inside = (ids >= low) & (ids < low + n_cols)
        v_tgt += jnp.where(inside, zmsg[h, 2:3, :] * f + v_sum, 0.0)
        v_sum += zmsg[h, 1:2, :] * f
    vmsg[v, 0:1, :] = v_max
    vmsg[v, 1:2, :] = v_sum
    vmsg[v, 2:3, :] = v_tgt

    for i in range(3):
        z_send(i).wait_send()
    for d in (2, 1, 3):
        v_send(d).start()
    for d in (1, 2, 3):
        frm = lax.rem(v + 4 - d, 4)
        with jax.named_scope(f"v{d}"):
            remote(vmsg.at[frm], vmsg.at[frm], vs.at[d - 1], vr.at[d - 1], vocab=frm).wait_recv()

    maxes = [vmsg[u, 0:1, :] for u in range(4)]
    g_max = functools.reduce(jnp.maximum, maxes)
    g_sum = jnp.zeros((1, rows), F32)
    g_tgt = jnp.zeros((1, rows), F32)
    g_before = jnp.zeros((1, rows), F32)
    for u in range(4):
        f = jnp.exp(maxes[u] - g_max)
        g_before = jnp.where(u == v, g_sum + mine_before * f, g_before)
        low = u * 4 * n_cols
        inside = (ids >= low) & (ids < low + 4 * n_cols)
        g_tgt += jnp.where(inside, vmsg[u, 2:3, :] * f + g_sum, 0.0)
        g_sum += vmsg[u, 1:2, :] * f
    tgt_out_ref[...] = g_tgt / g_sum
    factor_ref[0:1, :] = jnp.exp(zmsg[z, 0:1, :] - g_max) / g_sum
    factor_ref[1:2, :] = g_before / g_sum
    for d in (1, 2, 3):
        v_send(d).wait_send()


def finish_kernel(tiles, lanes, c_ref, coef_ref, factor_ref, tgt_ref, out_ref, tgt_out_ref, buf, factor_col, sems):
    slots, n, n_cols = buf.shape
    steps = c_ref.shape[0] // n

    def put(i):
        slot = lax.rem(i, slots)
        at = pl.ds(pl.multiple_of(i * n, n), n)
        return pltpu.make_async_copy(buf.at[slot], out_ref.at[at], sems.at[slot])

    @pl.loop(0, steps)
    def _(i):
        slot = lax.rem(i, slots)

        @pl.when(i >= slots)
        def _():
            put(i - slots).wait()

        at = pl.ds(pl.multiple_of(i * n, n), n)
        turn = max(n, LANES)

        @pl.when(lax.rem(i, turn // n) == 0)
        def _():
            some = pl.ds(pl.multiple_of(i // (turn // n) * turn, turn), turn)
            factor_col[some, :] = factor_ref[:, some].T

        lane = lax.broadcasted_iota(jnp.int32, (n, LANES), 1)
        coef = coef_ref[at, :] * factor_col[at, 0:1] + jnp.where(lane < SLOTS, 0.0, factor_col[at, 1:2])
        for (start, width), k in zip(tiles, lanes):
            span = slice(start, start + width)
            buf[slot, :, span] = c_ref[at, span] * coef[:, k : k + 1] + coef[:, SLOTS + k : SLOTS + k + 1]
        put(i).start()

    tgt_out_ref[...] = tgt_ref[...]
    for i in range(max(0, steps - slots), steps):
        with jax.named_scope(f"fe{i}"):
            put(i).wait()


def solution(mesh):
    n_hid, n_voc = mesh.shape["hid"], mesh.shape["vocab"]
    assert n_hid == 4 and n_voc == 4 and mesh.shape["data"] == 2

    def local_step(h_blk, w_blk, temp_blk, tgt_blk):
        rows, depth = h_blk.shape
        n_cols = w_blk.shape[1] // n_hid
        assert n_cols % LANES == 0
        tiles = tiles_of(n_cols // LANES)
        n_tiles = len(tiles)
        assert n_tiles <= SLOTS
        plan = chunks_of(n_cols // LANES)
        n_chunks = len(plan)
        vmem = pl.BlockSpec(memory_space=pltpu.VMEM)
        hbm = pl.BlockSpec(memory_space=pltpu.HBM)
        dma = pltpu.SemaphoreType.DMA
        table = pltpu.VMEM((rows, LANES), F32)
        c, coef, factor, tgt = pl.pallas_call(
            functools.partial(prefix_kernel, n_cols),
            out_shape=(
                pltpu.VMEM((rows, n_cols), F32),
                pltpu.VMEM((rows, LANES), F32),
                pltpu.VMEM((8, rows), F32),
                pltpu.VMEM((1, rows), F32),
            ),
            in_specs=[hbm] * 4,
            out_specs=[vmem] * 4,
            scratch_shapes=[
                pltpu.VMEM((4 * depth, n_cols), BF16),
                pltpu.VMEM((rows, 4 * depth), BF16),
                pltpu.VMEM((rows, TILE), F32),
                pltpu.VMEM((3 * TILE, TILE), BF16),
                pltpu.VMEM((3 * LANES, LANES), BF16),
                table,
                table,
                table,
                pltpu.VMEM((rows, LANES), jnp.int32),
                pltpu.VMEM((1, rows), F32),
                pltpu.VMEM((1, rows), jnp.int32),
                pltpu.VMEM((4, 3, rows), F32),
                pltpu.VMEM((4, 3, rows), F32),
                pltpu.VMEM((8, rows), F32),
                dma((3,)),
                dma((n_chunks, 3)),
                dma((4,)),
                dma((n_chunks,)),
                dma((2,)),
                dma,
                dma,
                dma,
                dma((6,)),
                dma((6,)),
                dma((3,)),
                dma((3,)),
                dma((3,)),
                dma((3,)),
                dma((2,)),
            ],
            compiler_params=pltpu.CompilerParams(
                collective_id=0, has_side_effects=True, vmem_limit_bytes=37 << 20
            ),
            name="prefix",
        )(h_blk, w_blk, temp_blk.reshape(1, rows), tgt_blk.reshape(1, rows))
        n = min(rows, 64)
        lanes = list(range(n_tiles))
        last_whole = sum(width == TILE for _, width in tiles) - 1
        first_end = [first for first, *_ in plan].index(2 * last_whole)
        for _, g0, g1 in folds_of(plan, first_end):
            lanes[g0:g1] = [g0] * (g1 - g0)
        cdf, cdf_tgt = pl.pallas_call(
            functools.partial(finish_kernel, tiles, lanes),
            out_shape=(
                jax.ShapeDtypeStruct((rows, n_cols), F32),
                jax.ShapeDtypeStruct((1, rows), F32),
            ),
            in_specs=[vmem] * 4,
            out_specs=[hbm, vmem],
            scratch_shapes=[pltpu.VMEM((4, n, n_cols), F32), pltpu.VMEM((rows, 8), F32), dma((4,))],
            compiler_params=pltpu.CompilerParams(vmem_limit_bytes=9 << 20),
            name="finish",
        )(c, coef, factor, tgt)
        return cdf, cdf_tgt.reshape(rows)

    return jax.shard_map(
        local_step,
        mesh=mesh,
        in_specs=(P("data", "hid"), P("hid", "vocab"), P("data"), P("data")),
        out_specs=(P("data", ("vocab", "hid")), P("data")),
        check_vma=False,
    )
```

```python
import functools

import jax
import jax.numpy as jnp
from jax import lax
from jax.experimental import pallas as pl
from jax.experimental.pallas import tpu as pltpu
from jax.sharding import PartitionSpec as P

MESH = pl.DeviceIdType.MESH
F32 = jnp.float32
BF16 = jnp.bfloat16
TILE = 256
LANES = 128
SLOTS = 32
LOWEST = float(jnp.finfo(jnp.float32).min)


def tiles_of(blocks):
    whole = (blocks - 3) // 2
    tiles = [(t * TILE, TILE) for t in range(whole)]
    return tiles + [(b * LANES, LANES) for b in range(2 * whole, blocks)]


def chunks_of(blocks):
    whole = (blocks - 3) // 2
    sizes, left = [], 2 * whole - 2
    for size in (2, 2, 2, 2, 4, 4):
        if left > size:
            sizes.append(size)
            left -= size
    while left > 0:
        sizes.append(min(6, left))
        left -= sizes[-1]
    plan, at = [], 0
    for size in reversed(sizes):
        plan.append((at, size, 0, 2))
        at += size
    plan += [(b, 1, 0, 2) for b in range(at, blocks - 2)]
    return plan + [(b, 1, r, 1) for b in (blocks - 2, blocks - 1) for r in (0, 1)]


def service_order(plan, blocks):
    events = [(0.15 * blocks, "h line", 0), (0.28 * blocks, "h chip", 0)]
    for j, (first, size, _, _) in enumerate(plan):
        end = first + size
        events.append((first + size / 3 + 2, 0, j))
        events.append((end + 2, 2, j))
        events.append((min(1.86 * end, 0.68 * blocks + 0.6 * end) + 2, 1, j))
    events.sort(key=lambda e: e[0])
    order = [e[1:] for e in events]
    for j in range(len(plan)):
        at = max(order.index((k, j)) for k in (0, 1, 2))
        order.remove((1, j))
        order.insert(at, (1, j))
    return order


def folds_of(plan, first_end):
    folds, at = [], 0
    for j in (first_end // 3, 3 * first_end // 5):
        stop = sum(plan[j][:2]) // 2 - 1
        if j < first_end and stop > at:
            folds.append((j, at, stop))
            at = stop
    return folds


def split3(e):
    hi = e.astype(BF16)
    rest = e - hi.astype(F32)
    mid = rest.astype(BF16)
    low = (rest - mid.astype(F32)).astype(BF16)
    return hi, mid, low


def prefix_kernel(
    n_cols, h_ref, w_ref, temp_hbm, tgt_hbm,
    c_ref, coef_ref, factor_ref, tgt_out_ref,
    wbuf, hbuf, zbuf, tri, tri_last, stats, t_all, temp_col, rel_col, temp_ref, tgt_ref, zmsg, vmsg, back,
    ws, wr, xs, xr, ts, tr, wl, hl, hs, hr, zs, zr, vs, vr, rl,
):
    x, z, v = lax.axis_index("data"), lax.axis_index("hid"), lax.axis_index("vocab")
    rows, depth = h_ref.shape
    half, quarter = depth // 2, rows // 4
    tiles = tiles_of(n_cols // LANES)
    n_tiles = len(tiles)
    n_whole = sum(width == TILE for _, width in tiles)
    plan = chunks_of(n_cols // LANES)
    n_chunks = len(plan)
    ends = [[j for j, (first, *_) in enumerate(plan) if first * LANES < sum(tiles[t])][-1] for t in range(n_whole - 1, n_tiles)]
    first_end = ends[0] - 1

    side = z // 2
    outer_far, inner_far, near = 3 - 3 * side, 2 - side, 1 - z + 4 * side
    is_outer = jnp.where(z == side * 3, 1, 0)
    z_two, z_one = lax.rem(z + 2, 4), near
    v_two, v_one = lax.rem(v + 2, 4), v + 1 - 2 * lax.rem(v, 2)
    sources = (near, inner_far, outer_far)

    def cols_of(j):
        first, size, _, _ = plan[j]
        return first * LANES, size * LANES

    def w_rows(source, part, j=None):
        at, n = (0, half) if j is None else (plan[j][2] * (half // 2), plan[j][3] * (half // 2))
        return pl.ds(pl.multiple_of(source * depth + part * half + at, half // 2), n)

    def w_place(j, source, part):
        start, n = cols_of(j)
        return wbuf.at[w_rows(source, part, j), pl.ds(start, n)]

    def h_place(q, block=None):
        at = pl.ds(pl.multiple_of(q * quarter, quarter), quarter)
        if block is None:
            return hbuf.at[at]
        return hbuf.at[at, pl.ds(pl.multiple_of(block * depth, depth), depth)]

    def remote(src, dst, send, recv, **to):
        return pltpu.make_async_remote_copy(
            src_ref=src, dst_ref=dst, send_sem=send, recv_sem=recv, device_id=to, device_id_type=MESH
        )

    def w_source(j, part, dest):
        start, n = cols_of(j)
        return w_ref.at[w_rows(0, part, j), pl.ds(pl.multiple_of(dest * n_cols + start, LANES), n)]

    def arrival(j, from_inner):
        early = min(j, first_end)
        return early + from_inner * (first_end + 1 + j - early)

    def direct(j, k, dest, from_inner):
        return remote(w_source(j, x, dest), w_place(j, z, x), ws.at[k], wr.at[arrival(j, from_inner)], hid=dest)

    def send_near(j):
        return direct(j, 0, near, 0)

    odd = lax.rem(v, 2)
    far_first = outer_far + odd * (inner_far - outer_far)
    far_second = inner_far + odd * (outer_far - inner_far)

    def send_far(j, i):
        return direct(j, 1 + i, (far_first, far_second)[i], 1 - is_outer)

    def send_twin(i):
        dest = (far_first, far_second)[i]
        return remote(w_source(n_chunks - 1, 1 - x, dest), w_place(n_chunks - 1, z, 1 - x), ts.at[i], tr, hid=dest)

    def twin_landed():
        place = w_place(n_chunks - 1, inner_far, 1 - x)
        remote(place, place, ts.at[0], tr, hid=inner_far).wait_recv()

    def landed(j):
        place = w_place(j, inner_far, x)
        remote(place, place, ws.at[1], wr.at[arrival(j, 1)], hid=inner_far).wait_recv()

    def landed_pair(j):
        start, n = cols_of(j)
        place = wbuf.at[pl.ds(0, 2 * half), pl.ds(start, n if j < first_end else n_cols - start)]
        remote(place, place, ws.at[0], wr.at[arrival(j, 0)], hid=near).wait_recv()

    def forward(j, k):
        place = w_place(j, sources[k], x)
        send = 3 if k == 1 and j == n_chunks - 2 else k
        return remote(place, place, xs.at[send], xr.at[cross(j, k)], data=1 - x)

    def cross(j, k):
        if j < first_end:
            return j
        return first_end if k != 1 else 1 + j

    def cross_wait(slot, count, start, stop):
        place = wbuf.at[pl.ds(0, count), pl.ds(start, stop - start)]
        remote(place, place, xs.at[0], xr.at[slot], data=1 - x).wait_recv()

    def forwarded(j):
        place = w_place(j, inner_far, 1 - x)
        remote(place, place, xs.at[1], xr.at[cross(j, 1)], data=1 - x).wait_recv()

    def own(j):
        start, n = cols_of(j)
        return pltpu.make_async_copy(
            w_ref.at[:, pl.ds(pl.multiple_of(z * n_cols + start, LANES), n)],
            wbuf.at[pl.ds(pl.multiple_of(z * depth, depth), depth), pl.ds(start, n)],
            wl,
        )

    h_mine = h_ref.at[pl.ds(pl.multiple_of(v * quarter, quarter), quarter)]
    h_own = pltpu.make_async_copy(h_mine, h_place(v, z), hl)
    h_two = remote(h_mine, h_place(v, z), hs, hr.at[0], hid=z_two)
    h_one = remote(h_mine, h_place(v, z), hs, hr.at[1], hid=z_one)
    h_relay = remote(h_place(v, z_two), h_place(v, z_two), hs, hr.at[2], hid=z_one)
    h_chip = remote(h_place(v), h_place(v), hs, hr.at[3], vocab=v_two)
    h_core = remote(h_place(v), h_place(v), hs, hr.at[4], vocab=v_one)
    h_both = remote(h_place(v_two), h_place(v_two), hs, hr.at[5], vocab=v_one)

    def arrived(place, i, **frm):
        remote(place, place, hs, hr.at[i], **frm).wait_recv()

    barrier = pltpu.get_barrier_semaphore()
    peers = [{"hid": lax.rem(z + d, 4)} for d in (1, 2, 3)]
    peers += [{"data": 1 - x}] + [{"vocab": lax.rem(v + d, 4)} for d in (1, 2, 3)]
    for peer in peers:
        pl.semaphore_signal(barrier, inc=1, device_id=peer, device_id_type=MESH)
    row_copies = [
        pltpu.make_async_copy(temp_hbm, temp_ref, rl.at[0]),
        pltpu.make_async_copy(tgt_hbm, tgt_ref, rl.at[1]),
    ]
    for copy in (h_own, *row_copies):
        copy.start()
    for j in range(n_chunks):
        if plan[j][2] == 0:
            own(j).start()
    with jax.named_scope("bar"):
        pl.semaphore_wait(barrier, len(peers))

    h_two.start()
    h_one.start()
    send_near(0).start()
    send_far(0, 0).start()

    def ones_below(ref, width):
        k = lax.broadcasted_iota(jnp.int32, (width, width), 0)
        c = lax.broadcasted_iota(jnp.int32, (width, width), 1)
        block = jnp.where(k <= c, 1.0, 0.0).astype(BF16)
        for i in range(3):
            ref[pl.ds(i * width, width), :] = block

    ones_below(tri, TILE)
    ones_below(tri_last, LANES)
    base = (v * 4 + z) * n_cols
    for copy in row_copies:
        copy.wait()
    back[0:1, :] = temp_ref[...]
    back[1:2, :] = (tgt_ref[...] - base).astype(F32)
    cols8 = back[...].T
    temp_col[...] = jnp.broadcast_to(cols8[:, 0:1], temp_col.shape)
    rel_col[...] = jnp.broadcast_to(cols8[:, 1:2], rel_col.shape).astype(jnp.int32)
    slot = lax.broadcasted_iota(jnp.int32, stats.shape, 1)
    stats[...] = jnp.where(slot < SLOTS, LOWEST, 0.0)
    t_all[...] = jnp.zeros(t_all.shape, F32)

    with jax.named_scope("h0"):
        arrived(h_place(v, z_two), 0, hid=z_two)
    h_relay.start()
    send_far(0, 1).start()
    for j in range(1, n_chunks):
        send_near(j).start()
        send_far(j, 0).start()
        send_far(j, 1).start()

    @pl.when(is_outer == 0)
    def _():
        send_twin(0).start()
        send_twin(1).start()


    part, few = min(rows, 512), min(rows, 128)

    def logits_and_sums(product, sums):
        some = part if product is not None or sums[2] == TILE else min(rows, 2 * part)

        @pl.loop(0, rows // some)
        def _(i):
            if product is not None:
                _, new_start, new_width = product
                at = pl.ds(pl.multiple_of(i * part, part), part)
                new = jnp.dot(
                    hbuf[at, :], wbuf[:, pl.ds(new_start, new_width)], preferred_element_type=F32
                )
            for k in range(0, some, few) if sums is not None else ():
                prefix(pl.ds(pl.multiple_of(i * some + k, few), few), *sums)
            if product is not None:
                zbuf[at, 0:new_width] = new

    def prefix(at, t, start, width):
        pieces = width // LANES
        logits = zbuf[at, 0:width] * jnp.concatenate([temp_col[at, :]] * pieces, axis=1)
        lane = lax.broadcasted_iota(jnp.int32, (few, LANES), 1)
        top = jnp.max(logits, axis=1, keepdims=True)
        e = jnp.exp(logits - top)
        total = jnp.sum(e, axis=1, keepdims=True)
        stats[at, :] = jnp.where(lane == t, top, jnp.where(lane == SLOTS + t, total, stats[at, :]))
        table = tri if width == TILE else tri_last
        run = jnp.dot(jnp.concatenate(split3(e), axis=1), table[...], preferred_element_type=F32)
        c_ref[at, pl.ds(start, width)] = run
        rel = rel_col[at, :] - start
        hit = t_all[at, :]
        for p in range(pieces):
            hit += jnp.where(lane == rel - p * LANES, run[:, p * LANES : (p + 1) * LANES], 0.0)
        t_all[at, :] = hit

    def whole(t):
        return t, pl.multiple_of(t * TILE, TILE), TILE

    def compute(j):
        first, size = (n // 2 for n in plan[j][:2])
        stop = first + size
        if first == 0:
            logits_and_sums(whole(0), None)
            first = 1
        if first < stop:

            @pl.loop(first, stop)
            def _(t):
                logits_and_sums(whole(t), whole(t - 1))

        if j == first_end - 1:
            logits_and_sums(None, whole(stop - 1))

    def block_dot(at, block, start, width):
        lanes = pl.ds(pl.multiple_of(block * depth, depth), depth)
        return jnp.dot(hbuf[at, lanes], wbuf[lanes, start : start + width], preferred_element_type=F32)

    def begin_end(i):
        start, width = tiles[n_whole - 1 + i]

        @pl.loop(0, rows // part)
        def _(k):
            at = pl.ds(pl.multiple_of(k * part, part), part)
            c_ref[at, start : start + width] = (
                block_dot(at, z, start, width)
                + block_dot(at, near, start, width)
                + block_dot(at, outer_far, start, width)
            )

    def finish_end(i):
        t = n_whole - 1 + i
        start, width = tiles[t]
        every = slice(0, rows)
        zbuf[:, 0:width] = c_ref[:, start : start + width] + block_dot(every, inner_far, start, width)
        logits_and_sums(None, (t, start, width))

    def fold(g0, g1):
        @pl.loop(0, rows // few)
        def _(i):
            at = pl.ds(pl.multiple_of(i * few, few), few)
            lane = lax.broadcasted_iota(jnp.int32, (few, LANES), 1)
            group = (lane >= g0) & (lane < g1)
            m = stats[at, :]
            s = pltpu.roll(m, LANES - SLOTS, 1)
            top = jnp.max(jnp.where(group, m, LOWEST), axis=1, keepdims=True)
            shrink = jnp.where(group, jnp.exp(m - top), 0.0)
            parts = jnp.where(group, s, 0.0) * shrink
            before = prefix_before(parts)
            for t in range(g0, g1):
                span = slice(t * TILE, (t + 1) * TILE)
                c_ref[at, span] = c_ref[at, span] * shrink[:, t : t + 1] + before[:, t : t + 1]
            rel = rel_col[at, :]
            holds = (rel >= lane * TILE) & (rel < (lane + 1) * TILE)
            old = t_all[at, :]
            moved = jnp.sum(old, axis=1, keepdims=True) * shrink + before
            inside = (rel >= g0 * TILE) & (rel < g1 * TILE)
            t_all[at, :] = jnp.where(inside, jnp.where(holds, moved, 0.0), old)
            total = jnp.sum(parts, axis=1, keepdims=True)
            sums = jnp.where(lane == SLOTS + g1 - 1, total, 0.0)
            of_sums = (lane >= SLOTS + g0) & (lane < SLOTS + g1)
            stats[at, :] = jnp.where(group, top, jnp.where(of_sums, sums, m))

    def close(i):
        first = ends[i - 1] + 1 if i else first_end
        with jax.named_scope(f"xe{i}"):
            for j in range(first, ends[i] + 1):
                if j < n_chunks - 1:
                    forwarded(j)
                else:
                    twin_landed()
        with jax.named_scope(f"ce{i}"):
            finish_end(i)

    def prefix_before(parts):
        k = lax.broadcasted_iota(jnp.int32, (LANES, LANES), 0)
        c = lax.broadcasted_iota(jnp.int32, (LANES, LANES), 1)
        strict = jnp.where(k < c, 1.0, 0.0).astype(BF16)
        return sum(jnp.dot(p, strict, preferred_element_type=F32) for p in split3(parts))

    def complete(j):
        start, n = cols_of(j)
        cross_wait(j, 3 * half, start, start + n)

    def own_complete():
        place = wbuf.at[pl.ds(pl.multiple_of(z * depth, depth), depth)]
        pltpu.make_async_copy(place, place, wl).wait()

    order = service_order(plan, n_cols // LANES)
    folds = {j: (g0, g1) for j, g0, g1 in folds_of(plan, first_end)}
    tail = range(first_end, n_chunks)
    known = max(order.index((k, j)) for k in (0, 2) for j in tail)
    early = min(j for j in range(max(0, first_end - 7), n_chunks - 1) if order.index((1, j + 1)) > known)
    assert early < first_end
    m = len(ends) - 1
    closes = {n_chunks - 3: range(m - 2), n_chunks - 2: [m - 2], n_chunks - 1: [m - 1]}

    pairs = [e for e in order if e[0] == 2 and e[1] > first_end]
    order = [e for e in order if e[0] != 0 and e not in pairs]
    order.remove((2, first_end))
    order.insert(order.index((1, early + 1)), (2, first_end))

    for what, j in order:
        if what == "h line":
            with jax.named_scope("hline"):
                arrived(h_place(v, z_one), 1, hid=z_one)
                arrived(h_place(v, lax.rem(z_one + 2, 4)), 2, hid=z_one)
                h_own.wait()
            h_chip.start()
            h_core.start()
        elif what == "h chip":
            with jax.named_scope("hchip"):
                arrived(h_place(v_two), 3, vocab=v_two)
            h_both.start()
        else:
            with jax.named_scope(f"w{what}_{j}"):
                landed(j) if what == 1 else landed_pair(j)
            if what == 2:
                for i in range(j, j + 1 if j < first_end else n_chunks):
                    forward(i, 0).start()
                    forward(i, 2).start()
                continue
            if j < n_chunks - 1:
                forward(j, 1).start()
            if j == 1:
                with jax.named_scope("hcore"):
                    arrived(h_place(v_one), 4, vocab=v_one)
                    arrived(h_place(lax.rem(v_one + 2, 4)), 5, vocab=v_one)
                    own_complete()
            if 0 < j <= first_end:
                with jax.named_scope(f"x{j - 1}"):
                    complete(j - 1)
                with jax.named_scope(f"c{j - 1}"):
                    compute(j - 1)
                if j - 1 in folds:
                    with jax.named_scope(f"f{j - 1}"):
                        fold(*folds[j - 1])
            if j - 1 == early:
                with jax.named_scope("begin"):
                    cross_wait(first_end, 2 * half, cols_of(first_end)[0], n_cols)
                    for i in range(len(ends)):
                        begin_end(i)
            for i in closes.get(j, ()):
                close(i)
    close(m)

    lane = lax.broadcasted_iota(jnp.int32, (rows, LANES), 1)
    at_tgt = jnp.sum(t_all[...], axis=1, keepdims=True)
    turned = jnp.where(lane == 2 * SLOTS, at_tgt, stats[...]).T
    m, at_tgt = turned[0:SLOTS, :], turned[2 * SLOTS : 2 * SLOTS + 1, :]
    top = jnp.max(m, axis=0, keepdims=True)
    shrink = jnp.exp(m - top)
    parts = turned[SLOTS : 2 * SLOTS, :] * shrink
    t = lax.broadcasted_iota(jnp.int32, (SLOTS, rows), 0)
    start = jnp.where(t < n_whole, t * TILE, n_whole * (TILE - LANES) + t * LANES)
    stop = start + jnp.where(t < n_whole, TILE, LANES)
    rel = tgt_ref[...] - base
    known = rel < n_cols
    holds = (rel >= start) & (rel < stop) & known
    ahead = (stop <= rel) & known
    found = jnp.where(holds, at_tgt * shrink, jnp.where(ahead, parts, 0.0))
    zmsg[z, 0:1, :] = top
    zmsg[z, 1:2, :] = jnp.sum(parts, axis=0, keepdims=True)
    zmsg[z, 2:3, :] = jnp.sum(found, axis=0, keepdims=True)

    for k in range(3):
        mine = wbuf.at[w_rows(sources[k], x)]
        remote(mine, mine, ws.at[k], wr.at[0], hid=near).wait_send()
        if k == 1:
            mine = wbuf.at[w_rows(sources[k], x), pl.ds(0, n_cols - LANES)]
        remote(mine, mine, xs.at[k], xr.at[0], data=1 - x).wait_send()
    forward(n_chunks - 2, 1).wait_send()

    @pl.when(is_outer == 0)
    def _():
        send_twin(0).wait_send()
        send_twin(1).wait_send()

    mine = hbuf.at[pl.ds(0, quarter * 15 // 4)]
    remote(mine, mine, hs, hr.at[0], hid=near).wait_send()

    def z_send(i):
        return remote(zmsg.at[z], zmsg.at[z], zs, zr, hid=(near, inner_far, outer_far)[i])

    def v_send(d):
        to = lax.rem(v + d, 4)
        return remote(vmsg.at[v], vmsg.at[v], vs, vr, vocab=to)

    for i in (2, 1, 0):
        z_send(i).start()
    k = lax.broadcasted_iota(jnp.int32, (SLOTS, SLOTS), 0)
    c = lax.broadcasted_iota(jnp.int32, (SLOTS, SLOTS), 1)
    strict = jnp.where(c < k, 1.0, 0.0).astype(BF16)
    before = sum(jnp.dot(strict, p, preferred_element_type=F32) for p in split3(parts))
    rest = jnp.zeros((LANES - 2 * SLOTS, rows), F32)
    coef_ref[...] = jnp.concatenate([shrink, before, rest], axis=0).T
    z_all = remote(zmsg.at[pl.ds(0, 3)], zmsg.at[pl.ds(0, 3)], zs, zr, hid=near)
    with jax.named_scope("z"):
        z_all.wait_recv()

    ids = tgt_ref[...]
    maxes = [zmsg[h, 0:1, :] for h in range(4)]
    v_max = functools.reduce(jnp.maximum, maxes)
    v_sum = jnp.zeros((1, rows), F32)
    v_tgt = jnp.zeros((1, rows), F32)
    mine_before = jnp.zeros((1, rows), F32)
    for h in range(4):
        mine_before = jnp.where(h == z, v_sum, mine_before)
        f = jnp.exp(maxes[h] - v_max)
        low = (v * 4 + h) * n_cols
        inside = (ids >= low) & (ids < low + n_cols)
        v_tgt += jnp.where(inside, zmsg[h, 2:3, :] * f + v_sum, 0.0)
        v_sum += zmsg[h, 1:2, :] * f
    vmsg[v, 0:1, :] = v_max
    vmsg[v, 1:2, :] = v_sum
    vmsg[v, 2:3, :] = v_tgt

    z_all.wait_send()
    for d in (2, 1, 3):
        v_send(d).start()
    v_all = remote(vmsg.at[pl.ds(0, 3)], vmsg.at[pl.ds(0, 3)], vs, vr, vocab=v_one)
    with jax.named_scope("v"):
        v_all.wait_recv()

    maxes = [vmsg[u, 0:1, :] for u in range(4)]
    g_max = functools.reduce(jnp.maximum, maxes)
    g_sum = jnp.zeros((1, rows), F32)
    g_tgt = jnp.zeros((1, rows), F32)
    g_before = jnp.zeros((1, rows), F32)
    for u in range(4):
        f = jnp.exp(maxes[u] - g_max)
        g_before = jnp.where(u == v, g_sum + mine_before * f, g_before)
        low = u * 4 * n_cols
        inside = (ids >= low) & (ids < low + 4 * n_cols)
        g_tgt += jnp.where(inside, vmsg[u, 2:3, :] * f + g_sum, 0.0)
        g_sum += vmsg[u, 1:2, :] * f
    tgt_out_ref[...] = g_tgt / g_sum
    factor_ref[0:1, :] = jnp.exp(zmsg[z, 0:1, :] - g_max) / g_sum
    factor_ref[1:2, :] = g_before / g_sum
    v_all.wait_send()


def finish_kernel(tiles, lanes, c_ref, coef_ref, factor_ref, tgt_ref, out_ref, tgt_out_ref, buf, factor_col, sems, tgt_sem):
    slots, n, n_cols = buf.shape
    steps = c_ref.shape[0] // n
    tgt_copy = pltpu.make_async_copy(tgt_ref, tgt_out_ref, tgt_sem)
    tgt_copy.start()

    def put(i):
        slot = lax.rem(i, slots)
        at = pl.ds(pl.multiple_of(i * n, n), n)
        return pltpu.make_async_copy(buf.at[slot], out_ref.at[at], sems.at[slot])

    @pl.loop(0, steps)
    def _(i):
        slot = lax.rem(i, slots)

        @pl.when(i >= slots)
        def _():
            put(i - slots).wait()

        at = pl.ds(pl.multiple_of(i * n, n), n)
        turn = max(n, LANES)

        @pl.when(lax.rem(i, turn // n) == 0)
        def _():
            some = pl.ds(pl.multiple_of(i // (turn // n) * turn, turn), turn)
            factor_col[some, :] = factor_ref[:, some].T

        lane = lax.broadcasted_iota(jnp.int32, (n, LANES), 1)
        coef = coef_ref[at, :] * factor_col[at, 0:1] + jnp.where(lane < SLOTS, 0.0, factor_col[at, 1:2])
        for (start, width), k in zip(tiles, lanes):
            span = slice(start, start + width)
            buf[slot, :, span] = c_ref[at, span] * coef[:, k : k + 1] + coef[:, SLOTS + k : SLOTS + k + 1]
        put(i).start()

    tgt_copy.wait()
    for i in range(max(0, steps - slots), steps):
        with jax.named_scope(f"fe{i}"):
            put(i).wait()


def solution(mesh):
    n_hid, n_voc = mesh.shape["hid"], mesh.shape["vocab"]
    assert n_hid == 4 and n_voc == 4 and mesh.shape["data"] == 2

    def local_step(h_blk, w_blk, temp_blk, tgt_blk):
        rows, depth = h_blk.shape
        n_cols = w_blk.shape[1] // n_hid
        assert n_cols % LANES == 0
        tiles = tiles_of(n_cols // LANES)
        n_tiles = len(tiles)
        assert n_tiles <= SLOTS
        plan = chunks_of(n_cols // LANES)
        n_chunks = len(plan)
        last_whole = sum(width == TILE for _, width in tiles) - 1
        first_end = [first for first, *_ in plan].index(2 * last_whole)
        vmem = pl.BlockSpec(memory_space=pltpu.VMEM)
        hbm = pl.BlockSpec(memory_space=pltpu.HBM)
        dma = pltpu.SemaphoreType.DMA
        table = pltpu.VMEM((rows, LANES), F32)
        c, coef, factor, tgt = pl.pallas_call(
            functools.partial(prefix_kernel, n_cols),
            out_shape=(
                pltpu.VMEM((rows, n_cols), F32),
                pltpu.VMEM((rows, LANES), F32),
                pltpu.VMEM((8, rows), F32),
                pltpu.VMEM((1, rows), F32),
            ),
            in_specs=[hbm] * 4,
            out_specs=[vmem] * 4,
            scratch_shapes=[
                pltpu.VMEM((4 * depth, n_cols), BF16),
                pltpu.VMEM((rows, 4 * depth), BF16),
                pltpu.VMEM((rows, TILE), F32),
                pltpu.VMEM((3 * TILE, TILE), BF16),
                pltpu.VMEM((3 * LANES, LANES), BF16),
                table,
                table,
                table,
                pltpu.VMEM((rows, LANES), jnp.int32),
                pltpu.VMEM((1, rows), F32),
                pltpu.VMEM((1, rows), jnp.int32),
                pltpu.VMEM((4, 3, rows), F32),
                pltpu.VMEM((4, 3, rows), F32),
                pltpu.VMEM((8, rows), F32),
                dma((3,)),
                dma((first_end + 1 + n_chunks,)),
                dma((4,)),
                dma((n_chunks,)),
                dma((2,)),
                dma,
                dma,
                dma,
                dma,
                dma((6,)),
                dma,
                dma,
                dma,
                dma,
                dma((2,)),
            ],
            compiler_params=pltpu.CompilerParams(
                collective_id=0, has_side_effects=True, vmem_limit_bytes=37 << 20
            ),
            name="prefix",
        )(h_blk, w_blk, temp_blk.reshape(1, rows), tgt_blk.reshape(1, rows))
        n = min(rows, 64)
        lanes = list(range(n_tiles))
        for _, g0, g1 in folds_of(plan, first_end):
            lanes[g0:g1] = [g0] * (g1 - g0)
        cdf, cdf_tgt = pl.pallas_call(
            functools.partial(finish_kernel, tiles, lanes),
            out_shape=(
                jax.ShapeDtypeStruct((rows, n_cols), F32),
                jax.ShapeDtypeStruct((1, rows), F32),
            ),
            in_specs=[vmem] * 4,
            out_specs=[hbm, hbm],
            scratch_shapes=[
                pltpu.VMEM((4, n, n_cols), F32),
                pltpu.VMEM((rows, 8), F32),
                dma((4,)),
                dma,
            ],
            compiler_params=pltpu.CompilerParams(vmem_limit_bytes=9 << 20),
            name="finish",
        )(c, coef, factor, tgt)
        return cdf, cdf_tgt.reshape(rows)

    return jax.shard_map(
        local_step,
        mesh=mesh,
        in_specs=(P("data", "hid"), P("hid", "vocab"), P("data"), P("data")),
        out_specs=(P("data", ("vocab", "hid")), P("data")),
        check_vma=False,
    )
```

```python
import functools

import jax
import jax.numpy as jnp
from jax import lax
from jax.experimental import pallas as pl
from jax.experimental.pallas import tpu as pltpu
from jax.sharding import PartitionSpec as P

MESH = pl.DeviceIdType.MESH
F32 = jnp.float32
BF16 = jnp.bfloat16
TILE = 256
LANES = 128
SLOTS = 32
LOWEST = float(jnp.finfo(jnp.float32).min)


def tiles_of(blocks):
    whole = (blocks - 3) // 2
    tiles = [(t * TILE, TILE) for t in range(whole)]
    return tiles + [(b * LANES, LANES) for b in range(2 * whole, blocks)]


def chunks_of(blocks):
    whole = (blocks - 3) // 2
    sizes, left = [], 2 * whole - 2
    for size in (2, 2, 2, 2, 4, 4):
        if left > size:
            sizes.append(size)
            left -= size
    while left > 0:
        sizes.append(min(6, left))
        left -= sizes[-1]
    plan, at = [], 0
    for size in reversed(sizes):
        plan.append((at, size, 0, 2))
        at += size
    plan += [(b, 1, 0, 2) for b in range(at, blocks - 2)]
    return plan + [(b, 1, r, 1) for b in (blocks - 2, blocks - 1) for r in (0, 1)]


def service_order(plan, blocks):
    events = [(0.15 * blocks, "h line", 0), (0.28 * blocks, "h chip", 0)]
    for j, (first, size, _, _) in enumerate(plan):
        end = first + size
        events.append((first + size / 3 + 2, 0, j))
        events.append((end + 2, 2, j))
        events.append((min(1.86 * end, 0.68 * blocks + 0.6 * end) + 2, 1, j))
    events.sort(key=lambda e: e[0])
    order = [e[1:] for e in events]
    for j in range(len(plan)):
        at = max(order.index((k, j)) for k in (0, 1, 2))
        order.remove((1, j))
        order.insert(at, (1, j))
    return order


def folds_of(plan, first_end):
    folds, at = [], 0
    for j in (first_end // 3, 3 * first_end // 5):
        stop = sum(plan[j][:2]) // 2 - 1
        if j < first_end and stop > at:
            folds.append((j, at, stop))
            at = stop
    return folds


def split3(e):
    hi = e.astype(BF16)
    rest = e - hi.astype(F32)
    mid = rest.astype(BF16)
    low = (rest - mid.astype(F32)).astype(BF16)
    return hi, mid, low


def prefix_kernel(
    n_cols, h_ref, w_ref, temp_hbm, tgt_hbm,
    c_ref, coef_ref, factor_ref, tgt_out_ref,
    wbuf, hbuf, zbuf, tri, tri_last, stats, t_all, temp_col, rel_col, temp_ref, tgt_ref, zmsg, vmsg, back,
    ws, wr, xs, xr, ts, tr, wl, hl, hs, hr, zs, zr, vs, vr, rl,
):
    x, z, v = lax.axis_index("data"), lax.axis_index("hid"), lax.axis_index("vocab")
    rows, depth = h_ref.shape
    half, quarter = depth // 2, rows // 4
    tiles = tiles_of(n_cols // LANES)
    n_tiles = len(tiles)
    n_whole = sum(width == TILE for _, width in tiles)
    plan = chunks_of(n_cols // LANES)
    n_chunks = len(plan)
    ends = [[j for j, (first, *_) in enumerate(plan) if first * LANES < sum(tiles[t])][-1] for t in range(n_whole - 1, n_tiles)]
    first_end = ends[0] - 1

    side = z // 2
    outer_far, inner_far, near = 3 - 3 * side, 2 - side, 1 - z + 4 * side
    is_outer = jnp.where(z == side * 3, 1, 0)
    z_two, z_one = lax.rem(z + 2, 4), near
    v_two, v_one = lax.rem(v + 2, 4), v + 1 - 2 * lax.rem(v, 2)
    sources = (near, inner_far, outer_far)

    def cols_of(j):
        first, size, _, _ = plan[j]
        return first * LANES, size * LANES

    def w_rows(source, part, j=None):
        at, n = (0, half) if j is None else (plan[j][2] * (half // 2), plan[j][3] * (half // 2))
        return pl.ds(pl.multiple_of(source * depth + part * half + at, half // 2), n)

    def w_place(j, source, part):
        start, n = cols_of(j)
        return wbuf.at[w_rows(source, part, j), pl.ds(start, n)]

    def h_place(q, block=None):
        at = pl.ds(pl.multiple_of(q * quarter, quarter), quarter)
        if block is None:
            return hbuf.at[at]
        return hbuf.at[at, pl.ds(pl.multiple_of(block * depth, depth), depth)]

    def remote(src, dst, send, recv, **to):
        return pltpu.make_async_remote_copy(
            src_ref=src, dst_ref=dst, send_sem=send, recv_sem=recv, device_id=to, device_id_type=MESH
        )

    def w_source(j, part, dest):
        start, n = cols_of(j)
        return w_ref.at[w_rows(0, part, j), pl.ds(pl.multiple_of(dest * n_cols + start, LANES), n)]

    def direct(j, k, dest, slot):
        return remote(w_source(j, x, dest), w_place(j, z, x), ws.at[k], wr.at[j, slot], hid=dest)

    def send_near(j):
        return direct(j, 0, near, 0)

    odd = lax.rem(v, 2)
    far_first = outer_far + odd * (inner_far - outer_far)
    far_second = inner_far + odd * (outer_far - inner_far)

    def send_far(j, i):
        return direct(j, 1 + i, (far_first, far_second)[i], 1 + is_outer)

    def send_twin(i):
        dest = (far_first, far_second)[i]
        return remote(w_source(n_chunks - 1, 1 - x, dest), w_place(n_chunks - 1, z, 1 - x), ts.at[i], tr, hid=dest)

    def twin_landed():
        place = w_place(n_chunks - 1, inner_far, 1 - x)
        remote(place, place, ts.at[0], tr, hid=inner_far).wait_recv()

    def landed(j, k):
        place = w_place(j, sources[k], x)
        remote(place, place, ws.at[k], wr.at[j, k], hid=sources[k]).wait_recv()

    def forward(j, k):
        place = w_place(j, sources[k], x)
        send = 3 if k == 1 and j == n_chunks - 2 else k
        return remote(place, place, xs.at[send], xr.at[cross(j, k)], data=1 - x)

    def cross(j, k):
        if j < first_end:
            return j
        return first_end if k != 1 else 1 + j

    def cross_wait(slot, count, start, stop):
        place = wbuf.at[pl.ds(0, count), pl.ds(start, stop - start)]
        remote(place, place, xs.at[0], xr.at[slot], data=1 - x).wait_recv()

    def forwarded(j):
        place = w_place(j, inner_far, 1 - x)
        remote(place, place, xs.at[1], xr.at[cross(j, 1)], data=1 - x).wait_recv()

    def own(j):
        start, n = cols_of(j)
        return pltpu.make_async_copy(
            w_ref.at[:, pl.ds(pl.multiple_of(z * n_cols + start, LANES), n)],
            wbuf.at[pl.ds(pl.multiple_of(z * depth, depth), depth), pl.ds(start, n)],
            wl,
        )

    h_mine = h_ref.at[pl.ds(pl.multiple_of(v * quarter, quarter), quarter)]
    h_own = pltpu.make_async_copy(h_mine, h_place(v, z), hl)
    h_two = remote(h_mine, h_place(v, z), hs, hr.at[0], hid=z_two)
    h_one = remote(h_mine, h_place(v, z), hs, hr.at[1], hid=z_one)
    h_relay = remote(h_place(v, z_two), h_place(v, z_two), hs, hr.at[2], hid=z_one)
    h_chip = remote(h_place(v), h_place(v), hs, hr.at[3], vocab=v_two)
    h_core = remote(h_place(v), h_place(v), hs, hr.at[4], vocab=v_one)
    h_both = remote(h_place(v_two), h_place(v_two), hs, hr.at[5], vocab=v_one)

    def arrived(place, i, **frm):
        remote(place, place, hs, hr.at[i], **frm).wait_recv()

    barrier = pltpu.get_barrier_semaphore()
    peers = [{"hid": lax.rem(z + d, 4)} for d in (1, 2, 3)]
    peers += [{"data": 1 - x}] + [{"vocab": lax.rem(v + d, 4)} for d in (1, 2, 3)]
    for peer in peers:
        pl.semaphore_signal(barrier, inc=1, device_id=peer, device_id_type=MESH)
    row_copies = [
        pltpu.make_async_copy(temp_hbm, temp_ref, rl.at[0]),
        pltpu.make_async_copy(tgt_hbm, tgt_ref, rl.at[1]),
    ]
    for copy in (h_own, *row_copies):
        copy.start()
    for j in range(n_chunks):
        if plan[j][2] == 0:
            own(j).start()
    with jax.named_scope("bar"):
        pl.semaphore_wait(barrier, len(peers))

    h_two.start()
    h_one.start()
    send_near(0).start()
    send_far(0, 0).start()

    def ones_below(ref, width):
        k = lax.broadcasted_iota(jnp.int32, (width, width), 0)
        c = lax.broadcasted_iota(jnp.int32, (width, width), 1)
        block = jnp.where(k <= c, 1.0, 0.0).astype(BF16)
        for i in range(3):
            ref[pl.ds(i * width, width), :] = block

    ones_below(tri, TILE)
    ones_below(tri_last, LANES)
    base = (v * 4 + z) * n_cols
    for copy in row_copies:
        copy.wait()
    back[0:1, :] = temp_ref[...]
    back[1:2, :] = (tgt_ref[...] - base).astype(F32)
    cols8 = back[...].T
    temp_col[...] = jnp.broadcast_to(cols8[:, 0:1], temp_col.shape)
    rel_col[...] = jnp.broadcast_to(cols8[:, 1:2], rel_col.shape).astype(jnp.int32)
    slot = lax.broadcasted_iota(jnp.int32, stats.shape, 1)
    stats[...] = jnp.where(slot < SLOTS, LOWEST, 0.0)
    t_all[...] = jnp.zeros(t_all.shape, F32)

    with jax.named_scope("h0"):
        arrived(h_place(v, z_two), 0, hid=z_two)
    h_relay.start()
    send_far(0, 1).start()
    for j in range(1, n_chunks):
        send_near(j).start()
        send_far(j, 0).start()
        send_far(j, 1).start()

    @pl.when(is_outer == 0)
    def _():
        send_twin(0).start()
        send_twin(1).start()


    part, few = min(rows, 512), min(rows, 128)

    def logits_and_sums(product, sums):
        some = part if product is not None or sums[2] == TILE else min(rows, 2 * part)

        @pl.loop(0, rows // some)
        def _(i):
            if product is not None:
                _, new_start, new_width = product
                at = pl.ds(pl.multiple_of(i * part, part), part)
                new = jnp.dot(
                    hbuf[at, :], wbuf[:, pl.ds(new_start, new_width)], preferred_element_type=F32
                )
            for k in range(0, some, few) if sums is not None else ():
                prefix(pl.ds(pl.multiple_of(i * some + k, few), few), *sums)
            if product is not None:
                zbuf[at, 0:new_width] = new

    def prefix(at, t, start, width):
        pieces = width // LANES
        logits = zbuf[at, 0:width] * jnp.concatenate([temp_col[at, :]] * pieces, axis=1)
        lane = lax.broadcasted_iota(jnp.int32, (few, LANES), 1)
        top = jnp.max(logits, axis=1, keepdims=True)
        e = jnp.exp(logits - top)
        total = jnp.sum(e, axis=1, keepdims=True)
        stats[at, :] = jnp.where(lane == t, top, jnp.where(lane == SLOTS + t, total, stats[at, :]))
        table = tri if width == TILE else tri_last
        run = jnp.dot(jnp.concatenate(split3(e), axis=1), table[...], preferred_element_type=F32)
        c_ref[at, pl.ds(start, width)] = run
        rel = rel_col[at, :] - start
        hit = t_all[at, :]
        for p in range(pieces):
            hit += jnp.where(lane == rel - p * LANES, run[:, p * LANES : (p + 1) * LANES], 0.0)
        t_all[at, :] = hit

    def whole(t):
        return t, pl.multiple_of(t * TILE, TILE), TILE

    def compute(j):
        first, size = (n // 2 for n in plan[j][:2])
        stop = first + size
        if first == 0:
            logits_and_sums(whole(0), None)
            first = 1
        if first < stop:

            @pl.loop(first, stop)
            def _(t):
                logits_and_sums(whole(t), whole(t - 1))

        if j == first_end - 1:
            logits_and_sums(None, whole(stop - 1))

    def block_dot(at, block, start, width):
        lanes = pl.ds(pl.multiple_of(block * depth, depth), depth)
        return jnp.dot(hbuf[at, lanes], wbuf[lanes, start : start + width], preferred_element_type=F32)

    def begin_end(i):
        start, width = tiles[n_whole - 1 + i]

        @pl.loop(0, rows // part)
        def _(k):
            at = pl.ds(pl.multiple_of(k * part, part), part)
            c_ref[at, start : start + width] = (
                block_dot(at, z, start, width)
                + block_dot(at, near, start, width)
                + block_dot(at, outer_far, start, width)
            )

    def finish_end(i):
        t = n_whole - 1 + i
        start, width = tiles[t]
        every = slice(0, rows)
        zbuf[:, 0:width] = c_ref[:, start : start + width] + block_dot(every, inner_far, start, width)
        logits_and_sums(None, (t, start, width))

    def fold(g0, g1):
        @pl.loop(0, rows // few)
        def _(i):
            at = pl.ds(pl.multiple_of(i * few, few), few)
            lane = lax.broadcasted_iota(jnp.int32, (few, LANES), 1)
            group = (lane >= g0) & (lane < g1)
            m = stats[at, :]
            s = pltpu.roll(m, LANES - SLOTS, 1)
            top = jnp.max(jnp.where(group, m, LOWEST), axis=1, keepdims=True)
            shrink = jnp.where(group, jnp.exp(m - top), 0.0)
            parts = jnp.where(group, s, 0.0) * shrink
            before = prefix_before(parts)
            for t in range(g0, g1):
                span = slice(t * TILE, (t + 1) * TILE)
                c_ref[at, span] = c_ref[at, span] * shrink[:, t : t + 1] + before[:, t : t + 1]
            rel = rel_col[at, :]
            holds = (rel >= lane * TILE) & (rel < (lane + 1) * TILE)
            old = t_all[at, :]
            moved = jnp.sum(old, axis=1, keepdims=True) * shrink + before
            inside = (rel >= g0 * TILE) & (rel < g1 * TILE)
            t_all[at, :] = jnp.where(inside, jnp.where(holds, moved, 0.0), old)
            total = jnp.sum(parts, axis=1, keepdims=True)
            sums = jnp.where(lane == SLOTS + g1 - 1, total, 0.0)
            of_sums = (lane >= SLOTS + g0) & (lane < SLOTS + g1)
            stats[at, :] = jnp.where(group, top, jnp.where(of_sums, sums, m))

    def close(i):
        first = ends[i - 1] + 1 if i else first_end
        with jax.named_scope(f"xe{i}"):
            for j in range(first, ends[i] + 1):
                if j < n_chunks - 1:
                    forwarded(j)
                else:
                    twin_landed()
        with jax.named_scope(f"ce{i}"):
            finish_end(i)

    def prefix_before(parts):
        k = lax.broadcasted_iota(jnp.int32, (LANES, LANES), 0)
        c = lax.broadcasted_iota(jnp.int32, (LANES, LANES), 1)
        strict = jnp.where(k < c, 1.0, 0.0).astype(BF16)
        return sum(jnp.dot(p, strict, preferred_element_type=F32) for p in split3(parts))

    def complete(j):
        start, n = cols_of(j)
        cross_wait(j, 3 * half, start, start + n)

    def own_complete():
        place = wbuf.at[pl.ds(pl.multiple_of(z * depth, depth), depth)]
        pltpu.make_async_copy(place, place, wl).wait()

    order = service_order(plan, n_cols // LANES)
    folds = {j: (g0, g1) for j, g0, g1 in folds_of(plan, first_end)}
    tail = range(first_end, n_chunks)
    known = max(order.index((k, j)) for k in (0, 2) for j in tail)
    early = min(j for j in range(max(0, first_end - 7), n_chunks - 1) if order.index((1, j + 1)) > known)
    assert early < first_end
    m = len(ends) - 1
    closes = {n_chunks - 3: range(m - 2), n_chunks - 2: [m - 2], n_chunks - 1: [m - 1]}

    for what, j in order:
        if what == "h line":
            with jax.named_scope("hline"):
                arrived(h_place(v, z_one), 1, hid=z_one)
                arrived(h_place(v, lax.rem(z_one + 2, 4)), 2, hid=z_one)
                h_own.wait()
            h_chip.start()
            h_core.start()
        elif what == "h chip":
            with jax.named_scope("hchip"):
                arrived(h_place(v_two), 3, vocab=v_two)
            h_both.start()
        else:
            with jax.named_scope(f"w{what}_{j}"):
                landed(j, what)
            if (what, j) != (1, n_chunks - 1):
                forward(j, what).start()
            if what != 1:
                continue
            if j == 1:
                with jax.named_scope("hcore"):
                    arrived(h_place(v_one), 4, vocab=v_one)
                    arrived(h_place(lax.rem(v_one + 2, 4)), 5, vocab=v_one)
                    own_complete()
            if 0 < j <= first_end:
                with jax.named_scope(f"x{j - 1}"):
                    complete(j - 1)
                with jax.named_scope(f"c{j - 1}"):
                    compute(j - 1)
                if j - 1 in folds:
                    with jax.named_scope(f"f{j - 1}"):
                        fold(*folds[j - 1])
            if j - 1 == early:
                with jax.named_scope("begin"):
                    cross_wait(first_end, 2 * half, cols_of(first_end)[0], n_cols)
                    for i in range(len(ends)):
                        begin_end(i)
            for i in closes.get(j, ()):
                close(i)
    close(m)

    lane = lax.broadcasted_iota(jnp.int32, (rows, LANES), 1)
    at_tgt = jnp.sum(t_all[...], axis=1, keepdims=True)
    turned = jnp.where(lane == 2 * SLOTS, at_tgt, stats[...]).T
    m, at_tgt = turned[0:SLOTS, :], turned[2 * SLOTS : 2 * SLOTS + 1, :]
    top = jnp.max(m, axis=0, keepdims=True)
    shrink = jnp.exp(m - top)
    parts = turned[SLOTS : 2 * SLOTS, :] * shrink
    t = lax.broadcasted_iota(jnp.int32, (SLOTS, rows), 0)
    start = jnp.where(t < n_whole, t * TILE, n_whole * (TILE - LANES) + t * LANES)
    stop = start + jnp.where(t < n_whole, TILE, LANES)
    rel = tgt_ref[...] - base
    known = rel < n_cols
    holds = (rel >= start) & (rel < stop) & known
    ahead = (stop <= rel) & known
    found = jnp.where(holds, at_tgt * shrink, jnp.where(ahead, parts, 0.0))
    zmsg[z, 0:1, :] = top
    zmsg[z, 1:2, :] = jnp.sum(parts, axis=0, keepdims=True)
    zmsg[z, 2:3, :] = jnp.sum(found, axis=0, keepdims=True)

    for k in range(3):
        mine = wbuf.at[w_rows(sources[k], x)]
        remote(mine, mine, ws.at[k], wr.at[0, k], hid=near).wait_send()
        if k == 1:
            mine = wbuf.at[w_rows(sources[k], x), pl.ds(0, n_cols - LANES)]
        remote(mine, mine, xs.at[k], xr.at[0], data=1 - x).wait_send()
    forward(n_chunks - 2, 1).wait_send()

    @pl.when(is_outer == 0)
    def _():
        send_twin(0).wait_send()
        send_twin(1).wait_send()

    mine = hbuf.at[pl.ds(0, quarter * 15 // 4)]
    remote(mine, mine, hs, hr.at[0], hid=near).wait_send()

    def z_send(i):
        return remote(zmsg.at[z], zmsg.at[z], zs, zr, hid=(near, inner_far, outer_far)[i])

    def v_send(d):
        to = lax.rem(v + d, 4)
        return remote(vmsg.at[v], vmsg.at[v], vs, vr, vocab=to)

    for i in (2, 1, 0):
        z_send(i).start()
    k = lax.broadcasted_iota(jnp.int32, (SLOTS, SLOTS), 0)
    c = lax.broadcasted_iota(jnp.int32, (SLOTS, SLOTS), 1)
    strict = jnp.where(c < k, 1.0, 0.0).astype(BF16)
    before = sum(jnp.dot(strict, p, preferred_element_type=F32) for p in split3(parts))
    rest = jnp.zeros((LANES - 2 * SLOTS, rows), F32)
    coef_ref[...] = jnp.concatenate([shrink, before, rest], axis=0).T
    z_all = remote(zmsg.at[pl.ds(0, 3)], zmsg.at[pl.ds(0, 3)], zs, zr, hid=near)
    with jax.named_scope("z"):
        z_all.wait_recv()

    ids = tgt_ref[...]
    maxes = [zmsg[h, 0:1, :] for h in range(4)]
    v_max = functools.reduce(jnp.maximum, maxes)
    v_sum = jnp.zeros((1, rows), F32)
    v_tgt = jnp.zeros((1, rows), F32)
    mine_before = jnp.zeros((1, rows), F32)
    for h in range(4):
        mine_before = jnp.where(h == z, v_sum, mine_before)
        f = jnp.exp(maxes[h] - v_max)
        low = (v * 4 + h) * n_cols
        inside = (ids >= low) & (ids < low + n_cols)
        v_tgt += jnp.where(inside, zmsg[h, 2:3, :] * f + v_sum, 0.0)
        v_sum += zmsg[h, 1:2, :] * f
    vmsg[v, 0:1, :] = v_max
    vmsg[v, 1:2, :] = v_sum
    vmsg[v, 2:3, :] = v_tgt

    z_all.wait_send()
    for d in (2, 1, 3):
        v_send(d).start()
    v_all = remote(vmsg.at[pl.ds(0, 3)], vmsg.at[pl.ds(0, 3)], vs, vr, vocab=v_one)
    with jax.named_scope("v"):
        v_all.wait_recv()

    maxes = [vmsg[u, 0:1, :] for u in range(4)]
    g_max = functools.reduce(jnp.maximum, maxes)
    g_sum = jnp.zeros((1, rows), F32)
    g_tgt = jnp.zeros((1, rows), F32)
    g_before = jnp.zeros((1, rows), F32)
    for u in range(4):
        f = jnp.exp(maxes[u] - g_max)
        g_before = jnp.where(u == v, g_sum + mine_before * f, g_before)
        low = u * 4 * n_cols
        inside = (ids >= low) & (ids < low + 4 * n_cols)
        g_tgt += jnp.where(inside, vmsg[u, 2:3, :] * f + g_sum, 0.0)
        g_sum += vmsg[u, 1:2, :] * f
    tgt_out_ref[...] = g_tgt / g_sum
    factor_ref[0:1, :] = jnp.exp(zmsg[z, 0:1, :] - g_max) / g_sum
    factor_ref[1:2, :] = g_before / g_sum
    v_all.wait_send()


def finish_kernel(tiles, lanes, c_ref, coef_ref, factor_ref, tgt_ref, out_ref, tgt_out_ref, buf, factor_col, sems, tgt_sem):
    slots, n, n_cols = buf.shape
    steps = c_ref.shape[0] // n
    tgt_copy = pltpu.make_async_copy(tgt_ref, tgt_out_ref, tgt_sem)
    tgt_copy.start()

    def put(i):
        slot = lax.rem(i, slots)
        at = pl.ds(pl.multiple_of(i * n, n), n)
        return pltpu.make_async_copy(buf.at[slot], out_ref.at[at], sems.at[slot])

    @pl.loop(0, steps)
    def _(i):
        slot = lax.rem(i, slots)

        @pl.when(i >= slots)
        def _():
            put(i - slots).wait()

        at = pl.ds(pl.multiple_of(i * n, n), n)
        turn = max(n, LANES)

        @pl.when(lax.rem(i, turn // n) == 0)
        def _():
            some = pl.ds(pl.multiple_of(i // (turn // n) * turn, turn), turn)
            factor_col[some, :] = factor_ref[:, some].T

        lane = lax.broadcasted_iota(jnp.int32, (n, LANES), 1)
        coef = coef_ref[at, :] * factor_col[at, 0:1] + jnp.where(lane < SLOTS, 0.0, factor_col[at, 1:2])
        for (start, width), k in zip(tiles, lanes):
            span = slice(start, start + width)
            buf[slot, :, span] = c_ref[at, span] * coef[:, k : k + 1] + coef[:, SLOTS + k : SLOTS + k + 1]
        put(i).start()

    tgt_copy.wait()
    for i in range(max(0, steps - slots), steps):
        with jax.named_scope(f"fe{i}"):
            put(i).wait()


def solution(mesh):
    n_hid, n_voc = mesh.shape["hid"], mesh.shape["vocab"]
    assert n_hid == 4 and n_voc == 4 and mesh.shape["data"] == 2

    def local_step(h_blk, w_blk, temp_blk, tgt_blk):
        rows, depth = h_blk.shape
        n_cols = w_blk.shape[1] // n_hid
        assert n_cols % LANES == 0
        tiles = tiles_of(n_cols // LANES)
        n_tiles = len(tiles)
        assert n_tiles <= SLOTS
        plan = chunks_of(n_cols // LANES)
        n_chunks = len(plan)
        last_whole = sum(width == TILE for _, width in tiles) - 1
        first_end = [first for first, *_ in plan].index(2 * last_whole)
        vmem = pl.BlockSpec(memory_space=pltpu.VMEM)
        hbm = pl.BlockSpec(memory_space=pltpu.HBM)
        dma = pltpu.SemaphoreType.DMA
        table = pltpu.VMEM((rows, LANES), F32)
        c, coef, factor, tgt = pl.pallas_call(
            functools.partial(prefix_kernel, n_cols),
            out_shape=(
                pltpu.VMEM((rows, n_cols), F32),
                pltpu.VMEM((rows, LANES), F32),
                pltpu.VMEM((8, rows), F32),
                pltpu.VMEM((1, rows), F32),
            ),
            in_specs=[hbm] * 4,
            out_specs=[vmem] * 4,
            scratch_shapes=[
                pltpu.VMEM((4 * depth, n_cols), BF16),
                pltpu.VMEM((rows, 4 * depth), BF16),
                pltpu.VMEM((rows, TILE), F32),
                pltpu.VMEM((3 * TILE, TILE), BF16),
                pltpu.VMEM((3 * LANES, LANES), BF16),
                table,
                table,
                table,
                pltpu.VMEM((rows, LANES), jnp.int32),
                pltpu.VMEM((1, rows), F32),
                pltpu.VMEM((1, rows), jnp.int32),
                pltpu.VMEM((4, 3, rows), F32),
                pltpu.VMEM((4, 3, rows), F32),
                pltpu.VMEM((8, rows), F32),
                dma((3,)),
                dma((n_chunks, 3)),
                dma((4,)),
                dma((n_chunks,)),
                dma((2,)),
                dma,
                dma,
                dma,
                dma,
                dma((6,)),
                dma,
                dma,
                dma,
                dma,
                dma((2,)),
            ],
            compiler_params=pltpu.CompilerParams(
                collective_id=0, has_side_effects=True, vmem_limit_bytes=37 << 20
            ),
            name="prefix",
        )(h_blk, w_blk, temp_blk.reshape(1, rows), tgt_blk.reshape(1, rows))
        n = min(rows, 64)
        lanes = list(range(n_tiles))
        for _, g0, g1 in folds_of(plan, first_end):
            lanes[g0:g1] = [g0] * (g1 - g0)
        cdf, cdf_tgt = pl.pallas_call(
            functools.partial(finish_kernel, tiles, lanes),
            out_shape=(
                jax.ShapeDtypeStruct((rows, n_cols), F32),
                jax.ShapeDtypeStruct((1, rows), F32),
            ),
            in_specs=[vmem] * 4,
            out_specs=[hbm, hbm],
            scratch_shapes=[
                pltpu.VMEM((4, n, n_cols), F32),
                pltpu.VMEM((rows, 8), F32),
                dma((4,)),
                dma,
            ],
            compiler_params=pltpu.CompilerParams(vmem_limit_bytes=9 << 20),
            name="finish",
        )(c, coef, factor, tgt)
        return cdf, cdf_tgt.reshape(rows)

    return jax.shard_map(
        local_step,
        mesh=mesh,
        in_specs=(P("data", "hid"), P("hid", "vocab"), P("data"), P("data")),
        out_specs=(P("data", ("vocab", "hid")), P("data")),
        check_vma=False,
    )
```

```python
import functools

import jax
import jax.numpy as jnp
from jax import lax
from jax.experimental import pallas as pl
from jax.experimental.pallas import tpu as pltpu
from jax.sharding import PartitionSpec as P

MESH = pl.DeviceIdType.MESH
F32 = jnp.float32
BF16 = jnp.bfloat16
TILE = 256
LANES = 128
SLOTS = 32
LOWEST = float(jnp.finfo(jnp.float32).min)


def tiles_of(blocks):
    whole = (blocks - 3) // 2
    tiles = [(t * TILE, TILE) for t in range(whole)]
    return tiles + [(b * LANES, LANES) for b in range(2 * whole, blocks)]


def chunks_of(blocks):
    whole = (blocks - 3) // 2
    sizes, left = [], 2 * whole - 2
    for size in (2, 2, 2, 2, 4, 4):
        if left > size:
            sizes.append(size)
            left -= size
    while left > 0:
        sizes.append(min(6, left))
        left -= sizes[-1]
    plan, at = [], 0
    for size in reversed(sizes):
        plan.append((at, size, 0, 2))
        at += size
    plan += [(b, 1, 0, 2) for b in range(at, blocks - 2)]
    return plan + [(b, 1, r, 1) for b in (blocks - 2, blocks - 1) for r in (0, 1)]


def service_order(plan, blocks):
    events = [(0.15 * blocks, "h line", 0), (0.28 * blocks, "h chip", 0)]
    for j, (first, size, _, _) in enumerate(plan):
        end = first + size
        events.append((first + size / 3 + 2, 0, j))
        events.append((end + 2, 2, j))
        events.append((min(1.86 * end, 0.68 * blocks + 0.6 * end) + 2, 1, j))
    events.sort(key=lambda e: e[0])
    order = [e[1:] for e in events]
    for j in range(len(plan)):
        at = max(order.index((k, j)) for k in (0, 1, 2))
        order.remove((1, j))
        order.insert(at, (1, j))
    return order


def folds_of(plan, first_end):
    folds, at = [], 0
    for j in (first_end // 3, 3 * first_end // 5):
        stop = sum(plan[j][:2]) // 2 - 1
        if j < first_end and stop > at:
            folds.append((j, at, stop))
            at = stop
    return folds


def split3(e):
    hi = e.astype(BF16)
    rest = e - hi.astype(F32)
    mid = rest.astype(BF16)
    low = (rest - mid.astype(F32)).astype(BF16)
    return hi, mid, low


def prefix_kernel(
    n_cols, h_ref, w_ref, temp_hbm, tgt_hbm,
    c_ref, coef_ref, factor_ref, tgt_out_ref,
    wbuf, hbuf, zbuf, tri, tri_last, stats, t_all, temp_col, rel_col, temp_ref, tgt_ref, zmsg, vmsg, back,
    ws, wr, xs, xr, ts, tr, wl, hl, hs, hr, zs, zr, vs, vr, rl,
):
    x, z, v = lax.axis_index("data"), lax.axis_index("hid"), lax.axis_index("vocab")
    rows, depth = h_ref.shape
    half, quarter = depth // 2, rows // 4
    tiles = tiles_of(n_cols // LANES)
    n_tiles = len(tiles)
    n_whole = sum(width == TILE for _, width in tiles)
    plan = chunks_of(n_cols // LANES)
    n_chunks = len(plan)
    ends = [[j for j, (first, *_) in enumerate(plan) if first * LANES < sum(tiles[t])][-1] for t in range(n_whole - 1, n_tiles)]
    first_end = ends[0] - 1

    side = z // 2
    outer_far, inner_far, near = 3 - 3 * side, 2 - side, 1 - z + 4 * side
    is_outer = jnp.where(z == side * 3, 1, 0)
    z_two, z_one = lax.rem(z + 2, 4), near
    v_two, v_one = lax.rem(v + 2, 4), v + 1 - 2 * lax.rem(v, 2)
    sources = (near, inner_far, outer_far)

    def cols_of(j):
        first, size, _, _ = plan[j]
        return first * LANES, size * LANES

    def w_rows(source, part, j=None):
        at, n = (0, half) if j is None else (plan[j][2] * (half // 2), plan[j][3] * (half // 2))
        return pl.ds(pl.multiple_of(source * depth + part * half + at, half // 2), n)

    def w_place(j, source, part):
        start, n = cols_of(j)
        return wbuf.at[w_rows(source, part, j), pl.ds(start, n)]

    def h_place(q, block=None):
        at = pl.ds(pl.multiple_of(q * quarter, quarter), quarter)
        if block is None:
            return hbuf.at[at]
        return hbuf.at[at, pl.ds(pl.multiple_of(block * depth, depth), depth)]

    def remote(src, dst, send, recv, **to):
        return pltpu.make_async_remote_copy(
            src_ref=src, dst_ref=dst, send_sem=send, recv_sem=recv, device_id=to, device_id_type=MESH
        )

    def w_source(j, part, dest):
        start, n = cols_of(j)
        return w_ref.at[w_rows(0, part, j), pl.ds(pl.multiple_of(dest * n_cols + start, LANES), n)]

    def direct(j, k, dest, slot):
        return remote(w_source(j, x, dest), w_place(j, z, x), ws.at[k], wr.at[j, slot], hid=dest)

    def send_near(j):
        return direct(j, 0, near, 0)

    odd = lax.rem(v, 2)
    far_first = outer_far + odd * (inner_far - outer_far)
    far_second = inner_far + odd * (outer_far - inner_far)

    def send_far(j, i):
        return direct(j, 1 + i, (far_first, far_second)[i], 1 + is_outer)

    def send_twin(i):
        dest = (far_first, far_second)[i]
        return remote(w_source(n_chunks - 1, 1 - x, dest), w_place(n_chunks - 1, z, 1 - x), ts.at[i], tr, hid=dest)

    def twin_landed():
        place = w_place(n_chunks - 1, inner_far, 1 - x)
        remote(place, place, ts.at[0], tr, hid=inner_far).wait_recv()

    def landed(j, k):
        place = w_place(j, sources[k], x)
        remote(place, place, ws.at[k], wr.at[j, k], hid=sources[k]).wait_recv()

    def forward(j, k):
        place = w_place(j, sources[k], x)
        send = 3 if k == 1 and j == n_chunks - 2 else k
        return remote(place, place, xs.at[send], xr.at[cross(j, k)], data=1 - x)

    def cross(j, k):
        if j < first_end:
            return j
        return first_end if k != 1 else 1 + j

    def cross_wait(slot, count, start, stop):
        place = wbuf.at[pl.ds(0, count), pl.ds(start, stop - start)]
        remote(place, place, xs.at[0], xr.at[slot], data=1 - x).wait_recv()

    def forwarded(j):
        place = w_place(j, inner_far, 1 - x)
        remote(place, place, xs.at[1], xr.at[cross(j, 1)], data=1 - x).wait_recv()

    def own(j):
        start, n = cols_of(j)
        return pltpu.make_async_copy(
            w_ref.at[:, pl.ds(pl.multiple_of(z * n_cols + start, LANES), n)],
            wbuf.at[pl.ds(pl.multiple_of(z * depth, depth), depth), pl.ds(start, n)],
            wl,
        )

    h_mine = h_ref.at[pl.ds(pl.multiple_of(v * quarter, quarter), quarter)]
    h_own = pltpu.make_async_copy(h_mine, h_place(v, z), hl)
    h_two = remote(h_place(v, z), h_place(v, z), hs, hr.at[0], hid=z_two)
    h_one = remote(h_place(v, z), h_place(v, z), hs, hr.at[1], hid=z_one)
    h_relay = remote(h_place(v, z_two), h_place(v, z_two), hs, hr.at[2], hid=z_one)
    h_chip = remote(h_place(v), h_place(v), hs, hr.at[3], vocab=v_two)
    h_core = remote(h_place(v), h_place(v), hs, hr.at[4], vocab=v_one)
    h_both = remote(h_place(v_two), h_place(v_two), hs, hr.at[5], vocab=v_one)

    def arrived(place, i, **frm):
        remote(place, place, hs, hr.at[i], **frm).wait_recv()

    barrier = pltpu.get_barrier_semaphore()
    peers = [{"hid": lax.rem(z + d, 4)} for d in (1, 2, 3)]
    peers += [{"data": 1 - x}] + [{"vocab": lax.rem(v + d, 4)} for d in (1, 2, 3)]
    for peer in peers:
        pl.semaphore_signal(barrier, inc=1, device_id=peer, device_id_type=MESH)
    row_copies = [
        pltpu.make_async_copy(temp_hbm, temp_ref, rl.at[0]),
        pltpu.make_async_copy(tgt_hbm, tgt_ref, rl.at[1]),
    ]
    for copy in (h_own, *row_copies):
        copy.start()
    for j in range(n_chunks):
        if plan[j][2] == 0:
            own(j).start()
    with jax.named_scope("bar"):
        pl.semaphore_wait(barrier, len(peers))

    h_own.wait()
    h_two.start()
    h_one.start()
    send_near(0).start()
    send_far(0, 0).start()

    def ones_below(ref, width):
        k = lax.broadcasted_iota(jnp.int32, (width, width), 0)
        c = lax.broadcasted_iota(jnp.int32, (width, width), 1)
        block = jnp.where(k <= c, 1.0, 0.0).astype(BF16)
        for i in range(3):
            ref[pl.ds(i * width, width), :] = block

    ones_below(tri, TILE)
    ones_below(tri_last, LANES)
    base = (v * 4 + z) * n_cols
    for copy in row_copies:
        copy.wait()
    back[0:1, :] = temp_ref[...]
    back[1:2, :] = (tgt_ref[...] - base).astype(F32)
    cols8 = back[...].T
    temp_col[...] = jnp.broadcast_to(cols8[:, 0:1], temp_col.shape)
    rel_col[...] = jnp.broadcast_to(cols8[:, 1:2], rel_col.shape).astype(jnp.int32)
    slot = lax.broadcasted_iota(jnp.int32, stats.shape, 1)
    stats[...] = jnp.where(slot < SLOTS, LOWEST, 0.0)
    t_all[...] = jnp.zeros(t_all.shape, F32)

    with jax.named_scope("h0"):
        arrived(h_place(v, z_two), 0, hid=z_two)
    h_relay.start()
    send_far(0, 1).start()
    for j in range(1, n_chunks):
        send_near(j).start()
        send_far(j, 0).start()
        send_far(j, 1).start()

    @pl.when(is_outer == 0)
    def _():
        send_twin(0).start()
        send_twin(1).start()


    part, few = min(rows, 512), min(rows, 128)

    def logits_and_sums(product, sums):
        some = part if product is not None or sums[2] == TILE else min(rows, 2 * part)

        @pl.loop(0, rows // some)
        def _(i):
            if product is not None:
                _, new_start, new_width = product
                at = pl.ds(pl.multiple_of(i * part, part), part)
                new = jnp.dot(
                    hbuf[at, :], wbuf[:, pl.ds(new_start, new_width)], preferred_element_type=F32
                )
            for k in range(0, some, few) if sums is not None else ():
                prefix(pl.ds(pl.multiple_of(i * some + k, few), few), *sums)
            if product is not None:
                zbuf[at, 0:new_width] = new

    def prefix(at, t, start, width):
        pieces = width // LANES
        logits = zbuf[at, 0:width] * jnp.concatenate([temp_col[at, :]] * pieces, axis=1)
        lane = lax.broadcasted_iota(jnp.int32, (few, LANES), 1)
        top = jnp.max(logits, axis=1, keepdims=True)
        e = jnp.exp(logits - top)
        total = jnp.sum(e, axis=1, keepdims=True)
        stats[at, :] = jnp.where(lane == t, top, jnp.where(lane == SLOTS + t, total, stats[at, :]))
        table = tri if width == TILE else tri_last
        run = jnp.dot(jnp.concatenate(split3(e), axis=1), table[...], preferred_element_type=F32)
        c_ref[at, pl.ds(start, width)] = run
        rel = rel_col[at, :] - start
        hit = t_all[at, :]
        for p in range(pieces):
            hit += jnp.where(lane == rel - p * LANES, run[:, p * LANES : (p + 1) * LANES], 0.0)
        t_all[at, :] = hit

    def whole(t):
        return t, pl.multiple_of(t * TILE, TILE), TILE

    def compute(j):
        first, size = (n // 2 for n in plan[j][:2])
        stop = first + size
        if first == 0:
            logits_and_sums(whole(0), None)
            first = 1
        if first < stop:

            @pl.loop(first, stop)
            def _(t):
                logits_and_sums(whole(t), whole(t - 1))

        if j == first_end - 1:
            logits_and_sums(None, whole(stop - 1))

    def block_dot(at, block, start, width):
        lanes = pl.ds(pl.multiple_of(block * depth, depth), depth)
        return jnp.dot(hbuf[at, lanes], wbuf[lanes, start : start + width], preferred_element_type=F32)

    def begin_end(i):
        start, width = tiles[n_whole - 1 + i]

        @pl.loop(0, rows // part)
        def _(k):
            at = pl.ds(pl.multiple_of(k * part, part), part)
            c_ref[at, start : start + width] = (
                block_dot(at, z, start, width)
                + block_dot(at, near, start, width)
                + block_dot(at, outer_far, start, width)
            )

    def finish_end(i):
        t = n_whole - 1 + i
        start, width = tiles[t]
        every = slice(0, rows)
        zbuf[:, 0:width] = c_ref[:, start : start + width] + block_dot(every, inner_far, start, width)
        logits_and_sums(None, (t, start, width))

    def fold(g0, g1):
        @pl.loop(0, rows // few)
        def _(i):
            at = pl.ds(pl.multiple_of(i * few, few), few)
            lane = lax.broadcasted_iota(jnp.int32, (few, LANES), 1)
            group = (lane >= g0) & (lane < g1)
            m = stats[at, :]
            s = pltpu.roll(m, LANES - SLOTS, 1)
            top = jnp.max(jnp.where(group, m, LOWEST), axis=1, keepdims=True)
            shrink = jnp.where(group, jnp.exp(m - top), 0.0)
            parts = jnp.where(group, s, 0.0) * shrink
            before = prefix_before(parts)
            for t in range(g0, g1):
                span = slice(t * TILE, (t + 1) * TILE)
                c_ref[at, span] = c_ref[at, span] * shrink[:, t : t + 1] + before[:, t : t + 1]
            rel = rel_col[at, :]
            holds = (rel >= lane * TILE) & (rel < (lane + 1) * TILE)
            old = t_all[at, :]
            moved = jnp.sum(old, axis=1, keepdims=True) * shrink + before
            inside = (rel >= g0 * TILE) & (rel < g1 * TILE)
            t_all[at, :] = jnp.where(inside, jnp.where(holds, moved, 0.0), old)
            total = jnp.sum(parts, axis=1, keepdims=True)
            sums = jnp.where(lane == SLOTS + g1 - 1, total, 0.0)
            of_sums = (lane >= SLOTS + g0) & (lane < SLOTS + g1)
            stats[at, :] = jnp.where(group, top, jnp.where(of_sums, sums, m))

    def close(i):
        first = ends[i - 1] + 1 if i else first_end
        with jax.named_scope(f"xe{i}"):
            for j in range(first, ends[i] + 1):
                if j < n_chunks - 1:
                    forwarded(j)
                else:
                    twin_landed()
        with jax.named_scope(f"ce{i}"):
            finish_end(i)

    def prefix_before(parts):
        k = lax.broadcasted_iota(jnp.int32, (LANES, LANES), 0)
        c = lax.broadcasted_iota(jnp.int32, (LANES, LANES), 1)
        strict = jnp.where(k < c, 1.0, 0.0).astype(BF16)
        return sum(jnp.dot(p, strict, preferred_element_type=F32) for p in split3(parts))

    def complete(j):
        start, n = cols_of(j)
        cross_wait(j, 3 * half, start, start + n)

    def own_complete():
        place = wbuf.at[pl.ds(pl.multiple_of(z * depth, depth), depth)]
        pltpu.make_async_copy(place, place, wl).wait()

    order = service_order(plan, n_cols // LANES)
    folds = {j: (g0, g1) for j, g0, g1 in folds_of(plan, first_end)}
    tail = range(first_end, n_chunks)
    known = max(order.index((k, j)) for k in (0, 2) for j in tail)
    early = min(j for j in range(max(0, first_end - 7), n_chunks - 1) if order.index((1, j + 1)) > known)
    assert early < first_end
    m = len(ends) - 1
    closes = {n_chunks - 3: range(m - 2), n_chunks - 2: [m - 2], n_chunks - 1: [m - 1]}

    for what, j in order:
        if what == "h line":
            with jax.named_scope("hline"):
                arrived(h_place(v, z_one), 1, hid=z_one)
                arrived(h_place(v, lax.rem(z_one + 2, 4)), 2, hid=z_one)
            h_chip.start()
            h_core.start()
        elif what == "h chip":
            with jax.named_scope("hchip"):
                arrived(h_place(v_two), 3, vocab=v_two)
            h_both.start()
        else:
            with jax.named_scope(f"w{what}_{j}"):
                landed(j, what)
            if (what, j) != (1, n_chunks - 1):
                forward(j, what).start()
            if what != 1:
                continue
            if j == 1:
                with jax.named_scope("hcore"):
                    arrived(h_place(v_one), 4, vocab=v_one)
                    arrived(h_place(lax.rem(v_one + 2, 4)), 5, vocab=v_one)
                    own_complete()
            if 0 < j <= first_end:
                with jax.named_scope(f"x{j - 1}"):
                    complete(j - 1)
                with jax.named_scope(f"c{j - 1}"):
                    compute(j - 1)
                if j - 1 in folds:
                    with jax.named_scope(f"f{j - 1}"):
                        fold(*folds[j - 1])
            if j - 1 == early:
                with jax.named_scope("begin"):
                    cross_wait(first_end, 2 * half, cols_of(first_end)[0], n_cols)
                    for i in range(len(ends)):
                        begin_end(i)
            for i in closes.get(j, ()):
                close(i)
    close(m)

    lane = lax.broadcasted_iota(jnp.int32, (rows, LANES), 1)
    at_tgt = jnp.sum(t_all[...], axis=1, keepdims=True)
    turned = jnp.where(lane == 2 * SLOTS, at_tgt, stats[...]).T
    m, at_tgt = turned[0:SLOTS, :], turned[2 * SLOTS : 2 * SLOTS + 1, :]
    top = jnp.max(m, axis=0, keepdims=True)
    shrink = jnp.exp(m - top)
    parts = turned[SLOTS : 2 * SLOTS, :] * shrink
    t = lax.broadcasted_iota(jnp.int32, (SLOTS, rows), 0)
    start = jnp.where(t < n_whole, t * TILE, n_whole * (TILE - LANES) + t * LANES)
    stop = start + jnp.where(t < n_whole, TILE, LANES)
    rel = tgt_ref[...] - base
    known = rel < n_cols
    holds = (rel >= start) & (rel < stop) & known
    ahead = (stop <= rel) & known
    found = jnp.where(holds, at_tgt * shrink, jnp.where(ahead, parts, 0.0))
    zmsg[z, 0:1, :] = top
    zmsg[z, 1:2, :] = jnp.sum(parts, axis=0, keepdims=True)
    zmsg[z, 2:3, :] = jnp.sum(found, axis=0, keepdims=True)

    for k in range(3):
        mine = wbuf.at[w_rows(sources[k], x)]
        remote(mine, mine, ws.at[k], wr.at[0, k], hid=near).wait_send()
        if k == 1:
            mine = wbuf.at[w_rows(sources[k], x), pl.ds(0, n_cols - LANES)]
        remote(mine, mine, xs.at[k], xr.at[0], data=1 - x).wait_send()
    forward(n_chunks - 2, 1).wait_send()

    @pl.when(is_outer == 0)
    def _():
        send_twin(0).wait_send()
        send_twin(1).wait_send()

    mine = hbuf.at[pl.ds(0, quarter * 15 // 4)]
    remote(mine, mine, hs, hr.at[0], hid=near).wait_send()

    def z_send(i):
        return remote(zmsg.at[z], zmsg.at[z], zs, zr, hid=(near, inner_far, outer_far)[i])

    def v_send(d):
        to = lax.rem(v + d, 4)
        return remote(vmsg.at[v], vmsg.at[v], vs, vr, vocab=to)

    for i in (2, 1, 0):
        z_send(i).start()
    k = lax.broadcasted_iota(jnp.int32, (SLOTS, SLOTS), 0)
    c = lax.broadcasted_iota(jnp.int32, (SLOTS, SLOTS), 1)
    strict = jnp.where(c < k, 1.0, 0.0).astype(BF16)
    before = sum(jnp.dot(strict, p, preferred_element_type=F32) for p in split3(parts))
    rest = jnp.zeros((LANES - 2 * SLOTS, rows), F32)
    coef_ref[...] = jnp.concatenate([shrink, before, rest], axis=0).T
    z_all = remote(zmsg.at[pl.ds(0, 3)], zmsg.at[pl.ds(0, 3)], zs, zr, hid=near)
    with jax.named_scope("z"):
        z_all.wait_recv()

    ids = tgt_ref[...]
    maxes = [zmsg[h, 0:1, :] for h in range(4)]
    v_max = functools.reduce(jnp.maximum, maxes)
    v_sum = jnp.zeros((1, rows), F32)
    v_tgt = jnp.zeros((1, rows), F32)
    mine_before = jnp.zeros((1, rows), F32)
    for h in range(4):
        mine_before = jnp.where(h == z, v_sum, mine_before)
        f = jnp.exp(maxes[h] - v_max)
        low = (v * 4 + h) * n_cols
        inside = (ids >= low) & (ids < low + n_cols)
        v_tgt += jnp.where(inside, zmsg[h, 2:3, :] * f + v_sum, 0.0)
        v_sum += zmsg[h, 1:2, :] * f
    vmsg[v, 0:1, :] = v_max
    vmsg[v, 1:2, :] = v_sum
    vmsg[v, 2:3, :] = v_tgt

    z_all.wait_send()
    for d in (2, 1, 3):
        v_send(d).start()
    v_all = remote(vmsg.at[pl.ds(0, 3)], vmsg.at[pl.ds(0, 3)], vs, vr, vocab=v_one)
    with jax.named_scope("v"):
        v_all.wait_recv()

    maxes = [vmsg[u, 0:1, :] for u in range(4)]
    g_max = functools.reduce(jnp.maximum, maxes)
    g_sum = jnp.zeros((1, rows), F32)
    g_tgt = jnp.zeros((1, rows), F32)
    g_before = jnp.zeros((1, rows), F32)
    for u in range(4):
        f = jnp.exp(maxes[u] - g_max)
        g_before = jnp.where(u == v, g_sum + mine_before * f, g_before)
        low = u * 4 * n_cols
        inside = (ids >= low) & (ids < low + 4 * n_cols)
        g_tgt += jnp.where(inside, vmsg[u, 2:3, :] * f + g_sum, 0.0)
        g_sum += vmsg[u, 1:2, :] * f
    tgt_out_ref[...] = g_tgt / g_sum
    factor_ref[0:1, :] = jnp.exp(zmsg[z, 0:1, :] - g_max) / g_sum
    factor_ref[1:2, :] = g_before / g_sum
    v_all.wait_send()


def finish_kernel(tiles, lanes, c_ref, coef_ref, factor_ref, tgt_ref, out_ref, tgt_out_ref, buf, factor_col, sems, tgt_sem):
    slots, n, n_cols = buf.shape
    steps = c_ref.shape[0] // n
    tgt_copy = pltpu.make_async_copy(tgt_ref, tgt_out_ref, tgt_sem)
    tgt_copy.start()

    def put(i):
        slot = lax.rem(i, slots)
        at = pl.ds(pl.multiple_of(i * n, n), n)
        return pltpu.make_async_copy(buf.at[slot], out_ref.at[at], sems.at[slot])

    @pl.loop(0, steps)
    def _(i):
        slot = lax.rem(i, slots)

        @pl.when(i >= slots)
        def _():
            put(i - slots).wait()

        at = pl.ds(pl.multiple_of(i * n, n), n)
        turn = max(n, LANES)

        @pl.when(lax.rem(i, turn // n) == 0)
        def _():
            some = pl.ds(pl.multiple_of(i // (turn // n) * turn, turn), turn)
            factor_col[some, :] = factor_ref[:, some].T

        lane = lax.broadcasted_iota(jnp.int32, (n, LANES), 1)
        coef = coef_ref[at, :] * factor_col[at, 0:1] + jnp.where(lane < SLOTS, 0.0, factor_col[at, 1:2])
        for (start, width), k in zip(tiles, lanes):
            span = slice(start, start + width)
            buf[slot, :, span] = c_ref[at, span] * coef[:, k : k + 1] + coef[:, SLOTS + k : SLOTS + k + 1]
        put(i).start()

    tgt_copy.wait()
    for i in range(max(0, steps - slots), steps):
        with jax.named_scope(f"fe{i}"):
            put(i).wait()


def solution(mesh):
    n_hid, n_voc = mesh.shape["hid"], mesh.shape["vocab"]
    assert n_hid == 4 and n_voc == 4 and mesh.shape["data"] == 2

    def local_step(h_blk, w_blk, temp_blk, tgt_blk):
        rows, depth = h_blk.shape
        n_cols = w_blk.shape[1] // n_hid
        assert n_cols % LANES == 0
        tiles = tiles_of(n_cols // LANES)
        n_tiles = len(tiles)
        assert n_tiles <= SLOTS
        plan = chunks_of(n_cols // LANES)
        n_chunks = len(plan)
        last_whole = sum(width == TILE for _, width in tiles) - 1
        first_end = [first for first, *_ in plan].index(2 * last_whole)
        vmem = pl.BlockSpec(memory_space=pltpu.VMEM)
        hbm = pl.BlockSpec(memory_space=pltpu.HBM)
        dma = pltpu.SemaphoreType.DMA
        table = pltpu.VMEM((rows, LANES), F32)
        c, coef, factor, tgt = pl.pallas_call(
            functools.partial(prefix_kernel, n_cols),
            out_shape=(
                pltpu.VMEM((rows, n_cols), F32),
                pltpu.VMEM((rows, LANES), F32),
                pltpu.VMEM((8, rows), F32),
                pltpu.VMEM((1, rows), F32),
            ),
            in_specs=[hbm] * 4,
            out_specs=[vmem] * 4,
            scratch_shapes=[
                pltpu.VMEM((4 * depth, n_cols), BF16),
                pltpu.VMEM((rows, 4 * depth), BF16),
                pltpu.VMEM((rows, TILE), F32),
                pltpu.VMEM((3 * TILE, TILE), BF16),
                pltpu.VMEM((3 * LANES, LANES), BF16),
                table,
                table,
                table,
                pltpu.VMEM((rows, LANES), jnp.int32),
                pltpu.VMEM((1, rows), F32),
                pltpu.VMEM((1, rows), jnp.int32),
                pltpu.VMEM((4, 3, rows), F32),
                pltpu.VMEM((4, 3, rows), F32),
                pltpu.VMEM((8, rows), F32),
                dma((3,)),
                dma((n_chunks, 3)),
                dma((4,)),
                dma((n_chunks,)),
                dma((2,)),
                dma,
                dma,
                dma,
                dma,
                dma((6,)),
                dma,
                dma,
                dma,
                dma,
                dma((2,)),
            ],
            compiler_params=pltpu.CompilerParams(
                collective_id=0, has_side_effects=True, vmem_limit_bytes=37 << 20
            ),
            name="prefix",
        )(h_blk, w_blk, temp_blk.reshape(1, rows), tgt_blk.reshape(1, rows))
        n = min(rows, 64)
        lanes = list(range(n_tiles))
        for _, g0, g1 in folds_of(plan, first_end):
            lanes[g0:g1] = [g0] * (g1 - g0)
        cdf, cdf_tgt = pl.pallas_call(
            functools.partial(finish_kernel, tiles, lanes),
            out_shape=(
                jax.ShapeDtypeStruct((rows, n_cols), F32),
                jax.ShapeDtypeStruct((1, rows), F32),
            ),
            in_specs=[vmem] * 4,
            out_specs=[hbm, hbm],
            scratch_shapes=[
                pltpu.VMEM((4, n, n_cols), F32),
                pltpu.VMEM((rows, 8), F32),
                dma((4,)),
                dma,
            ],
            compiler_params=pltpu.CompilerParams(vmem_limit_bytes=9 << 20),
            name="finish",
        )(c, coef, factor, tgt)
        return cdf, cdf_tgt.reshape(rows)

    return jax.shard_map(
        local_step,
        mesh=mesh,
        in_specs=(P("data", "hid"), P("hid", "vocab"), P("data"), P("data")),
        out_specs=(P("data", ("vocab", "hid")), P("data")),
        check_vma=False,
    )
```

```python
import functools

import jax
import jax.numpy as jnp
from jax import lax
from jax.experimental import pallas as pl
from jax.experimental.pallas import tpu as pltpu
from jax.sharding import PartitionSpec as P

MESH = pl.DeviceIdType.MESH
F32 = jnp.float32
BF16 = jnp.bfloat16
TILE = 256
LANES = 128
SLOTS = 32
LOWEST = float(jnp.finfo(jnp.float32).min)


def tiles_of(blocks):
    whole = (blocks - 3) // 2
    tiles = [(t * TILE, TILE) for t in range(whole)]
    return tiles + [(b * LANES, LANES) for b in range(2 * whole, blocks)]


def chunks_of(blocks):
    whole = (blocks - 3) // 2
    sizes, left = [], 2 * whole - 2
    for size in (2, 2, 2, 2, 4, 4):
        if left > size:
            sizes.append(size)
            left -= size
    while left > 0:
        sizes.append(min(6, left))
        left -= sizes[-1]
    plan, at = [], 0
    for size in reversed(sizes):
        plan.append((at, size, 0, 2))
        at += size
    plan += [(b, 1, 0, 2) for b in range(at, blocks - 2)]
    return plan + [(b, 1, r, 1) for b in (blocks - 2, blocks - 1) for r in (0, 1)]


def service_order(plan, blocks):
    events = [(0.15 * blocks, "h line", 0), (0.28 * blocks, "h chip", 0)]
    for j, (first, size, _, _) in enumerate(plan):
        end = first + size
        events.append((first + size / 3 + 2, 0, j))
        events.append((end + 2, 2, j))
        events.append((min(1.86 * end, 0.68 * blocks + 0.6 * end) + 2, 1, j))
    events.sort(key=lambda e: e[0])
    order = [e[1:] for e in events]
    for j in range(len(plan)):
        at = max(order.index((k, j)) for k in (0, 1, 2))
        order.remove((1, j))
        order.insert(at, (1, j))
    return order


def folds_of(plan, first_end):
    folds, at = [], 0
    for j in (first_end // 3, 3 * first_end // 5):
        stop = sum(plan[j][:2]) // 2 - 1
        if j < first_end and stop > at:
            folds.append((j, at, stop))
            at = stop
    return folds


def split3(e):
    hi = e.astype(BF16)
    rest = e - hi.astype(F32)
    mid = rest.astype(BF16)
    low = (rest - mid.astype(F32)).astype(BF16)
    return hi, mid, low


def prefix_kernel(
    n_cols, h_ref, w_ref, temp_hbm, tgt_hbm,
    c_ref, coef_ref, factor_ref, tgt_out_ref,
    wbuf, hbuf, zbuf, tri, tri_last, stats, t_all, temp_col, rel_col, temp_ref, tgt_ref, zmsg, vmsg, back,
    ws, wr, xs, xr, ts, tr, wl, hl, hs, hr, zs, zr, vs, vr, rl,
):
    x, z, v = lax.axis_index("data"), lax.axis_index("hid"), lax.axis_index("vocab")
    rows, depth = h_ref.shape
    half, quarter = depth // 2, rows // 4
    tiles = tiles_of(n_cols // LANES)
    n_tiles = len(tiles)
    n_whole = sum(width == TILE for _, width in tiles)
    plan = chunks_of(n_cols // LANES)
    n_chunks = len(plan)
    ends = [[j for j, (first, *_) in enumerate(plan) if first * LANES < sum(tiles[t])][-1] for t in range(n_whole - 1, n_tiles)]
    first_end = ends[0] - 1

    side = z // 2
    outer_far, inner_far, near = 3 - 3 * side, 2 - side, 1 - z + 4 * side
    is_outer = jnp.where(z == side * 3, 1, 0)
    z_two, z_one = lax.rem(z + 2, 4), near
    v_two, v_one = lax.rem(v + 2, 4), v + 1 - 2 * lax.rem(v, 2)
    sources = (near, inner_far, outer_far)

    def cols_of(j):
        first, size, _, _ = plan[j]
        return first * LANES, size * LANES

    def w_rows(source, part, j=None):
        at, n = (0, half) if j is None else (plan[j][2] * (half // 2), plan[j][3] * (half // 2))
        return pl.ds(pl.multiple_of(source * depth + part * half + at, half // 2), n)

    def w_place(j, source, part):
        start, n = cols_of(j)
        return wbuf.at[w_rows(source, part, j), pl.ds(start, n)]

    def h_place(q, block=None):
        at = pl.ds(pl.multiple_of(q * quarter, quarter), quarter)
        if block is None:
            return hbuf.at[at]
        return hbuf.at[at, pl.ds(pl.multiple_of(block * depth, depth), depth)]

    def remote(src, dst, send, recv, **to):
        return pltpu.make_async_remote_copy(
            src_ref=src, dst_ref=dst, send_sem=send, recv_sem=recv, device_id=to, device_id_type=MESH
        )

    def w_source(j, part, dest):
        start, n = cols_of(j)
        return w_ref.at[w_rows(0, part, j), pl.ds(pl.multiple_of(dest * n_cols + start, LANES), n)]

    def direct(j, k, dest, slot):
        return remote(w_source(j, x, dest), w_place(j, z, x), ws.at[k], wr.at[j, slot], hid=dest)

    def send_near(j):
        return direct(j, 0, near, 0)

    odd = lax.rem(v, 2)
    far_first = outer_far + odd * (inner_far - outer_far)
    far_second = inner_far + odd * (outer_far - inner_far)

    def send_far(j, i):
        return direct(j, 1 + i, (far_first, far_second)[i], 1 + is_outer)

    def send_twin(i):
        dest = (far_first, far_second)[i]
        return remote(w_source(n_chunks - 1, 1 - x, dest), w_place(n_chunks - 1, z, 1 - x), ts.at[i], tr, hid=dest)

    def twin_landed():
        place = w_place(n_chunks - 1, inner_far, 1 - x)
        remote(place, place, ts.at[0], tr, hid=inner_far).wait_recv()

    def landed(j, k):
        place = w_place(j, sources[k], x)
        remote(place, place, ws.at[k], wr.at[j, k], hid=sources[k]).wait_recv()

    def forward(j, k):
        place = w_place(j, sources[k], x)
        send = 5 - n_chunks + j if k == 1 and j >= n_chunks - 2 else k
        return remote(place, place, xs.at[send], xr.at[cross(j, k)], data=1 - x)

    def cross(j, k):
        if j < first_end:
            return j
        return first_end if k != 1 else 1 + j

    def cross_wait(slot, count, start, stop):
        place = wbuf.at[pl.ds(0, count), pl.ds(start, stop - start)]
        remote(place, place, xs.at[0], xr.at[slot], data=1 - x).wait_recv()

    def forwarded(j):
        place = w_place(j, inner_far, 1 - x)
        remote(place, place, xs.at[1], xr.at[cross(j, 1)], data=1 - x).wait_recv()

    def own(j):
        start, n = cols_of(j)
        return pltpu.make_async_copy(
            w_ref.at[:, pl.ds(pl.multiple_of(z * n_cols + start, LANES), n)],
            wbuf.at[pl.ds(pl.multiple_of(z * depth, depth), depth), pl.ds(start, n)],
            wl,
        )

    h_mine = h_ref.at[pl.ds(pl.multiple_of(v * quarter, quarter), quarter)]
    h_own = pltpu.make_async_copy(h_mine, h_place(v, z), hl)
    h_two = remote(h_mine, h_place(v, z), hs, hr.at[0], hid=z_two)
    h_one = remote(h_mine, h_place(v, z), hs, hr.at[1], hid=z_one)
    h_relay = remote(h_place(v, z_two), h_place(v, z_two), hs, hr.at[2], hid=z_one)
    h_chip = remote(h_place(v), h_place(v), hs, hr.at[3], vocab=v_two)
    h_core = remote(h_place(v), h_place(v), hs, hr.at[4], vocab=v_one)
    h_both = remote(h_place(v_two), h_place(v_two), hs, hr.at[5], vocab=v_one)

    def arrived(place, i, **frm):
        remote(place, place, hs, hr.at[i], **frm).wait_recv()

    barrier = pltpu.get_barrier_semaphore()
    peers = [{"hid": lax.rem(z + d, 4)} for d in (1, 2, 3)]
    peers += [{"data": 1 - x}] + [{"vocab": lax.rem(v + d, 4)} for d in (1, 2, 3)]
    for peer in peers:
        pl.semaphore_signal(barrier, inc=1, device_id=peer, device_id_type=MESH)
    row_copies = [
        pltpu.make_async_copy(temp_hbm, temp_ref, rl.at[0]),
        pltpu.make_async_copy(tgt_hbm, tgt_ref, rl.at[1]),
    ]
    for copy in (h_own, *row_copies):
        copy.start()
    for j in range(n_chunks):
        if plan[j][2] == 0:
            own(j).start()
    with jax.named_scope("bar"):
        pl.semaphore_wait(barrier, len(peers))

    h_two.start()
    h_one.start()
    send_near(0).start()
    send_far(0, 0).start()

    def ones_below(ref, width):
        k = lax.broadcasted_iota(jnp.int32, (width, width), 0)
        c = lax.broadcasted_iota(jnp.int32, (width, width), 1)
        block = jnp.where(k <= c, 1.0, 0.0).astype(BF16)
        for i in range(3):
            ref[pl.ds(i * width, width), :] = block

    ones_below(tri, TILE)
    ones_below(tri_last, LANES)
    base = (v * 4 + z) * n_cols
    for copy in row_copies:
        copy.wait()
    back[0:1, :] = temp_ref[...]
    back[1:2, :] = (tgt_ref[...] - base).astype(F32)
    cols8 = back[...].T
    temp_col[...] = jnp.broadcast_to(cols8[:, 0:1], temp_col.shape)
    rel_col[...] = jnp.broadcast_to(cols8[:, 1:2], rel_col.shape).astype(jnp.int32)
    slot = lax.broadcasted_iota(jnp.int32, stats.shape, 1)
    stats[...] = jnp.where(slot < SLOTS, LOWEST, 0.0)
    t_all[...] = jnp.zeros(t_all.shape, F32)

    with jax.named_scope("h0"):
        arrived(h_place(v, z_two), 0, hid=z_two)
    h_relay.start()
    send_far(0, 1).start()
    for j in range(1, n_chunks):
        send_near(j).start()
        send_far(j, 0).start()
        send_far(j, 1).start()

    twins = (is_outer == 0) & (odd == 0)

    @pl.when(twins)
    def _():
        send_twin(0).start()
        send_twin(1).start()


    part, few = min(rows, 512), min(rows, 128)

    def logits_and_sums(product, sums):
        some = part if product is not None or sums[2] == TILE else min(rows, 2 * part)

        @pl.loop(0, rows // some)
        def _(i):
            if product is not None:
                _, new_start, new_width = product
                at = pl.ds(pl.multiple_of(i * part, part), part)
                new = jnp.dot(
                    hbuf[at, :], wbuf[:, pl.ds(new_start, new_width)], preferred_element_type=F32
                )
            for k in range(0, some, few) if sums is not None else ():
                prefix(pl.ds(pl.multiple_of(i * some + k, few), few), *sums)
            if product is not None:
                zbuf[at, 0:new_width] = new

    def prefix(at, t, start, width):
        pieces = width // LANES
        logits = zbuf[at, 0:width] * jnp.concatenate([temp_col[at, :]] * pieces, axis=1)
        lane = lax.broadcasted_iota(jnp.int32, (few, LANES), 1)
        top = jnp.max(logits, axis=1, keepdims=True)
        e = jnp.exp(logits - top)
        total = jnp.sum(e, axis=1, keepdims=True)
        stats[at, :] = jnp.where(lane == t, top, jnp.where(lane == SLOTS + t, total, stats[at, :]))
        table = tri if width == TILE else tri_last
        run = jnp.dot(jnp.concatenate(split3(e), axis=1), table[...], preferred_element_type=F32)
        c_ref[at, pl.ds(start, width)] = run
        rel = rel_col[at, :] - start
        hit = t_all[at, :]
        for p in range(pieces):
            hit += jnp.where(lane == rel - p * LANES, run[:, p * LANES : (p + 1) * LANES], 0.0)
        t_all[at, :] = hit

    def whole(t):
        return t, pl.multiple_of(t * TILE, TILE), TILE

    def compute(j):
        first, size = (n // 2 for n in plan[j][:2])
        stop = first + size
        if first == 0:
            logits_and_sums(whole(0), None)
            first = 1
        if first < stop:

            @pl.loop(first, stop)
            def _(t):
                logits_and_sums(whole(t), whole(t - 1))

        if j == first_end - 1:
            logits_and_sums(None, whole(stop - 1))

    def block_dot(at, block, start, width):
        lanes = pl.ds(pl.multiple_of(block * depth, depth), depth)
        return jnp.dot(hbuf[at, lanes], wbuf[lanes, start : start + width], preferred_element_type=F32)

    def begin_end(i):
        start, width = tiles[n_whole - 1 + i]

        @pl.loop(0, rows // part)
        def _(k):
            at = pl.ds(pl.multiple_of(k * part, part), part)
            c_ref[at, start : start + width] = (
                block_dot(at, z, start, width)
                + block_dot(at, near, start, width)
                + block_dot(at, outer_far, start, width)
            )

    def finish_end(i):
        t = n_whole - 1 + i
        start, width = tiles[t]
        every = slice(0, rows)
        zbuf[:, 0:width] = c_ref[:, start : start + width] + block_dot(every, inner_far, start, width)
        logits_and_sums(None, (t, start, width))

    def fold(g0, g1):
        @pl.loop(0, rows // few)
        def _(i):
            at = pl.ds(pl.multiple_of(i * few, few), few)
            lane = lax.broadcasted_iota(jnp.int32, (few, LANES), 1)
            group = (lane >= g0) & (lane < g1)
            m = stats[at, :]
            s = pltpu.roll(m, LANES - SLOTS, 1)
            top = jnp.max(jnp.where(group, m, LOWEST), axis=1, keepdims=True)
            shrink = jnp.where(group, jnp.exp(m - top), 0.0)
            parts = jnp.where(group, s, 0.0) * shrink
            before = prefix_before(parts)
            for t in range(g0, g1):
                span = slice(t * TILE, (t + 1) * TILE)
                c_ref[at, span] = c_ref[at, span] * shrink[:, t : t + 1] + before[:, t : t + 1]
            rel = rel_col[at, :]
            holds = (rel >= lane * TILE) & (rel < (lane + 1) * TILE)
            old = t_all[at, :]
            moved = jnp.sum(old, axis=1, keepdims=True) * shrink + before
            inside = (rel >= g0 * TILE) & (rel < g1 * TILE)
            t_all[at, :] = jnp.where(inside, jnp.where(holds, moved, 0.0), old)
            total = jnp.sum(parts, axis=1, keepdims=True)
            sums = jnp.where(lane == SLOTS + g1 - 1, total, 0.0)
            of_sums = (lane >= SLOTS + g0) & (lane < SLOTS + g1)
            stats[at, :] = jnp.where(group, top, jnp.where(of_sums, sums, m))

    def close(i):
        first = ends[i - 1] + 1 if i else first_end
        with jax.named_scope(f"xe{i}"):
            for j in range(first, ends[i] + 1):
                if j < n_chunks - 1:
                    forwarded(j)
                else:
                    pl.when(odd == 1)(lambda: forwarded(n_chunks - 1))
                    pl.when(odd == 0)(twin_landed)
        with jax.named_scope(f"ce{i}"):
            finish_end(i)

    def prefix_before(parts):
        k = lax.broadcasted_iota(jnp.int32, (LANES, LANES), 0)
        c = lax.broadcasted_iota(jnp.int32, (LANES, LANES), 1)
        strict = jnp.where(k < c, 1.0, 0.0).astype(BF16)
        return sum(jnp.dot(p, strict, preferred_element_type=F32) for p in split3(parts))

    def complete(j):
        start, n = cols_of(j)
        cross_wait(j, 3 * half, start, start + n)

    def own_complete():
        place = wbuf.at[pl.ds(pl.multiple_of(z * depth, depth), depth)]
        pltpu.make_async_copy(place, place, wl).wait()

    order = service_order(plan, n_cols // LANES)
    folds = {j: (g0, g1) for j, g0, g1 in folds_of(plan, first_end)}
    tail = range(first_end, n_chunks)
    known = max(order.index((k, j)) for k in (0, 2) for j in tail)
    early = min(j for j in range(max(0, first_end - 7), n_chunks - 1) if order.index((1, j + 1)) > known)
    assert early < first_end
    m = len(ends) - 1
    closes = {n_chunks - 3: range(m - 2), n_chunks - 2: [m - 2], n_chunks - 1: [m - 1]}

    for what, j in order:
        if what == "h line":
            with jax.named_scope("hline"):
                arrived(h_place(v, z_one), 1, hid=z_one)
                arrived(h_place(v, lax.rem(z_one + 2, 4)), 2, hid=z_one)
                h_own.wait()
            h_chip.start()
            h_core.start()
        elif what == "h chip":
            with jax.named_scope("hchip"):
                arrived(h_place(v_two), 3, vocab=v_two)
            h_both.start()
        else:
            with jax.named_scope(f"w{what}_{j}"):
                landed(j, what)
            if (what, j) != (1, n_chunks - 1):
                forward(j, what).start()
            else:
                pl.when(odd == 1)(lambda: forward(n_chunks - 1, 1).start())
            if what != 1:
                continue
            if j == 1:
                with jax.named_scope("hcore"):
                    arrived(h_place(v_one), 4, vocab=v_one)
                    arrived(h_place(lax.rem(v_one + 2, 4)), 5, vocab=v_one)
                    own_complete()
            if 0 < j <= first_end:
                with jax.named_scope(f"x{j - 1}"):
                    complete(j - 1)
                with jax.named_scope(f"c{j - 1}"):
                    compute(j - 1)
                if j - 1 in folds:
                    with jax.named_scope(f"f{j - 1}"):
                        fold(*folds[j - 1])
            if j - 1 == early:
                with jax.named_scope("begin"):
                    cross_wait(first_end, 2 * half, cols_of(first_end)[0], n_cols)
                    for i in range(len(ends)):
                        begin_end(i)
            for i in closes.get(j, ()):
                close(i)
    close(m)

    lane = lax.broadcasted_iota(jnp.int32, (rows, LANES), 1)
    at_tgt = jnp.sum(t_all[...], axis=1, keepdims=True)
    turned = jnp.where(lane == 2 * SLOTS, at_tgt, stats[...]).T
    m, at_tgt = turned[0:SLOTS, :], turned[2 * SLOTS : 2 * SLOTS + 1, :]
    top = jnp.max(m, axis=0, keepdims=True)
    shrink = jnp.exp(m - top)
    parts = turned[SLOTS : 2 * SLOTS, :] * shrink
    t = lax.broadcasted_iota(jnp.int32, (SLOTS, rows), 0)
    start = jnp.where(t < n_whole, t * TILE, n_whole * (TILE - LANES) + t * LANES)
    stop = start + jnp.where(t < n_whole, TILE, LANES)
    rel = tgt_ref[...] - base
    known = rel < n_cols
    holds = (rel >= start) & (rel < stop) & known
    ahead = (stop <= rel) & known
    found = jnp.where(holds, at_tgt * shrink, jnp.where(ahead, parts, 0.0))
    zmsg[z, 0:1, :] = top
    zmsg[z, 1:2, :] = jnp.sum(parts, axis=0, keepdims=True)
    zmsg[z, 2:3, :] = jnp.sum(found, axis=0, keepdims=True)

    for k in range(3):
        mine = wbuf.at[w_rows(sources[k], x)]
        remote(mine, mine, ws.at[k], wr.at[0, k], hid=near).wait_send()
        if k == 1:
            mine = wbuf.at[w_rows(sources[k], x), pl.ds(0, n_cols - LANES)]
        remote(mine, mine, xs.at[k], xr.at[0], data=1 - x).wait_send()
    forward(n_chunks - 2, 1).wait_send()
    pl.when(odd == 1)(lambda: forward(n_chunks - 1, 1).wait_send())

    @pl.when(twins)
    def _():
        send_twin(0).wait_send()
        send_twin(1).wait_send()

    mine = hbuf.at[pl.ds(0, quarter * 15 // 4)]
    remote(mine, mine, hs, hr.at[0], hid=near).wait_send()

    def z_send(i):
        return remote(zmsg.at[z], zmsg.at[z], zs, zr, hid=(near, inner_far, outer_far)[i])

    def v_send(d):
        to = lax.rem(v + d, 4)
        return remote(vmsg.at[v], vmsg.at[v], vs, vr, vocab=to)

    for i in (2, 1, 0):
        z_send(i).start()
    k = lax.broadcasted_iota(jnp.int32, (SLOTS, SLOTS), 0)
    c = lax.broadcasted_iota(jnp.int32, (SLOTS, SLOTS), 1)
    strict = jnp.where(c < k, 1.0, 0.0).astype(BF16)
    before = sum(jnp.dot(strict, p, preferred_element_type=F32) for p in split3(parts))
    rest = jnp.zeros((LANES - 2 * SLOTS, rows), F32)
    coef_ref[...] = jnp.concatenate([shrink, before, rest], axis=0).T
    z_all = remote(zmsg.at[pl.ds(0, 3)], zmsg.at[pl.ds(0, 3)], zs, zr, hid=near)
    with jax.named_scope("z"):
        z_all.wait_recv()

    ids = tgt_ref[...]
    maxes = [zmsg[h, 0:1, :] for h in range(4)]
    v_max = functools.reduce(jnp.maximum, maxes)
    v_sum = jnp.zeros((1, rows), F32)
    v_tgt = jnp.zeros((1, rows), F32)
    mine_before = jnp.zeros((1, rows), F32)
    for h in range(4):
        mine_before = jnp.where(h == z, v_sum, mine_before)
        f = jnp.exp(maxes[h] - v_max)
        low = (v * 4 + h) * n_cols
        inside = (ids >= low) & (ids < low + n_cols)
        v_tgt += jnp.where(inside, zmsg[h, 2:3, :] * f + v_sum, 0.0)
        v_sum += zmsg[h, 1:2, :] * f
    vmsg[v, 0:1, :] = v_max
    vmsg[v, 1:2, :] = v_sum
    vmsg[v, 2:3, :] = v_tgt

    z_all.wait_send()
    for d in (2, 1, 3):
        v_send(d).start()
    v_all = remote(vmsg.at[pl.ds(0, 3)], vmsg.at[pl.ds(0, 3)], vs, vr, vocab=v_one)
    with jax.named_scope("v"):
        v_all.wait_recv()

    maxes = [vmsg[u, 0:1, :] for u in range(4)]
    g_max = functools.reduce(jnp.maximum, maxes)
    g_sum = jnp.zeros((1, rows), F32)
    g_tgt = jnp.zeros((1, rows), F32)
    g_before = jnp.zeros((1, rows), F32)
    for u in range(4):
        f = jnp.exp(maxes[u] - g_max)
        g_before = jnp.where(u == v, g_sum + mine_before * f, g_before)
        low = u * 4 * n_cols
        inside = (ids >= low) & (ids < low + 4 * n_cols)
        g_tgt += jnp.where(inside, vmsg[u, 2:3, :] * f + g_sum, 0.0)
        g_sum += vmsg[u, 1:2, :] * f
    tgt_out_ref[...] = g_tgt / g_sum
    factor_ref[0:1, :] = jnp.exp(zmsg[z, 0:1, :] - g_max) / g_sum
    factor_ref[1:2, :] = g_before / g_sum
    v_all.wait_send()


def finish_kernel(tiles, lanes, c_ref, coef_ref, factor_ref, tgt_ref, out_ref, tgt_out_ref, buf, factor_col, sems, tgt_sem):
    slots, n, n_cols = buf.shape
    steps = c_ref.shape[0] // n
    tgt_copy = pltpu.make_async_copy(tgt_ref, tgt_out_ref, tgt_sem)
    tgt_copy.start()

    def put(i):
        slot = lax.rem(i, slots)
        at = pl.ds(pl.multiple_of(i * n, n), n)
        return pltpu.make_async_copy(buf.at[slot], out_ref.at[at], sems.at[slot])

    @pl.loop(0, steps)
    def _(i):
        slot = lax.rem(i, slots)

        @pl.when(i >= slots)
        def _():
            put(i - slots).wait()

        at = pl.ds(pl.multiple_of(i * n, n), n)
        turn = max(n, LANES)

        @pl.when(lax.rem(i, turn // n) == 0)
        def _():
            some = pl.ds(pl.multiple_of(i // (turn // n) * turn, turn), turn)
            factor_col[some, :] = factor_ref[:, some].T

        lane = lax.broadcasted_iota(jnp.int32, (n, LANES), 1)
        coef = coef_ref[at, :] * factor_col[at, 0:1] + jnp.where(lane < SLOTS, 0.0, factor_col[at, 1:2])
        for (start, width), k in zip(tiles, lanes):
            span = slice(start, start + width)
            buf[slot, :, span] = c_ref[at, span] * coef[:, k : k + 1] + coef[:, SLOTS + k : SLOTS + k + 1]
        put(i).start()

    tgt_copy.wait()
    for i in range(max(0, steps - slots), steps):
        with jax.named_scope(f"fe{i}"):
            put(i).wait()


def solution(mesh):
    n_hid, n_voc = mesh.shape["hid"], mesh.shape["vocab"]
    assert n_hid == 4 and n_voc == 4 and mesh.shape["data"] == 2

    def local_step(h_blk, w_blk, temp_blk, tgt_blk):
        rows, depth = h_blk.shape
        n_cols = w_blk.shape[1] // n_hid
        assert n_cols % LANES == 0
        tiles = tiles_of(n_cols // LANES)
        n_tiles = len(tiles)
        assert n_tiles <= SLOTS
        plan = chunks_of(n_cols // LANES)
        n_chunks = len(plan)
        last_whole = sum(width == TILE for _, width in tiles) - 1
        first_end = [first for first, *_ in plan].index(2 * last_whole)
        vmem = pl.BlockSpec(memory_space=pltpu.VMEM)
        hbm = pl.BlockSpec(memory_space=pltpu.HBM)
        dma = pltpu.SemaphoreType.DMA
        table = pltpu.VMEM((rows, LANES), F32)
        c, coef, factor, tgt = pl.pallas_call(
            functools.partial(prefix_kernel, n_cols),
            out_shape=(
                pltpu.VMEM((rows, n_cols), F32),
                pltpu.VMEM((rows, LANES), F32),
                pltpu.VMEM((8, rows), F32),
                pltpu.VMEM((1, rows), F32),
            ),
            in_specs=[hbm] * 4,
            out_specs=[vmem] * 4,
            scratch_shapes=[
                pltpu.VMEM((4 * depth, n_cols), BF16),
                pltpu.VMEM((rows, 4 * depth), BF16),
                pltpu.VMEM((rows, TILE), F32),
                pltpu.VMEM((3 * TILE, TILE), BF16),
                pltpu.VMEM((3 * LANES, LANES), BF16),
                table,
                table,
                table,
                pltpu.VMEM((rows, LANES), jnp.int32),
                pltpu.VMEM((1, rows), F32),
                pltpu.VMEM((1, rows), jnp.int32),
                pltpu.VMEM((4, 3, rows), F32),
                pltpu.VMEM((4, 3, rows), F32),
                pltpu.VMEM((8, rows), F32),
                dma((3,)),
                dma((n_chunks, 3)),
                dma((5,)),
                dma((n_chunks + 1,)),
                dma((2,)),
                dma,
                dma,
                dma,
                dma,
                dma((6,)),
                dma,
                dma,
                dma,
                dma,
                dma((2,)),
            ],
            compiler_params=pltpu.CompilerParams(
                collective_id=0, has_side_effects=True, vmem_limit_bytes=37 << 20
            ),
            name="prefix",
        )(h_blk, w_blk, temp_blk.reshape(1, rows), tgt_blk.reshape(1, rows))
        n = min(rows, 64)
        lanes = list(range(n_tiles))
        for _, g0, g1 in folds_of(plan, first_end):
            lanes[g0:g1] = [g0] * (g1 - g0)
        cdf, cdf_tgt = pl.pallas_call(
            functools.partial(finish_kernel, tiles, lanes),
            out_shape=(
                jax.ShapeDtypeStruct((rows, n_cols), F32),
                jax.ShapeDtypeStruct((1, rows), F32),
            ),
            in_specs=[vmem] * 4,
            out_specs=[hbm, hbm],
            scratch_shapes=[
                pltpu.VMEM((4, n, n_cols), F32),
                pltpu.VMEM((rows, 8), F32),
                dma((4,)),
                dma,
            ],
            compiler_params=pltpu.CompilerParams(vmem_limit_bytes=9 << 20),
            name="finish",
        )(c, coef, factor, tgt)
        return cdf, cdf_tgt.reshape(rows)

    return jax.shard_map(
        local_step,
        mesh=mesh,
        in_specs=(P("data", "hid"), P("hid", "vocab"), P("data"), P("data")),
        out_specs=(P("data", ("vocab", "hid")), P("data")),
        check_vma=False,
    )
```

```python
import functools

import jax
import jax.numpy as jnp
from jax import lax
from jax.experimental import pallas as pl
from jax.experimental.pallas import tpu as pltpu
from jax.sharding import PartitionSpec as P

MESH = pl.DeviceIdType.MESH
F32 = jnp.float32
BF16 = jnp.bfloat16
TILE = 256
LANES = 128
SLOTS = 32
LOWEST = float(jnp.finfo(jnp.float32).min)


def tiles_of(blocks):
    whole = (blocks - 3) // 2
    tiles = [(t * TILE, TILE) for t in range(whole)]
    return tiles + [(b * LANES, LANES) for b in range(2 * whole, blocks)]


def chunks_of(blocks):
    whole = (blocks - 3) // 2
    sizes, left = [], 2 * whole - 2
    for size in (2, 2, 2, 2, 4, 4):
        if left > size:
            sizes.append(size)
            left -= size
    while left > 0:
        sizes.append(min(6, left))
        left -= sizes[-1]
    plan, at = [], 0
    for size in reversed(sizes):
        plan.append((at, size, 0, 2))
        at += size
    plan += [(b, 1, 0, 2) for b in range(at, blocks - 2)]
    return plan + [(b, 1, r, 1) for b in (blocks - 2, blocks - 1) for r in (0, 1)]


def service_order(plan, blocks):
    events = [(0.15 * blocks, "h line", 0), (0.28 * blocks, "h chip", 0)]
    for j, (first, size, _, _) in enumerate(plan):
        end = first + size
        events.append((first + size / 3 + 2, 0, j))
        events.append((end + 2, 2, j))
        events.append((min(1.86 * end, 0.68 * blocks + 0.6 * end) + 2, 1, j))
    events.sort(key=lambda e: e[0])
    order = [e[1:] for e in events]
    for j in range(len(plan)):
        at = max(order.index((k, j)) for k in (0, 1, 2))
        order.remove((1, j))
        order.insert(at, (1, j))
    return order


def folds_of(plan, first_end):
    folds, at = [], 0
    for j in (first_end // 3, 3 * first_end // 5):
        stop = sum(plan[j][:2]) // 2 - 1
        if j < first_end and stop > at:
            folds.append((j, at, stop))
            at = stop
    return folds


def split3(e):
    hi = e.astype(BF16)
    rest = e - hi.astype(F32)
    mid = rest.astype(BF16)
    low = (rest - mid.astype(F32)).astype(BF16)
    return hi, mid, low


def prefix_kernel(
    n_cols, h_ref, w_ref, temp_hbm, tgt_hbm,
    c_ref, coef_ref, factor_ref, tgt_out_ref,
    wbuf, hbuf, zbuf, tri, tri_last, stats, t_all, temp_col, rel_col, temp_ref, tgt_ref, zmsg, vmsg, back,
    ws, wr, xs, xr, ts, tr, wl, hl, hs, hr, zs, zr, vs, vr, rl,
):
    x, z, v = lax.axis_index("data"), lax.axis_index("hid"), lax.axis_index("vocab")
    rows, depth = h_ref.shape
    half, quarter = depth // 2, rows // 4
    tiles = tiles_of(n_cols // LANES)
    n_tiles = len(tiles)
    n_whole = sum(width == TILE for _, width in tiles)
    plan = chunks_of(n_cols // LANES)
    n_chunks = len(plan)
    ends = [[j for j, (first, *_) in enumerate(plan) if first * LANES < sum(tiles[t])][-1] for t in range(n_whole - 1, n_tiles)]
    first_end = ends[0] - 1

    side = z // 2
    outer_far, inner_far, near = 3 - 3 * side, 2 - side, 1 - z + 4 * side
    is_outer = jnp.where(z == side * 3, 1, 0)
    z_two, z_one = lax.rem(z + 2, 4), near
    v_two, v_one = lax.rem(v + 2, 4), v + 1 - 2 * lax.rem(v, 2)
    sources = (near, inner_far, outer_far)

    def cols_of(j):
        first, size, _, _ = plan[j]
        return first * LANES, size * LANES

    def w_rows(source, part, j=None):
        at, n = (0, half) if j is None else (plan[j][2] * (half // 2), plan[j][3] * (half // 2))
        return pl.ds(pl.multiple_of(source * depth + part * half + at, half // 2), n)

    def w_place(j, source, part):
        start, n = cols_of(j)
        return wbuf.at[w_rows(source, part, j), pl.ds(start, n)]

    def h_place(q, block=None):
        at = pl.ds(pl.multiple_of(q * quarter, quarter), quarter)
        if block is None:
            return hbuf.at[at]
        return hbuf.at[at, pl.ds(pl.multiple_of(block * depth, depth), depth)]

    def remote(src, dst, send, recv, **to):
        return pltpu.make_async_remote_copy(
            src_ref=src, dst_ref=dst, send_sem=send, recv_sem=recv, device_id=to, device_id_type=MESH
        )

    def w_source(j, part, dest):
        start, n = cols_of(j)
        return w_ref.at[w_rows(0, part, j), pl.ds(pl.multiple_of(dest * n_cols + start, LANES), n)]

    def direct(j, k, dest, slot):
        return remote(w_source(j, x, dest), w_place(j, z, x), ws.at[k], wr.at[j, slot], hid=dest)

    def send_near(j):
        return direct(j, 0, near, 0)

    odd = lax.rem(v, 2)
    far_first = outer_far + odd * (inner_far - outer_far)
    far_second = inner_far + odd * (outer_far - inner_far)

    def send_far(j, i):
        dests = (far_first, far_second) if j < first_end else (outer_far, inner_far)
        return direct(j, 1 + i, dests[i], 1 + is_outer)

    def send_twin(i):
        dest = (outer_far, inner_far)[i]
        return remote(w_source(n_chunks - 1, 1 - x, dest), w_place(n_chunks - 1, z, 1 - x), ts.at[i], tr, hid=dest)

    def twin_landed():
        place = w_place(n_chunks - 1, inner_far, 1 - x)
        remote(place, place, ts.at[0], tr, hid=inner_far).wait_recv()

    def landed(j, k):
        place = w_place(j, sources[k], x)
        remote(place, place, ws.at[k], wr.at[j, k], hid=sources[k]).wait_recv()

    def forward(j, k):
        place = w_place(j, sources[k], x)
        send = 3 if k == 1 and j == n_chunks - 2 else k
        return remote(place, place, xs.at[send], xr.at[cross(j, k)], data=1 - x)

    def cross(j, k):
        if j < first_end:
            return j
        return first_end if k != 1 else 1 + j

    def cross_wait(slot, count, start, stop):
        place = wbuf.at[pl.ds(0, count), pl.ds(start, stop - start)]
        remote(place, place, xs.at[0], xr.at[slot], data=1 - x).wait_recv()

    def forwarded(j):
        place = w_place(j, inner_far, 1 - x)
        remote(place, place, xs.at[1], xr.at[cross(j, 1)], data=1 - x).wait_recv()

    def own(j):
        start, n = cols_of(j)
        return pltpu.make_async_copy(
            w_ref.at[:, pl.ds(pl.multiple_of(z * n_cols + start, LANES), n)],
            wbuf.at[pl.ds(pl.multiple_of(z * depth, depth), depth), pl.ds(start, n)],
            wl,
        )

    h_mine = h_ref.at[pl.ds(pl.multiple_of(v * quarter, quarter), quarter)]
    h_own = pltpu.make_async_copy(h_mine, h_place(v, z), hl)
    h_two = remote(h_mine, h_place(v, z), hs, hr.at[0], hid=z_two)
    h_one = remote(h_mine, h_place(v, z), hs, hr.at[1], hid=z_one)
    h_relay = remote(h_place(v, z_two), h_place(v, z_two), hs, hr.at[2], hid=z_one)
    h_chip = remote(h_place(v), h_place(v), hs, hr.at[3], vocab=v_two)
    h_core = remote(h_place(v), h_place(v), hs, hr.at[4], vocab=v_one)
    h_both = remote(h_place(v_two), h_place(v_two), hs, hr.at[5], vocab=v_one)

    def arrived(place, i, **frm):
        remote(place, place, hs, hr.at[i], **frm).wait_recv()

    barrier = pltpu.get_barrier_semaphore()
    peers = [{"hid": lax.rem(z + d, 4)} for d in (1, 2, 3)]
    peers += [{"data": 1 - x}] + [{"vocab": lax.rem(v + d, 4)} for d in (1, 2, 3)]
    for peer in peers:
        pl.semaphore_signal(barrier, inc=1, device_id=peer, device_id_type=MESH)
    row_copies = [
        pltpu.make_async_copy(temp_hbm, temp_ref, rl.at[0]),
        pltpu.make_async_copy(tgt_hbm, tgt_ref, rl.at[1]),
    ]
    for copy in (h_own, *row_copies):
        copy.start()
    for j in range(n_chunks):
        if plan[j][2] == 0:
            own(j).start()
    with jax.named_scope("bar"):
        pl.semaphore_wait(barrier, len(peers))

    h_two.start()
    h_one.start()
    send_near(0).start()
    send_far(0, 0).start()

    def ones_below(ref, width):
        k = lax.broadcasted_iota(jnp.int32, (width, width), 0)
        c = lax.broadcasted_iota(jnp.int32, (width, width), 1)
        block = jnp.where(k <= c, 1.0, 0.0).astype(BF16)
        for i in range(3):
            ref[pl.ds(i * width, width), :] = block

    ones_below(tri, TILE)
    ones_below(tri_last, LANES)
    base = (v * 4 + z) * n_cols
    for copy in row_copies:
        copy.wait()
    back[0:1, :] = temp_ref[...]
    back[1:2, :] = (tgt_ref[...] - base).astype(F32)
    cols8 = back[...].T
    temp_col[...] = jnp.broadcast_to(cols8[:, 0:1], temp_col.shape)
    rel_col[...] = jnp.broadcast_to(cols8[:, 1:2], rel_col.shape).astype(jnp.int32)
    slot = lax.broadcasted_iota(jnp.int32, stats.shape, 1)
    stats[...] = jnp.where(slot < SLOTS, LOWEST, 0.0)
    t_all[...] = jnp.zeros(t_all.shape, F32)

    with jax.named_scope("h0"):
        arrived(h_place(v, z_two), 0, hid=z_two)
    h_relay.start()
    send_far(0, 1).start()
    for j in range(1, n_chunks):
        send_near(j).start()
        send_far(j, 0).start()
        send_far(j, 1).start()

    @pl.when(is_outer == 0)
    def _():
        send_twin(0).start()
        send_twin(1).start()


    part, few = min(rows, 512), min(rows, 128)

    def logits_and_sums(product, sums):
        some = part if product is not None or sums[2] == TILE else min(rows, 2 * part)

        @pl.loop(0, rows // some)
        def _(i):
            if product is not None:
                _, new_start, new_width = product
                at = pl.ds(pl.multiple_of(i * part, part), part)
                new = jnp.dot(
                    hbuf[at, :], wbuf[:, pl.ds(new_start, new_width)], preferred_element_type=F32
                )
            for k in range(0, some, few) if sums is not None else ():
                prefix(pl.ds(pl.multiple_of(i * some + k, few), few), *sums)
            if product is not None:
                zbuf[at, 0:new_width] = new

    def prefix(at, t, start, width):
        pieces = width // LANES
        logits = zbuf[at, 0:width] * jnp.concatenate([temp_col[at, :]] * pieces, axis=1)
        lane = lax.broadcasted_iota(jnp.int32, (few, LANES), 1)
        top = jnp.max(logits, axis=1, keepdims=True)
        e = jnp.exp(logits - top)
        total = jnp.sum(e, axis=1, keepdims=True)
        stats[at, :] = jnp.where(lane == t, top, jnp.where(lane == SLOTS + t, total, stats[at, :]))
        table = tri if width == TILE else tri_last
        run = jnp.dot(jnp.concatenate(split3(e), axis=1), table[...], preferred_element_type=F32)
        c_ref[at, pl.ds(start, width)] = run
        rel = rel_col[at, :] - start
        hit = t_all[at, :]
        for p in range(pieces):
            hit += jnp.where(lane == rel - p * LANES, run[:, p * LANES : (p + 1) * LANES], 0.0)
        t_all[at, :] = hit

    def whole(t):
        return t, pl.multiple_of(t * TILE, TILE), TILE

    def compute(j):
        first, size = (n // 2 for n in plan[j][:2])
        stop = first + size
        if first == 0:
            logits_and_sums(whole(0), None)
            first = 1
        if first < stop:

            @pl.loop(first, stop)
            def _(t):
                logits_and_sums(whole(t), whole(t - 1))

        if j == first_end - 1:
            logits_and_sums(None, whole(stop - 1))

    def block_dot(at, block, start, width):
        lanes = pl.ds(pl.multiple_of(block * depth, depth), depth)
        return jnp.dot(hbuf[at, lanes], wbuf[lanes, start : start + width], preferred_element_type=F32)

    def begin_end(i):
        start, width = tiles[n_whole - 1 + i]

        @pl.loop(0, rows // part)
        def _(k):
            at = pl.ds(pl.multiple_of(k * part, part), part)
            c_ref[at, start : start + width] = (
                block_dot(at, z, start, width)
                + block_dot(at, near, start, width)
                + block_dot(at, outer_far, start, width)
            )

    def finish_end(i):
        t = n_whole - 1 + i
        start, width = tiles[t]
        every = slice(0, rows)
        zbuf[:, 0:width] = c_ref[:, start : start + width] + block_dot(every, inner_far, start, width)
        logits_and_sums(None, (t, start, width))

    def fold(g0, g1):
        @pl.loop(0, rows // few)
        def _(i):
            at = pl.ds(pl.multiple_of(i * few, few), few)
            lane = lax.broadcasted_iota(jnp.int32, (few, LANES), 1)
            group = (lane >= g0) & (lane < g1)
            m = stats[at, :]
            s = pltpu.roll(m, LANES - SLOTS, 1)
            top = jnp.max(jnp.where(group, m, LOWEST), axis=1, keepdims=True)
            shrink = jnp.where(group, jnp.exp(m - top), 0.0)
            parts = jnp.where(group, s, 0.0) * shrink
            before = prefix_before(parts)
            for t in range(g0, g1):
                span = slice(t * TILE, (t + 1) * TILE)
                c_ref[at, span] = c_ref[at, span] * shrink[:, t : t + 1] + before[:, t : t + 1]
            rel = rel_col[at, :]
            holds = (rel >= lane * TILE) & (rel < (lane + 1) * TILE)
            old = t_all[at, :]
            moved = jnp.sum(old, axis=1, keepdims=True) * shrink + before
            inside = (rel >= g0 * TILE) & (rel < g1 * TILE)
            t_all[at, :] = jnp.where(inside, jnp.where(holds, moved, 0.0), old)
            total = jnp.sum(parts, axis=1, keepdims=True)
            sums = jnp.where(lane == SLOTS + g1 - 1, total, 0.0)
            of_sums = (lane >= SLOTS + g0) & (lane < SLOTS + g1)
            stats[at, :] = jnp.where(group, top, jnp.where(of_sums, sums, m))

    def close(i):
        first = ends[i - 1] + 1 if i else first_end
        with jax.named_scope(f"xe{i}"):
            for j in range(first, ends[i] + 1):
                if j < n_chunks - 1:
                    forwarded(j)
                else:
                    twin_landed()
        with jax.named_scope(f"ce{i}"):
            finish_end(i)

    def prefix_before(parts):
        k = lax.broadcasted_iota(jnp.int32, (LANES, LANES), 0)
        c = lax.broadcasted_iota(jnp.int32, (LANES, LANES), 1)
        strict = jnp.where(k < c, 1.0, 0.0).astype(BF16)
        return sum(jnp.dot(p, strict, preferred_element_type=F32) for p in split3(parts))

    def complete(j):
        start, n = cols_of(j)
        cross_wait(j, 3 * half, start, start + n)

    def own_complete():
        place = wbuf.at[pl.ds(pl.multiple_of(z * depth, depth), depth)]
        pltpu.make_async_copy(place, place, wl).wait()

    order = service_order(plan, n_cols // LANES)
    folds = {j: (g0, g1) for j, g0, g1 in folds_of(plan, first_end)}
    tail = range(first_end, n_chunks)
    known = max(order.index((k, j)) for k in (0, 2) for j in tail)
    early = min(j for j in range(max(0, first_end - 7), n_chunks - 1) if order.index((1, j + 1)) > known)
    assert early < first_end
    m = len(ends) - 1
    closes = {n_chunks - 3: range(m - 2), n_chunks - 2: [m - 2], n_chunks - 1: [m - 1]}

    for what, j in order:
        if what == "h line":
            with jax.named_scope("hline"):
                arrived(h_place(v, z_one), 1, hid=z_one)
                arrived(h_place(v, lax.rem(z_one + 2, 4)), 2, hid=z_one)
                h_own.wait()
            h_chip.start()
            h_core.start()
        elif what == "h chip":
            with jax.named_scope("hchip"):
                arrived(h_place(v_two), 3, vocab=v_two)
            h_both.start()
        else:
            with jax.named_scope(f"w{what}_{j}"):
                landed(j, what)
            if (what, j) != (1, n_chunks - 1):
                forward(j, what).start()
            if what != 1:
                continue
            if j == 1:
                with jax.named_scope("hcore"):
                    arrived(h_place(v_one), 4, vocab=v_one)
                    arrived(h_place(lax.rem(v_one + 2, 4)), 5, vocab=v_one)
                    own_complete()
            if 0 < j <= first_end:
                with jax.named_scope(f"x{j - 1}"):
                    complete(j - 1)
                with jax.named_scope(f"c{j - 1}"):
                    compute(j - 1)
                if j - 1 in folds:
                    with jax.named_scope(f"f{j - 1}"):
                        fold(*folds[j - 1])
            if j - 1 == early:
                with jax.named_scope("begin"):
                    cross_wait(first_end, 2 * half, cols_of(first_end)[0], n_cols)
                    for i in range(len(ends)):
                        begin_end(i)
            for i in closes.get(j, ()):
                close(i)
    close(m)

    lane = lax.broadcasted_iota(jnp.int32, (rows, LANES), 1)
    at_tgt = jnp.sum(t_all[...], axis=1, keepdims=True)
    turned = jnp.where(lane == 2 * SLOTS, at_tgt, stats[...]).T
    m, at_tgt = turned[0:SLOTS, :], turned[2 * SLOTS : 2 * SLOTS + 1, :]
    top = jnp.max(m, axis=0, keepdims=True)
    shrink = jnp.exp(m - top)
    parts = turned[SLOTS : 2 * SLOTS, :] * shrink
    t = lax.broadcasted_iota(jnp.int32, (SLOTS, rows), 0)
    start = jnp.where(t < n_whole, t * TILE, n_whole * (TILE - LANES) + t * LANES)
    stop = start + jnp.where(t < n_whole, TILE, LANES)
    rel = tgt_ref[...] - base
    known = rel < n_cols
    holds = (rel >= start) & (rel < stop) & known
    ahead = (stop <= rel) & known
    found = jnp.where(holds, at_tgt * shrink, jnp.where(ahead, parts, 0.0))
    zmsg[z, 0:1, :] = top
    zmsg[z, 1:2, :] = jnp.sum(parts, axis=0, keepdims=True)
    zmsg[z, 2:3, :] = jnp.sum(found, axis=0, keepdims=True)

    for k in range(3):
        mine = wbuf.at[w_rows(sources[k], x)]
        remote(mine, mine, ws.at[k], wr.at[0, k], hid=near).wait_send()
        if k == 1:
            mine = wbuf.at[w_rows(sources[k], x), pl.ds(0, n_cols - LANES)]
        remote(mine, mine, xs.at[k], xr.at[0], data=1 - x).wait_send()
    forward(n_chunks - 2, 1).wait_send()

    @pl.when(is_outer == 0)
    def _():
        send_twin(0).wait_send()
        send_twin(1).wait_send()

    mine = hbuf.at[pl.ds(0, quarter * 15 // 4)]
    remote(mine, mine, hs, hr.at[0], hid=near).wait_send()

    def z_send(i):
        return remote(zmsg.at[z], zmsg.at[z], zs, zr, hid=(near, inner_far, outer_far)[i])

    def v_send(d):
        to = lax.rem(v + d, 4)
        return remote(vmsg.at[v], vmsg.at[v], vs, vr, vocab=to)

    for i in (2, 1, 0):
        z_send(i).start()
    k = lax.broadcasted_iota(jnp.int32, (SLOTS, SLOTS), 0)
    c = lax.broadcasted_iota(jnp.int32, (SLOTS, SLOTS), 1)
    strict = jnp.where(c < k, 1.0, 0.0).astype(BF16)
    before = sum(jnp.dot(strict, p, preferred_element_type=F32) for p in split3(parts))
    rest = jnp.zeros((LANES - 2 * SLOTS, rows), F32)
    coef_ref[...] = jnp.concatenate([shrink, before, rest], axis=0).T
    z_all = remote(zmsg.at[pl.ds(0, 3)], zmsg.at[pl.ds(0, 3)], zs, zr, hid=near)
    with jax.named_scope("z"):
        z_all.wait_recv()

    ids = tgt_ref[...]
    maxes = [zmsg[h, 0:1, :] for h in range(4)]
    v_max = functools.reduce(jnp.maximum, maxes)
    v_sum = jnp.zeros((1, rows), F32)
    v_tgt = jnp.zeros((1, rows), F32)
    mine_before = jnp.zeros((1, rows), F32)
    for h in range(4):
        mine_before = jnp.where(h == z, v_sum, mine_before)
        f = jnp.exp(maxes[h] - v_max)
        low = (v * 4 + h) * n_cols
        inside = (ids >= low) & (ids < low + n_cols)
        v_tgt += jnp.where(inside, zmsg[h, 2:3, :] * f + v_sum, 0.0)
        v_sum += zmsg[h, 1:2, :] * f
    vmsg[v, 0:1, :] = v_max
    vmsg[v, 1:2, :] = v_sum
    vmsg[v, 2:3, :] = v_tgt

    z_all.wait_send()
    for d in (2, 1, 3):
        v_send(d).start()
    v_all = remote(vmsg.at[pl.ds(0, 3)], vmsg.at[pl.ds(0, 3)], vs, vr, vocab=v_one)
    with jax.named_scope("v"):
        v_all.wait_recv()

    maxes = [vmsg[u, 0:1, :] for u in range(4)]
    g_max = functools.reduce(jnp.maximum, maxes)
    g_sum = jnp.zeros((1, rows), F32)
    g_tgt = jnp.zeros((1, rows), F32)
    g_before = jnp.zeros((1, rows), F32)
    for u in range(4):
        f = jnp.exp(maxes[u] - g_max)
        g_before = jnp.where(u == v, g_sum + mine_before * f, g_before)
        low = u * 4 * n_cols
        inside = (ids >= low) & (ids < low + 4 * n_cols)
        g_tgt += jnp.where(inside, vmsg[u, 2:3, :] * f + g_sum, 0.0)
        g_sum += vmsg[u, 1:2, :] * f
    tgt_out_ref[...] = g_tgt / g_sum
    factor_ref[0:1, :] = jnp.exp(zmsg[z, 0:1, :] - g_max) / g_sum
    factor_ref[1:2, :] = g_before / g_sum
    v_all.wait_send()


def finish_kernel(tiles, lanes, c_ref, coef_ref, factor_ref, tgt_ref, out_ref, tgt_out_ref, buf, factor_col, sems, tgt_sem):
    slots, n, n_cols = buf.shape
    steps = c_ref.shape[0] // n
    tgt_copy = pltpu.make_async_copy(tgt_ref, tgt_out_ref, tgt_sem)
    tgt_copy.start()

    def put(i):
        slot = lax.rem(i, slots)
        at = pl.ds(pl.multiple_of(i * n, n), n)
        return pltpu.make_async_copy(buf.at[slot], out_ref.at[at], sems.at[slot])

    @pl.loop(0, steps)
    def _(i):
        slot = lax.rem(i, slots)

        @pl.when(i >= slots)
        def _():
            put(i - slots).wait()

        at = pl.ds(pl.multiple_of(i * n, n), n)
        turn = max(n, LANES)

        @pl.when(lax.rem(i, turn // n) == 0)
        def _():
            some = pl.ds(pl.multiple_of(i // (turn // n) * turn, turn), turn)
            factor_col[some, :] = factor_ref[:, some].T

        lane = lax.broadcasted_iota(jnp.int32, (n, LANES), 1)
        coef = coef_ref[at, :] * factor_col[at, 0:1] + jnp.where(lane < SLOTS, 0.0, factor_col[at, 1:2])
        for (start, width), k in zip(tiles, lanes):
            span = slice(start, start + width)
            buf[slot, :, span] = c_ref[at, span] * coef[:, k : k + 1] + coef[:, SLOTS + k : SLOTS + k + 1]
        put(i).start()

    tgt_copy.wait()
    for i in range(max(0, steps - slots), steps):
        with jax.named_scope(f"fe{i}"):
            put(i).wait()


def solution(mesh):
    n_hid, n_voc = mesh.shape["hid"], mesh.shape["vocab"]
    assert n_hid == 4 and n_voc == 4 and mesh.shape["data"] == 2

    def local_step(h_blk, w_blk, temp_blk, tgt_blk):
        rows, depth = h_blk.shape
        n_cols = w_blk.shape[1] // n_hid
        assert n_cols % LANES == 0
        tiles = tiles_of(n_cols // LANES)
        n_tiles = len(tiles)
        assert n_tiles <= SLOTS
        plan = chunks_of(n_cols // LANES)
        n_chunks = len(plan)
        last_whole = sum(width == TILE for _, width in tiles) - 1
        first_end = [first for first, *_ in plan].index(2 * last_whole)
        vmem = pl.BlockSpec(memory_space=pltpu.VMEM)
        hbm = pl.BlockSpec(memory_space=pltpu.HBM)
        dma = pltpu.SemaphoreType.DMA
        table = pltpu.VMEM((rows, LANES), F32)
        c, coef, factor, tgt = pl.pallas_call(
            functools.partial(prefix_kernel, n_cols),
            out_shape=(
                pltpu.VMEM((rows, n_cols), F32),
                pltpu.VMEM((rows, LANES), F32),
                pltpu.VMEM((8, rows), F32),
                pltpu.VMEM((1, rows), F32),
            ),
            in_specs=[hbm] * 4,
            out_specs=[vmem] * 4,
            scratch_shapes=[
                pltpu.VMEM((4 * depth, n_cols), BF16),
                pltpu.VMEM((rows, 4 * depth), BF16),
                pltpu.VMEM((rows, TILE), F32),
                pltpu.VMEM((3 * TILE, TILE), BF16),
                pltpu.VMEM((3 * LANES, LANES), BF16),
                table,
                table,
                table,
                pltpu.VMEM((rows, LANES), jnp.int32),
                pltpu.VMEM((1, rows), F32),
                pltpu.VMEM((1, rows), jnp.int32),
                pltpu.VMEM((4, 3, rows), F32),
                pltpu.VMEM((4, 3, rows), F32),
                pltpu.VMEM((8, rows), F32),
                dma((3,)),
                dma((n_chunks, 3)),
                dma((4,)),
                dma((n_chunks,)),
                dma((2,)),
                dma,
                dma,
                dma,
                dma,
                dma((6,)),
                dma,
                dma,
                dma,
                dma,
                dma((2,)),
            ],
            compiler_params=pltpu.CompilerParams(
                collective_id=0, has_side_effects=True, vmem_limit_bytes=37 << 20
            ),
            name="prefix",
        )(h_blk, w_blk, temp_blk.reshape(1, rows), tgt_blk.reshape(1, rows))
        n = min(rows, 64)
        lanes = list(range(n_tiles))
        for _, g0, g1 in folds_of(plan, first_end):
            lanes[g0:g1] = [g0] * (g1 - g0)
        cdf, cdf_tgt = pl.pallas_call(
            functools.partial(finish_kernel, tiles, lanes),
            out_shape=(
                jax.ShapeDtypeStruct((rows, n_cols), F32),
                jax.ShapeDtypeStruct((1, rows), F32),
            ),
            in_specs=[vmem] * 4,
            out_specs=[hbm, hbm],
            scratch_shapes=[
                pltpu.VMEM((4, n, n_cols), F32),
                pltpu.VMEM((rows, 8), F32),
                dma((4,)),
                dma,
            ],
            compiler_params=pltpu.CompilerParams(vmem_limit_bytes=9 << 20),
            name="finish",
        )(c, coef, factor, tgt)
        return cdf, cdf_tgt.reshape(rows)

    return jax.shard_map(
        local_step,
        mesh=mesh,
        in_specs=(P("data", "hid"), P("hid", "vocab"), P("data"), P("data")),
        out_specs=(P("data", ("vocab", "hid")), P("data")),
        check_vma=False,
    )
```

```python
import functools

import jax
import jax.numpy as jnp
from jax import lax
from jax.experimental import pallas as pl
from jax.experimental.pallas import tpu as pltpu
from jax.sharding import PartitionSpec as P

MESH = pl.DeviceIdType.MESH
F32 = jnp.float32
BF16 = jnp.bfloat16
TILE = 256
LANES = 128
SLOTS = 32
LOWEST = float(jnp.finfo(jnp.float32).min)


def tiles_of(blocks):
    whole = (blocks - 3) // 2
    tiles = [(t * TILE, TILE) for t in range(whole)]
    return tiles + [(b * LANES, LANES) for b in range(2 * whole, blocks)]


def chunks_of(blocks):
    whole = (blocks - 3) // 2
    sizes, left = [], 2 * whole - 2
    for size in (2, 2, 2, 2, 4, 4):
        if left > size:
            sizes.append(size)
            left -= size
    while left > 0:
        sizes.append(min(6, left))
        left -= sizes[-1]
    plan, at = [], 0
    for size in reversed(sizes):
        plan.append((at, size, 0, 2))
        at += size
    plan += [(b, 1, 0, 2) for b in range(at, blocks - 2)]
    return plan + [(b, 1, r, 1) for b in (blocks - 2, blocks - 1) for r in (0, 1)]


def service_order(plan, blocks):
    events = [(0.15 * blocks, "h line", 0), (0.28 * blocks, "h chip", 0)]
    for j, (first, size, _, _) in enumerate(plan):
        end = first + size
        events.append((first + size / 3 + 2, 0, j))
        events.append((end + 2, 2, j))
        events.append((min(1.86 * end, 0.68 * blocks + 0.6 * end) + 2, 1, j))
    events.sort(key=lambda e: e[0])
    order = [e[1:] for e in events]
    for j in range(len(plan)):
        at = max(order.index((k, j)) for k in (0, 1, 2))
        order.remove((1, j))
        order.insert(at, (1, j))
    return order


def folds_of(plan, first_end):
    folds, at = [], 0
    for j in (first_end // 3, 3 * first_end // 5):
        stop = sum(plan[j][:2]) // 2 - 1
        if j < first_end and stop > at:
            folds.append((j, at, stop))
            at = stop
    return folds


def split3(e):
    hi = e.astype(BF16)
    rest = e - hi.astype(F32)
    mid = rest.astype(BF16)
    low = (rest - mid.astype(F32)).astype(BF16)
    return hi, mid, low


def prefix_kernel(
    n_cols, h_ref, w_ref, temp_hbm, tgt_hbm,
    c_ref, coef_ref, factor_ref, tgt_out_ref,
    wbuf, hbuf, zbuf, tri, tri_last, stats, t_all, temp_col, rel_col, temp_ref, tgt_ref, zmsg, vmsg, back,
    ws, wr, xs, xr, ts, tr, wl, hl, hs, hr, zs, zr, vs, vr, rl,
):
    x, z, v = lax.axis_index("data"), lax.axis_index("hid"), lax.axis_index("vocab")
    rows, depth = h_ref.shape
    half, quarter = depth // 2, rows // 4
    tiles = tiles_of(n_cols // LANES)
    n_tiles = len(tiles)
    n_whole = sum(width == TILE for _, width in tiles)
    plan = chunks_of(n_cols // LANES)
    n_chunks = len(plan)
    ends = [[j for j, (first, *_) in enumerate(plan) if first * LANES < sum(tiles[t])][-1] for t in range(n_whole - 1, n_tiles)]
    first_end = ends[0] - 1

    side = z // 2
    outer_far, inner_far, near = 3 - 3 * side, 2 - side, 1 - z + 4 * side
    is_outer = jnp.where(z == side * 3, 1, 0)
    z_two, z_one = lax.rem(z + 2, 4), near
    v_two, v_one = lax.rem(v + 2, 4), v + 1 - 2 * lax.rem(v, 2)
    sources = (near, inner_far, outer_far)

    def cols_of(j):
        first, size, _, _ = plan[j]
        return first * LANES, size * LANES

    def w_rows(source, part, j=None):
        at, n = (0, half) if j is None else (plan[j][2] * (half // 2), plan[j][3] * (half // 2))
        return pl.ds(pl.multiple_of(source * depth + part * half + at, half // 2), n)

    def w_place(j, source, part):
        start, n = cols_of(j)
        return wbuf.at[w_rows(source, part, j), pl.ds(start, n)]

    def h_place(q, block=None):
        at = pl.ds(pl.multiple_of(q * quarter, quarter), quarter)
        if block is None:
            return hbuf.at[at]
        return hbuf.at[at, pl.ds(pl.multiple_of(block * depth, depth), depth)]

    def remote(src, dst, send, recv, **to):
        return pltpu.make_async_remote_copy(
            src_ref=src, dst_ref=dst, send_sem=send, recv_sem=recv, device_id=to, device_id_type=MESH
        )

    def w_source(j, part, dest):
        start, n = cols_of(j)
        return w_ref.at[w_rows(0, part, j), pl.ds(pl.multiple_of(dest * n_cols + start, LANES), n)]

    def direct(j, k, dest, slot):
        return remote(w_source(j, x, dest), w_place(j, z, x), ws.at[k], wr.at[j, slot], hid=dest)

    def send_near(j):
        return direct(j, 0, near, 0)

    odd = lax.rem(v, 2)
    far_first = outer_far + odd * (inner_far - outer_far)
    far_second = inner_far + odd * (outer_far - inner_far)

    def send_far(j, i):
        return direct(j, 1 + i, (far_first, far_second)[i], 1 + is_outer)

    def send_twin(i):
        dest = (far_first, far_second)[i]
        return remote(w_source(n_chunks - 1, 1 - x, dest), w_place(n_chunks - 1, z, 1 - x), ts.at[i], tr, hid=dest)

    def twin_landed():
        place = w_place(n_chunks - 1, inner_far, 1 - x)
        remote(place, place, ts.at[0], tr, hid=inner_far).wait_recv()

    def landed(j, k):
        place = w_place(j, sources[k], x)
        remote(place, place, ws.at[k], wr.at[j, k], hid=sources[k]).wait_recv()

    def forward(j, k):
        place = w_place(j, sources[k], x)
        send = 3 if k == 1 and j == n_chunks - 2 else k
        return remote(place, place, xs.at[send], xr.at[cross(j, k)], data=1 - x)

    def cross(j, k):
        if j < first_end:
            return j
        return first_end if k != 1 else 1 + j

    def cross_wait(slot, count, start, stop):
        place = wbuf.at[pl.ds(0, count), pl.ds(start, stop - start)]
        remote(place, place, xs.at[0], xr.at[slot], data=1 - x).wait_recv()

    def forwarded(j):
        place = w_place(j, inner_far, 1 - x)
        remote(place, place, xs.at[1], xr.at[cross(j, 1)], data=1 - x).wait_recv()

    def own(j):
        start, n = cols_of(j)
        return pltpu.make_async_copy(
            w_ref.at[:, pl.ds(pl.multiple_of(z * n_cols + start, LANES), n)],
            wbuf.at[pl.ds(pl.multiple_of(z * depth, depth), depth), pl.ds(start, n)],
            wl,
        )

    h_mine = h_ref.at[pl.ds(pl.multiple_of(v * quarter, quarter), quarter)]
    h_own = pltpu.make_async_copy(h_mine, h_place(v, z), hl)
    h_two = remote(h_mine, h_place(v, z), hs, hr.at[0], hid=z_two)
    h_one = remote(h_mine, h_place(v, z), hs, hr.at[1], hid=z_one)
    h_relay = remote(h_place(v, z_two), h_place(v, z_two), hs, hr.at[2], hid=z_one)
    h_chip = remote(h_place(v), h_place(v), hs, hr.at[3], vocab=v_two)
    h_core = remote(h_place(v), h_place(v), hs, hr.at[4], vocab=v_one)
    h_both = remote(h_place(v_two), h_place(v_two), hs, hr.at[5], vocab=v_one)

    def arrived(place, i, **frm):
        remote(place, place, hs, hr.at[i], **frm).wait_recv()

    barrier = pltpu.get_barrier_semaphore()
    peers = [{"hid": outer_far}, {"hid": inner_far}, {"hid": near}, {"data": 1 - x}]
    peers += [{"vocab": lax.rem(v + d, 4)} for d in (2, 1, 3)]
    for peer in peers:
        pl.semaphore_signal(barrier, inc=1, device_id=peer, device_id_type=MESH)
    row_copies = [
        pltpu.make_async_copy(temp_hbm, temp_ref, rl.at[0]),
        pltpu.make_async_copy(tgt_hbm, tgt_ref, rl.at[1]),
    ]
    for copy in (h_own, *row_copies):
        copy.start()
    for j in range(n_chunks):
        if plan[j][2] == 0:
            own(j).start()
    with jax.named_scope("bar"):
        pl.semaphore_wait(barrier, len(peers))

    h_two.start()
    h_one.start()
    send_near(0).start()
    send_far(0, 0).start()

    def ones_below(ref, width):
        k = lax.broadcasted_iota(jnp.int32, (width, width), 0)
        c = lax.broadcasted_iota(jnp.int32, (width, width), 1)
        block = jnp.where(k <= c, 1.0, 0.0).astype(BF16)
        for i in range(3):
            ref[pl.ds(i * width, width), :] = block

    ones_below(tri, TILE)
    ones_below(tri_last, LANES)
    base = (v * 4 + z) * n_cols
    for copy in row_copies:
        copy.wait()
    back[0:1, :] = temp_ref[...]
    back[1:2, :] = (tgt_ref[...] - base).astype(F32)
    cols8 = back[...].T
    temp_col[...] = jnp.broadcast_to(cols8[:, 0:1], temp_col.shape)
    rel_col[...] = jnp.broadcast_to(cols8[:, 1:2], rel_col.shape).astype(jnp.int32)
    slot = lax.broadcasted_iota(jnp.int32, stats.shape, 1)
    stats[...] = jnp.where(slot < SLOTS, LOWEST, 0.0)
    t_all[...] = jnp.zeros(t_all.shape, F32)

    with jax.named_scope("h0"):
        arrived(h_place(v, z_two), 0, hid=z_two)
    h_relay.start()
    send_far(0, 1).start()
    for j in range(1, n_chunks):
        send_near(j).start()
        send_far(j, 0).start()
        send_far(j, 1).start()

    @pl.when(is_outer == 0)
    def _():
        send_twin(0).start()
        send_twin(1).start()


    part, few = min(rows, 512), min(rows, 128)

    def logits_and_sums(product, sums):
        some = part if product is not None or sums[2] == TILE else min(rows, 2 * part)

        @pl.loop(0, rows // some)
        def _(i):
            if product is not None:
                _, new_start, new_width = product
                at = pl.ds(pl.multiple_of(i * part, part), part)
                new = jnp.dot(
                    hbuf[at, :], wbuf[:, pl.ds(new_start, new_width)], preferred_element_type=F32
                )
            for k in range(0, some, few) if sums is not None else ():
                prefix(pl.ds(pl.multiple_of(i * some + k, few), few), *sums)
            if product is not None:
                zbuf[at, 0:new_width] = new

    def prefix(at, t, start, width, ending=False):
        pieces = width // LANES
        logits = zbuf[at, 0:width] * jnp.concatenate([temp_col[at, :]] * pieces, axis=1)
        lane = lax.broadcasted_iota(jnp.int32, (few, LANES), 1)
        top = jnp.max(logits, axis=1, keepdims=True)
        e = jnp.exp(logits - top)
        total = jnp.sum(e, axis=1, keepdims=True)
        old = stats[at, :]
        table = tri if width == TILE else tri_last
        run = jnp.dot(jnp.concatenate(split3(e), axis=1), table[...], preferred_element_type=F32)
        c_ref[at, pl.ds(start, width)] = run
        rel = rel_col[at, :] - start
        if ending:
            hit = jnp.where(lane == rel, run, 0.0)
            old = jnp.where(lane == 2 * SLOTS, old + jnp.sum(hit, axis=1, keepdims=True), old)
        else:
            hit = t_all[at, :]
            for p in range(pieces):
                hit += jnp.where(lane == rel - p * LANES, run[:, p * LANES : (p + 1) * LANES], 0.0)
            t_all[at, :] = hit
        stats[at, :] = jnp.where(lane == t, top, jnp.where(lane == SLOTS + t, total, old))

    def collect():
        lane = lax.broadcasted_iota(jnp.int32, stats.shape, 1)
        stats[...] = jnp.where(lane == 2 * SLOTS, jnp.sum(t_all[...], axis=1, keepdims=True), stats[...])

    def whole(t):
        return t, pl.multiple_of(t * TILE, TILE), TILE

    def compute(j):
        first, size = (n // 2 for n in plan[j][:2])
        stop = first + size
        if first == 0:
            logits_and_sums(whole(0), None)
            first = 1
        if first < stop:

            @pl.loop(first, stop)
            def _(t):
                logits_and_sums(whole(t), whole(t - 1))

        if j == first_end - 1:
            logits_and_sums(None, whole(stop - 1))

    def block_dot(at, block, start, width):
        lanes = pl.ds(pl.multiple_of(block * depth, depth), depth)
        return jnp.dot(hbuf[at, lanes], wbuf[lanes, start : start + width], preferred_element_type=F32)

    def begin_end(i):
        start, width = tiles[n_whole - 1 + i]

        @pl.loop(0, rows // part)
        def _(k):
            at = pl.ds(pl.multiple_of(k * part, part), part)
            c_ref[at, start : start + width] = (
                block_dot(at, z, start, width)
                + block_dot(at, near, start, width)
                + block_dot(at, outer_far, start, width)
            )

    def finish_end(i):
        t = n_whole - 1 + i
        start, width = tiles[t]
        every = slice(0, rows)
        zbuf[:, 0:width] = c_ref[:, start : start + width] + block_dot(every, inner_far, start, width)
        logits_and_sums(None, (t, start, width, t == n_tiles - 1))

    def fold(g0, g1):
        @pl.loop(0, rows // few)
        def _(i):
            at = pl.ds(pl.multiple_of(i * few, few), few)
            lane = lax.broadcasted_iota(jnp.int32, (few, LANES), 1)
            group = (lane >= g0) & (lane < g1)
            m = stats[at, :]
            s = pltpu.roll(m, LANES - SLOTS, 1)
            top = jnp.max(jnp.where(group, m, LOWEST), axis=1, keepdims=True)
            shrink = jnp.where(group, jnp.exp(m - top), 0.0)
            parts = jnp.where(group, s, 0.0) * shrink
            before = prefix_before(parts)
            for t in range(g0, g1):
                span = slice(t * TILE, (t + 1) * TILE)
                c_ref[at, span] = c_ref[at, span] * shrink[:, t : t + 1] + before[:, t : t + 1]
            rel = rel_col[at, :]
            holds = (rel >= lane * TILE) & (rel < (lane + 1) * TILE)
            old = t_all[at, :]
            moved = jnp.sum(old, axis=1, keepdims=True) * shrink + before
            inside = (rel >= g0 * TILE) & (rel < g1 * TILE)
            t_all[at, :] = jnp.where(inside, jnp.where(holds, moved, 0.0), old)
            total = jnp.sum(parts, axis=1, keepdims=True)
            sums = jnp.where(lane == SLOTS + g1 - 1, total, 0.0)
            of_sums = (lane >= SLOTS + g0) & (lane < SLOTS + g1)
            stats[at, :] = jnp.where(group, top, jnp.where(of_sums, sums, m))

    def close(i):
        first = ends[i - 1] + 1 if i else first_end
        with jax.named_scope(f"xe{i}"):
            for j in range(first, ends[i] + 1):
                if j < n_chunks - 1:
                    forwarded(j)
                else:
                    twin_landed()
        with jax.named_scope(f"ce{i}"):
            finish_end(i)

    def prefix_before(parts):
        k = lax.broadcasted_iota(jnp.int32, (LANES, LANES), 0)
        c = lax.broadcasted_iota(jnp.int32, (LANES, LANES), 1)
        strict = jnp.where(k < c, 1.0, 0.0).astype(BF16)
        return sum(jnp.dot(p, strict, preferred_element_type=F32) for p in split3(parts))

    def complete(j):
        start, n = cols_of(j)
        cross_wait(j, 3 * half, start, start + n)

    def own_complete():
        place = wbuf.at[pl.ds(pl.multiple_of(z * depth, depth), depth)]
        pltpu.make_async_copy(place, place, wl).wait()

    order = service_order(plan, n_cols // LANES)
    folds = {j: (g0, g1) for j, g0, g1 in folds_of(plan, first_end)}
    tail = range(first_end, n_chunks)
    known = max(order.index((k, j)) for k in (0, 2) for j in tail)
    early = min(j for j in range(max(0, first_end - 7), n_chunks - 1) if order.index((1, j + 1)) > known)
    assert early < first_end
    m = len(ends) - 1
    closes = {n_chunks - 3: range(m - 2), n_chunks - 2: [m - 2], n_chunks - 1: [m - 1]}

    for what, j in order:
        if what == "h line":
            with jax.named_scope("hline"):
                arrived(h_place(v, z_one), 1, hid=z_one)
                arrived(h_place(v, lax.rem(z_one + 2, 4)), 2, hid=z_one)
                h_own.wait()
            h_chip.start()
            h_core.start()
        elif what == "h chip":
            with jax.named_scope("hchip"):
                arrived(h_place(v_two), 3, vocab=v_two)
            h_both.start()
        else:
            with jax.named_scope(f"w{what}_{j}"):
                landed(j, what)
            if (what, j) != (1, n_chunks - 1):
                forward(j, what).start()
            if what != 1:
                continue
            if j == 1:
                with jax.named_scope("hcore"):
                    arrived(h_place(v_one), 4, vocab=v_one)
                    arrived(h_place(lax.rem(v_one + 2, 4)), 5, vocab=v_one)
                    own_complete()
            if 0 < j <= first_end:
                with jax.named_scope(f"x{j - 1}"):
                    complete(j - 1)
                with jax.named_scope(f"c{j - 1}"):
                    compute(j - 1)
                if j - 1 in folds:
                    with jax.named_scope(f"f{j - 1}"):
                        fold(*folds[j - 1])
            if j - 1 == early:
                with jax.named_scope("begin"):
                    cross_wait(first_end, 2 * half, cols_of(first_end)[0], n_cols)
                    for i in range(len(ends)):
                        begin_end(i)
            for i in closes.get(j, ()):
                close(i)
    collect()
    close(m)

    lane = lax.broadcasted_iota(jnp.int32, (rows, LANES), 1)
    turned = stats[...].T
    m, at_tgt = turned[0:SLOTS, :], turned[2 * SLOTS : 2 * SLOTS + 1, :]
    top = jnp.max(m, axis=0, keepdims=True)
    shrink = jnp.exp(m - top)
    parts = turned[SLOTS : 2 * SLOTS, :] * shrink
    t = lax.broadcasted_iota(jnp.int32, (SLOTS, rows), 0)
    start = jnp.where(t < n_whole, t * TILE, n_whole * (TILE - LANES) + t * LANES)
    stop = start + jnp.where(t < n_whole, TILE, LANES)
    rel = tgt_ref[...] - base
    known = rel < n_cols
    holds = (rel >= start) & (rel < stop) & known
    ahead = (stop <= rel) & known
    found = jnp.where(holds, at_tgt * shrink, jnp.where(ahead, parts, 0.0))
    zmsg[z, 0:1, :] = top
    zmsg[z, 1:2, :] = jnp.sum(parts, axis=0, keepdims=True)
    zmsg[z, 2:3, :] = jnp.sum(found, axis=0, keepdims=True)

    for k in range(3):
        mine = wbuf.at[w_rows(sources[k], x)]
        remote(mine, mine, ws.at[k], wr.at[0, k], hid=near).wait_send()
        if k == 1:
            mine = wbuf.at[w_rows(sources[k], x), pl.ds(0, n_cols - LANES)]
        remote(mine, mine, xs.at[k], xr.at[0], data=1 - x).wait_send()
    forward(n_chunks - 2, 1).wait_send()

    @pl.when(is_outer == 0)
    def _():
        send_twin(0).wait_send()
        send_twin(1).wait_send()

    mine = hbuf.at[pl.ds(0, quarter * 15 // 4)]
    remote(mine, mine, hs, hr.at[0], hid=near).wait_send()

    def z_send(i):
        return remote(zmsg.at[z], zmsg.at[z], zs, zr, hid=(near, inner_far, outer_far)[i])

    def v_send(d):
        to = lax.rem(v + d, 4)
        return remote(vmsg.at[v], vmsg.at[v], vs, vr, vocab=to)

    for i in (2, 1, 0):
        z_send(i).start()
    k = lax.broadcasted_iota(jnp.int32, (SLOTS, SLOTS), 0)
    c = lax.broadcasted_iota(jnp.int32, (SLOTS, SLOTS), 1)
    strict = jnp.where(c < k, 1.0, 0.0).astype(BF16)
    before = sum(jnp.dot(strict, p, preferred_element_type=F32) for p in split3(parts))
    rest = jnp.zeros((LANES - 2 * SLOTS, rows), F32)
    coef_ref[...] = jnp.concatenate([shrink, before, rest], axis=0).T
    z_all = remote(zmsg.at[pl.ds(0, 3)], zmsg.at[pl.ds(0, 3)], zs, zr, hid=near)
    with jax.named_scope("z"):
        z_all.wait_recv()

    ids = tgt_ref[...]
    maxes = [zmsg[h, 0:1, :] for h in range(4)]
    v_max = functools.reduce(jnp.maximum, maxes)
    v_sum = jnp.zeros((1, rows), F32)
    v_tgt = jnp.zeros((1, rows), F32)
    mine_before = jnp.zeros((1, rows), F32)
    for h in range(4):
        mine_before = jnp.where(h == z, v_sum, mine_before)
        f = jnp.exp(maxes[h] - v_max)
        low = (v * 4 + h) * n_cols
        inside = (ids >= low) & (ids < low + n_cols)
        v_tgt += jnp.where(inside, zmsg[h, 2:3, :] * f + v_sum, 0.0)
        v_sum += zmsg[h, 1:2, :] * f
    vmsg[v, 0:1, :] = v_max
    vmsg[v, 1:2, :] = v_sum
    vmsg[v, 2:3, :] = v_tgt

    z_all.wait_send()
    for d in (2, 1, 3):
        v_send(d).start()
    v_all = remote(vmsg.at[pl.ds(0, 3)], vmsg.at[pl.ds(0, 3)], vs, vr, vocab=v_one)
    with jax.named_scope("v"):
        v_all.wait_recv()

    maxes = [vmsg[u, 0:1, :] for u in range(4)]
    g_max = functools.reduce(jnp.maximum, maxes)
    g_sum = jnp.zeros((1, rows), F32)
    g_tgt = jnp.zeros((1, rows), F32)
    g_before = jnp.zeros((1, rows), F32)
    for u in range(4):
        f = jnp.exp(maxes[u] - g_max)
        g_before = jnp.where(u == v, g_sum + mine_before * f, g_before)
        low = u * 4 * n_cols
        inside = (ids >= low) & (ids < low + 4 * n_cols)
        g_tgt += jnp.where(inside, vmsg[u, 2:3, :] * f + g_sum, 0.0)
        g_sum += vmsg[u, 1:2, :] * f
    tgt_out_ref[...] = g_tgt / g_sum
    factor_ref[0:1, :] = jnp.exp(zmsg[z, 0:1, :] - g_max) / g_sum
    factor_ref[1:2, :] = g_before / g_sum
    v_all.wait_send()


def finish_kernel(tiles, lanes, c_ref, coef_ref, factor_ref, tgt_ref, out_ref, tgt_out_ref, buf, factor_col, sems, tgt_sem):
    slots, n, n_cols = buf.shape
    steps = c_ref.shape[0] // n
    tgt_copy = pltpu.make_async_copy(tgt_ref, tgt_out_ref, tgt_sem)
    tgt_copy.start()

    def put(i):
        slot = lax.rem(i, slots)
        at = pl.ds(pl.multiple_of(i * n, n), n)
        return pltpu.make_async_copy(buf.at[slot], out_ref.at[at], sems.at[slot])

    @pl.loop(0, steps)
    def _(i):
        slot = lax.rem(i, slots)

        @pl.when(i >= slots)
        def _():
            put(i - slots).wait()

        at = pl.ds(pl.multiple_of(i * n, n), n)
        turn = max(n, LANES)

        @pl.when(lax.rem(i, turn // n) == 0)
        def _():
            some = pl.ds(pl.multiple_of(i // (turn // n) * turn, turn), turn)
            factor_col[some, :] = factor_ref[:, some].T

        lane = lax.broadcasted_iota(jnp.int32, (n, LANES), 1)
        coef = coef_ref[at, :] * factor_col[at, 0:1] + jnp.where(lane < SLOTS, 0.0, factor_col[at, 1:2])
        for (start, width), k in zip(tiles, lanes):
            span = slice(start, start + width)
            buf[slot, :, span] = c_ref[at, span] * coef[:, k : k + 1] + coef[:, SLOTS + k : SLOTS + k + 1]
        put(i).start()

    tgt_copy.wait()
    for i in range(max(0, steps - slots), steps):
        with jax.named_scope(f"fe{i}"):
            put(i).wait()


def solution(mesh):
    n_hid, n_voc = mesh.shape["hid"], mesh.shape["vocab"]
    assert n_hid == 4 and n_voc == 4 and mesh.shape["data"] == 2

    def local_step(h_blk, w_blk, temp_blk, tgt_blk):
        rows, depth = h_blk.shape
        n_cols = w_blk.shape[1] // n_hid
        assert n_cols % LANES == 0
        tiles = tiles_of(n_cols // LANES)
        n_tiles = len(tiles)
        assert n_tiles <= SLOTS
        plan = chunks_of(n_cols // LANES)
        n_chunks = len(plan)
        last_whole = sum(width == TILE for _, width in tiles) - 1
        first_end = [first for first, *_ in plan].index(2 * last_whole)
        vmem = pl.BlockSpec(memory_space=pltpu.VMEM)
        hbm = pl.BlockSpec(memory_space=pltpu.HBM)
        dma = pltpu.SemaphoreType.DMA
        table = pltpu.VMEM((rows, LANES), F32)
        c, coef, factor, tgt = pl.pallas_call(
            functools.partial(prefix_kernel, n_cols),
            out_shape=(
                pltpu.VMEM((rows, n_cols), F32),
                pltpu.VMEM((rows, LANES), F32),
                pltpu.VMEM((8, rows), F32),
                pltpu.VMEM((1, rows), F32),
            ),
            in_specs=[hbm] * 4,
            out_specs=[vmem] * 4,
            scratch_shapes=[
                pltpu.VMEM((4 * depth, n_cols), BF16),
                pltpu.VMEM((rows, 4 * depth), BF16),
                pltpu.VMEM((rows, TILE), F32),
                pltpu.VMEM((3 * TILE, TILE), BF16),
                pltpu.VMEM((3 * LANES, LANES), BF16),
                table,
                table,
                table,
                pltpu.VMEM((rows, LANES), jnp.int32),
                pltpu.VMEM((1, rows), F32),
                pltpu.VMEM((1, rows), jnp.int32),
                pltpu.VMEM((4, 3, rows), F32),
                pltpu.VMEM((4, 3, rows), F32),
                pltpu.VMEM((8, rows), F32),
                dma((3,)),
                dma((n_chunks, 3)),
                dma((4,)),
                dma((n_chunks,)),
                dma((2,)),
                dma,
                dma,
                dma,
                dma,
                dma((6,)),
                dma,
                dma,
                dma,
                dma,
                dma((2,)),
            ],
            compiler_params=pltpu.CompilerParams(
                collective_id=0, has_side_effects=True, vmem_limit_bytes=37 << 20
            ),
            name="prefix",
        )(h_blk, w_blk, temp_blk.reshape(1, rows), tgt_blk.reshape(1, rows))
        n = min(rows, 64)
        lanes = list(range(n_tiles))
        for _, g0, g1 in folds_of(plan, first_end):
            lanes[g0:g1] = [g0] * (g1 - g0)
        cdf, cdf_tgt = pl.pallas_call(
            functools.partial(finish_kernel, tiles, lanes),
            out_shape=(
                jax.ShapeDtypeStruct((rows, n_cols), F32),
                jax.ShapeDtypeStruct((1, rows), F32),
            ),
            in_specs=[vmem] * 4,
            out_specs=[hbm, hbm],
            scratch_shapes=[
                pltpu.VMEM((4, n, n_cols), F32),
                pltpu.VMEM((rows, 8), F32),
                dma((4,)),
                dma,
            ],
            compiler_params=pltpu.CompilerParams(vmem_limit_bytes=9 << 20),
            name="finish",
        )(c, coef, factor, tgt)
        return cdf, cdf_tgt.reshape(rows)

    return jax.shard_map(
        local_step,
        mesh=mesh,
        in_specs=(P("data", "hid"), P("hid", "vocab"), P("data"), P("data")),
        out_specs=(P("data", ("vocab", "hid")), P("data")),
        check_vma=False,
    )
```

```python
import functools

import jax
import jax.numpy as jnp
from jax import lax
from jax.experimental import pallas as pl
from jax.experimental.pallas import tpu as pltpu
from jax.sharding import PartitionSpec as P

MESH = pl.DeviceIdType.MESH
F32 = jnp.float32
BF16 = jnp.bfloat16
TILE = 256
LANES = 128
SLOTS = 32
LOWEST = float(jnp.finfo(jnp.float32).min)


def tiles_of(blocks):
    whole = (blocks - 3) // 2
    tiles = [(t * TILE, TILE) for t in range(whole)]
    return tiles + [(b * LANES, LANES) for b in range(2 * whole, blocks)]


def chunks_of(blocks):
    whole = (blocks - 3) // 2
    sizes, left = [], 2 * whole - 2
    for size in (2, 2, 2, 2, 4, 4):
        if left > size:
            sizes.append(size)
            left -= size
    while left > 0:
        sizes.append(min(6, left))
        left -= sizes[-1]
    plan, at = [], 0
    for size in reversed(sizes):
        plan.append((at, size, 0, 2))
        at += size
    plan += [(b, 1, 0, 2) for b in range(at, blocks - 2)]
    return plan + [(b, 1, r, 1) for b in (blocks - 2, blocks - 1) for r in (0, 1)]


def service_order(plan, blocks):
    events = [(0.15 * blocks, "h line", 0), (0.28 * blocks, "h chip", 0)]
    for j, (first, size, _, _) in enumerate(plan):
        end = first + size
        events.append((first + size / 3 + 2, 0, j))
        events.append((end + 2, 2, j))
        events.append((min(1.86 * end, 0.68 * blocks + 0.6 * end) + 2, 1, j))
    events.sort(key=lambda e: e[0])
    order = [e[1:] for e in events]
    for j in range(len(plan)):
        at = max(order.index((k, j)) for k in (0, 1, 2))
        order.remove((1, j))
        order.insert(at, (1, j))
    return order


def folds_of(plan, first_end):
    folds, at = [], 0
    for j in (first_end // 3, 3 * first_end // 5):
        stop = sum(plan[j][:2]) // 2 - 1
        if j < first_end and stop > at:
            folds.append((j, at, stop))
            at = stop
    return folds


def split3(e):
    hi = e.astype(BF16)
    rest = e - hi.astype(F32)
    mid = rest.astype(BF16)
    low = (rest - mid.astype(F32)).astype(BF16)
    return hi, mid, low


def prefix_kernel(
    n_cols, h_ref, w_ref, temp_hbm, tgt_hbm,
    c_ref, coef_ref, factor_ref, tgt_out_ref,
    wbuf, hbuf, zbuf, tri, tri_last, stats, t_all, temp_col, rel_col, temp_ref, tgt_ref, zmsg, vmsg, back,
    ws, wr, xs, xr, ts, tr, wl, hl, hs, hr, zs, zr, vs, vr, rl,
):
    x, z, v = lax.axis_index("data"), lax.axis_index("hid"), lax.axis_index("vocab")
    rows, depth = h_ref.shape
    half, quarter = depth // 2, rows // 4
    tiles = tiles_of(n_cols // LANES)
    n_tiles = len(tiles)
    n_whole = sum(width == TILE for _, width in tiles)
    plan = chunks_of(n_cols // LANES)
    n_chunks = len(plan)
    ends = [[j for j, (first, *_) in enumerate(plan) if first * LANES < sum(tiles[t])][-1] for t in range(n_whole - 1, n_tiles)]
    first_end = ends[0] - 1

    side = z // 2
    outer_far, inner_far, near = 3 - 3 * side, 2 - side, 1 - z + 4 * side
    is_outer = jnp.where(z == side * 3, 1, 0)
    z_two, z_one = lax.rem(z + 2, 4), near
    v_two, v_one = lax.rem(v + 2, 4), v + 1 - 2 * lax.rem(v, 2)
    sources = (near, inner_far, outer_far)

    def cols_of(j):
        first, size, _, _ = plan[j]
        return first * LANES, size * LANES

    def w_rows(source, part, j=None):
        at, n = (0, half) if j is None else (plan[j][2] * (half // 2), plan[j][3] * (half // 2))
        return pl.ds(pl.multiple_of(source * depth + part * half + at, half // 2), n)

    def w_place(j, source, part):
        start, n = cols_of(j)
        return wbuf.at[w_rows(source, part, j), pl.ds(start, n)]

    def h_place(q, block=None):
        at = pl.ds(pl.multiple_of(q * quarter, quarter), quarter)
        if block is None:
            return hbuf.at[at]
        return hbuf.at[at, pl.ds(pl.multiple_of(block * depth, depth), depth)]

    def remote(src, dst, send, recv, **to):
        return pltpu.make_async_remote_copy(
            src_ref=src, dst_ref=dst, send_sem=send, recv_sem=recv, device_id=to, device_id_type=MESH
        )

    def w_source(j, part, dest):
        start, n = cols_of(j)
        return w_ref.at[w_rows(0, part, j), pl.ds(pl.multiple_of(dest * n_cols + start, LANES), n)]

    def direct(j, k, dest, slot):
        return remote(w_source(j, x, dest), w_place(j, z, x), ws.at[k], wr.at[j, slot], hid=dest)

    def send_near(j):
        return direct(j, 0, near, 0)

    odd = lax.rem(v, 2)
    far_first = outer_far + odd * (inner_far - outer_far)
    far_second = inner_far + odd * (outer_far - inner_far)

    def send_far(j, i):
        return direct(j, 1 + i, (far_first, far_second)[i], 1 + is_outer)

    def send_twin(i):
        dest = (far_first, far_second)[i]
        return remote(w_source(n_chunks - 1, 1 - x, dest), w_place(n_chunks - 1, z, 1 - x), ts.at[i], tr, hid=dest)

    def twin_landed():
        place = w_place(n_chunks - 1, inner_far, 1 - x)
        remote(place, place, ts.at[0], tr, hid=inner_far).wait_recv()

    def landed(j, k):
        place = w_place(j, sources[k], x)
        remote(place, place, ws.at[k], wr.at[j, k], hid=sources[k]).wait_recv()

    def forward(j, k):
        place = w_place(j, sources[k], x)
        send = 3 if k == 1 and j == n_chunks - 2 else k
        return remote(place, place, xs.at[send], xr.at[cross(j, k)], data=1 - x)

    def cross(j, k):
        if j < first_end:
            return j
        return first_end if k != 1 else 1 + j

    def cross_wait(slot, count, start, stop):
        place = wbuf.at[pl.ds(0, count), pl.ds(start, stop - start)]
        remote(place, place, xs.at[0], xr.at[slot], data=1 - x).wait_recv()

    def forwarded(j):
        place = w_place(j, inner_far, 1 - x)
        remote(place, place, xs.at[1], xr.at[cross(j, 1)], data=1 - x).wait_recv()

    def own(j):
        start, n = cols_of(j)
        return pltpu.make_async_copy(
            w_ref.at[:, pl.ds(pl.multiple_of(z * n_cols + start, LANES), n)],
            wbuf.at[pl.ds(pl.multiple_of(z * depth, depth), depth), pl.ds(start, n)],
            wl,
        )

    h_mine = h_ref.at[pl.ds(pl.multiple_of(v * quarter, quarter), quarter)]
    h_own = pltpu.make_async_copy(h_mine, h_place(v, z), hl)
    h_two = remote(h_mine, h_place(v, z), hs, hr.at[0], hid=z_two)
    h_one = remote(h_mine, h_place(v, z), hs, hr.at[1], hid=z_one)
    h_relay = remote(h_place(v, z_two), h_place(v, z_two), hs, hr.at[2], hid=z_one)
    h_chip = remote(h_place(v), h_place(v), hs, hr.at[3], vocab=v_two)
    h_core = remote(h_place(v), h_place(v), hs, hr.at[4], vocab=v_one)
    h_both = remote(h_place(v_two), h_place(v_two), hs, hr.at[5], vocab=v_one)

    def arrived(place, i, **frm):
        remote(place, place, hs, hr.at[i], **frm).wait_recv()

    barrier = pltpu.get_barrier_semaphore()
    peers = [{"hid": outer_far}, {"hid": inner_far}, {"hid": near}, {"data": 1 - x}]
    peers += [{"vocab": lax.rem(v + d, 4)} for d in (2, 1, 3)]
    for peer in peers:
        pl.semaphore_signal(barrier, inc=1, device_id=peer, device_id_type=MESH)
    row_copies = [
        pltpu.make_async_copy(temp_hbm, temp_ref, rl.at[0]),
        pltpu.make_async_copy(tgt_hbm, tgt_ref, rl.at[1]),
    ]
    for copy in (h_own, *row_copies):
        copy.start()
    with jax.named_scope("bar"):
        pl.semaphore_wait(barrier, len(peers))

    h_two.start()
    h_one.start()
    send_near(0).start()
    send_far(0, 0).start()
    for j in range(n_chunks):
        if plan[j][2] == 0:
            own(j).start()

    def ones_below(ref, width):
        k = lax.broadcasted_iota(jnp.int32, (width, width), 0)
        c = lax.broadcasted_iota(jnp.int32, (width, width), 1)
        block = jnp.where(k <= c, 1.0, 0.0).astype(BF16)
        for i in range(3):
            ref[pl.ds(i * width, width), :] = block

    ones_below(tri, TILE)
    ones_below(tri_last, LANES)
    base = (v * 4 + z) * n_cols
    for copy in row_copies:
        copy.wait()
    back[0:1, :] = temp_ref[...]
    back[1:2, :] = (tgt_ref[...] - base).astype(F32)
    cols8 = back[...].T
    temp_col[...] = jnp.broadcast_to(cols8[:, 0:1], temp_col.shape)
    rel_col[...] = jnp.broadcast_to(cols8[:, 1:2], rel_col.shape).astype(jnp.int32)
    slot = lax.broadcasted_iota(jnp.int32, stats.shape, 1)
    stats[...] = jnp.where(slot < SLOTS, LOWEST, 0.0)
    t_all[...] = jnp.zeros(t_all.shape, F32)

    with jax.named_scope("h0"):
        arrived(h_place(v, z_two), 0, hid=z_two)
    h_relay.start()
    send_far(0, 1).start()
    for j in range(1, n_chunks):
        send_near(j).start()
        send_far(j, 0).start()
        send_far(j, 1).start()

    @pl.when(is_outer == 0)
    def _():
        send_twin(0).start()
        send_twin(1).start()


    part, few = min(rows, 512), min(rows, 128)

    def logits_and_sums(product, sums):
        some = part if product is not None or sums[2] == TILE else min(rows, 2 * part)

        @pl.loop(0, rows // some)
        def _(i):
            if product is not None:
                _, new_start, new_width = product
                at = pl.ds(pl.multiple_of(i * part, part), part)
                new = jnp.dot(
                    hbuf[at, :], wbuf[:, pl.ds(new_start, new_width)], preferred_element_type=F32
                )
            for k in range(0, some, few) if sums is not None else ():
                prefix(pl.ds(pl.multiple_of(i * some + k, few), few), *sums)
            if product is not None:
                zbuf[at, 0:new_width] = new

    def prefix(at, t, start, width, ending=False):
        pieces = width // LANES
        logits = zbuf[at, 0:width] * jnp.concatenate([temp_col[at, :]] * pieces, axis=1)
        lane = lax.broadcasted_iota(jnp.int32, (few, LANES), 1)
        top = jnp.max(logits, axis=1, keepdims=True)
        e = jnp.exp(logits - top)
        total = jnp.sum(e, axis=1, keepdims=True)
        old = stats[at, :]
        table = tri if width == TILE else tri_last
        run = jnp.dot(jnp.concatenate(split3(e), axis=1), table[...], preferred_element_type=F32)
        c_ref[at, pl.ds(start, width)] = run
        rel = rel_col[at, :] - start
        if ending:
            hit = jnp.where(lane == rel, run, 0.0)
            old = jnp.where(lane == 2 * SLOTS, old + jnp.sum(hit, axis=1, keepdims=True), old)
        else:
            hit = t_all[at, :]
            for p in range(pieces):
                hit += jnp.where(lane == rel - p * LANES, run[:, p * LANES : (p + 1) * LANES], 0.0)
            t_all[at, :] = hit
        stats[at, :] = jnp.where(lane == t, top, jnp.where(lane == SLOTS + t, total, old))

    def collect():
        lane = lax.broadcasted_iota(jnp.int32, stats.shape, 1)
        stats[...] = jnp.where(lane == 2 * SLOTS, jnp.sum(t_all[...], axis=1, keepdims=True), stats[...])

    def whole(t):
        return t, pl.multiple_of(t * TILE, TILE), TILE

    def compute(j):
        first, size = (n // 2 for n in plan[j][:2])
        stop = first + size
        if first == 0:
            logits_and_sums(whole(0), None)
            first = 1
        if first < stop:

            @pl.loop(first, stop)
            def _(t):
                logits_and_sums(whole(t), whole(t - 1))

        if j == first_end - 1:
            logits_and_sums(None, whole(stop - 1))

    def block_dot(at, block, start, width):
        lanes = pl.ds(pl.multiple_of(block * depth, depth), depth)
        return jnp.dot(hbuf[at, lanes], wbuf[lanes, start : start + width], preferred_element_type=F32)

    def begin_end(i):
        start, width = tiles[n_whole - 1 + i]

        @pl.loop(0, rows // part)
        def _(k):
            at = pl.ds(pl.multiple_of(k * part, part), part)
            c_ref[at, start : start + width] = (
                block_dot(at, z, start, width)
                + block_dot(at, near, start, width)
                + block_dot(at, outer_far, start, width)
            )

    def finish_end(i):
        t = n_whole - 1 + i
        start, width = tiles[t]
        every = slice(0, rows)
        zbuf[:, 0:width] = c_ref[:, start : start + width] + block_dot(every, inner_far, start, width)
        logits_and_sums(None, (t, start, width, t == n_tiles - 1))

    def fold(g0, g1):
        @pl.loop(0, rows // few)
        def _(i):
            at = pl.ds(pl.multiple_of(i * few, few), few)
            lane = lax.broadcasted_iota(jnp.int32, (few, LANES), 1)
            group = (lane >= g0) & (lane < g1)
            m = stats[at, :]
            s = pltpu.roll(m, LANES - SLOTS, 1)
            top = jnp.max(jnp.where(group, m, LOWEST), axis=1, keepdims=True)
            shrink = jnp.where(group, jnp.exp(m - top), 0.0)
            parts = jnp.where(group, s, 0.0) * shrink
            before = prefix_before(parts)
            for t in range(g0, g1):
                span = slice(t * TILE, (t + 1) * TILE)
                c_ref[at, span] = c_ref[at, span] * shrink[:, t : t + 1] + before[:, t : t + 1]
            rel = rel_col[at, :]
            holds = (rel >= lane * TILE) & (rel < (lane + 1) * TILE)
            old = t_all[at, :]
            moved = jnp.sum(old, axis=1, keepdims=True) * shrink + before
            inside = (rel >= g0 * TILE) & (rel < g1 * TILE)
            t_all[at, :] = jnp.where(inside, jnp.where(holds, moved, 0.0), old)
            total = jnp.sum(parts, axis=1, keepdims=True)
            sums = jnp.where(lane == SLOTS + g1 - 1, total, 0.0)
            of_sums = (lane >= SLOTS + g0) & (lane < SLOTS + g1)
            stats[at, :] = jnp.where(group, top, jnp.where(of_sums, sums, m))

    def close(i):
        first = ends[i - 1] + 1 if i else first_end
        with jax.named_scope(f"xe{i}"):
            for j in range(first, ends[i] + 1):
                if j < n_chunks - 1:
                    forwarded(j)
                else:
                    twin_landed()
        with jax.named_scope(f"ce{i}"):
            finish_end(i)

    def prefix_before(parts):
        k = lax.broadcasted_iota(jnp.int32, (LANES, LANES), 0)
        c = lax.broadcasted_iota(jnp.int32, (LANES, LANES), 1)
        strict = jnp.where(k < c, 1.0, 0.0).astype(BF16)
        return sum(jnp.dot(p, strict, preferred_element_type=F32) for p in split3(parts))

    def complete(j):
        start, n = cols_of(j)
        cross_wait(j, 3 * half, start, start + n)

    def own_complete():
        place = wbuf.at[pl.ds(pl.multiple_of(z * depth, depth), depth)]
        pltpu.make_async_copy(place, place, wl).wait()

    order = service_order(plan, n_cols // LANES)
    folds = {j: (g0, g1) for j, g0, g1 in folds_of(plan, first_end)}
    tail = range(first_end, n_chunks)
    known = max(order.index((k, j)) for k in (0, 2) for j in tail)
    early = min(j for j in range(max(0, first_end - 7), n_chunks - 1) if order.index((1, j + 1)) > known)
    assert early < first_end
    m = len(ends) - 1
    closes = {n_chunks - 3: range(m - 2), n_chunks - 2: [m - 2], n_chunks - 1: [m - 1]}

    for what, j in order:
        if what == "h line":
            with jax.named_scope("hline"):
                arrived(h_place(v, z_one), 1, hid=z_one)
                arrived(h_place(v, lax.rem(z_one + 2, 4)), 2, hid=z_one)
                h_own.wait()
            h_chip.start()
            h_core.start()
        elif what == "h chip":
            with jax.named_scope("hchip"):
                arrived(h_place(v_two), 3, vocab=v_two)
            h_both.start()
        else:
            with jax.named_scope(f"w{what}_{j}"):
                landed(j, what)
            if (what, j) != (1, n_chunks - 1):
                forward(j, what).start()
            if what != 1:
                continue
            if j == 1:
                with jax.named_scope("hcore"):
                    arrived(h_place(v_one), 4, vocab=v_one)
                    arrived(h_place(lax.rem(v_one + 2, 4)), 5, vocab=v_one)
                    own_complete()
            if 0 < j <= first_end:
                with jax.named_scope(f"x{j - 1}"):
                    complete(j - 1)
                with jax.named_scope(f"c{j - 1}"):
                    compute(j - 1)
                if j - 1 in folds:
                    with jax.named_scope(f"f{j - 1}"):
                        fold(*folds[j - 1])
            if j - 1 == early:
                with jax.named_scope("begin"):
                    cross_wait(first_end, 2 * half, cols_of(first_end)[0], n_cols)
                    for i in range(len(ends)):
                        begin_end(i)
            for i in closes.get(j, ()):
                close(i)
    collect()
    close(m)

    lane = lax.broadcasted_iota(jnp.int32, (rows, LANES), 1)
    turned = stats[...].T
    m, at_tgt = turned[0:SLOTS, :], turned[2 * SLOTS : 2 * SLOTS + 1, :]
    top = jnp.max(m, axis=0, keepdims=True)
    shrink = jnp.exp(m - top)
    parts = turned[SLOTS : 2 * SLOTS, :] * shrink
    t = lax.broadcasted_iota(jnp.int32, (SLOTS, rows), 0)
    start = jnp.where(t < n_whole, t * TILE, n_whole * (TILE - LANES) + t * LANES)
    stop = start + jnp.where(t < n_whole, TILE, LANES)
    rel = tgt_ref[...] - base
    known = rel < n_cols
    holds = (rel >= start) & (rel < stop) & known
    ahead = (stop <= rel) & known
    found = jnp.where(holds, at_tgt * shrink, jnp.where(ahead, parts, 0.0))
    zmsg[z, 0:1, :] = top
    zmsg[z, 1:2, :] = jnp.sum(parts, axis=0, keepdims=True)
    zmsg[z, 2:3, :] = jnp.sum(found, axis=0, keepdims=True)

    for k in range(3):
        mine = wbuf.at[w_rows(sources[k], x)]
        remote(mine, mine, ws.at[k], wr.at[0, k], hid=near).wait_send()
        if k == 1:
            mine = wbuf.at[w_rows(sources[k], x), pl.ds(0, n_cols - LANES)]
        remote(mine, mine, xs.at[k], xr.at[0], data=1 - x).wait_send()
    forward(n_chunks - 2, 1).wait_send()

    @pl.when(is_outer == 0)
    def _():
        send_twin(0).wait_send()
        send_twin(1).wait_send()

    mine = hbuf.at[pl.ds(0, quarter * 15 // 4)]
    remote(mine, mine, hs, hr.at[0], hid=near).wait_send()

    def z_send(i):
        return remote(zmsg.at[z], zmsg.at[z], zs, zr, hid=(near, inner_far, outer_far)[i])

    def v_send(d):
        to = lax.rem(v + d, 4)
        return remote(vmsg.at[v], vmsg.at[v], vs, vr, vocab=to)

    for i in (2, 1, 0):
        z_send(i).start()
    k = lax.broadcasted_iota(jnp.int32, (SLOTS, SLOTS), 0)
    c = lax.broadcasted_iota(jnp.int32, (SLOTS, SLOTS), 1)
    strict = jnp.where(c < k, 1.0, 0.0).astype(BF16)
    before = sum(jnp.dot(strict, p, preferred_element_type=F32) for p in split3(parts))
    rest = jnp.zeros((LANES - 2 * SLOTS, rows), F32)
    coef_ref[...] = jnp.concatenate([shrink, before, rest], axis=0).T
    z_all = remote(zmsg.at[pl.ds(0, 3)], zmsg.at[pl.ds(0, 3)], zs, zr, hid=near)
    with jax.named_scope("z"):
        z_all.wait_recv()

    ids = tgt_ref[...]
    maxes = [zmsg[h, 0:1, :] for h in range(4)]
    v_max = functools.reduce(jnp.maximum, maxes)
    v_sum = jnp.zeros((1, rows), F32)
    v_tgt = jnp.zeros((1, rows), F32)
    mine_before = jnp.zeros((1, rows), F32)
    for h in range(4):
        mine_before = jnp.where(h == z, v_sum, mine_before)
        f = jnp.exp(maxes[h] - v_max)
        low = (v * 4 + h) * n_cols
        inside = (ids >= low) & (ids < low + n_cols)
        v_tgt += jnp.where(inside, zmsg[h, 2:3, :] * f + v_sum, 0.0)
        v_sum += zmsg[h, 1:2, :] * f
    vmsg[v, 0:1, :] = v_max
    vmsg[v, 1:2, :] = v_sum
    vmsg[v, 2:3, :] = v_tgt

    z_all.wait_send()
    for d in (2, 1, 3):
        v_send(d).start()
    v_all = remote(vmsg.at[pl.ds(0, 3)], vmsg.at[pl.ds(0, 3)], vs, vr, vocab=v_one)
    with jax.named_scope("v"):
        v_all.wait_recv()

    maxes = [vmsg[u, 0:1, :] for u in range(4)]
    g_max = functools.reduce(jnp.maximum, maxes)
    g_sum = jnp.zeros((1, rows), F32)
    g_tgt = jnp.zeros((1, rows), F32)
    g_before = jnp.zeros((1, rows), F32)
    for u in range(4):
        f = jnp.exp(maxes[u] - g_max)
        g_before = jnp.where(u == v, g_sum + mine_before * f, g_before)
        low = u * 4 * n_cols
        inside = (ids >= low) & (ids < low + 4 * n_cols)
        g_tgt += jnp.where(inside, vmsg[u, 2:3, :] * f + g_sum, 0.0)
        g_sum += vmsg[u, 1:2, :] * f
    tgt_out_ref[...] = g_tgt / g_sum
    factor_ref[0:1, :] = jnp.exp(zmsg[z, 0:1, :] - g_max) / g_sum
    factor_ref[1:2, :] = g_before / g_sum
    v_all.wait_send()


def finish_kernel(tiles, lanes, c_ref, coef_ref, factor_ref, tgt_ref, out_ref, tgt_out_ref, buf, factor_col, sems, tgt_sem):
    slots, n, n_cols = buf.shape
    steps = c_ref.shape[0] // n
    tgt_copy = pltpu.make_async_copy(tgt_ref, tgt_out_ref, tgt_sem)
    tgt_copy.start()

    def put(i):
        slot = lax.rem(i, slots)
        at = pl.ds(pl.multiple_of(i * n, n), n)
        return pltpu.make_async_copy(buf.at[slot], out_ref.at[at], sems.at[slot])

    @pl.loop(0, steps)
    def _(i):
        slot = lax.rem(i, slots)

        @pl.when(i >= slots)
        def _():
            put(i - slots).wait()

        at = pl.ds(pl.multiple_of(i * n, n), n)
        turn = max(n, LANES)

        @pl.when(lax.rem(i, turn // n) == 0)
        def _():
            some = pl.ds(pl.multiple_of(i // (turn // n) * turn, turn), turn)
            factor_col[some, :] = factor_ref[:, some].T

        lane = lax.broadcasted_iota(jnp.int32, (n, LANES), 1)
        coef = coef_ref[at, :] * factor_col[at, 0:1] + jnp.where(lane < SLOTS, 0.0, factor_col[at, 1:2])
        for (start, width), k in zip(tiles, lanes):
            span = slice(start, start + width)
            buf[slot, :, span] = c_ref[at, span] * coef[:, k : k + 1] + coef[:, SLOTS + k : SLOTS + k + 1]
        put(i).start()

    tgt_copy.wait()
    for i in range(max(0, steps - slots), steps):
        with jax.named_scope(f"fe{i}"):
            put(i).wait()


def solution(mesh):
    n_hid, n_voc = mesh.shape["hid"], mesh.shape["vocab"]
    assert n_hid == 4 and n_voc == 4 and mesh.shape["data"] == 2

    def local_step(h_blk, w_blk, temp_blk, tgt_blk):
        rows, depth = h_blk.shape
        n_cols = w_blk.shape[1] // n_hid
        assert n_cols % LANES == 0
        tiles = tiles_of(n_cols // LANES)
        n_tiles = len(tiles)
        assert n_tiles <= SLOTS
        plan = chunks_of(n_cols // LANES)
        n_chunks = len(plan)
        last_whole = sum(width == TILE for _, width in tiles) - 1
        first_end = [first for first, *_ in plan].index(2 * last_whole)
        vmem = pl.BlockSpec(memory_space=pltpu.VMEM)
        hbm = pl.BlockSpec(memory_space=pltpu.HBM)
        dma = pltpu.SemaphoreType.DMA
        table = pltpu.VMEM((rows, LANES), F32)
        c, coef, factor, tgt = pl.pallas_call(
            functools.partial(prefix_kernel, n_cols),
            out_shape=(
                pltpu.VMEM((rows, n_cols), F32),
                pltpu.VMEM((rows, LANES), F32),
                pltpu.VMEM((8, rows), F32),
                pltpu.VMEM((1, rows), F32),
            ),
            in_specs=[hbm] * 4,
            out_specs=[vmem] * 4,
            scratch_shapes=[
                pltpu.VMEM((4 * depth, n_cols), BF16),
                pltpu.VMEM((rows, 4 * depth), BF16),
                pltpu.VMEM((rows, TILE), F32),
                pltpu.VMEM((3 * TILE, TILE), BF16),
                pltpu.VMEM((3 * LANES, LANES), BF16),
                table,
                table,
                table,
                pltpu.VMEM((rows, LANES), jnp.int32),
                pltpu.VMEM((1, rows), F32),
                pltpu.VMEM((1, rows), jnp.int32),
                pltpu.VMEM((4, 3, rows), F32),
                pltpu.VMEM((4, 3, rows), F32),
                pltpu.VMEM((8, rows), F32),
                dma((3,)),
                dma((n_chunks, 3)),
                dma((4,)),
                dma((n_chunks,)),
                dma((2,)),
                dma,
                dma,
                dma,
                dma,
                dma((6,)),
                dma,
                dma,
                dma,
                dma,
                dma((2,)),
            ],
            compiler_params=pltpu.CompilerParams(
                collective_id=0, has_side_effects=True, vmem_limit_bytes=37 << 20
            ),
            name="prefix",
        )(h_blk, w_blk, temp_blk.reshape(1, rows), tgt_blk.reshape(1, rows))
        n = min(rows, 64)
        lanes = list(range(n_tiles))
        for _, g0, g1 in folds_of(plan, first_end):
            lanes[g0:g1] = [g0] * (g1 - g0)
        cdf, cdf_tgt = pl.pallas_call(
            functools.partial(finish_kernel, tiles, lanes),
            out_shape=(
                jax.ShapeDtypeStruct((rows, n_cols), F32),
                jax.ShapeDtypeStruct((1, rows), F32),
            ),
            in_specs=[vmem] * 4,
            out_specs=[hbm, hbm],
            scratch_shapes=[
                pltpu.VMEM((4, n, n_cols), F32),
                pltpu.VMEM((rows, 8), F32),
                dma((4,)),
                dma,
            ],
            compiler_params=pltpu.CompilerParams(vmem_limit_bytes=9 << 20),
            name="finish",
        )(c, coef, factor, tgt)
        return cdf, cdf_tgt.reshape(rows)

    return jax.shard_map(
        local_step,
        mesh=mesh,
        in_specs=(P("data", "hid"), P("hid", "vocab"), P("data"), P("data")),
        out_specs=(P("data", ("vocab", "hid")), P("data")),
        check_vma=False,
    )
```

```python
import functools

import jax
import jax.numpy as jnp
from jax import lax
from jax.experimental import pallas as pl
from jax.experimental.pallas import tpu as pltpu
from jax.sharding import PartitionSpec as P

MESH = pl.DeviceIdType.MESH
F32 = jnp.float32
BF16 = jnp.bfloat16
TILE = 256
LANES = 128
SLOTS = 32
LOWEST = float(jnp.finfo(jnp.float32).min)


def tiles_of(blocks):
    whole = (blocks - 3) // 2
    tiles = [(t * TILE, TILE) for t in range(whole)]
    return tiles + [(b * LANES, LANES) for b in range(2 * whole, blocks)]


def chunks_of(blocks):
    whole = (blocks - 3) // 2
    sizes, left = [], 2 * whole - 2
    for size in (2, 2, 2, 2, 4, 4):
        if left > size:
            sizes.append(size)
            left -= size
    while left > 0:
        sizes.append(min(6, left))
        left -= sizes[-1]
    plan, at = [], 0
    for size in reversed(sizes):
        plan.append((at, size, 0, 2))
        at += size
    plan += [(b, 1, 0, 2) for b in range(at, blocks - 2)]
    return plan + [(b, 1, r, 1) for b in (blocks - 2, blocks - 1) for r in (0, 1)]


def service_order(plan, blocks):
    events = [(0.15 * blocks, "h line", 0), (0.28 * blocks, "h chip", 0)]
    for j, (first, size, _, _) in enumerate(plan):
        end = first + size
        events.append((first + size / 3 + 2, 0, j))
        events.append((end + 2, 2, j))
        events.append((min(1.86 * end, 0.68 * blocks + 0.6 * end) + 2, 1, j))
    events.sort(key=lambda e: e[0])
    order = [e[1:] for e in events]
    for j in range(len(plan)):
        at = max(order.index((k, j)) for k in (0, 1, 2))
        order.remove((1, j))
        order.insert(at, (1, j))
    return order


def folds_of(plan, first_end):
    folds, at = [], 0
    for j in (first_end // 3, 3 * first_end // 5):
        stop = sum(plan[j][:2]) // 2 - 1
        if j < first_end and stop > at:
            folds.append((j, at, stop))
            at = stop
    return folds


def split3(e):
    hi = e.astype(BF16)
    rest = e - hi.astype(F32)
    mid = rest.astype(BF16)
    low = (rest - mid.astype(F32)).astype(BF16)
    return hi, mid, low


def prefix_kernel(
    n_cols, h_ref, w_ref, temp_hbm, tgt_hbm,
    c_ref, coef_ref, factor_ref, tgt_out_ref,
    wbuf, hbuf, zbuf, tri, tri_last, stats, t_all, temp_col, rel_col, temp_ref, tgt_ref, zmsg, vmsg, back,
    ws, wr, xs, xr, ts, tr, wl, hl, hs, hr, zs, zr, vs, vr, rl,
):
    x, z, v = lax.axis_index("data"), lax.axis_index("hid"), lax.axis_index("vocab")
    rows, depth = h_ref.shape
    half, quarter = depth // 2, rows // 4
    tiles = tiles_of(n_cols // LANES)
    n_tiles = len(tiles)
    n_whole = sum(width == TILE for _, width in tiles)
    plan = chunks_of(n_cols // LANES)
    n_chunks = len(plan)
    ends = [[j for j, (first, *_) in enumerate(plan) if first * LANES < sum(tiles[t])][-1] for t in range(n_whole - 1, n_tiles)]
    first_end = ends[0] - 1

    side = z // 2
    outer_far, inner_far, near = 3 - 3 * side, 2 - side, 1 - z + 4 * side
    is_outer = jnp.where(z == side * 3, 1, 0)
    z_two, z_one = lax.rem(z + 2, 4), near
    v_two, v_one = lax.rem(v + 2, 4), v + 1 - 2 * lax.rem(v, 2)
    sources = (near, inner_far, outer_far)

    def cols_of(j):
        first, size, _, _ = plan[j]
        return first * LANES, size * LANES

    def w_rows(source, part, j=None):
        at, n = (0, half) if j is None else (plan[j][2] * (half // 2), plan[j][3] * (half // 2))
        return pl.ds(pl.multiple_of(source * depth + part * half + at, half // 2), n)

    def w_place(j, source, part):
        start, n = cols_of(j)
        return wbuf.at[w_rows(source, part, j), pl.ds(start, n)]

    def h_place(q, block=None):
        at = pl.ds(pl.multiple_of(q * quarter, quarter), quarter)
        if block is None:
            return hbuf.at[at]
        return hbuf.at[at, pl.ds(pl.multiple_of(block * depth, depth), depth)]

    def remote(src, dst, send, recv, **to):
        return pltpu.make_async_remote_copy(
            src_ref=src, dst_ref=dst, send_sem=send, recv_sem=recv, device_id=to, device_id_type=MESH
        )

    def w_source(j, part, dest):
        start, n = cols_of(j)
        return w_ref.at[w_rows(0, part, j), pl.ds(pl.multiple_of(dest * n_cols + start, LANES), n)]

    def direct(j, k, dest, slot):
        return remote(w_source(j, x, dest), w_place(j, z, x), ws.at[k], wr.at[j, slot], hid=dest)

    def send_near(j):
        return direct(j, 0, near, 0)

    odd = lax.rem(v, 2)
    far_first = outer_far + odd * (inner_far - outer_far)
    far_second = inner_far + odd * (outer_far - inner_far)

    def send_far(j, i):
        return direct(j, 1 + i, (far_first, far_second)[i], 1 + is_outer)

    def send_twin(i):
        dest = (far_first, far_second)[i]
        return remote(w_source(n_chunks - 1, 1 - x, dest), w_place(n_chunks - 1, z, 1 - x), ts.at[i], tr, hid=dest)

    def twin_landed():
        place = w_place(n_chunks - 1, inner_far, 1 - x)
        remote(place, place, ts.at[0], tr, hid=inner_far).wait_recv()

    def landed(j, k):
        place = w_place(j, sources[k], x)
        remote(place, place, ws.at[k], wr.at[j, k], hid=sources[k]).wait_recv()

    def forward(j, k):
        place = w_place(j, sources[k], x)
        send = 3 if k == 1 and j == n_chunks - 2 else k
        return remote(place, place, xs.at[send], xr.at[cross(j, k)], data=1 - x)

    def cross(j, k):
        if j < first_end:
            return j
        return first_end if k != 1 else 1 + j

    def cross_wait(slot, count, start, stop):
        place = wbuf.at[pl.ds(0, count), pl.ds(start, stop - start)]
        remote(place, place, xs.at[0], xr.at[slot], data=1 - x).wait_recv()

    def forwarded(j):
        place = w_place(j, inner_far, 1 - x)
        remote(place, place, xs.at[1], xr.at[cross(j, 1)], data=1 - x).wait_recv()

    def own(j):
        start, n = cols_of(j)
        return pltpu.make_async_copy(
            w_ref.at[:, pl.ds(pl.multiple_of(z * n_cols + start, LANES), n)],
            wbuf.at[pl.ds(pl.multiple_of(z * depth, depth), depth), pl.ds(start, n)],
            wl,
        )

    h_mine = h_ref.at[pl.ds(pl.multiple_of(v * quarter, quarter), quarter)]
    h_own = pltpu.make_async_copy(h_mine, h_place(v, z), hl)
    h_two = remote(h_mine, h_place(v, z), hs, hr.at[0], hid=z_two)
    h_one = remote(h_mine, h_place(v, z), hs, hr.at[1], hid=z_one)
    h_relay = remote(h_place(v, z_two), h_place(v, z_two), hs, hr.at[2], hid=z_one)
    h_chip = remote(h_place(v), h_place(v), hs, hr.at[3], vocab=v_two)
    h_core = remote(h_place(v), h_place(v), hs, hr.at[4], vocab=v_one)
    h_both = remote(h_place(v_two), h_place(v_two), hs, hr.at[5], vocab=v_one)

    def arrived(place, i, **frm):
        remote(place, place, hs, hr.at[i], **frm).wait_recv()

    barrier = pltpu.get_barrier_semaphore()
    peers = [{"hid": outer_far}, {"hid": inner_far}, {"hid": near}, {"data": 1 - x}]
    peers += [{"vocab": lax.rem(v + d, 4)} for d in (2, 1, 3)]
    for peer in peers:
        pl.semaphore_signal(barrier, inc=1, device_id=peer, device_id_type=MESH)
    row_copies = [
        pltpu.make_async_copy(temp_hbm, temp_ref, rl.at[0]),
        pltpu.make_async_copy(tgt_hbm, tgt_ref, rl.at[1]),
    ]
    for copy in (h_own, *row_copies):
        copy.start()
    for j in range(n_chunks):
        if plan[j][2] == 0:
            own(j).start()
    with jax.named_scope("bar"):
        pl.semaphore_wait(barrier, len(peers))

    h_two.start()
    h_one.start()
    send_near(0).start()
    send_far(0, 0).start()

    def ones_below(ref, width):
        k = lax.broadcasted_iota(jnp.int32, (width, width), 0)
        c = lax.broadcasted_iota(jnp.int32, (width, width), 1)
        block = jnp.where(k <= c, 1.0, 0.0).astype(BF16)
        for i in range(3):
            ref[pl.ds(i * width, width), :] = block

    ones_below(tri, TILE)
    ones_below(tri_last, LANES)
    base = (v * 4 + z) * n_cols
    for copy in row_copies:
        copy.wait()
    back[0:1, :] = temp_ref[...]
    back[1:2, :] = (tgt_ref[...] - base).astype(F32)
    cols8 = back[...].T
    temp_col[...] = jnp.broadcast_to(cols8[:, 0:1], temp_col.shape)
    rel_col[...] = jnp.broadcast_to(cols8[:, 1:2], rel_col.shape).astype(jnp.int32)
    slot = lax.broadcasted_iota(jnp.int32, stats.shape, 1)
    stats[...] = jnp.where(slot < SLOTS, LOWEST, 0.0)
    t_all[...] = jnp.zeros(t_all.shape, F32)

    with jax.named_scope("h0"):
        arrived(h_place(v, z_two), 0, hid=z_two)
    h_relay.start()
    send_far(0, 1).start()
    for j in range(1, n_chunks):
        send_near(j).start()
        send_far(j, 0).start()
        send_far(j, 1).start()

    @pl.when(is_outer == 0)
    def _():
        send_twin(0).start()
        send_twin(1).start()


    part, few = min(rows, 512), min(rows, 128)

    def logits_and_sums(product, sums):
        some = part if product is not None or sums[2] == TILE else min(rows, 2 * part)

        @pl.loop(0, rows // some)
        def _(i):
            if product is not None:
                _, new_start, new_width = product
                at = pl.ds(pl.multiple_of(i * part, part), part)
                new = jnp.dot(
                    hbuf[at, :], wbuf[:, pl.ds(new_start, new_width)], preferred_element_type=F32
                )
            for k in range(0, some, few) if sums is not None else ():
                prefix(pl.ds(pl.multiple_of(i * some + k, few), few), *sums)
            if product is not None:
                zbuf[at, 0:new_width] = new

    def prefix(at, t, start, width, ending=False):
        pieces = width // LANES
        logits = zbuf[at, 0:width] * jnp.concatenate([temp_col[at, :]] * pieces, axis=1)
        lane = lax.broadcasted_iota(jnp.int32, (few, LANES), 1)
        top = jnp.max(logits, axis=1, keepdims=True)
        e = jnp.exp(logits - top)
        total = jnp.sum(e, axis=1, keepdims=True)
        old = stats[at, :]
        table = tri if width == TILE else tri_last
        run = jnp.dot(jnp.concatenate(split3(e), axis=1), table[...], preferred_element_type=F32)
        c_ref[at, pl.ds(start, width)] = run
        rel = rel_col[at, :] - start
        if ending:
            hit = jnp.where(lane == rel, run, 0.0)
            old = jnp.where(lane == 2 * SLOTS, old + jnp.sum(hit, axis=1, keepdims=True), old)
        else:
            hit = t_all[at, :]
            for p in range(pieces):
                hit += jnp.where(lane == rel - p * LANES, run[:, p * LANES : (p + 1) * LANES], 0.0)
            t_all[at, :] = hit
        stats[at, :] = jnp.where(lane == t, top, jnp.where(lane == SLOTS + t, total, old))

    def collect():
        lane = lax.broadcasted_iota(jnp.int32, stats.shape, 1)
        stats[...] = jnp.where(lane == 2 * SLOTS, jnp.sum(t_all[...], axis=1, keepdims=True), stats[...])

    def whole(t):
        return t, pl.multiple_of(t * TILE, TILE), TILE

    def compute(j):
        first, size = (n // 2 for n in plan[j][:2])
        stop = first + size
        if first == 0:
            logits_and_sums(whole(0), None)
            first = 1
        if first < stop:

            @pl.loop(first, stop)
            def _(t):
                logits_and_sums(whole(t), whole(t - 1))

        if j == first_end - 1:
            logits_and_sums(None, whole(stop - 1))

    def block_dot(at, block, start, width):
        lanes = pl.ds(pl.multiple_of(block * depth, depth), depth)
        return jnp.dot(hbuf[at, lanes], wbuf[lanes, start : start + width], preferred_element_type=F32)

    def begin_end(i):
        start, width = tiles[n_whole - 1 + i]

        @pl.loop(0, rows // part)
        def _(k):
            at = pl.ds(pl.multiple_of(k * part, part), part)
            c_ref[at, start : start + width] = (
                block_dot(at, z, start, width)
                + block_dot(at, near, start, width)
                + block_dot(at, outer_far, start, width)
            )

    def finish_end(i):
        t = n_whole - 1 + i
        start, width = tiles[t]
        every = slice(0, rows)
        zbuf[:, 0:width] = c_ref[:, start : start + width] + block_dot(every, inner_far, start, width)
        logits_and_sums(None, (t, start, width, t == n_tiles - 1))

    def fold(g0, g1):
        @pl.loop(0, rows // few)
        def _(i):
            at = pl.ds(pl.multiple_of(i * few, few), few)
            lane = lax.broadcasted_iota(jnp.int32, (few, LANES), 1)
            group = (lane >= g0) & (lane < g1)
            m = stats[at, :]
            s = pltpu.roll(m, LANES - SLOTS, 1)
            top = jnp.max(jnp.where(group, m, LOWEST), axis=1, keepdims=True)
            shrink = jnp.where(group, jnp.exp(m - top), 0.0)
            parts = jnp.where(group, s, 0.0) * shrink
            before = prefix_before(parts)
            for t in range(g0, g1):
                span = slice(t * TILE, (t + 1) * TILE)
                c_ref[at, span] = c_ref[at, span] * shrink[:, t : t + 1] + before[:, t : t + 1]
            rel = rel_col[at, :]
            holds = (rel >= lane * TILE) & (rel < (lane + 1) * TILE)
            old = t_all[at, :]
            moved = jnp.sum(old, axis=1, keepdims=True) * shrink + before
            inside = (rel >= g0 * TILE) & (rel < g1 * TILE)
            t_all[at, :] = jnp.where(inside, jnp.where(holds, moved, 0.0), old)
            total = jnp.sum(parts, axis=1, keepdims=True)
            sums = jnp.where(lane == SLOTS + g1 - 1, total, 0.0)
            of_sums = (lane >= SLOTS + g0) & (lane < SLOTS + g1)
            stats[at, :] = jnp.where(group, top, jnp.where(of_sums, sums, m))

    def close(i):
        first = ends[i - 1] + 1 if i else first_end
        with jax.named_scope(f"xe{i}"):
            for j in range(first, ends[i] + 1):
                if j < n_chunks - 1:
                    forwarded(j)
                else:
                    twin_landed()
        with jax.named_scope(f"ce{i}"):
            finish_end(i)

    def prefix_before(parts):
        k = lax.broadcasted_iota(jnp.int32, (LANES, LANES), 0)
        c = lax.broadcasted_iota(jnp.int32, (LANES, LANES), 1)
        strict = jnp.where(k < c, 1.0, 0.0).astype(BF16)
        return sum(jnp.dot(p, strict, preferred_element_type=F32) for p in split3(parts))

    def complete(j):
        start, n = cols_of(j)
        cross_wait(j, 3 * half, start, start + n)

    def own_complete():
        place = wbuf.at[pl.ds(pl.multiple_of(z * depth, depth), depth)]
        pltpu.make_async_copy(place, place, wl).wait()

    order = service_order(plan, n_cols // LANES)
    folds = {j: (g0, g1) for j, g0, g1 in folds_of(plan, first_end)}
    tail = range(first_end, n_chunks)
    known = max(order.index((k, j)) for k in (0, 2) for j in tail)
    early = min(j for j in range(max(0, first_end - 7), n_chunks - 1) if order.index((1, j + 1)) > known)
    assert early < first_end
    m = len(ends) - 1
    closes = {n_chunks - 3: range(m - 2), n_chunks - 2: [m - 2], n_chunks - 1: [m - 1]}

    for what, j in order:
        if what == "h line":
            with jax.named_scope("hline"):
                arrived(h_place(v, z_one), 1, hid=z_one)
                arrived(h_place(v, lax.rem(z_one + 2, 4)), 2, hid=z_one)
                h_own.wait()
            h_chip.start()
            h_core.start()
        elif what == "h chip":
            with jax.named_scope("hchip"):
                arrived(h_place(v_two), 3, vocab=v_two)
            h_both.start()
        else:
            with jax.named_scope(f"w{what}_{j}"):
                landed(j, what)
            if (what, j) != (1, n_chunks - 1):
                forward(j, what).start()
            if what != 1:
                continue
            if j == 1:
                with jax.named_scope("hcore"):
                    arrived(h_place(v_one), 4, vocab=v_one)
                    arrived(h_place(lax.rem(v_one + 2, 4)), 5, vocab=v_one)
                    own_complete()
            if 0 < j <= first_end:
                with jax.named_scope(f"x{j - 1}"):
                    complete(j - 1)
                with jax.named_scope(f"c{j - 1}"):
                    compute(j - 1)
                if j - 1 in folds:
                    with jax.named_scope(f"f{j - 1}"):
                        fold(*folds[j - 1])
            if j - 1 == early:
                with jax.named_scope("begin"):
                    cross_wait(first_end, 2 * half, cols_of(first_end)[0], n_cols)
                    for i in range(len(ends)):
                        begin_end(i)
            for i in closes.get(j, ()):
                close(i)
    collect()
    close(m)

    lane = lax.broadcasted_iota(jnp.int32, (rows, LANES), 1)
    turned = stats[...].T
    m, at_tgt = turned[0:SLOTS, :], turned[2 * SLOTS : 2 * SLOTS + 1, :]
    top = jnp.max(m, axis=0, keepdims=True)
    shrink = jnp.exp(m - top)
    parts = turned[SLOTS : 2 * SLOTS, :] * shrink
    t = lax.broadcasted_iota(jnp.int32, (SLOTS, rows), 0)
    start = jnp.where(t < n_whole, t * TILE, n_whole * (TILE - LANES) + t * LANES)
    stop = start + jnp.where(t < n_whole, TILE, LANES)
    rel = tgt_ref[...] - base
    known = rel < n_cols
    holds = (rel >= start) & (rel < stop) & known
    ahead = (stop <= rel) & known
    found = jnp.where(holds, at_tgt * shrink, jnp.where(ahead, parts, 0.0))
    zmsg[z, 0:1, :] = top
    zmsg[z, 1:2, :] = jnp.sum(parts, axis=0, keepdims=True)
    zmsg[z, 2:3, :] = jnp.sum(found, axis=0, keepdims=True)

    for k in range(3):
        mine = wbuf.at[w_rows(sources[k], x)]
        remote(mine, mine, ws.at[k], wr.at[0, k], hid=near).wait_send()
        if k == 1:
            mine = wbuf.at[w_rows(sources[k], x), pl.ds(0, n_cols - LANES)]
        remote(mine, mine, xs.at[k], xr.at[0], data=1 - x).wait_send()
    forward(n_chunks - 2, 1).wait_send()

    @pl.when(is_outer == 0)
    def _():
        send_twin(0).wait_send()
        send_twin(1).wait_send()

    mine = hbuf.at[pl.ds(0, quarter * 15 // 4)]
    remote(mine, mine, hs, hr.at[0], hid=near).wait_send()

    def z_send(i):
        return remote(zmsg.at[z], zmsg.at[z], zs, zr, hid=(near, inner_far, outer_far)[i])

    def v_send(d):
        to = lax.rem(v + d, 4)
        return remote(vmsg.at[v], vmsg.at[v], vs, vr, vocab=to)

    for i in (2, 1, 0):
        z_send(i).start()
    k = lax.broadcasted_iota(jnp.int32, (SLOTS, SLOTS), 0)
    c = lax.broadcasted_iota(jnp.int32, (SLOTS, SLOTS), 1)
    strict = jnp.where(c < k, 1.0, 0.0).astype(BF16)
    before = sum(jnp.dot(strict, p, preferred_element_type=F32) for p in split3(parts))
    rest = jnp.zeros((LANES - 2 * SLOTS, rows), F32)
    spare = t == SLOTS - 1
    coef_ref[...] = jnp.concatenate([jnp.where(spare, 1.0, shrink), jnp.where(spare, 0.0, before), rest], axis=0).T

    @pl.loop(0, rows // few)
    def _(i):
        at = pl.ds(pl.multiple_of(i * few, few), few)
        coef = coef_ref[at, :]
        for q in range(folds_of(plan, first_end)[-1][2], n_whole):
            span = slice(tiles[q][0], sum(tiles[q]))
            c_ref[at, span] = c_ref[at, span] * coef[:, q : q + 1] + coef[:, SLOTS + q : SLOTS + q + 1]

    z_all = remote(zmsg.at[pl.ds(0, 3)], zmsg.at[pl.ds(0, 3)], zs, zr, hid=near)
    with jax.named_scope("z"):
        z_all.wait_recv()

    ids = tgt_ref[...]
    maxes = [zmsg[h, 0:1, :] for h in range(4)]
    v_max = functools.reduce(jnp.maximum, maxes)
    v_sum = jnp.zeros((1, rows), F32)
    v_tgt = jnp.zeros((1, rows), F32)
    mine_before = jnp.zeros((1, rows), F32)
    for h in range(4):
        mine_before = jnp.where(h == z, v_sum, mine_before)
        f = jnp.exp(maxes[h] - v_max)
        low = (v * 4 + h) * n_cols
        inside = (ids >= low) & (ids < low + n_cols)
        v_tgt += jnp.where(inside, zmsg[h, 2:3, :] * f + v_sum, 0.0)
        v_sum += zmsg[h, 1:2, :] * f
    vmsg[v, 0:1, :] = v_max
    vmsg[v, 1:2, :] = v_sum
    vmsg[v, 2:3, :] = v_tgt

    z_all.wait_send()
    for d in (2, 1, 3):
        v_send(d).start()
    v_all = remote(vmsg.at[pl.ds(0, 3)], vmsg.at[pl.ds(0, 3)], vs, vr, vocab=v_one)
    with jax.named_scope("v"):
        v_all.wait_recv()

    maxes = [vmsg[u, 0:1, :] for u in range(4)]
    g_max = functools.reduce(jnp.maximum, maxes)
    g_sum = jnp.zeros((1, rows), F32)
    g_tgt = jnp.zeros((1, rows), F32)
    g_before = jnp.zeros((1, rows), F32)
    for u in range(4):
        f = jnp.exp(maxes[u] - g_max)
        g_before = jnp.where(u == v, g_sum + mine_before * f, g_before)
        low = u * 4 * n_cols
        inside = (ids >= low) & (ids < low + 4 * n_cols)
        g_tgt += jnp.where(inside, vmsg[u, 2:3, :] * f + g_sum, 0.0)
        g_sum += vmsg[u, 1:2, :] * f
    tgt_out_ref[...] = g_tgt / g_sum
    factor_ref[0:1, :] = jnp.exp(zmsg[z, 0:1, :] - g_max) / g_sum
    factor_ref[1:2, :] = g_before / g_sum
    v_all.wait_send()


def finish_kernel(tiles, lanes, c_ref, coef_ref, factor_ref, tgt_ref, out_ref, tgt_out_ref, buf, factor_col, sems, ends):
    slots, n, n_cols = buf.shape
    steps = c_ref.shape[0] // n
    turn = max(n, LANES)
    tgt_copy = pltpu.make_async_copy(tgt_ref, tgt_out_ref, ends.at[2])
    tgt_copy.start()

    def put(i):
        at = pl.ds(pl.multiple_of(i * n, n), n)
        slot = lax.rem(i - 1, slots)
        return pltpu.make_async_copy(buf.at[slot], out_ref.at[at], sems.at[slot])

    def turn_factors(i):
        some = pl.ds(pl.multiple_of(i // (turn // n) * turn, turn), turn)
        factor_col[some, :] = factor_ref[:, some].T

    def table(at, count, to):
        lane = lax.broadcasted_iota(jnp.int32, (count, LANES), 1)
        coef = coef_ref[at, :] * factor_col[at, 0:1] + jnp.where(lane < SLOTS, 0.0, factor_col[at, 1:2])
        for (start, width), k in zip(tiles, lanes):
            span = slice(start, start + width)
            buf[(*to, span)] = c_ref[at, span] * coef[:, k : k + 1] + coef[:, SLOTS + k : SLOTS + k + 1]

    turn_factors(0)
    half = n // 2

    def put_half(h):
        at = pl.ds(pl.multiple_of(h * half, half), half)
        return pltpu.make_async_copy(buf.at[slots - 1, at], out_ref.at[at], ends.at[h])

    @pl.loop(0, 2)
    def _(h):
        at = pl.ds(pl.multiple_of(h * half, half), half)
        table(at, half, (slots - 1, at))
        put_half(h).start()

    @pl.loop(1, steps)
    def _(i):
        @pl.when(i == slots)
        def _():
            put_half(0).wait()
            put_half(1).wait()

        @pl.when(i > slots)
        def _():
            put(i - slots).wait()

        @pl.when(lax.rem(i, turn // n) == 0)
        def _():
            turn_factors(i)

        table(pl.ds(pl.multiple_of(i * n, n), n), n, (lax.rem(i - 1, slots), slice(None)))
        put(i).start()

    tgt_copy.wait()
    for i in range(max(0, steps - slots), steps):
        with jax.named_scope(f"fe{i}"):
            put(i).wait()


def solution(mesh):
    n_hid, n_voc = mesh.shape["hid"], mesh.shape["vocab"]
    assert n_hid == 4 and n_voc == 4 and mesh.shape["data"] == 2

    def local_step(h_blk, w_blk, temp_blk, tgt_blk):
        rows, depth = h_blk.shape
        n_cols = w_blk.shape[1] // n_hid
        assert n_cols % LANES == 0
        tiles = tiles_of(n_cols // LANES)
        n_tiles = len(tiles)
        assert n_tiles < SLOTS
        plan = chunks_of(n_cols // LANES)
        n_chunks = len(plan)
        last_whole = sum(width == TILE for _, width in tiles) - 1
        first_end = [first for first, *_ in plan].index(2 * last_whole)
        vmem = pl.BlockSpec(memory_space=pltpu.VMEM)
        hbm = pl.BlockSpec(memory_space=pltpu.HBM)
        dma = pltpu.SemaphoreType.DMA
        table = pltpu.VMEM((rows, LANES), F32)
        c, coef, factor, tgt = pl.pallas_call(
            functools.partial(prefix_kernel, n_cols),
            out_shape=(
                pltpu.VMEM((rows, n_cols), F32),
                pltpu.VMEM((rows, LANES), F32),
                pltpu.VMEM((8, rows), F32),
                pltpu.VMEM((1, rows), F32),
            ),
            in_specs=[hbm] * 4,
            out_specs=[vmem] * 4,
            scratch_shapes=[
                pltpu.VMEM((4 * depth, n_cols), BF16),
                pltpu.VMEM((rows, 4 * depth), BF16),
                pltpu.VMEM((rows, TILE), F32),
                pltpu.VMEM((3 * TILE, TILE), BF16),
                pltpu.VMEM((3 * LANES, LANES), BF16),
                table,
                table,
                table,
                pltpu.VMEM((rows, LANES), jnp.int32),
                pltpu.VMEM((1, rows), F32),
                pltpu.VMEM((1, rows), jnp.int32),
                pltpu.VMEM((4, 3, rows), F32),
                pltpu.VMEM((4, 3, rows), F32),
                pltpu.VMEM((8, rows), F32),
                dma((3,)),
                dma((n_chunks, 3)),
                dma((4,)),
                dma((n_chunks,)),
                dma((2,)),
                dma,
                dma,
                dma,
                dma,
                dma((6,)),
                dma,
                dma,
                dma,
                dma,
                dma((2,)),
            ],
            compiler_params=pltpu.CompilerParams(
                collective_id=0, has_side_effects=True, vmem_limit_bytes=37 << 20
            ),
            name="prefix",
        )(h_blk, w_blk, temp_blk.reshape(1, rows), tgt_blk.reshape(1, rows))
        n = min(rows // 8, 64)
        assert rows // n > 4
        lanes = list(range(n_tiles))
        for _, g0, g1 in folds_of(plan, first_end):
            lanes[g0:g1] = [g0] * (g1 - g0)
        lanes[g1 : last_whole + 1] = [SLOTS - 1] * (last_whole + 1 - g1)
        cdf, cdf_tgt = pl.pallas_call(
            functools.partial(finish_kernel, tiles, lanes),
            out_shape=(
                jax.ShapeDtypeStruct((rows, n_cols), F32),
                jax.ShapeDtypeStruct((1, rows), F32),
            ),
            in_specs=[vmem] * 4,
            out_specs=[hbm, hbm],
            scratch_shapes=[
                pltpu.VMEM((4, n, n_cols), F32),
                pltpu.VMEM((rows, 8), F32),
                dma((4,)),
                dma((3,)),
            ],
            compiler_params=pltpu.CompilerParams(vmem_limit_bytes=9 << 20),
            name="finish",
        )(c, coef, factor, tgt)
        return cdf, cdf_tgt.reshape(rows)

    return jax.shard_map(
        local_step,
        mesh=mesh,
        in_specs=(P("data", "hid"), P("hid", "vocab"), P("data"), P("data")),
        out_specs=(P("data", ("vocab", "hid")), P("data")),
        check_vma=False,
    )
```

```python
import functools

import jax
import jax.numpy as jnp
from jax import lax
from jax.experimental import pallas as pl
from jax.experimental.pallas import tpu as pltpu
from jax.sharding import PartitionSpec as P

MESH = pl.DeviceIdType.MESH
F32 = jnp.float32
BF16 = jnp.bfloat16
TILE = 256
LANES = 128
SLOTS = 32
LOWEST = float(jnp.finfo(jnp.float32).min)


def tiles_of(blocks):
    whole = (blocks - 3) // 2
    tiles = [(t * TILE, TILE) for t in range(whole)]
    return tiles + [(b * LANES, LANES) for b in range(2 * whole, blocks)]


def chunks_of(blocks):
    whole = (blocks - 3) // 2
    sizes, left = [], 2 * whole - 2
    for size in (2, 2, 2, 2, 4, 4):
        if left > size:
            sizes.append(size)
            left -= size
    while left > 0:
        sizes.append(min(6, left))
        left -= sizes[-1]
    plan, at = [], 0
    for size in reversed(sizes):
        plan.append((at, size, 0, 2))
        at += size
    plan += [(b, 1, 0, 2) for b in range(at, blocks - 2)]
    return plan + [(b, 1, r, 1) for b in (blocks - 2, blocks - 1) for r in (0, 1)]


def service_order(plan, blocks):
    events = [(0.15 * blocks, "h line", 0), (0.28 * blocks, "h chip", 0)]
    for j, (first, size, _, _) in enumerate(plan):
        end = first + size
        events.append((first + size / 3 + 2, 0, j))
        events.append((end + 2, 2, j))
        events.append((min(1.86 * end, 0.68 * blocks + 0.6 * end) + 2, 1, j))
    events.sort(key=lambda e: e[0])
    order = [e[1:] for e in events]
    for j in range(len(plan)):
        at = max(order.index((k, j)) for k in (0, 1, 2))
        order.remove((1, j))
        order.insert(at, (1, j))
    return order


def folds_of(plan, first_end):
    folds, at = [], 0
    for j in (first_end // 3, 3 * first_end // 5):
        stop = sum(plan[j][:2]) // 2 - 1
        if j < first_end and stop > at:
            folds.append((j, at, stop))
            at = stop
    return folds


def split3(e):
    hi = e.astype(BF16)
    rest = e - hi.astype(F32)
    mid = rest.astype(BF16)
    low = (rest - mid.astype(F32)).astype(BF16)
    return hi, mid, low


def prefix_kernel(
    n_cols, h_ref, w_ref, temp_hbm, tgt_hbm,
    c_ref, coef_ref, factor_ref, tgt_out_ref,
    wbuf, hbuf, zbuf, tri, tri_last, stats, t_all, temp_col, rel_col, temp_ref, tgt_ref, zmsg, vmsg, back,
    ws, wr, xs, xr, ts, tr, wl, hl, hs, hr, zs, zr, vs, vr, rl,
):
    x, z, v = lax.axis_index("data"), lax.axis_index("hid"), lax.axis_index("vocab")
    rows, depth = h_ref.shape
    half, quarter = depth // 2, rows // 4
    tiles = tiles_of(n_cols // LANES)
    n_tiles = len(tiles)
    n_whole = sum(width == TILE for _, width in tiles)
    plan = chunks_of(n_cols // LANES)
    n_chunks = len(plan)
    ends = [[j for j, (first, *_) in enumerate(plan) if first * LANES < sum(tiles[t])][-1] for t in range(n_whole - 1, n_tiles)]
    first_end = ends[0] - 1

    side = z // 2
    outer_far, inner_far, near = 3 - 3 * side, 2 - side, 1 - z + 4 * side
    is_outer = jnp.where(z == side * 3, 1, 0)
    z_two, z_one = lax.rem(z + 2, 4), near
    v_two, v_one = lax.rem(v + 2, 4), v + 1 - 2 * lax.rem(v, 2)
    sources = (near, inner_far, outer_far)

    def cols_of(j):
        first, size, _, _ = plan[j]
        return first * LANES, size * LANES

    def w_rows(source, part, j=None):
        at, n = (0, half) if j is None else (plan[j][2] * (half // 2), plan[j][3] * (half // 2))
        return pl.ds(pl.multiple_of(source * depth + part * half + at, half // 2), n)

    def w_place(j, source, part):
        start, n = cols_of(j)
        return wbuf.at[w_rows(source, part, j), pl.ds(start, n)]

    def h_place(q, block=None):
        at = pl.ds(pl.multiple_of(q * quarter, quarter), quarter)
        if block is None:
            return hbuf.at[at]
        return hbuf.at[at, pl.ds(pl.multiple_of(block * depth, depth), depth)]

    def remote(src, dst, send, recv, **to):
        return pltpu.make_async_remote_copy(
            src_ref=src, dst_ref=dst, send_sem=send, recv_sem=recv, device_id=to, device_id_type=MESH
        )

    def w_source(j, part, dest):
        start, n = cols_of(j)
        return w_ref.at[w_rows(0, part, j), pl.ds(pl.multiple_of(dest * n_cols + start, LANES), n)]

    def direct(j, k, dest, slot):
        return remote(w_source(j, x, dest), w_place(j, z, x), ws.at[k], wr.at[j, slot], hid=dest)

    def send_near(j):
        return direct(j, 0, near, 0)

    odd = lax.rem(v, 2)
    far_first = outer_far + odd * (inner_far - outer_far)
    far_second = inner_far + odd * (outer_far - inner_far)

    def send_far(j, i):
        return direct(j, 1 + i, (far_first, far_second)[i], 1 + is_outer)

    def send_twin(i):
        dest = (far_first, far_second)[i]
        return remote(w_source(n_chunks - 1, 1 - x, dest), w_place(n_chunks - 1, z, 1 - x), ts.at[i], tr, hid=dest)

    def twin_landed():
        place = w_place(n_chunks - 1, inner_far, 1 - x)
        remote(place, place, ts.at[0], tr, hid=inner_far).wait_recv()

    def landed(j, k):
        place = w_place(j, sources[k], x)
        remote(place, place, ws.at[k], wr.at[j, k], hid=sources[k]).wait_recv()

    def forward(j, k):
        place = w_place(j, sources[k], x)
        send = 3 if k == 1 and j == n_chunks - 2 else k
        return remote(place, place, xs.at[send], xr.at[cross(j, k)], data=1 - x)

    def cross(j, k):
        if j < first_end:
            return j
        return first_end if k != 1 else 1 + j

    def cross_wait(slot, count, start, stop):
        place = wbuf.at[pl.ds(0, count), pl.ds(start, stop - start)]
        remote(place, place, xs.at[0], xr.at[slot], data=1 - x).wait_recv()

    def forwarded(j):
        place = w_place(j, inner_far, 1 - x)
        remote(place, place, xs.at[1], xr.at[cross(j, 1)], data=1 - x).wait_recv()

    def own(j):
        start, n = cols_of(j)
        return pltpu.make_async_copy(
            w_ref.at[:, pl.ds(pl.multiple_of(z * n_cols + start, LANES), n)],
            wbuf.at[pl.ds(pl.multiple_of(z * depth, depth), depth), pl.ds(start, n)],
            wl,
        )

    h_mine = h_ref.at[pl.ds(pl.multiple_of(v * quarter, quarter), quarter)]
    h_own = pltpu.make_async_copy(h_mine, h_place(v, z), hl)
    h_two = remote(h_mine, h_place(v, z), hs, hr.at[0], hid=z_two)
    h_one = remote(h_mine, h_place(v, z), hs, hr.at[1], hid=z_one)
    h_relay = remote(h_place(v, z_two), h_place(v, z_two), hs, hr.at[2], hid=z_one)
    h_chip = remote(h_place(v), h_place(v), hs, hr.at[3], vocab=v_two)
    h_core = remote(h_place(v), h_place(v), hs, hr.at[4], vocab=v_one)
    h_both = remote(h_place(v_two), h_place(v_two), hs, hr.at[5], vocab=v_one)

    def arrived(place, i, **frm):
        remote(place, place, hs, hr.at[i], **frm).wait_recv()

    barrier = pltpu.get_barrier_semaphore()
    peers = [{"hid": outer_far}, {"hid": inner_far}, {"hid": near}, {"data": 1 - x}]
    peers += [{"vocab": lax.rem(v + d, 4)} for d in (2, 1, 3)]
    for peer in peers:
        pl.semaphore_signal(barrier, inc=1, device_id=peer, device_id_type=MESH)
    row_copies = [
        pltpu.make_async_copy(temp_hbm, temp_ref, rl.at[0]),
        pltpu.make_async_copy(tgt_hbm, tgt_ref, rl.at[1]),
    ]
    for copy in (h_own, *row_copies):
        copy.start()
    for j in range(n_chunks):
        if plan[j][2] == 0:
            own(j).start()
    with jax.named_scope("bar"):
        pl.semaphore_wait(barrier, len(peers))

    h_two.start()
    h_one.start()
    send_near(0).start()
    send_far(0, 0).start()

    def ones_below(ref, width):
        k = lax.broadcasted_iota(jnp.int32, (width, width), 0)
        c = lax.broadcasted_iota(jnp.int32, (width, width), 1)
        block = jnp.where(k <= c, 1.0, 0.0).astype(BF16)
        for i in range(3):
            ref[pl.ds(i * width, width), :] = block

    ones_below(tri, TILE)
    ones_below(tri_last, LANES)
    base = (v * 4 + z) * n_cols
    for copy in row_copies:
        copy.wait()
    back[0:1, :] = temp_ref[...]
    back[1:2, :] = (tgt_ref[...] - base).astype(F32)
    cols8 = back[...].T
    temp_col[...] = jnp.broadcast_to(cols8[:, 0:1], temp_col.shape)
    rel_col[...] = jnp.broadcast_to(cols8[:, 1:2], rel_col.shape).astype(jnp.int32)
    slot = lax.broadcasted_iota(jnp.int32, stats.shape, 1)
    stats[...] = jnp.where(slot < SLOTS, LOWEST, 0.0)
    t_all[...] = jnp.zeros(t_all.shape, F32)

    with jax.named_scope("h0"):
        arrived(h_place(v, z_two), 0, hid=z_two)
    h_relay.start()
    send_far(0, 1).start()
    for j in range(1, n_chunks):
        send_near(j).start()
        send_far(j, 0).start()
        send_far(j, 1).start()

    @pl.when(is_outer == 0)
    def _():
        send_twin(0).start()
        send_twin(1).start()


    part, few = min(rows, 512), min(rows, 128)

    def logits_and_sums(product, sums):
        some = part if product is not None or sums[2] == TILE else min(rows, 2 * part)

        @pl.loop(0, rows // some)
        def _(i):
            if product is not None:
                _, new_start, new_width = product
                at = pl.ds(pl.multiple_of(i * part, part), part)
                new = jnp.dot(
                    hbuf[at, :], wbuf[:, pl.ds(new_start, new_width)], preferred_element_type=F32
                )
            for k in range(0, some, few) if sums is not None else ():
                prefix(pl.ds(pl.multiple_of(i * some + k, few), few), *sums)
            if product is not None:
                zbuf[at, 0:new_width] = new

    def prefix(at, t, start, width, ending=False):
        pieces = width // LANES
        logits = zbuf[at, 0:width] * jnp.concatenate([temp_col[at, :]] * pieces, axis=1)
        lane = lax.broadcasted_iota(jnp.int32, (few, LANES), 1)
        top = jnp.max(logits, axis=1, keepdims=True)
        e = jnp.exp(logits - top)
        total = jnp.sum(e, axis=1, keepdims=True)
        old = stats[at, :]
        table = tri if width == TILE else tri_last
        run = jnp.dot(jnp.concatenate(split3(e), axis=1), table[...], preferred_element_type=F32)
        c_ref[at, pl.ds(start, width)] = run
        rel = rel_col[at, :] - start
        if ending:
            hit = jnp.where(lane == rel, run, 0.0)
            old = jnp.where(lane == 2 * SLOTS, old + jnp.sum(hit, axis=1, keepdims=True), old)
        else:
            hit = t_all[at, :]
            for p in range(pieces):
                hit += jnp.where(lane == rel - p * LANES, run[:, p * LANES : (p + 1) * LANES], 0.0)
            t_all[at, :] = hit
        stats[at, :] = jnp.where(lane == t, top, jnp.where(lane == SLOTS + t, total, old))

    def collect():
        lane = lax.broadcasted_iota(jnp.int32, stats.shape, 1)
        stats[...] = jnp.where(lane == 2 * SLOTS, jnp.sum(t_all[...], axis=1, keepdims=True), stats[...])

    def whole(t):
        return t, pl.multiple_of(t * TILE, TILE), TILE

    def compute(j):
        first, size = (n // 2 for n in plan[j][:2])
        stop = first + size
        if first == 0:
            logits_and_sums(whole(0), None)
            first = 1
        if first < stop:

            @pl.loop(first, stop)
            def _(t):
                logits_and_sums(whole(t), whole(t - 1))

        if j == first_end - 1:
            logits_and_sums(None, whole(stop - 1))

    def block_dot(at, block, start, width):
        lanes = pl.ds(pl.multiple_of(block * depth, depth), depth)
        return jnp.dot(hbuf[at, lanes], wbuf[lanes, start : start + width], preferred_element_type=F32)

    def begin_end(i):
        start, width = tiles[n_whole - 1 + i]

        @pl.loop(0, rows // part)
        def _(k):
            at = pl.ds(pl.multiple_of(k * part, part), part)
            c_ref[at, start : start + width] = (
                block_dot(at, z, start, width)
                + block_dot(at, near, start, width)
                + block_dot(at, outer_far, start, width)
            )

    def finish_end(i):
        t = n_whole - 1 + i
        start, width = tiles[t]
        every = slice(0, rows)
        zbuf[:, 0:width] = c_ref[:, start : start + width] + block_dot(every, inner_far, start, width)
        logits_and_sums(None, (t, start, width, t == n_tiles - 1))

    def fold(g0, g1):
        @pl.loop(0, rows // few)
        def _(i):
            at = pl.ds(pl.multiple_of(i * few, few), few)
            lane = lax.broadcasted_iota(jnp.int32, (few, LANES), 1)
            group = (lane >= g0) & (lane < g1)
            m = stats[at, :]
            s = pltpu.roll(m, LANES - SLOTS, 1)
            top = jnp.max(jnp.where(group, m, LOWEST), axis=1, keepdims=True)
            shrink = jnp.where(group, jnp.exp(m - top), 0.0)
            parts = jnp.where(group, s, 0.0) * shrink
            before = prefix_before(parts)
            for t in range(g0, g1):
                span = slice(t * TILE, (t + 1) * TILE)
                c_ref[at, span] = c_ref[at, span] * shrink[:, t : t + 1] + before[:, t : t + 1]
            rel = rel_col[at, :]
            holds = (rel >= lane * TILE) & (rel < (lane + 1) * TILE)
            old = t_all[at, :]
            moved = jnp.sum(old, axis=1, keepdims=True) * shrink + before
            inside = (rel >= g0 * TILE) & (rel < g1 * TILE)
            t_all[at, :] = jnp.where(inside, jnp.where(holds, moved, 0.0), old)
            total = jnp.sum(parts, axis=1, keepdims=True)
            sums = jnp.where(lane == SLOTS + g1 - 1, total, 0.0)
            of_sums = (lane >= SLOTS + g0) & (lane < SLOTS + g1)
            stats[at, :] = jnp.where(group, top, jnp.where(of_sums, sums, m))

    def close(i):
        first = ends[i - 1] + 1 if i else first_end
        with jax.named_scope(f"xe{i}"):
            for j in range(first, ends[i] + 1):
                if j < n_chunks - 1:
                    forwarded(j)
                else:
                    twin_landed()
        with jax.named_scope(f"ce{i}"):
            finish_end(i)

    def prefix_before(parts):
        k = lax.broadcasted_iota(jnp.int32, (LANES, LANES), 0)
        c = lax.broadcasted_iota(jnp.int32, (LANES, LANES), 1)
        strict = jnp.where(k < c, 1.0, 0.0).astype(BF16)
        return sum(jnp.dot(p, strict, preferred_element_type=F32) for p in split3(parts))

    def complete(j):
        start, n = cols_of(j)
        cross_wait(j, 3 * half, start, start + n)

    def own_complete():
        place = wbuf.at[pl.ds(pl.multiple_of(z * depth, depth), depth)]
        pltpu.make_async_copy(place, place, wl).wait()

    order = service_order(plan, n_cols // LANES)
    folds = {j: (g0, g1) for j, g0, g1 in folds_of(plan, first_end)}
    tail = range(first_end, n_chunks)
    known = max(order.index((k, j)) for k in (0, 2) for j in tail)
    early = min(j for j in range(max(0, first_end - 7), n_chunks - 1) if order.index((1, j + 1)) > known)
    assert early < first_end
    m = len(ends) - 1
    closes = {n_chunks - 3: range(m - 2), n_chunks - 2: [m - 2], n_chunks - 1: [m - 1]}

    for what, j in order:
        if what == "h line":
            with jax.named_scope("hline"):
                arrived(h_place(v, z_one), 1, hid=z_one)
                arrived(h_place(v, lax.rem(z_one + 2, 4)), 2, hid=z_one)
                h_own.wait()
            h_chip.start()
            h_core.start()
        elif what == "h chip":
            with jax.named_scope("hchip"):
                arrived(h_place(v_two), 3, vocab=v_two)
            h_both.start()
        else:
            with jax.named_scope(f"w{what}_{j}"):
                landed(j, what)
            if (what, j) != (1, n_chunks - 1):
                forward(j, what).start()
            if what != 1:
                continue
            if j == 1:
                with jax.named_scope("hcore"):
                    arrived(h_place(v_one), 4, vocab=v_one)
                    arrived(h_place(lax.rem(v_one + 2, 4)), 5, vocab=v_one)
                    own_complete()
            if 0 < j <= first_end:
                with jax.named_scope(f"x{j - 1}"):
                    complete(j - 1)
                with jax.named_scope(f"c{j - 1}"):
                    compute(j - 1)
                if j - 1 in folds:
                    with jax.named_scope(f"f{j - 1}"):
                        fold(*folds[j - 1])
            if j - 1 == early:
                with jax.named_scope("begin"):
                    cross_wait(first_end, 2 * half, cols_of(first_end)[0], n_cols)
                    for i in range(len(ends)):
                        begin_end(i)
            for i in closes.get(j, ()):
                close(i)
    collect()
    close(m)

    lane = lax.broadcasted_iota(jnp.int32, (rows, LANES), 1)
    turned = stats[...].T
    m, at_tgt = turned[0:SLOTS, :], turned[2 * SLOTS : 2 * SLOTS + 1, :]
    top = jnp.max(m, axis=0, keepdims=True)
    shrink = jnp.exp(m - top)
    parts = turned[SLOTS : 2 * SLOTS, :] * shrink
    t = lax.broadcasted_iota(jnp.int32, (SLOTS, rows), 0)
    start = jnp.where(t < n_whole, t * TILE, n_whole * (TILE - LANES) + t * LANES)
    stop = start + jnp.where(t < n_whole, TILE, LANES)
    rel = tgt_ref[...] - base
    known = rel < n_cols
    holds = (rel >= start) & (rel < stop) & known
    ahead = (stop <= rel) & known
    found = jnp.where(holds, at_tgt * shrink, jnp.where(ahead, parts, 0.0))
    zmsg[z, 0:1, :] = top
    zmsg[z, 1:2, :] = jnp.sum(parts, axis=0, keepdims=True)
    zmsg[z, 2:3, :] = jnp.sum(found, axis=0, keepdims=True)

    for k in range(3):
        mine = wbuf.at[w_rows(sources[k], x)]
        remote(mine, mine, ws.at[k], wr.at[0, k], hid=near).wait_send()
        if k == 1:
            mine = wbuf.at[w_rows(sources[k], x), pl.ds(0, n_cols - LANES)]
        remote(mine, mine, xs.at[k], xr.at[0], data=1 - x).wait_send()
    forward(n_chunks - 2, 1).wait_send()

    @pl.when(is_outer == 0)
    def _():
        send_twin(0).wait_send()
        send_twin(1).wait_send()

    mine = hbuf.at[pl.ds(0, quarter * 15 // 4)]
    remote(mine, mine, hs, hr.at[0], hid=near).wait_send()

    def z_send(i):
        return remote(zmsg.at[z], zmsg.at[z], zs, zr, hid=(near, inner_far, outer_far)[i])

    def v_send(d):
        to = lax.rem(v + d, 4)
        return remote(vmsg.at[v], vmsg.at[v], vs, vr, vocab=to)

    for i in (2, 1, 0):
        z_send(i).start()
    k = lax.broadcasted_iota(jnp.int32, (SLOTS, SLOTS), 0)
    c = lax.broadcasted_iota(jnp.int32, (SLOTS, SLOTS), 1)
    strict = jnp.where(c < k, 1.0, 0.0).astype(BF16)
    before = sum(jnp.dot(strict, p, preferred_element_type=F32) for p in split3(parts))
    rest = jnp.zeros((LANES - 2 * SLOTS, rows), F32)
    spare = t == SLOTS - 1
    coef_ref[...] = jnp.concatenate([jnp.where(spare, 1.0, shrink), jnp.where(spare, 0.0, before), rest], axis=0).T

    @pl.loop(0, rows // few)
    def _(i):
        at = pl.ds(pl.multiple_of(i * few, few), few)
        coef = coef_ref[at, :]
        for q in range(folds_of(plan, first_end)[-1][2], n_whole):
            span = slice(tiles[q][0], sum(tiles[q]))
            c_ref[at, span] = c_ref[at, span] * coef[:, q : q + 1] + coef[:, SLOTS + q : SLOTS + q + 1]

    z_all = remote(zmsg.at[pl.ds(0, 3)], zmsg.at[pl.ds(0, 3)], zs, zr, hid=near)
    with jax.named_scope("z"):
        z_all.wait_recv()

    ids = tgt_ref[...]
    maxes = [zmsg[h, 0:1, :] for h in range(4)]
    v_max = functools.reduce(jnp.maximum, maxes)
    v_sum = jnp.zeros((1, rows), F32)
    v_tgt = jnp.zeros((1, rows), F32)
    mine_before = jnp.zeros((1, rows), F32)
    for h in range(4):
        mine_before = jnp.where(h == z, v_sum, mine_before)
        f = jnp.exp(maxes[h] - v_max)
        low = (v * 4 + h) * n_cols
        inside = (ids >= low) & (ids < low + n_cols)
        v_tgt += jnp.where(inside, zmsg[h, 2:3, :] * f + v_sum, 0.0)
        v_sum += zmsg[h, 1:2, :] * f
    vmsg[v, 0:1, :] = v_max
    vmsg[v, 1:2, :] = v_sum
    vmsg[v, 2:3, :] = v_tgt

    z_all.wait_send()
    for d in (2, 1, 3):
        v_send(d).start()
    v_all = remote(vmsg.at[pl.ds(0, 3)], vmsg.at[pl.ds(0, 3)], vs, vr, vocab=v_one)
    with jax.named_scope("v"):
        v_all.wait_recv()

    maxes = [vmsg[u, 0:1, :] for u in range(4)]
    g_max = functools.reduce(jnp.maximum, maxes)
    g_sum = jnp.zeros((1, rows), F32)
    g_tgt = jnp.zeros((1, rows), F32)
    g_before = jnp.zeros((1, rows), F32)
    for u in range(4):
        f = jnp.exp(maxes[u] - g_max)
        g_before = jnp.where(u == v, g_sum + mine_before * f, g_before)
        low = u * 4 * n_cols
        inside = (ids >= low) & (ids < low + 4 * n_cols)
        g_tgt += jnp.where(inside, vmsg[u, 2:3, :] * f + g_sum, 0.0)
        g_sum += vmsg[u, 1:2, :] * f
    tgt_out_ref[...] = g_tgt / g_sum
    factor_ref[0:1, :] = jnp.exp(zmsg[z, 0:1, :] - g_max) / g_sum
    factor_ref[1:2, :] = g_before / g_sum
    v_all.wait_send()


def finish_kernel(tiles, lanes, c_ref, coef_ref, factor_ref, tgt_ref, out_ref, tgt_out_ref, buf, factor_col, sems, ends):
    slots, n, n_cols = buf.shape
    steps = c_ref.shape[0] // n
    turn = max(n, LANES)
    tgt_copy = pltpu.make_async_copy(tgt_ref, tgt_out_ref, ends.at[4])
    tgt_copy.start()

    def put(i):
        at = pl.ds(pl.multiple_of(i * n, n), n)
        slot = lax.rem(i - 1, slots)
        return pltpu.make_async_copy(buf.at[slot], out_ref.at[at], sems.at[slot])

    def turn_factors(i):
        some = pl.ds(pl.multiple_of(i // (turn // n) * turn, turn), turn)
        factor_col[some, :] = factor_ref[:, some].T

    def table(at, count, to):
        lane = lax.broadcasted_iota(jnp.int32, (count, LANES), 1)
        coef = coef_ref[at, :] * factor_col[at, 0:1] + jnp.where(lane < SLOTS, 0.0, factor_col[at, 1:2])
        for (start, width), k in zip(tiles, lanes):
            span = slice(start, start + width)
            buf[(*to, span)] = c_ref[at, span] * coef[:, k : k + 1] + coef[:, SLOTS + k : SLOTS + k + 1]

    turn_factors(0)
    n_parts = 4
    part = n // n_parts

    def put_part(h):
        at = pl.ds(pl.multiple_of(h * part, part), part)
        return pltpu.make_async_copy(buf.at[slots - 1, at], out_ref.at[at], ends.at[h])

    @pl.loop(0, n_parts)
    def _(h):
        at = pl.ds(pl.multiple_of(h * part, part), part)
        table(at, part, (slots - 1, at))
        put_part(h).start()

    @pl.loop(1, steps)
    def _(i):
        @pl.when(i == slots)
        def _():
            for h in range(n_parts):
                put_part(h).wait()

        @pl.when(i > slots)
        def _():
            put(i - slots).wait()

        @pl.when(lax.rem(i, turn // n) == 0)
        def _():
            turn_factors(i)

        table(pl.ds(pl.multiple_of(i * n, n), n), n, (lax.rem(i - 1, slots), slice(None)))
        put(i).start()

    tgt_copy.wait()
    for i in range(max(0, steps - slots), steps):
        with jax.named_scope(f"fe{i}"):
            put(i).wait()


def solution(mesh):
    n_hid, n_voc = mesh.shape["hid"], mesh.shape["vocab"]
    assert n_hid == 4 and n_voc == 4 and mesh.shape["data"] == 2

    def local_step(h_blk, w_blk, temp_blk, tgt_blk):
        rows, depth = h_blk.shape
        n_cols = w_blk.shape[1] // n_hid
        assert n_cols % LANES == 0
        tiles = tiles_of(n_cols // LANES)
        n_tiles = len(tiles)
        assert n_tiles < SLOTS
        plan = chunks_of(n_cols // LANES)
        n_chunks = len(plan)
        last_whole = sum(width == TILE for _, width in tiles) - 1
        first_end = [first for first, *_ in plan].index(2 * last_whole)
        vmem = pl.BlockSpec(memory_space=pltpu.VMEM)
        hbm = pl.BlockSpec(memory_space=pltpu.HBM)
        dma = pltpu.SemaphoreType.DMA
        table = pltpu.VMEM((rows, LANES), F32)
        c, coef, factor, tgt = pl.pallas_call(
            functools.partial(prefix_kernel, n_cols),
            out_shape=(
                pltpu.VMEM((rows, n_cols), F32),
                pltpu.VMEM((rows, LANES), F32),
                pltpu.VMEM((8, rows), F32),
                pltpu.VMEM((1, rows), F32),
            ),
            in_specs=[hbm] * 4,
            out_specs=[vmem] * 4,
            scratch_shapes=[
                pltpu.VMEM((4 * depth, n_cols), BF16),
                pltpu.VMEM((rows, 4 * depth), BF16),
                pltpu.VMEM((rows, TILE), F32),
                pltpu.VMEM((3 * TILE, TILE), BF16),
                pltpu.VMEM((3 * LANES, LANES), BF16),
                table,
                table,
                table,
                pltpu.VMEM((rows, LANES), jnp.int32),
                pltpu.VMEM((1, rows), F32),
                pltpu.VMEM((1, rows), jnp.int32),
                pltpu.VMEM((4, 3, rows), F32),
                pltpu.VMEM((4, 3, rows), F32),
                pltpu.VMEM((8, rows), F32),
                dma((3,)),
                dma((n_chunks, 3)),
                dma((4,)),
                dma((n_chunks,)),
                dma((2,)),
                dma,
                dma,
                dma,
                dma,
                dma((6,)),
                dma,
                dma,
                dma,
                dma,
                dma((2,)),
            ],
            compiler_params=pltpu.CompilerParams(
                collective_id=0, has_side_effects=True, vmem_limit_bytes=37 << 20
            ),
            name="prefix",
        )(h_blk, w_blk, temp_blk.reshape(1, rows), tgt_blk.reshape(1, rows))
        n = min(rows // 8, 64)
        assert rows // n > 4
        lanes = list(range(n_tiles))
        for _, g0, g1 in folds_of(plan, first_end):
            lanes[g0:g1] = [g0] * (g1 - g0)
        lanes[g1 : last_whole + 1] = [SLOTS - 1] * (last_whole + 1 - g1)
        cdf, cdf_tgt = pl.pallas_call(
            functools.partial(finish_kernel, tiles, lanes),
            out_shape=(
                jax.ShapeDtypeStruct((rows, n_cols), F32),
                jax.ShapeDtypeStruct((1, rows), F32),
            ),
            in_specs=[vmem] * 4,
            out_specs=[hbm, hbm],
            scratch_shapes=[
                pltpu.VMEM((4, n, n_cols), F32),
                pltpu.VMEM((rows, 8), F32),
                dma((4,)),
                dma((5,)),
            ],
            compiler_params=pltpu.CompilerParams(vmem_limit_bytes=9 << 20),
            name="finish",
        )(c, coef, factor, tgt)
        return cdf, cdf_tgt.reshape(rows)

    return jax.shard_map(
        local_step,
        mesh=mesh,
        in_specs=(P("data", "hid"), P("hid", "vocab"), P("data"), P("data")),
        out_specs=(P("data", ("vocab", "hid")), P("data")),
        check_vma=False,
    )
```

```python
import functools

import jax
import jax.numpy as jnp
from jax import lax
from jax.experimental import pallas as pl
from jax.experimental.pallas import tpu as pltpu
from jax.sharding import PartitionSpec as P

MESH = pl.DeviceIdType.MESH
F32 = jnp.float32
BF16 = jnp.bfloat16
TILE = 256
LANES = 128
SLOTS = 32
LOWEST = float(jnp.finfo(jnp.float32).min)


def tiles_of(blocks):
    whole = (blocks - 3) // 2
    tiles = [(t * TILE, TILE) for t in range(whole)]
    return tiles + [(b * LANES, LANES) for b in range(2 * whole, blocks)]


def chunks_of(blocks):
    whole = (blocks - 3) // 2
    sizes, left = [], 2 * whole - 2
    for size in (2, 2, 2, 2, 4, 4):
        if left > size:
            sizes.append(size)
            left -= size
    while left > 0:
        sizes.append(min(6, left))
        left -= sizes[-1]
    plan, at = [], 0
    for size in reversed(sizes):
        plan.append((at, size, 0, 2))
        at += size
    plan += [(b, 1, 0, 2) for b in range(at, blocks - 2)]
    return plan + [(b, 1, r, 1) for b in (blocks - 2, blocks - 1) for r in (0, 1)]


def service_order(plan, blocks):
    events = [(0.15 * blocks, "h line", 0), (0.28 * blocks, "h chip", 0)]
    for j, (first, size, _, _) in enumerate(plan):
        end = first + size
        events.append((first + size / 3 + 2, 0, j))
        events.append((end + 2, 2, j))
        events.append((min(1.86 * end, 0.68 * blocks + 0.6 * end) + 2, 1, j))
    events.sort(key=lambda e: e[0])
    order = [e[1:] for e in events]
    for j in range(len(plan)):
        at = max(order.index((k, j)) for k in (0, 1, 2))
        order.remove((1, j))
        order.insert(at, (1, j))
    return order


def folds_of(plan, first_end):
    folds, at = [], 0
    for j in (first_end // 3, 3 * first_end // 5):
        stop = sum(plan[j][:2]) // 2 - 1
        if j < first_end and stop > at:
            folds.append((j, at, stop))
            at = stop
    return folds


def split3(e):
    hi = e.astype(BF16)
    rest = e - hi.astype(F32)
    mid = rest.astype(BF16)
    low = (rest - mid.astype(F32)).astype(BF16)
    return hi, mid, low


def prefix_kernel(
    n_cols, h_ref, w_ref, temp_hbm, tgt_hbm,
    c_ref, coef_ref, factor_ref, tgt_out_ref,
    wbuf, hbuf, zbuf, tri, tri_last, stats, t_all, temp_col, rel_col, temp_ref, tgt_ref, zmsg, vmsg, back,
    ws, wr, xs, xr, ts, tr, wl, hl, hs, hr, zs, zr, vs, vr, rl,
):
    x, z, v = lax.axis_index("data"), lax.axis_index("hid"), lax.axis_index("vocab")
    rows, depth = h_ref.shape
    half, quarter = depth // 2, rows // 4
    tiles = tiles_of(n_cols // LANES)
    n_tiles = len(tiles)
    n_whole = sum(width == TILE for _, width in tiles)
    plan = chunks_of(n_cols // LANES)
    n_chunks = len(plan)
    ends = [[j for j, (first, *_) in enumerate(plan) if first * LANES < sum(tiles[t])][-1] for t in range(n_whole - 1, n_tiles)]
    first_end = ends[0] - 1

    side = z // 2
    outer_far, inner_far, near = 3 - 3 * side, 2 - side, 1 - z + 4 * side
    is_outer = jnp.where(z == side * 3, 1, 0)
    z_two, z_one = lax.rem(z + 2, 4), near
    v_two, v_one = lax.rem(v + 2, 4), v + 1 - 2 * lax.rem(v, 2)
    sources = (near, inner_far, outer_far)

    def cols_of(j):
        first, size, _, _ = plan[j]
        return first * LANES, size * LANES

    def w_rows(source, part, j=None):
        at, n = (0, half) if j is None else (plan[j][2] * (half // 2), plan[j][3] * (half // 2))
        return pl.ds(pl.multiple_of(source * depth + part * half + at, half // 2), n)

    def w_place(j, source, part):
        start, n = cols_of(j)
        return wbuf.at[w_rows(source, part, j), pl.ds(start, n)]

    def h_place(q, block=None):
        at = pl.ds(pl.multiple_of(q * quarter, quarter), quarter)
        if block is None:
            return hbuf.at[at]
        return hbuf.at[at, pl.ds(pl.multiple_of(block * depth, depth), depth)]

    def remote(src, dst, send, recv, **to):
        return pltpu.make_async_remote_copy(
            src_ref=src, dst_ref=dst, send_sem=send, recv_sem=recv, device_id=to, device_id_type=MESH
        )

    def w_source(j, part, dest):
        start, n = cols_of(j)
        return w_ref.at[w_rows(0, part, j), pl.ds(pl.multiple_of(dest * n_cols + start, LANES), n)]

    def direct(j, k, dest, slot):
        return remote(w_source(j, x, dest), w_place(j, z, x), ws.at[k], wr.at[j, slot], hid=dest)

    def send_near(j):
        return direct(j, 0, near, 0)

    odd = lax.rem(v, 2)
    far_first = outer_far + odd * (inner_far - outer_far)
    far_second = inner_far + odd * (outer_far - inner_far)

    def send_far(j, i):
        return direct(j, 1 + i, (far_first, far_second)[i], 1 + is_outer)

    def send_twin(i):
        dest = (far_first, far_second)[i]
        return remote(w_source(n_chunks - 1, 1 - x, dest), w_place(n_chunks - 1, z, 1 - x), ts.at[i], tr, hid=dest)

    def twin_landed():
        place = w_place(n_chunks - 1, inner_far, 1 - x)
        remote(place, place, ts.at[0], tr, hid=inner_far).wait_recv()

    def landed(j, k):
        place = w_place(j, sources[k], x)
        remote(place, place, ws.at[k], wr.at[j, k], hid=sources[k]).wait_recv()

    def forward(j, k):
        place = w_place(j, sources[k], x)
        send = 3 if k == 1 and j == n_chunks - 2 else k
        return remote(place, place, xs.at[send], xr.at[cross(j, k)], data=1 - x)

    def cross(j, k):
        if j < first_end:
            return j
        return first_end if k != 1 else 1 + j

    def cross_wait(slot, count, start, stop):
        place = wbuf.at[pl.ds(0, count), pl.ds(start, stop - start)]
        remote(place, place, xs.at[0], xr.at[slot], data=1 - x).wait_recv()

    def forwarded(j):
        place = w_place(j, inner_far, 1 - x)
        remote(place, place, xs.at[1], xr.at[cross(j, 1)], data=1 - x).wait_recv()

    def own(j):
        start, n = cols_of(j)
        return pltpu.make_async_copy(
            w_ref.at[:, pl.ds(pl.multiple_of(z * n_cols + start, LANES), n)],
            wbuf.at[pl.ds(pl.multiple_of(z * depth, depth), depth), pl.ds(start, n)],
            wl,
        )

    h_mine = h_ref.at[pl.ds(pl.multiple_of(v * quarter, quarter), quarter)]
    h_own = pltpu.make_async_copy(h_mine, h_place(v, z), hl)
    h_two = remote(h_mine, h_place(v, z), hs, hr.at[0], hid=z_two)
    h_one = remote(h_mine, h_place(v, z), hs, hr.at[1], hid=z_one)
    h_relay = remote(h_place(v, z_two), h_place(v, z_two), hs, hr.at[2], hid=z_one)
    h_chip = remote(h_place(v), h_place(v), hs, hr.at[3], vocab=v_two)
    h_core = remote(h_place(v), h_place(v), hs, hr.at[4], vocab=v_one)
    h_both = remote(h_place(v_two), h_place(v_two), hs, hr.at[5], vocab=v_one)

    def arrived(place, i, **frm):
        remote(place, place, hs, hr.at[i], **frm).wait_recv()

    barrier = pltpu.get_barrier_semaphore()
    peers = [{"hid": outer_far}, {"hid": inner_far}, {"hid": near}, {"data": 1 - x}]
    peers += [{"vocab": lax.rem(v + d, 4)} for d in (2, 1, 3)]
    for peer in peers:
        pl.semaphore_signal(barrier, inc=1, device_id=peer, device_id_type=MESH)
    row_copies = [
        pltpu.make_async_copy(temp_hbm, temp_ref, rl.at[0]),
        pltpu.make_async_copy(tgt_hbm, tgt_ref, rl.at[1]),
    ]
    for copy in (h_own, *row_copies):
        copy.start()
    for j in range(n_chunks):
        if plan[j][2] == 0:
            own(j).start()
    with jax.named_scope("bar"):
        pl.semaphore_wait(barrier, len(peers))

    h_two.start()
    h_one.start()
    send_near(0).start()
    send_far(0, 0).start()

    def ones_below(ref, width):
        k = lax.broadcasted_iota(jnp.int32, (width, width), 0)
        c = lax.broadcasted_iota(jnp.int32, (width, width), 1)
        block = jnp.where(k <= c, 1.0, 0.0).astype(BF16)
        for i in range(3):
            ref[pl.ds(i * width, width), :] = block

    ones_below(tri, TILE)
    ones_below(tri_last, LANES)
    base = (v * 4 + z) * n_cols
    for copy in row_copies:
        copy.wait()
    back[0:1, :] = temp_ref[...]
    back[1:2, :] = (tgt_ref[...] - base).astype(F32)
    cols8 = back[...].T
    temp_col[...] = jnp.broadcast_to(cols8[:, 0:1], temp_col.shape)
    rel_col[...] = jnp.broadcast_to(cols8[:, 1:2], rel_col.shape).astype(jnp.int32)
    slot = lax.broadcasted_iota(jnp.int32, stats.shape, 1)
    stats[...] = jnp.where(slot < SLOTS, LOWEST, 0.0)
    t_all[...] = jnp.zeros(t_all.shape, F32)

    with jax.named_scope("h0"):
        arrived(h_place(v, z_two), 0, hid=z_two)
    h_relay.start()
    send_far(0, 1).start()
    for j in range(1, n_chunks):
        send_near(j).start()
        send_far(j, 0).start()
        send_far(j, 1).start()

    @pl.when(is_outer == 0)
    def _():
        send_twin(0).start()
        send_twin(1).start()


    part, few = min(rows, 512), min(rows, 128)

    def logits_and_sums(product, sums):
        some = part if product is not None or sums[2] == TILE else min(rows, 2 * part)

        @pl.loop(0, rows // some)
        def _(i):
            if product is not None:
                _, new_start, new_width = product
                at = pl.ds(pl.multiple_of(i * part, part), part)
                new = jnp.dot(
                    hbuf[at, :], wbuf[:, pl.ds(new_start, new_width)], preferred_element_type=F32
                )
            for k in range(0, some, few) if sums is not None else ():
                prefix(pl.ds(pl.multiple_of(i * some + k, few), few), *sums)
            if product is not None:
                zbuf[at, 0:new_width] = new

    def prefix(at, t, start, width, ending=False):
        pieces = width // LANES
        logits = zbuf[at, 0:width] * jnp.concatenate([temp_col[at, :]] * pieces, axis=1)
        lane = lax.broadcasted_iota(jnp.int32, (few, LANES), 1)
        top = jnp.max(logits, axis=1, keepdims=True)
        e = jnp.exp(logits - top)
        total = jnp.sum(e, axis=1, keepdims=True)
        old = stats[at, :]
        table = tri if width == TILE else tri_last
        run = jnp.dot(jnp.concatenate(split3(e), axis=1), table[...], preferred_element_type=F32)
        c_ref[at, pl.ds(start, width)] = run
        rel = rel_col[at, :] - start
        if ending:
            hit = jnp.where(lane == rel, run, 0.0)
            old = jnp.where(lane == 2 * SLOTS, old + jnp.sum(hit, axis=1, keepdims=True), old)
        else:
            hit = t_all[at, :]
            for p in range(pieces):
                hit += jnp.where(lane == rel - p * LANES, run[:, p * LANES : (p + 1) * LANES], 0.0)
            t_all[at, :] = hit
        stats[at, :] = jnp.where(lane == t, top, jnp.where(lane == SLOTS + t, total, old))

    def collect():
        lane = lax.broadcasted_iota(jnp.int32, stats.shape, 1)
        stats[...] = jnp.where(lane == 2 * SLOTS, jnp.sum(t_all[...], axis=1, keepdims=True), stats[...])

    def whole(t):
        return t, pl.multiple_of(t * TILE, TILE), TILE

    def compute(j):
        first, size = (n // 2 for n in plan[j][:2])
        stop = first + size
        if first == 0:
            logits_and_sums(whole(0), None)
            first = 1
        if first < stop:

            @pl.loop(first, stop)
            def _(t):
                logits_and_sums(whole(t), whole(t - 1))

        if j == first_end - 1:
            logits_and_sums(None, whole(stop - 1))

    def block_dot(at, block, start, width):
        lanes = pl.ds(pl.multiple_of(block * depth, depth), depth)
        return jnp.dot(hbuf[at, lanes], wbuf[lanes, start : start + width], preferred_element_type=F32)

    def begin_end(i):
        start, width = tiles[n_whole - 1 + i]

        @pl.loop(0, rows // part)
        def _(k):
            at = pl.ds(pl.multiple_of(k * part, part), part)
            c_ref[at, start : start + width] = (
                block_dot(at, z, start, width)
                + block_dot(at, near, start, width)
                + block_dot(at, outer_far, start, width)
            )

    def finish_end(i):
        t = n_whole - 1 + i
        start, width = tiles[t]
        every = slice(0, rows)
        zbuf[:, 0:width] = c_ref[:, start : start + width] + block_dot(every, inner_far, start, width)
        logits_and_sums(None, (t, start, width, t == n_tiles - 1))

    def fold(g0, g1):
        @pl.loop(0, rows // few)
        def _(i):
            at = pl.ds(pl.multiple_of(i * few, few), few)
            lane = lax.broadcasted_iota(jnp.int32, (few, LANES), 1)
            group = (lane >= g0) & (lane < g1)
            m = stats[at, :]
            s = pltpu.roll(m, LANES - SLOTS, 1)
            top = jnp.max(jnp.where(group, m, LOWEST), axis=1, keepdims=True)
            shrink = jnp.where(group, jnp.exp(m - top), 0.0)
            parts = jnp.where(group, s, 0.0) * shrink
            before = prefix_before(parts)
            for t in range(g0, g1):
                span = slice(t * TILE, (t + 1) * TILE)
                c_ref[at, span] = c_ref[at, span] * shrink[:, t : t + 1] + before[:, t : t + 1]
            rel = rel_col[at, :]
            holds = (rel >= lane * TILE) & (rel < (lane + 1) * TILE)
            old = t_all[at, :]
            moved = jnp.sum(old, axis=1, keepdims=True) * shrink + before
            inside = (rel >= g0 * TILE) & (rel < g1 * TILE)
            t_all[at, :] = jnp.where(inside, jnp.where(holds, moved, 0.0), old)
            total = jnp.sum(parts, axis=1, keepdims=True)
            sums = jnp.where(lane == SLOTS + g1 - 1, total, 0.0)
            of_sums = (lane >= SLOTS + g0) & (lane < SLOTS + g1)
            stats[at, :] = jnp.where(group, top, jnp.where(of_sums, sums, m))

    def close(i):
        first = ends[i - 1] + 1 if i else first_end
        with jax.named_scope(f"xe{i}"):
            for j in range(first, ends[i] + 1):
                if j < n_chunks - 1:
                    forwarded(j)
                else:
                    twin_landed()
        with jax.named_scope(f"ce{i}"):
            finish_end(i)

    def prefix_before(parts):
        k = lax.broadcasted_iota(jnp.int32, (LANES, LANES), 0)
        c = lax.broadcasted_iota(jnp.int32, (LANES, LANES), 1)
        strict = jnp.where(k < c, 1.0, 0.0).astype(BF16)
        return sum(jnp.dot(p, strict, preferred_element_type=F32) for p in split3(parts))

    def complete(j):
        start, n = cols_of(j)
        cross_wait(j, 3 * half, start, start + n)

    def own_complete():
        place = wbuf.at[pl.ds(pl.multiple_of(z * depth, depth), depth)]
        pltpu.make_async_copy(place, place, wl).wait()

    order = service_order(plan, n_cols // LANES)
    folds = {j: (g0, g1) for j, g0, g1 in folds_of(plan, first_end)}
    tail = range(first_end, n_chunks)
    known = max(order.index((k, j)) for k in (0, 2) for j in tail)
    early = min(j for j in range(max(0, first_end - 7), n_chunks - 1) if order.index((1, j + 1)) > known)
    assert early < first_end
    m = len(ends) - 1
    closes = {n_chunks - 3: range(m - 2), n_chunks - 2: [m - 2], n_chunks - 1: [m - 1]}

    for what, j in order:
        if what == "h line":
            with jax.named_scope("hline"):
                arrived(h_place(v, z_one), 1, hid=z_one)
                arrived(h_place(v, lax.rem(z_one + 2, 4)), 2, hid=z_one)
                h_own.wait()
            h_chip.start()
            h_core.start()
        elif what == "h chip":
            with jax.named_scope("hchip"):
                arrived(h_place(v_two), 3, vocab=v_two)
            h_both.start()
        else:
            with jax.named_scope(f"w{what}_{j}"):
                landed(j, what)
            if (what, j) != (1, n_chunks - 1):
                forward(j, what).start()
            if what != 1:
                continue
            if j == 1:
                with jax.named_scope("hcore"):
                    arrived(h_place(v_one), 4, vocab=v_one)
                    arrived(h_place(lax.rem(v_one + 2, 4)), 5, vocab=v_one)
                    own_complete()
            if 0 < j <= first_end:
                with jax.named_scope(f"x{j - 1}"):
                    complete(j - 1)
                with jax.named_scope(f"c{j - 1}"):
                    compute(j - 1)
                if j - 1 in folds:
                    with jax.named_scope(f"f{j - 1}"):
                        fold(*folds[j - 1])
            if j - 1 == early:
                with jax.named_scope("begin"):
                    cross_wait(first_end, 2 * half, cols_of(first_end)[0], n_cols)
                    for i in range(len(ends)):
                        begin_end(i)
            for i in closes.get(j, ()):
                close(i)
    collect()
    close(m)

    lane = lax.broadcasted_iota(jnp.int32, (rows, LANES), 1)
    turned = stats[...].T
    m, at_tgt = turned[0:SLOTS, :], turned[2 * SLOTS : 2 * SLOTS + 1, :]
    top = jnp.max(m, axis=0, keepdims=True)
    shrink = jnp.exp(m - top)
    parts = turned[SLOTS : 2 * SLOTS, :] * shrink
    t = lax.broadcasted_iota(jnp.int32, (SLOTS, rows), 0)
    start = jnp.where(t < n_whole, t * TILE, n_whole * (TILE - LANES) + t * LANES)
    stop = start + jnp.where(t < n_whole, TILE, LANES)
    rel = tgt_ref[...] - base
    known = rel < n_cols
    holds = (rel >= start) & (rel < stop) & known
    ahead = (stop <= rel) & known
    found = jnp.where(holds, at_tgt * shrink, jnp.where(ahead, parts, 0.0))
    zmsg[z, 0:1, :] = top
    zmsg[z, 1:2, :] = jnp.sum(parts, axis=0, keepdims=True)
    zmsg[z, 2:3, :] = jnp.sum(found, axis=0, keepdims=True)

    for k in range(3):
        mine = wbuf.at[w_rows(sources[k], x)]
        remote(mine, mine, ws.at[k], wr.at[0, k], hid=near).wait_send()
        if k == 1:
            mine = wbuf.at[w_rows(sources[k], x), pl.ds(0, n_cols - LANES)]
        remote(mine, mine, xs.at[k], xr.at[0], data=1 - x).wait_send()
    forward(n_chunks - 2, 1).wait_send()

    @pl.when(is_outer == 0)
    def _():
        send_twin(0).wait_send()
        send_twin(1).wait_send()

    mine = hbuf.at[pl.ds(0, quarter * 15 // 4)]
    remote(mine, mine, hs, hr.at[0], hid=near).wait_send()

    def z_send(i):
        return remote(zmsg.at[z], zmsg.at[z], zs, zr, hid=(near, inner_far, outer_far)[i])

    def v_send(d):
        to = lax.rem(v + d, 4)
        return remote(vmsg.at[v], vmsg.at[v], vs, vr, vocab=to)

    for i in (2, 1, 0):
        z_send(i).start()
    k = lax.broadcasted_iota(jnp.int32, (SLOTS, SLOTS), 0)
    c = lax.broadcasted_iota(jnp.int32, (SLOTS, SLOTS), 1)
    strict = jnp.where(c < k, 1.0, 0.0).astype(BF16)
    before = sum(jnp.dot(strict, p, preferred_element_type=F32) for p in split3(parts))
    rest = jnp.zeros((LANES - 2 * SLOTS, rows), F32)
    spare = t == SLOTS - 1
    coef_ref[...] = jnp.concatenate([jnp.where(spare, 1.0, shrink), jnp.where(spare, 0.0, before), rest], axis=0).T

    @pl.loop(0, rows // few)
    def _(i):
        at = pl.ds(pl.multiple_of(i * few, few), few)
        coef = coef_ref[at, :]
        for q in range(folds_of(plan, first_end)[-1][2], n_whole - 1):
            span = slice(tiles[q][0], sum(tiles[q]))
            c_ref[at, span] = c_ref[at, span] * coef[:, q : q + 1] + coef[:, SLOTS + q : SLOTS + q + 1]

    z_all = remote(zmsg.at[pl.ds(0, 3)], zmsg.at[pl.ds(0, 3)], zs, zr, hid=near)
    with jax.named_scope("z"):
        z_all.wait_recv()

    ids = tgt_ref[...]
    maxes = [zmsg[h, 0:1, :] for h in range(4)]
    v_max = functools.reduce(jnp.maximum, maxes)
    v_sum = jnp.zeros((1, rows), F32)
    v_tgt = jnp.zeros((1, rows), F32)
    mine_before = jnp.zeros((1, rows), F32)
    for h in range(4):
        mine_before = jnp.where(h == z, v_sum, mine_before)
        f = jnp.exp(maxes[h] - v_max)
        low = (v * 4 + h) * n_cols
        inside = (ids >= low) & (ids < low + n_cols)
        v_tgt += jnp.where(inside, zmsg[h, 2:3, :] * f + v_sum, 0.0)
        v_sum += zmsg[h, 1:2, :] * f
    vmsg[v, 0:1, :] = v_max
    vmsg[v, 1:2, :] = v_sum
    vmsg[v, 2:3, :] = v_tgt

    z_all.wait_send()
    for d in (2, 1, 3):
        v_send(d).start()
    v_all = remote(vmsg.at[pl.ds(0, 3)], vmsg.at[pl.ds(0, 3)], vs, vr, vocab=v_one)
    with jax.named_scope("v"):
        v_all.wait_recv()

    maxes = [vmsg[u, 0:1, :] for u in range(4)]
    g_max = functools.reduce(jnp.maximum, maxes)
    g_sum = jnp.zeros((1, rows), F32)
    g_tgt = jnp.zeros((1, rows), F32)
    g_before = jnp.zeros((1, rows), F32)
    for u in range(4):
        f = jnp.exp(maxes[u] - g_max)
        g_before = jnp.where(u == v, g_sum + mine_before * f, g_before)
        low = u * 4 * n_cols
        inside = (ids >= low) & (ids < low + 4 * n_cols)
        g_tgt += jnp.where(inside, vmsg[u, 2:3, :] * f + g_sum, 0.0)
        g_sum += vmsg[u, 1:2, :] * f
    tgt_out_ref[...] = g_tgt / g_sum
    factor_ref[0:1, :] = jnp.exp(zmsg[z, 0:1, :] - g_max) / g_sum
    factor_ref[1:2, :] = g_before / g_sum
    v_all.wait_send()


def finish_kernel(tiles, lanes, c_ref, coef_ref, factor_ref, tgt_ref, out_ref, tgt_out_ref, buf, factor_col, sems, ends):
    slots, n, n_cols = buf.shape
    steps = c_ref.shape[0] // n
    turn = max(n, LANES)
    tgt_copy = pltpu.make_async_copy(tgt_ref, tgt_out_ref, ends.at[2])
    tgt_copy.start()

    def put(i):
        at = pl.ds(pl.multiple_of(i * n, n), n)
        slot = lax.rem(i - 1, slots)
        return pltpu.make_async_copy(buf.at[slot], out_ref.at[at], sems.at[slot])

    def turn_factors(i):
        some = pl.ds(pl.multiple_of(i // (turn // n) * turn, turn), turn)
        factor_col[some, :] = factor_ref[:, some].T

    def table(at, count, to):
        lane = lax.broadcasted_iota(jnp.int32, (count, LANES), 1)
        coef = coef_ref[at, :] * factor_col[at, 0:1] + jnp.where(lane < SLOTS, 0.0, factor_col[at, 1:2])
        for (start, width), k in zip(tiles, lanes):
            span = slice(start, start + width)
            buf[(*to, span)] = c_ref[at, span] * coef[:, k : k + 1] + coef[:, SLOTS + k : SLOTS + k + 1]

    turn_factors(0)
    half = n // 2

    def put_half(h):
        at = pl.ds(pl.multiple_of(h * half, half), half)
        return pltpu.make_async_copy(buf.at[slots - 1, at], out_ref.at[at], ends.at[h])

    @pl.loop(0, 2)
    def _(h):
        at = pl.ds(pl.multiple_of(h * half, half), half)
        table(at, half, (slots - 1, at))
        put_half(h).start()

    @pl.loop(1, steps)
    def _(i):
        @pl.when(i == slots)
        def _():
            put_half(0).wait()
            put_half(1).wait()

        @pl.when(i > slots)
        def _():
            put(i - slots).wait()

        @pl.when(lax.rem(i, turn // n) == 0)
        def _():
            turn_factors(i)

        table(pl.ds(pl.multiple_of(i * n, n), n), n, (lax.rem(i - 1, slots), slice(None)))
        put(i).start()

    tgt_copy.wait()
    for i in range(max(0, steps - slots), steps):
        with jax.named_scope(f"fe{i}"):
            put(i).wait()


def solution(mesh):
    n_hid, n_voc = mesh.shape["hid"], mesh.shape["vocab"]
    assert n_hid == 4 and n_voc == 4 and mesh.shape["data"] == 2

    def local_step(h_blk, w_blk, temp_blk, tgt_blk):
        rows, depth = h_blk.shape
        n_cols = w_blk.shape[1] // n_hid
        assert n_cols % LANES == 0
        tiles = tiles_of(n_cols // LANES)
        n_tiles = len(tiles)
        assert n_tiles < SLOTS
        plan = chunks_of(n_cols // LANES)
        n_chunks = len(plan)
        last_whole = sum(width == TILE for _, width in tiles) - 1
        first_end = [first for first, *_ in plan].index(2 * last_whole)
        vmem = pl.BlockSpec(memory_space=pltpu.VMEM)
        hbm = pl.BlockSpec(memory_space=pltpu.HBM)
        dma = pltpu.SemaphoreType.DMA
        table = pltpu.VMEM((rows, LANES), F32)
        c, coef, factor, tgt = pl.pallas_call(
            functools.partial(prefix_kernel, n_cols),
            out_shape=(
                pltpu.VMEM((rows, n_cols), F32),
                pltpu.VMEM((rows, LANES), F32),
                pltpu.VMEM((8, rows), F32),
                pltpu.VMEM((1, rows), F32),
            ),
            in_specs=[hbm] * 4,
            out_specs=[vmem] * 4,
            scratch_shapes=[
                pltpu.VMEM((4 * depth, n_cols), BF16),
                pltpu.VMEM((rows, 4 * depth), BF16),
                pltpu.VMEM((rows, TILE), F32),
                pltpu.VMEM((3 * TILE, TILE), BF16),
                pltpu.VMEM((3 * LANES, LANES), BF16),
                table,
                table,
                table,
                pltpu.VMEM((rows, LANES), jnp.int32),
                pltpu.VMEM((1, rows), F32),
                pltpu.VMEM((1, rows), jnp.int32),
                pltpu.VMEM((4, 3, rows), F32),
                pltpu.VMEM((4, 3, rows), F32),
                pltpu.VMEM((8, rows), F32),
                dma((3,)),
                dma((n_chunks, 3)),
                dma((4,)),
                dma((n_chunks,)),
                dma((2,)),
                dma,
                dma,
                dma,
                dma,
                dma((6,)),
                dma,
                dma,
                dma,
                dma,
                dma((2,)),
            ],
            compiler_params=pltpu.CompilerParams(
                collective_id=0, has_side_effects=True, vmem_limit_bytes=37 << 20
            ),
            name="prefix",
        )(h_blk, w_blk, temp_blk.reshape(1, rows), tgt_blk.reshape(1, rows))
        n = min(rows // 8, 64)
        assert rows // n > 4
        lanes = list(range(n_tiles))
        for _, g0, g1 in folds_of(plan, first_end):
            lanes[g0:g1] = [g0] * (g1 - g0)
        lanes[g1:last_whole] = [SLOTS - 1] * (last_whole - g1)
        cdf, cdf_tgt = pl.pallas_call(
            functools.partial(finish_kernel, tiles, lanes),
            out_shape=(
                jax.ShapeDtypeStruct((rows, n_cols), F32),
                jax.ShapeDtypeStruct((1, rows), F32),
            ),
            in_specs=[vmem] * 4,
            out_specs=[hbm, hbm],
            scratch_shapes=[
                pltpu.VMEM((4, n, n_cols), F32),
                pltpu.VMEM((rows, 8), F32),
                dma((4,)),
                dma((3,)),
            ],
            compiler_params=pltpu.CompilerParams(vmem_limit_bytes=9 << 20),
            name="finish",
        )(c, coef, factor, tgt)
        return cdf, cdf_tgt.reshape(rows)

    return jax.shard_map(
        local_step,
        mesh=mesh,
        in_specs=(P("data", "hid"), P("hid", "vocab"), P("data"), P("data")),
        out_specs=(P("data", ("vocab", "hid")), P("data")),
        check_vma=False,
    )
```
